128 devices in a mesh: dp: 16 (over x_lo, z, core), tensor: 8 (over y, x_hi).
Axes of the slice: x: 4 (x_hi: 2, x_lo: 2; x = x_hi * 2 + x_lo), y: 4, z: 4, core: 2. Of those that a mesh axis runs over, the one named last changes fastest.
Arguments:
- token_ids: int32 [16, 1024], P('dp', 'tensor'), may hold values from 0 to 30527
- lengths: int32 [16], P('dp'), may hold values from 256 to 1024, as said below
- teacher_bins: int32 [16], P('dp'), may hold values from 0 to 127
- embed_table: bfloat16 [30528, 1024], P('tensor'), may hold values from -6 to 6
- query_key_value_matrix: bfloat16 [1024, 3, 1024], P('dp', None, 'tensor'), may hold values from -2 to 2
- output_matrix: bfloat16 [1024, 1024], P('tensor', 'dp'), may hold values from -0.1875 to 0.1875
- up_matrix: bfloat16 [1024, 4096], P('dp', 'tensor'), may hold values from -0.1875 to 0.1875
- down_matrix: bfloat16 [4096, 1024], P('tensor', 'dp'), may hold values from -0.09375 to 0.09375
- w_head: bfloat16 [1024, 128], P('dp'), may hold values from -64 to 64
Outputs:
- loss: float32 [], replicated
- query_key_value_gradient: float32 [1024, 3, 1024], P('dp', None, 'tensor')
- output_weight_gradient: float32 [1024, 1024], P('tensor', 'dp')
- up_weight_gradient: float32 [1024, 4096], P('dp', 'tensor')
- down_weight_gradient: float32 [4096, 1024], P('tensor', 'dp')
- grad_head: float32 [1024, 128], P('dp')
The draws below stay inside these ranges and needn't reach their ends.
Inputs may be any that keep to these rules, and one draw needn't show every extreme that they name: lengths[0] is 1024.
All inputs are finite; a program needn't handle non-finite values.
Results may differ from the reference program's by a relative error of at most 0.02.
Values may be sent and summed in bfloat16 or wider, within the bound.
A program may use at most 128 MiB of HBM per device.

```python
import math
import jax
import jax.numpy as jnp
import numpy as np
from jax import lax

D = 1024
HEAD_COUNT = 16
HEAD_WIDTH = 64
FF = 4096
VOCAB = 30528
NBINS = 128
LEN = 1024
SEQS = 16
N_TENSOR = 8


def draw_lengths(key, part):
    values = jax.random.randint(jax.random.fold_in(key, 11), (SEQS,), LEN // 4, LEN + 1, dtype=jnp.int32)
    return values.at[0].set(LEN)


def draw_embed_table(key, part):
    normal_rows = jax.random.normal(jax.random.fold_in(key, 21), (VOCAB, D), jnp.float32)
    values = normal_rows
    return jnp.clip(values, -6.0, 6.0).astype(jnp.bfloat16)


def draw_query_key_value_matrix(key, part):
    scaled = jnp.clip(jax.random.normal(jax.random.fold_in(key, 31), (D, 3, D), jnp.float32), -6.0, 6.0) * (1.0 / math.sqrt(D))
    return jnp.clip(scaled, -2.0, 2.0).astype(jnp.bfloat16)


def draw_w_head(key, part):
    drawn_cols = jnp.clip(jax.random.normal(jax.random.fold_in(key, 41), (D, NBINS), jnp.float32), -6.0, 6.0) * 0.1
    return jnp.clip(drawn_cols, -64.0, 64.0).astype(jnp.bfloat16)


def plant(entries, rng, least, top_value):
    longest = entries.shape.index(max(entries.shape))
    spots = []
    for shift in (0, 1):
        where = [jax.random.randint(jax.random.fold_in(rng, axis), (), 0, length) for axis, length in enumerate(entries.shape)]
        where[longest] = (where[longest] + shift) % entries.shape[longest]
        spots.append(tuple(where))
    return entries.at[spots[0]].set(least).at[spots[1]].set(top_value)


def shard_levels(own_key, extent, cuts, smallest, high):
    def one(axis_at, parts):
        heights = jax.random.uniform(jax.random.fold_in(jax.random.fold_in(own_key, 6), axis_at), (parts,), jnp.float32, smallest / len(cuts), high / len(cuts))
        return jnp.repeat(jnp.exp(heights), extent[axis_at] // parts).reshape((-1,) + (1,) * (len(extent) - axis_at - 1))

    loudness = one(*cuts[0])
    for cut in cuts[1:]:
        loudness = loudness * one(*cut)
    return loudness


def rank_table(amount, slope):
    portions = [(1 << 20) // math.isqrt(standing ** slope) + 1 for standing in range(1, amount + 1)]
    scale = 1 + sum(portions) // (1 << 30)
    return np.cumsum(np.array([max(1, weight // scale) for weight in portions]))


def skewed_ids(stream_key, extent, amount, lean):
    listing = rank_table(amount, lean)
    ticket = jax.random.randint(jax.random.fold_in(stream_key, 1), extent, 0, int(listing[amount - 1]))
    rank = jnp.searchsorted(jnp.asarray(listing, jnp.int32), ticket, side="right")
    return jax.random.permutation(jax.random.fold_in(stream_key, 2), amount)[rank].astype(jnp.int32)


def normal_values(key, shape, scale, reach, shards=(), held_as=jnp.bfloat16):
    values = jax.random.normal(key, shape, jnp.float32) * scale
    if len(shards) > 0:
        values = shard_levels(key, shape, shards, -0.22, 0.18) * values
    return jnp.clip(values, min=-reach, max=reach).astype(held_as)


def setup_inputs(seed: int = 0) -> dict:
    streams_of = jax.random.split(jax.random.key(seed), 10)
    token_ids = plant(skewed_ids(streams_of[0], (SEQS, LEN), VOCAB, 2), jax.random.fold_in(streams_of[0], 3), 0, VOCAB - 1).astype(jnp.int32)
    lengths = draw_lengths(jax.random.fold_in(streams_of[9], 71), 0)
    teacher_bins = plant(jax.random.randint(streams_of[2], (SEQS,), 0, NBINS), jax.random.fold_in(streams_of[2], 1), 0, NBINS - 1).astype(jnp.int32)
    embed_table = draw_embed_table(jax.random.fold_in(streams_of[9], 71), 0)
    query_key_value_matrix = draw_query_key_value_matrix(jax.random.fold_in(streams_of[9], 71), 0)
    output_matrix = normal_values(streams_of[5], (D, D), D ** -0.5, 0.1875, ((0, 8), (1, 16)))
    up_matrix = normal_values(streams_of[6], (D, FF), D ** -0.5, 0.1875, ((0, 16), (1, 8)))
    down_matrix = normal_values(streams_of[7], (FF, D), FF ** -0.5, 0.09375, ((0, 8), (1, 16)))
    w_head = draw_w_head(jax.random.fold_in(streams_of[9], 71), 0)
    return dict(token_ids=token_ids, lengths=lengths, teacher_bins=teacher_bins, embed_table=embed_table, query_key_value_matrix=query_key_value_matrix, output_matrix=output_matrix, up_matrix=up_matrix, down_matrix=down_matrix, w_head=w_head)


EPS = 1e-05

def normalize(values):
    mean = lax.optimization_barrier(jnp.mean(values, axis=-1, keepdims=True))
    centered = values - mean
    return centered * lax.rsqrt(lax.optimization_barrier(jnp.mean(centered * centered, axis=-1, keepdims=True)) + EPS)

def gelu_tanh(values):
    return 0.5 * values * (1.0 + jnp.tanh(0.7978845608028654 * (values + 0.044715 * values * values * values)))

def attend(query, keys, values_in, lengths):
    scale = query.shape[-1] ** (-0.5)
    scores = jnp.einsum('sqhe,skhe->shqk', query, keys) * scale
    visible = jnp.arange(keys.shape[1], dtype=jnp.int32)[None, :] < lengths[:, None]
    scores = jnp.where(visible[:, None, None, :], scores, -1e+30)
    top = lax.optimization_barrier(jnp.max(scores, axis=-1, keepdims=True))
    expo = jnp.exp(scores - top)
    probs = expo / lax.optimization_barrier(jnp.sum(expo, axis=-1, keepdims=True))
    rounded = lax.optimization_barrier(probs.astype(jnp.bfloat16)).astype(jnp.float32)
    return jnp.einsum('shqk,skhe->sqhe', rounded, values_in)

def rounded_sum(left_operand, right_operand, blocks, inner_value):
    total = None
    for layer_block in range(blocks):
        slice_portion = jnp.einsum('wou,ue->woe', left_operand[:, :, layer_block * inner_value:(layer_block + 1) * inner_value].astype(jnp.float32), right_operand[layer_block * inner_value:(layer_block + 1) * inner_value].astype(jnp.float32))
        slice_portion = lax.optimization_barrier(slice_portion.astype(jnp.bfloat16)).astype(jnp.float32)
        total = slice_portion if total is None else total + slice_portion
    return total

def reference(token_ids, lengths, teacher_bins, embed_table, query_key_value_matrix, output_matrix, up_matrix, down_matrix, w_head):
    sequence_batch, sequence_length = token_ids.shape
    width = embed_table.shape[1]
    first = jnp.take(embed_table, token_ids, axis=0)
    first_normed_rows = normalize(first.astype(jnp.float32)).astype(jnp.bfloat16)
    mixed_output = jnp.einsum('fxw,wvr->fxvr', first_normed_rows.astype(jnp.float32), query_key_value_matrix.astype(jnp.float32)).astype(jnp.bfloat16)
    split = mixed_output.astype(jnp.float32).reshape(sequence_batch, sequence_length, 3, HEAD_COUNT, HEAD_WIDTH)

    def forward_one(item):
        query, keys, vals, count = item
        return attend(query[None], keys[None], vals[None], count[None])[0]
    attended_rows = lax.map(forward_one, (split[:, :, 0], split[:, :, 1], split[:, :, 2], lengths))
    attended_rows = attended_rows.astype(jnp.bfloat16).reshape(sequence_batch, sequence_length, width)
    attn = rounded_sum(attended_rows, output_matrix, N_TENSOR, width // N_TENSOR)
    second = (first.astype(jnp.float32) + attn).astype(jnp.bfloat16)
    second_normed_rows = normalize(second.astype(jnp.float32)).astype(jnp.bfloat16)
    hidden_preactivation = jnp.einsum('ntp,pk->ntk', second_normed_rows.astype(jnp.float32), up_matrix.astype(jnp.float32))
    hidden_activated = gelu_tanh(hidden_preactivation).astype(jnp.bfloat16)
    ffn = rounded_sum(hidden_activated, down_matrix, N_TENSOR, FF // N_TENSOR)
    third = second.astype(jnp.float32) + ffn
    live = (jnp.arange(sequence_length, dtype=jnp.int32)[None, :] < lengths[:, None]).astype(jnp.float32)
    counts = lengths.astype(jnp.float32)[:, None]
    pooled = lax.optimization_barrier(jnp.sum(third * live[:, :, None], axis=1)) / counts
    final, final_back = jax.vjp(normalize, pooled)
    head = w_head.astype(jnp.float32)
    logits = jnp.dot(final, head, precision=lax.Precision.HIGHEST)
    top = lax.optimization_barrier(jnp.max(logits, axis=-1, keepdims=True))
    total_exp = jnp.log(lax.optimization_barrier(jnp.sum(jnp.exp(logits - top), axis=-1, keepdims=True))) + top
    labels = (teacher_bins[:, None] == jnp.arange(logits.shape[1], dtype=jnp.int32)[None, :]).astype(jnp.float32)
    losses = total_exp[:, 0] - lax.optimization_barrier(jnp.sum(logits * labels, axis=-1))
    loss = jnp.sum(losses) / sequence_batch
    g_logits = (jnp.exp(logits - total_exp) - labels) / sequence_batch
    grad_head = jnp.dot(final.T, g_logits, precision=lax.Precision.HIGHEST)
    g_final = jnp.dot(g_logits, head.T, precision=lax.Precision.HIGHEST)
    g_pooled = final_back(g_final)[0]
    per_token = g_pooled / counts
    g_third = per_token[:, None, :] * live[:, :, None]
    third_gradient_batch = g_third.astype(jnp.bfloat16)
    down_weight_gradient = jnp.einsum('omi,omy->iy', hidden_activated.astype(jnp.float32), third_gradient_batch.astype(jnp.float32))
    hidden_gradient = jnp.einsum('tpu,bu->tpb', third_gradient_batch.astype(jnp.float32), down_matrix.astype(jnp.float32))
    gelu_back = jax.vjp(gelu_tanh, hidden_preactivation)[1]
    preact_gradient = gelu_back(hidden_gradient)[0].astype(jnp.bfloat16)
    up_weight_gradient = jnp.einsum('qon,qom->nm', second_normed_rows.astype(jnp.float32), preact_gradient.astype(jnp.float32))
    g_normed_two = rounded_sum(preact_gradient, up_matrix.T, N_TENSOR, FF // N_TENSOR)
    norm_back = jax.vjp(normalize, second.astype(jnp.float32))[1]
    second_gradient = (g_third + norm_back(g_normed_two)[0]).astype(jnp.bfloat16)
    output_weight_gradient = jnp.einsum('jxm,jxn->mn', attended_rows.astype(jnp.float32), second_gradient.astype(jnp.float32))
    attended_gradient = jnp.einsum('kmi,qi->kmq', second_gradient.astype(jnp.float32), output_matrix.astype(jnp.float32)).reshape(sequence_batch, sequence_length, HEAD_COUNT, HEAD_WIDTH)

    def backward_one(item):
        query, keys, vals, count, grad = item
        back = jax.vjp(lambda a, b, c: attend(a[None], b[None], c[None], count[None])[0], query, keys, vals)[1]
        return back(grad)
    g_query, g_keys, g_vals = lax.map(backward_one, (split[:, :, 0], split[:, :, 1], split[:, :, 2], lengths, attended_gradient))
    mixed_gradient = jnp.stack([g_query, g_keys, g_vals], axis=2).reshape(sequence_batch, sequence_length, 3, width).astype(jnp.bfloat16)
    query_key_value_gradient = jnp.einsum('rvt,rvzx->tzx', first_normed_rows.astype(jnp.float32), mixed_gradient.astype(jnp.float32))
    return (loss, query_key_value_gradient, output_weight_gradient, up_weight_gradient, down_weight_gradient, grad_head)
```

```python
import functools

import jax
import jax.numpy as jnp
from jax import lax
from jax.experimental import pallas as pl
from jax.experimental.pallas import tpu as pltpu
from jax.sharding import Mesh
from jax.sharding import PartitionSpec as P

MESH = pl.DeviceIdType.MESH
EPS = 1e-05
F32 = jnp.float32
BF16 = jnp.bfloat16
HIGH = lax.Precision.HIGHEST
VM = pl.BlockSpec(memory_space=pltpu.VMEM)
SM = pl.BlockSpec(memory_space=pltpu.SMEM)


def where_am_i():
    return {name: lax.axis_index(name) for name in ("xl", "z", "c", "y", "xh")}


def add_mod(value, step, size):
    return lax.rem(value + step, size)


def params(number):
    return pltpu.CompilerParams(collective_id=number, has_side_effects=True)


def remote(src, dst, send, recv, device):
    return pltpu.make_async_remote_copy(
        src_ref=src, dst_ref=dst, send_sem=send, recv_sem=recv, device_id=device, device_id_type=MESH
    )


def signal(device):
    pl.semaphore_signal(pltpu.get_barrier_semaphore(), inc=1, device_id=device, device_id_type=MESH)


def normalize(values):
    mean = jnp.mean(values, axis=-1, keepdims=True)
    centered = values - mean
    return centered * lax.rsqrt(jnp.mean(centered * centered, axis=-1, keepdims=True) + EPS)


def normalize_back(values, grad):
    mean = jnp.mean(values, axis=-1, keepdims=True)
    centered = values - mean
    scale = lax.rsqrt(jnp.mean(centered * centered, axis=-1, keepdims=True) + EPS)
    normed = centered * scale
    return scale * (
        grad
        - jnp.mean(grad, axis=-1, keepdims=True)
        - normed * jnp.mean(grad * normed, axis=-1, keepdims=True)
    )


def spread_ids_kernel(src, out, send, recv):
    me = where_am_i()
    xl, z, c, y, xh = (me[n] for n in ("xl", "z", "c", "y", "xh"))
    here = xh == c

    for role in range(2):
        for k in range(4):
            source = dict(
                xl=add_mod(xl, role, 2), c=add_mod(xh, role, 2), xh=c, y=add_mod(y, 4 - k, 4), z=z
            )
            if role == 0 and k == 0:

                @pl.when(jnp.logical_not(here))
                def _(source=source):
                    signal(source)
            else:
                signal(source)
    pl.semaphore_wait(pltpu.get_barrier_semaphore(), jnp.where(here, 7, 8))

    def copy(role, k):
        return remote(
            src,
            out.at[role, y],
            send.at[role, k],
            recv.at[role, k],
            dict(xl=add_mod(xl, role, 2), c=xh, xh=add_mod(c, role, 2), y=add_mod(y, k, 4), z=z),
        )

    for role in range(2):
        for k in range(4):
            if role == 0 and k == 0:

                @pl.when(jnp.logical_not(here))
                def _():
                    copy(0, 0).start()

                @pl.when(here)
                def _():
                    pltpu.make_async_copy(src, out.at[0, y], recv.at[0, 0]).start()
            else:
                copy(role, k).start()
    for role in range(2):
        for k in range(4):
            if role == 0 and k == 0:

                @pl.when(jnp.logical_not(here))
                def _():
                    copy(0, 0).wait_send()
            else:
                copy(role, k).wait_send()
            pltpu.make_async_copy(src, out.at[role, add_mod(y, 4 - k, 4)], recv.at[role, k]).wait()


def spread_ids(packet):
    return pl.pallas_call(
        spread_ids_kernel,
        out_shape=jax.ShapeDtypeStruct((2, 4, 8, 128), jnp.int32),
        in_specs=[VM],
        out_specs=VM,
        scratch_shapes=[pltpu.SemaphoreType.DMA((2, 4)), pltpu.SemaphoreType.DMA((2, 4))],
        compiler_params=params(1),
        name="spread_ids",
    )(packet)


def plane_kernel(count, collect, *refs):
    me = where_am_i()
    xl, z, c, y, xh = (me[n] for n in ("xl", "z", "c", "y", "xh"))
    here = xh == c
    srcs, dsts = refs[:count], refs[count : 2 * count]
    send, recv = refs[2 * count :]
    mine, other = (xh, c) if collect else (c, xh)

    def target(a, k, e):
        swapped = dict(c=e, xh=c) if collect else dict(c=xh, xh=e)
        return dict(xl=add_mod(xl, a, 2), z=add_mod(z, k, 4), y=y, **swapped)

    def origin(a, k, e):
        swapped = dict(c=xh, xh=e) if collect else dict(c=e, xh=c)
        return dict(xl=add_mod(xl, a, 2), z=add_mod(z, 4 - k, 4), y=y, **swapped)

    def number(a, k, e, back):
        return (add_mod(xl, a, 2) * 4 + add_mod(z, 4 - k if back else k, 4)) * 2 + e

    slot = (xl * 4 + z) * 2 + mine

    def block(i, a, k, e):
        if collect and len(srcs[i].shape) == 3 and srcs[i].shape[0] == 16:
            return srcs[i].at[number(a, k, e, False)]
        return srcs[i]

    def copy(i, a, k, e):
        return remote(
            block(i, a, k, e),
            dsts[i].at[slot],
            send.at[i, a, k, e],
            recv.at[i, a, k, mine],
            target(a, k, e),
        )

    places = [(a, k, e) for k in (1, 3, 2, 0) for a in (1, 0) for e in range(2)]

    def is_self(a, k, e):
        return jnp.logical_and(here, e == other)

    for a, k, e in places:
        if a == 0 and k == 0:
            @pl.when(jnp.logical_not(jnp.logical_and(here, e == mine)))
            def _(a=a, k=k, e=e):
                signal(origin(a, k, e))
        else:
            signal(origin(a, k, e))
    pl.semaphore_wait(pltpu.get_barrier_semaphore(), jnp.where(here, 15, 16))
    for i in range(count):
        for a, k, e in places:
            if a == 0 and k == 0:

                @pl.when(jnp.logical_not(is_self(a, k, e)))
                def _(i=i, a=a, k=k, e=e):
                    copy(i, a, k, e).start()

                @pl.when(is_self(a, k, e))
                def _(i=i, a=a, k=k, e=e):
                    pltpu.make_async_copy(
                        block(i, a, k, e), dsts[i].at[slot], recv.at[i, a, k, mine]
                    ).start()
            else:
                copy(i, a, k, e).start()

    def finish(i):
        for a, k, e in places:
            if a == 0 and k == 0:

                @pl.when(jnp.logical_not(is_self(a, k, e)))
                def _(a=a, k=k, e=e):
                    copy(i, a, k, e).wait_send()
            else:
                copy(i, a, k, e).wait_send()
            pltpu.make_async_copy(
                block(i, 0, 0, 0), dsts[i].at[number(a, k, e, True)], recv.at[i, a, k, e]
            ).wait()

    return finish


def spread_kernel(count, *refs):
    finish = plane_kernel(count, False, *refs)
    for i in range(count):
        finish(i)


def spread(shards):
    count = len(shards)
    return pl.pallas_call(
        functools.partial(spread_kernel, count),
        out_shape=[jax.ShapeDtypeStruct((16, *s.shape), s.dtype) for s in shards],
        in_specs=[VM] * count,
        out_specs=[VM] * count,
        scratch_shapes=[pltpu.SemaphoreType.DMA((count, 2, 4, 2))] * 2,
        compiler_params=params(2),
        name="spread_weights",
    )(*shards)


def collect_kernel(count, *refs):
    ins, outs = refs[:count], refs[count : 2 * count]
    bufs = refs[2 * count : 3 * count - 1]
    sems = refs[3 * count - 1 :]
    finish = plane_kernel(count, True, *ins, outs[0], *bufs, *sems)
    finish(0)
    for i in range(1, count):
        finish(i)
        total = bufs[i - 1][0].astype(F32)
        for s in range(1, 16):
            total = total + bufs[i - 1][s].astype(F32)
        outs[i][...] = total


def collect(packet, grads):
    count = 1 + len(grads)
    shapes = [jax.ShapeDtypeStruct((16, *packet.shape), packet.dtype)]
    shapes += [jax.ShapeDtypeStruct(g.shape[1:], F32) for g in grads]
    return pl.pallas_call(
        functools.partial(collect_kernel, count),
        out_shape=shapes,
        in_specs=[VM] * count,
        out_specs=[VM] * count,
        scratch_shapes=[pltpu.VMEM(g.shape, g.dtype) for g in grads]
        + [pltpu.SemaphoreType.DMA((count, 2, 4, 2))] * 2,
        compiler_params=params(3),
        name="collect_gradients",
    )(packet, *grads)


def ring_places():
    me = where_am_i()
    y, c = me["y"], me["c"]
    return me, y, c, add_mod(y, 1, 4), add_mod(y, 3, 4), add_mod(y, 2, 4), 1 - c


HALVES = (pl.ds(0, 64), pl.ds(64, 64))


def to_owner(blocks, stage, far, near, send, recv):
    me, y, c, up, dn, op, oc = ring_places()
    first = [
        remote(blocks(op).at[HALVES[0]], far.at[0], send.at[0], recv.at[0], dict(y=up)),
        remote(blocks(op).at[HALVES[1]], far.at[1], send.at[1], recv.at[1], dict(y=dn)),
    ]
    for step in first:
        step.start()

    def second(side):
        return remote(
            stage.at[side], near.at[side], send.at[2 + side], recv.at[2 + side], dict(y=(up, dn)[side])
        )

    stage[0, 64:128] = blocks(up)[64:128]
    stage[1, 0:64] = blocks(dn)[0:64]
    first[0].wait_recv()
    stage[0, 0:64] = (blocks(up)[0:64].astype(F32) + far[0].astype(F32)).astype(BF16)
    second(0).start()
    first[1].wait_recv()
    stage[1, 64:128] = (blocks(dn)[64:128].astype(F32) + far[1].astype(F32)).astype(BF16)
    second(1).start()

    def finish():
        for step in first:
            step.wait_send()
        second(0).wait()
        second(1).wait()
        return blocks(y)[...].astype(F32) + near[0].astype(F32) + near[1].astype(F32)

    return finish


def to_all(out, send, recv):
    me, y, c, up, dn, op, oc = ring_places()

    def go(k, row, col, part, device):
        ref = out.at[row, col] if part is None else out.at[row, col, HALVES[part]]
        return remote(ref, ref, send.at[k], recv.at[k], device)

    begin = [
        go(0, y, c, None, dict(y=up)),
        go(1, y, c, None, dict(y=dn)),
        go(2, y, c, None, dict(c=oc)),
    ]
    for step in begin:
        step.start()
    begin[0].wait_recv()
    later = [go(3, dn, c, 0, dict(y=up)), go(4, dn, c, None, dict(c=oc))]
    for step in later:
        step.start()
    begin[1].wait_recv()
    later += [go(5, up, c, 1, dict(y=dn)), go(6, up, c, None, dict(c=oc))]
    for step in later[2:]:
        step.start()
    later[0].wait_recv()
    last = [go(7, op, c, 0, dict(c=oc)), go(8, op, c, 1, dict(c=oc))]
    last[0].start()
    later[2].wait_recv()
    last[1].start()
    begin[2].wait_recv()
    later[1].wait_recv()
    later[3].wait_recv()
    last[0].wait_recv()
    last[1].wait_recv()
    for step in begin + later + last:
        step.wait_send()


def embed_kernel(rows, first_out, normed_out, stage, far, near, other, total, rsend, rrecv, asend, arecv):
    me, y, c, up, dn, op, oc = ring_places()
    partner = dict(xl=1 - me["xl"], xh=1 - me["xh"])
    for device in (dict(y=up), dict(y=dn), dict(c=oc), partner):
        signal(device)
    pl.semaphore_wait(pltpu.get_barrier_semaphore(), 4)
    done = [
        to_owner(
            lambda b, role=role: rows.at[role, b],
            stage.at[role],
            far.at[role],
            near.at[role],
            rsend.at[role],
            rrecv.at[role],
        )
        for role in (1, 0)
    ]
    total[...] = done[0]().astype(BF16)
    cross = remote(total, other, rsend.at[2, 0], rrecv.at[2, 0], partner)
    cross.start()
    mine = done[1]()
    cross.wait()
    first = mine + other[...].astype(F32)
    first_out[...] = first.astype(BF16)
    normed_out[y, c] = normalize(first).astype(BF16)
    to_all(normed_out, asend, arecv)


def embed(rows):
    return pl.pallas_call(
        embed_kernel,
        out_shape=[
            jax.ShapeDtypeStruct((128, 1024), BF16),
            jax.ShapeDtypeStruct((4, 2, 128, 1024), BF16),
        ],
        in_specs=[VM],
        out_specs=[VM, VM],
        scratch_shapes=[
            pltpu.VMEM((2, 2, 128, 1024), BF16),
            pltpu.VMEM((2, 2, 64, 1024), BF16),
            pltpu.VMEM((2, 2, 128, 1024), BF16),
            pltpu.VMEM((128, 1024), BF16),
            pltpu.VMEM((128, 1024), BF16),
            pltpu.SemaphoreType.DMA((3, 4)),
            pltpu.SemaphoreType.DMA((3, 4)),
            pltpu.SemaphoreType.DMA((9,)),
            pltpu.SemaphoreType.DMA((9,)),
        ],
        compiler_params=params(4),
        name="embed_exchange",
    )(rows)


def pair_sum_to_owner(terms, pair, summed, stage, far, near, psend, precv, rsend, rrecv):
    me, y, c, up, dn, op, oc = ring_places()
    order = (op, up, dn, y)
    for device in (dict(y=up), dict(y=dn), dict(c=oc)):
        signal(device)
    pl.semaphore_wait(pltpu.get_barrier_semaphore(), 3)
    steps = [
        remote(terms.at[b, oc], pair.at[b], psend.at[i], precv.at[i], dict(c=oc))
        for i, b in enumerate(order)
    ]
    for step in steps:
        step.start()
    for i, b in enumerate(order):
        steps[i].wait_recv()
        summed[b] = (terms[b, c].astype(F32) + pair[b].astype(F32)).astype(BF16)
    total = to_owner(lambda b: summed.at[b], stage, far, near, rsend, rrecv)()
    for step in steps:
        step.wait_send()
    return total


PAIR_SCRATCH = [
    pltpu.VMEM((4, 128, 1024), BF16),
    pltpu.VMEM((4, 128, 1024), BF16),
    pltpu.VMEM((2, 128, 1024), BF16),
    pltpu.VMEM((2, 64, 1024), BF16),
    pltpu.VMEM((2, 128, 1024), BF16),
    pltpu.SemaphoreType.DMA((4,)),
    pltpu.SemaphoreType.DMA((4,)),
    pltpu.SemaphoreType.DMA((4,)),
    pltpu.SemaphoreType.DMA((4,)),
    pltpu.SemaphoreType.DMA((9,)),
    pltpu.SemaphoreType.DMA((9,)),
]


def residual_kernel(terms, first, second_out, normed_out, *scratch):
    me, y, c, up, dn, op, oc = ring_places()
    attn = pair_sum_to_owner(terms, *scratch[:9])
    second = (first[...].astype(F32) + attn).astype(BF16)
    second_out[...] = second
    normed_out[y, c] = normalize(second.astype(F32)).astype(BF16)
    to_all(normed_out, *scratch[9:])


def residual(terms, first):
    return pl.pallas_call(
        residual_kernel,
        out_shape=[
            jax.ShapeDtypeStruct((128, 1024), BF16),
            jax.ShapeDtypeStruct((4, 2, 128, 1024), BF16),
        ],
        in_specs=[VM, VM],
        out_specs=[VM, VM],
        scratch_shapes=PAIR_SCRATCH,
        compiler_params=params(5),
        name="residual_exchange",
    )(terms, first)


def backward_kernel(terms, second, g_third, g_out, *scratch):
    me, y, c, up, dn, op, oc = ring_places()
    grad = pair_sum_to_owner(terms, *scratch[:9])
    g_out[y, c] = (g_third[...] + normalize_back(second[...].astype(F32), grad)).astype(BF16)
    to_all(g_out, *scratch[9:])


def backward(terms, second, g_third):
    return pl.pallas_call(
        backward_kernel,
        out_shape=jax.ShapeDtypeStruct((4, 2, 128, 1024), BF16),
        in_specs=[VM, VM, VM],
        out_specs=VM,
        scratch_shapes=PAIR_SCRATCH,
        compiler_params=params(6),
        name="backward_exchange",
    )(terms, second, g_third)


PACKET = 512 + 1024 + 1024 + 128 + 128


def head_kernel(
    length, label, hidden_sum, second_sum, down_t, head, per_token_out, pulled_out, packet_out, parts, send, recv
):
    me, y, c, up, dn, op, oc = ring_places()
    slot = y * 2 + c
    peers = [(k, e) for k in (0, 1, 3, 2) for e in range(2) if (k, e) != (0, 0)]

    def device(k, e):
        return dict(y=add_mod(y, k, 4), c=add_mod(c, e, 2))

    for k, e in peers:
        signal(device(4 - k if k else 0, e))
    pl.semaphore_wait(pltpu.get_barrier_semaphore(), 7)
    contract = (((1,), (1,)), ((), ()))
    parts[slot] = second_sum[...] + lax.dot_general(
        hidden_sum[...], down_t[...].astype(F32), contract, precision=HIGH, preferred_element_type=F32
    )
    steps = [
        remote(parts.at[slot], parts.at[slot], send.at[k, e], recv.at[k, e], device(k, e)) for k, e in peers
    ]
    for step in steps:
        step.start()
    for step in steps:
        step.wait()
    pooled = parts[0]
    for s in range(1, 8):
        pooled = pooled + parts[s]
    count = length[0].astype(F32)
    pooled = pooled / count
    final = normalize(pooled)
    wide = head[...].astype(F32)
    logits = jnp.dot(final, wide, precision=HIGH, preferred_element_type=F32)
    top = jnp.max(logits, axis=-1, keepdims=True)
    total = jnp.log(jnp.sum(jnp.exp(logits - top), axis=-1, keepdims=True)) + top
    labels = (lax.broadcasted_iota(jnp.int32, logits.shape, 1) == label[0]).astype(F32)
    loss = total - jnp.sum(logits * labels, axis=-1, keepdims=True)
    g_logits = (jnp.exp(logits - total) - labels) / 16.0
    g_final = lax.dot_general(g_logits, wide, contract, precision=HIGH, preferred_element_type=F32)
    per_token = normalize_back(pooled, g_final) / count
    rounded = per_token.astype(BF16)
    per_token_out[...] = per_token
    pulled_out[...] = jnp.dot(rounded, down_t[...], preferred_element_type=F32)
    packet_out[:, 0:512] = hidden_sum[...]
    packet_out[:, 512:1536] = rounded.astype(F32)
    packet_out[:, 1536:2560] = final
    packet_out[:, 2560:2688] = g_logits
    packet_out[:, 2688:2816] = jnp.broadcast_to(loss, (1, 128))


def classify(length, label, hidden_sum, second_sum, down_t, head):
    return pl.pallas_call(
        head_kernel,
        out_shape=[
            jax.ShapeDtypeStruct((1, 1024), F32),
            jax.ShapeDtypeStruct((1, 512), F32),
            jax.ShapeDtypeStruct((1, PACKET), F32),
        ],
        in_specs=[SM, SM, VM, VM, VM, VM],
        out_specs=[VM, VM, VM],
        scratch_shapes=[
            pltpu.VMEM((8, 1, 1024), F32),
            pltpu.SemaphoreType.DMA((4, 2)),
            pltpu.SemaphoreType.DMA((4, 2)),
        ],
        compiler_params=params(7),
        name="classify",
    )(length, label, hidden_sum, second_sum, down_t, head)


SCALE = 0.125
WIDE = 256


def head_rows(value, head):
    rows = lax.broadcasted_iota(jnp.int32, value.shape, 0)
    return jnp.where((rows >= 64) == (head == 1), value, jnp.zeros_like(value))


def head_cols(value, head):
    cols = lax.broadcasted_iota(jnp.int32, value.shape, 1)
    return jnp.where((cols >= 64) == (head == 1), value, jnp.zeros_like(value))


def attend_kernel(length, qkv, context, context_t, probs_t):
    keys = qkv[:, 128:256]
    query_t = qkv[:, 0:128].T
    values_t = qkv[:, 256:384].T
    seen = lax.broadcasted_iota(jnp.int32, (1024, WIDE), 0) < length[0]
    for block in range(1024 // WIDE):
        cols = slice(block * WIDE, (block + 1) * WIDE)
        for head in range(2):
            scores = jnp.dot(keys, head_rows(query_t[:, cols], head), preferred_element_type=F32) * SCALE
            scores = jnp.where(seen, scores, -1e30)
            expo = jnp.exp(scores - jnp.max(scores, axis=0, keepdims=True))
            probs = (expo * (1.0 / jnp.sum(expo, axis=0, keepdims=True))).astype(BF16)
            probs_t[head, :, cols] = probs
            rows = slice(head * 64, head * 64 + 64)
            context_t[rows, cols] = jnp.dot(values_t[rows], probs, preferred_element_type=F32).astype(BF16)
    context[...] = context_t[...].T


def attend(length, qkv):
    return pl.pallas_call(
        attend_kernel,
        out_shape=[
            jax.ShapeDtypeStruct((1024, 128), BF16),
            jax.ShapeDtypeStruct((128, 1024), BF16),
            jax.ShapeDtypeStruct((2, 1024, 1024), BF16),
        ],
        in_specs=[SM, VM],
        out_specs=[VM, VM, VM],
        compiler_params=pltpu.CompilerParams(vmem_limit_bytes=48 * 2**20),
        name="attend",
    )(length, qkv)


def attend_back_kernel(qkv, probs_t, context_t, grad, out, grad_q, grad_k, grad_v):
    query = qkv[:, 0:128]
    keys_t = qkv[:, 128:256].T
    values = qkv[:, 256:384]
    grad_t = grad[...].T
    product = grad_t * context_t[...].astype(F32)
    for block in range(1024 // WIDE):
        cols = slice(block * WIDE, (block + 1) * WIDE)
        for head in range(2):
            rows = slice(head * 64, head * 64 + 64)
            probs = probs_t[head, :, cols]
            delta = jnp.sum(product[rows, cols], axis=0, keepdims=True)
            pulled = jnp.dot(values, head_rows(grad_t[:, cols], head).astype(BF16), preferred_element_type=F32)
            g_scores = (probs.astype(F32) * (pulled - delta) * SCALE).astype(BF16)
            grad_q[rows, cols] = jnp.dot(keys_t[rows], g_scores, preferred_element_type=F32)
            g_keys = jnp.dot(g_scores, head_cols(query[cols], head), preferred_element_type=F32)
            g_vals = jnp.dot(probs, head_cols(grad[cols], head).astype(BF16), preferred_element_type=F32)
            if block == 0 and head == 0:
                grad_k[...] = g_keys
                grad_v[...] = g_vals
            else:
                grad_k[...] += g_keys
                grad_v[...] += g_vals
    out[:, 0:128] = grad_q[...].T.astype(BF16)
    out[:, 128:256] = grad_k[...].astype(BF16)
    out[:, 256:384] = grad_v[...].astype(BF16)


def attend_back(qkv, probs_t, context_t, grad):
    return pl.pallas_call(
        attend_back_kernel,
        out_shape=jax.ShapeDtypeStruct((1024, 384), BF16),
        in_specs=[VM, VM, VM, VM],
        out_specs=VM,
        scratch_shapes=[
            pltpu.VMEM((128, 1024), F32),
            pltpu.VMEM((1024, 128), F32),
            pltpu.VMEM((1024, 128), F32),
        ],
        compiler_params=pltpu.CompilerParams(vmem_limit_bytes=48 * 2**20),
        name="attend_back",
    )(qkv, probs_t, context_t, grad)


def gelu(values):
    inner = jnp.tanh(0.7978845608028654 * (values + 0.044715 * values * values * values))
    return 0.5 * values * (1.0 + inner)


def gelu_slope(values):
    inner = jnp.tanh(0.7978845608028654 * (values + 0.044715 * values * values * values))
    return 0.5 * (1.0 + inner) + 0.5 * values * (1.0 - inner * inner) * 0.7978845608028654 * (
        1.0 + 3.0 * 0.044715 * values * values
    )


def per_device(token_ids, lengths, teacher_bins, table, qkv_shard, out_shard, up_shard, down_shard, head_shard):
    me = where_am_i()
    spot = (me["xl"] * 4 + me["z"]) * 2 + me["c"]
    vocab = table.shape[0]

    packet = jnp.concatenate(
        [
            token_ids,
            jnp.broadcast_to(lengths[:, None], (1, 128)),
            jnp.broadcast_to(teacher_bins[:, None], (1, 128)),
            jnp.zeros((5, 128), jnp.int32),
        ],
        axis=0,
    )
    got = spread_ids(packet)
    length = got[0, 0, 1, 0:1]
    label = got[0, 0, 2, 0:1]
    qkv_w, out_w, up_w, down_w, head_w = spread(
        [qkv_shard.reshape(64, 384), out_shard.T, up_shard, down_shard.T, head_shard]
    )
    qkv_w = qkv_w.reshape(1024, 384)
    out_w = out_w.reshape(1024, 128)
    up_w = up_w.reshape(1024, 512)
    down_w = down_w.reshape(1024, 512)
    head_w = head_w.reshape(1024, 128)

    shifted = got[:, :, 0, :] - (me["y"] * 2 + me["xh"]) * vocab
    inside = (shifted >= 0) & (shifted < vocab)
    rows = jnp.take(table, jnp.clip(shifted, 0, vocab - 1), axis=0)
    rows = jnp.where(inside[..., None], rows, jnp.zeros_like(rows))
    first, normed = embed(rows)
    normed = normed.reshape(1024, 1024)
    qkv = jnp.dot(normed, qkv_w, preferred_element_type=F32).astype(BF16)
    context, context_t, probs_t = attend(length, qkv)
    terms = jnp.einsum("ph,dh->pd", context, out_w, preferred_element_type=F32).astype(BF16)
    second, normed_two = residual(terms.reshape(4, 2, 128, 1024), first)
    normed_two = normed_two.reshape(1024, 1024)
    hidden = jnp.dot(normed_two, up_w, preferred_element_type=F32)
    live = (jnp.arange(1024, dtype=jnp.int32)[:, None] < length[0]).astype(F32)
    own = (me["y"] * 2 + me["c"]) * 128 + jnp.arange(128, dtype=jnp.int32)[:, None]
    live_own = (own < length[0]).astype(F32)
    hidden_sum = jnp.sum(gelu(hidden).astype(BF16).astype(F32) * live, axis=0, keepdims=True)
    second_sum = jnp.sum(second.astype(F32) * live_own, axis=0, keepdims=True)
    per_token, pulled, packet = classify(length, label, hidden_sum, second_sum, down_w, head_w)
    g_pre = (gelu_slope(hidden) * (pulled * live)).astype(BF16)
    up_term = jnp.einsum("pd,pf->df", normed_two, g_pre, preferred_element_type=F32).astype(BF16)
    terms = jnp.einsum("pf,df->pd", g_pre, up_w, preferred_element_type=F32).astype(BF16)
    g_second = backward(terms.reshape(4, 2, 128, 1024), second, per_token * live_own).reshape(1024, 1024)
    out_term = jnp.einsum("pd,ph->dh", g_second, context, preferred_element_type=F32).astype(BF16)
    g_context = jnp.einsum("pd,dh->ph", g_second, out_w, preferred_element_type=F32)
    g_qkv = attend_back(qkv, probs_t, context_t, g_context)
    qkv_term = jnp.einsum("pd,pr->dr", normed, g_qkv, preferred_element_type=F32).astype(BF16)
    packets, up_grad, out_grad, qkv_grad = collect(
        packet,
        [up_term.reshape(16, 64, 512), out_term.reshape(16, 64, 128), qkv_term.reshape(16, 64, 384)],
    )
    packets = packets.reshape(16, PACKET)
    loss = jnp.sum(packets[:, 2688]) / 16.0
    part = lax.dynamic_slice_in_dim(packets[:, 512:1536], spot * 64, 64, axis=1)
    down_grad = jnp.einsum("sf,sd->fd", packets[:, 0:512], part, precision=HIGH)
    part = lax.dynamic_slice_in_dim(packets[:, 1536:2560], spot * 64, 64, axis=1)
    head_grad = jnp.einsum("sd,sn->dn", part, packets[:, 2560:2688], precision=HIGH)
    return loss, qkv_grad.reshape(64, 3, 128), out_grad.T, up_grad, down_grad, head_grad


def solution(mesh):
    fine = Mesh(mesh.devices.reshape(2, 4, 2, 4, 2), ("xl", "z", "c", "y", "xh"))
    dp, tensor = ("xl", "z", "c"), ("y", "xh")
    return jax.shard_map(
        per_device,
        mesh=fine,
        in_specs=(
            P(dp, tensor),
            P(dp),
            P(dp),
            P(tensor, None),
            P(dp, None, tensor),
            P(tensor, dp),
            P(dp, tensor),
            P(tensor, dp),
            P(dp, None),
        ),
        out_specs=(
            P(),
            P(dp, None, tensor),
            P(tensor, dp),
            P(dp, tensor),
            P(tensor, dp),
            P(dp, None),
        ),
        check_vma=False,
    )
```

```python
import functools

import jax
import jax.numpy as jnp
from jax import lax
from jax.experimental import pallas as pl
from jax.experimental.pallas import tpu as pltpu
from jax.sharding import Mesh
from jax.sharding import PartitionSpec as P

MESH = pl.DeviceIdType.MESH
EPS = 1e-05
F32 = jnp.float32
BF16 = jnp.bfloat16
HIGH = lax.Precision.HIGHEST
VM = pl.BlockSpec(memory_space=pltpu.VMEM)
SM = pl.BlockSpec(memory_space=pltpu.SMEM)


def where_am_i():
    return {name: lax.axis_index(name) for name in ("xl", "z", "c", "y", "xh")}


def add_mod(value, step, size):
    return lax.rem(value + step, size)


def params(number):
    return pltpu.CompilerParams(collective_id=number, has_side_effects=True)


def remote(src, dst, send, recv, device):
    return pltpu.make_async_remote_copy(
        src_ref=src, dst_ref=dst, send_sem=send, recv_sem=recv, device_id=device, device_id_type=MESH
    )


def signal(device):
    pl.semaphore_signal(pltpu.get_barrier_semaphore(), inc=1, device_id=device, device_id_type=MESH)


def normalize(values):
    mean = jnp.mean(values, axis=-1, keepdims=True)
    centered = values - mean
    return centered * lax.rsqrt(jnp.mean(centered * centered, axis=-1, keepdims=True) + EPS)


def normalize_back(values, grad):
    mean = jnp.mean(values, axis=-1, keepdims=True)
    centered = values - mean
    scale = lax.rsqrt(jnp.mean(centered * centered, axis=-1, keepdims=True) + EPS)
    normed = centered * scale
    return scale * (
        grad
        - jnp.mean(grad, axis=-1, keepdims=True)
        - normed * jnp.mean(grad * normed, axis=-1, keepdims=True)
    )


def spread_ids_kernel(src, out, send, recv):
    me = where_am_i()
    xl, z, c, y, xh = (me[n] for n in ("xl", "z", "c", "y", "xh"))
    here = xh == c

    for role in range(2):
        for k in range(4):
            source = dict(
                xl=add_mod(xl, role, 2), c=add_mod(xh, role, 2), xh=c, y=add_mod(y, 4 - k, 4), z=z
            )
            if role == 0 and k == 0:

                @pl.when(jnp.logical_not(here))
                def _(source=source):
                    signal(source)
            else:
                signal(source)
    pl.semaphore_wait(pltpu.get_barrier_semaphore(), jnp.where(here, 7, 8))

    def copy(role, k):
        return remote(
            src,
            out.at[role, y],
            send.at[role, k],
            recv.at[role, k],
            dict(xl=add_mod(xl, role, 2), c=xh, xh=add_mod(c, role, 2), y=add_mod(y, k, 4), z=z),
        )

    for role in range(2):
        for k in range(4):
            if role == 0 and k == 0:

                @pl.when(jnp.logical_not(here))
                def _():
                    copy(0, 0).start()

                @pl.when(here)
                def _():
                    pltpu.make_async_copy(src, out.at[0, y], recv.at[0, 0]).start()
            else:
                copy(role, k).start()
    for role in range(2):
        for k in range(4):
            if role == 0 and k == 0:

                @pl.when(jnp.logical_not(here))
                def _():
                    copy(0, 0).wait_send()
            else:
                copy(role, k).wait_send()
            pltpu.make_async_copy(src, out.at[role, add_mod(y, 4 - k, 4)], recv.at[role, k]).wait()


def spread_ids(packet):
    return pl.pallas_call(
        spread_ids_kernel,
        out_shape=jax.ShapeDtypeStruct((2, 4, 8, 128), jnp.int32),
        in_specs=[VM],
        out_specs=VM,
        scratch_shapes=[pltpu.SemaphoreType.DMA((2, 4)), pltpu.SemaphoreType.DMA((2, 4))],
        compiler_params=params(1),
        name="spread_ids",
    )(packet)


class Plane:
    def __init__(self, srcs, dsts, send, recv, collect):
        self.srcs, self.dsts, self.send, self.recv, self.collect = srcs, dsts, send, recv, collect
        self.me = where_am_i()
        c, xh = self.me["c"], self.me["xh"]
        self.here = xh == c
        self.mine, self.other = (xh, c) if collect else (c, xh)
        self.slot = (self.me["xl"] * 4 + self.me["z"]) * 2 + self.mine
        self.places = [(a, k, e) for k in (2, 1, 3, 0) for a in (1, 0) for e in range(2)]

    def target(self, a, k, e):
        me = self.me
        swapped = dict(c=e, xh=me["c"]) if self.collect else dict(c=me["xh"], xh=e)
        return dict(xl=add_mod(me["xl"], a, 2), z=add_mod(me["z"], k, 4), y=me["y"], **swapped)

    def origin(self, a, k, e):
        me = self.me
        swapped = dict(c=me["xh"], xh=e) if self.collect else dict(c=e, xh=me["c"])
        return dict(xl=add_mod(me["xl"], a, 2), z=add_mod(me["z"], 4 - k, 4), y=me["y"], **swapped)

    def number(self, a, k, e, back):
        me = self.me
        return (add_mod(me["xl"], a, 2) * 4 + add_mod(me["z"], 4 - k if back else k, 4)) * 2 + e

    def block(self, i, a, k, e):
        if self.collect and len(self.srcs[i].shape) == 3 and self.srcs[i].shape[0] == 16:
            return self.srcs[i].at[self.number(a, k, e, False)]
        return self.srcs[i]

    def copy(self, i, a, k, e):
        return remote(
            self.block(i, a, k, e),
            self.dsts[i].at[self.slot],
            self.send.at[i, a, k, e],
            self.recv.at[i, a, k, self.mine],
            self.target(a, k, e),
        )

    def greet(self):
        for a, k, e in self.places:
            if a == 0 and k == 0:

                @pl.when(jnp.logical_not(jnp.logical_and(self.here, e == self.mine)))
                def _(a=a, k=k, e=e):
                    signal(self.origin(a, k, e))
            else:
                signal(self.origin(a, k, e))
        return jnp.where(self.here, 15, 16)

    def is_self(self, e):
        return jnp.logical_and(self.here, e == self.other)

    def start(self, i):
        for a, k, e in self.places:
            if a == 0 and k == 0:

                @pl.when(jnp.logical_not(self.is_self(e)))
                def _(a=a, k=k, e=e):
                    self.copy(i, a, k, e).start()

                @pl.when(self.is_self(e))
                def _(a=a, k=k, e=e):
                    pltpu.make_async_copy(
                        self.block(i, a, k, e), self.dsts[i].at[self.slot], self.recv.at[i, a, k, self.mine]
                    ).start()
            else:
                self.copy(i, a, k, e).start()

    def finish(self, i):
        for a, k, e in self.places:
            if a == 0 and k == 0:

                @pl.when(jnp.logical_not(self.is_self(e)))
                def _(a=a, k=k, e=e):
                    self.copy(i, a, k, e).wait_send()
            else:
                self.copy(i, a, k, e).wait_send()
            pltpu.make_async_copy(
                self.block(i, 0, 0, 0), self.dsts[i].at[self.number(a, k, e, True)], self.recv.at[i, a, k, e]
            ).wait()


def plane_sems(count):
    return [pltpu.SemaphoreType.DMA((count, 2, 4, 2))] * 2


def gathered(shard):
    return jax.ShapeDtypeStruct((16, *shard.shape), shard.dtype)


def total_of(buf):
    total = buf[0].astype(F32)
    for s in range(1, 16):
        total = total + buf[s].astype(F32)
    return total


def thirds(row):
    high = row.astype(BF16).astype(F32)
    middle = (row - high).astype(BF16).astype(F32)
    low = row - high - middle
    index = lax.broadcasted_iota(jnp.int32, (8, row.shape[1]), 0)
    rows = jnp.where(index == 0, high, jnp.where(index == 1, middle, jnp.where(index == 2, low, 0.0)))
    return rows.astype(BF16)


def picked(values, start):
    rows = lax.broadcasted_iota(jnp.int32, (values.shape[1], 64), 0)
    cols = lax.broadcasted_iota(jnp.int32, (values.shape[1], 64), 1)
    chosen = (rows == cols + start).astype(F32)
    return jnp.dot(values, chosen, precision=HIGH, preferred_element_type=F32)


def collect_kernel(packets, out_term, qkv_term, out_grad, qkv_grad, down_grad, head_grad, loss, out_buf, qkv_buf, send, recv):
    plane = Plane([out_term, qkv_term], [out_buf, qkv_buf], send, recv, True)
    pl.semaphore_wait(pltpu.get_barrier_semaphore(), plane.greet())
    plane.start(0)
    plane.start(1)
    me = plane.me
    start = ((me["xl"] * 4 + me["z"]) * 2 + me["c"]) * 64
    over = (((0,), (0,)), ((), ()))
    down_grad[...] = lax.dot_general(
        packets[:, 0:512], picked(packets[:, 512:1536], start), over, precision=HIGH, preferred_element_type=F32
    )
    head_grad[...] = lax.dot_general(
        picked(packets[:, 1536:2560], start), packets[:, 2560:2688], over, precision=HIGH, preferred_element_type=F32
    )
    loss[...] = jnp.sum(packets[:, 2688:2816], axis=0, keepdims=True) / 16.0
    plane.finish(0)
    out_grad[...] = total_of(out_buf)
    plane.finish(1)
    qkv_grad[...] = total_of(qkv_buf)


def collect(packets, out_term, qkv_term):
    return pl.pallas_call(
        collect_kernel,
        out_shape=[
            jax.ShapeDtypeStruct((64, 128), F32),
            jax.ShapeDtypeStruct((64, 384), F32),
            jax.ShapeDtypeStruct((512, 64), F32),
            jax.ShapeDtypeStruct((64, 128), F32),
            jax.ShapeDtypeStruct((1, 128), F32),
        ],
        in_specs=[VM] * 3,
        out_specs=[VM] * 5,
        scratch_shapes=[pltpu.VMEM((16, 64, 128), BF16), pltpu.VMEM((16, 64, 384), BF16), *plane_sems(2)],
        compiler_params=params(3),
        name="collect_gradients",
    )(packets, out_term, qkv_term)


def ring_places():
    me = where_am_i()
    y, c = me["y"], me["c"]
    return me, y, c, add_mod(y, 1, 4), add_mod(y, 3, 4), add_mod(y, 2, 4), 1 - c


HALVES = (pl.ds(0, 64), pl.ds(64, 64))


def to_owner(blocks, stage, far, near, send, recv, meanwhile=None):
    me, y, c, up, dn, op, oc = ring_places()
    first = [
        remote(blocks(op).at[HALVES[0]], far.at[0], send.at[0], recv.at[0], dict(y=up)),
        remote(blocks(op).at[HALVES[1]], far.at[1], send.at[1], recv.at[1], dict(y=dn)),
    ]
    for step in first:
        step.start()
    if meanwhile is not None:
        meanwhile()

    def second(side):
        return remote(
            stage.at[side], near.at[side], send.at[2 + side], recv.at[2 + side], dict(y=(up, dn)[side])
        )

    stage[0, 64:128] = blocks(up)[64:128]
    stage[1, 0:64] = blocks(dn)[0:64]
    first[0].wait_recv()
    stage[0, 0:64] = (blocks(up)[0:64].astype(F32) + far[0].astype(F32)).astype(BF16)
    second(0).start()
    first[1].wait_recv()
    stage[1, 64:128] = (blocks(dn)[64:128].astype(F32) + far[1].astype(F32)).astype(BF16)
    second(1).start()

    def finish():
        for step in first:
            step.wait_send()
        second(0).wait()
        second(1).wait()
        return blocks(y)[...].astype(F32) + near[0].astype(F32) + near[1].astype(F32)

    return finish


def to_all(out, send, recv):
    me, y, c, up, dn, op, oc = ring_places()

    def go(k, row, col, part, device):
        ref = out.at[row, col] if part is None else out.at[row, col, HALVES[part]]
        return remote(ref, ref, send.at[k], recv.at[k], device)

    begin = [
        go(0, y, c, None, dict(y=up)),
        go(1, y, c, None, dict(y=dn)),
        go(2, y, c, None, dict(c=oc)),
    ]
    for step in begin:
        step.start()
    begin[0].wait_recv()
    later = [go(3, dn, c, 0, dict(y=up)), go(4, dn, c, None, dict(c=oc))]
    for step in later:
        step.start()
    begin[1].wait_recv()
    later += [go(5, up, c, 1, dict(y=dn)), go(6, up, c, None, dict(c=oc))]
    for step in later[2:]:
        step.start()
    later[0].wait_recv()
    last = [go(7, op, c, 0, dict(c=oc)), go(8, op, c, 1, dict(c=oc))]
    last[0].start()
    later[2].wait_recv()
    last[1].start()
    begin[2].wait_recv()
    later[1].wait_recv()
    later[3].wait_recv()
    last[0].wait_recv()
    last[1].wait_recv()
    for step in begin + later + last:
        step.wait_send()


def embed_kernel(
    rows, qkv_s, out_s, head_s, first_out, normed_out, qkv_w, out_w, head_w,
    stage, far, near, other, total, rsend, rrecv, asend, arecv, psend, precv,
):
    me, y, c, up, dn, op, oc = ring_places()
    plane = Plane([qkv_s, out_s, head_s], [qkv_w, out_w, head_w], psend, precv, False)
    partner = dict(xl=1 - me["xl"], xh=1 - me["xh"])
    for device in (dict(y=up), dict(y=dn), dict(c=oc), partner):
        signal(device)
    pl.semaphore_wait(pltpu.get_barrier_semaphore(), plane.greet() + 4)
    done = [
        to_owner(
            lambda b, role=role: rows.at[role, b],
            stage.at[role],
            far.at[role],
            near.at[role],
            rsend.at[role],
            rrecv.at[role],
            (lambda: [plane.start(i) for i in range(3)]) if role == 1 else None,
        )
        for role in (1, 0)
    ]
    total[...] = done[0]().astype(BF16)
    cross = remote(total, other, rsend.at[2, 0], rrecv.at[2, 0], partner)
    cross.start()
    mine = done[1]()
    cross.wait()
    first = mine + other[...].astype(F32)
    first_out[...] = first.astype(BF16)
    normed_out[y, c] = normalize(first).astype(BF16)
    to_all(normed_out, asend, arecv)
    for i in range(3):
        plane.finish(i)


def embed(rows, shards):
    return pl.pallas_call(
        embed_kernel,
        out_shape=[
            jax.ShapeDtypeStruct((128, 1024), BF16),
            jax.ShapeDtypeStruct((4, 2, 128, 1024), BF16),
            *map(gathered, shards),
        ],
        in_specs=[VM] * 4,
        out_specs=[VM] * 5,
        scratch_shapes=[
            pltpu.VMEM((2, 2, 128, 1024), BF16),
            pltpu.VMEM((2, 2, 64, 1024), BF16),
            pltpu.VMEM((2, 2, 128, 1024), BF16),
            pltpu.VMEM((128, 1024), BF16),
            pltpu.VMEM((128, 1024), BF16),
            pltpu.SemaphoreType.DMA((3, 4)),
            pltpu.SemaphoreType.DMA((3, 4)),
            pltpu.SemaphoreType.DMA((9,)),
            pltpu.SemaphoreType.DMA((9,)),
            *plane_sems(3),
        ],
        compiler_params=params(4),
        name="embed_exchange",
    )(rows, *shards)


def pair_sum_to_owner(plane, terms, pair, summed, stage, far, near, psend, precv, rsend, rrecv):
    me, y, c, up, dn, op, oc = ring_places()
    order = (op, up, dn, y)
    for device in (dict(y=up), dict(y=dn), dict(c=oc)):
        signal(device)
    pl.semaphore_wait(pltpu.get_barrier_semaphore(), plane.greet() + 3)
    steps = [
        remote(terms.at[b, oc], pair.at[b], psend.at[i], precv.at[i], dict(c=oc))
        for i, b in enumerate(order)
    ]
    for step in steps:
        step.start()
    for i in range(len(plane.srcs)):
        plane.start(i)
    for i, b in enumerate(order):
        steps[i].wait_recv()
        summed[b] = (terms[b, c].astype(F32) + pair[b].astype(F32)).astype(BF16)
    total = to_owner(lambda b: summed.at[b], stage, far, near, rsend, rrecv)()
    for step in steps:
        step.wait_send()
    return total


PAIR_SCRATCH = [
    pltpu.VMEM((4, 128, 1024), BF16),
    pltpu.VMEM((4, 128, 1024), BF16),
    pltpu.VMEM((2, 128, 1024), BF16),
    pltpu.VMEM((2, 64, 1024), BF16),
    pltpu.VMEM((2, 128, 1024), BF16),
    pltpu.SemaphoreType.DMA((4,)),
    pltpu.SemaphoreType.DMA((4,)),
    pltpu.SemaphoreType.DMA((4,)),
    pltpu.SemaphoreType.DMA((4,)),
    pltpu.SemaphoreType.DMA((9,)),
    pltpu.SemaphoreType.DMA((9,)),
    *plane_sems(2),
]


def residual_kernel(terms, first, up_s, down_s, second_out, normed_out, up_w, down_w, *scratch):
    me, y, c, up, dn, op, oc = ring_places()
    plane = Plane([up_s, down_s], [up_w, down_w], *scratch[11:], False)
    attn = pair_sum_to_owner(plane, terms, *scratch[:9])
    second = (first[...].astype(F32) + attn).astype(BF16)
    second_out[...] = second
    normed_out[y, c] = normalize(second.astype(F32)).astype(BF16)
    to_all(normed_out, *scratch[9:11])
    plane.finish(0)
    plane.finish(1)


def residual(terms, first, shards):
    return pl.pallas_call(
        residual_kernel,
        out_shape=[
            jax.ShapeDtypeStruct((128, 1024), BF16),
            jax.ShapeDtypeStruct((4, 2, 128, 1024), BF16),
            *map(gathered, shards),
        ],
        in_specs=[VM] * 4,
        out_specs=[VM] * 4,
        scratch_shapes=PAIR_SCRATCH,
        compiler_params=params(5),
        name="residual_exchange",
    )(terms, first, *shards)


def backward_kernel(terms, second, g_third, up_term, packet, g_out, up_grad, packets, up_buf, *scratch):
    me, y, c, up, dn, op, oc = ring_places()
    plane = Plane([packet, up_term], [packets, up_buf], *scratch[11:], True)
    grad = pair_sum_to_owner(plane, terms, *scratch[:9])
    g_out[y, c] = (g_third[...] + normalize_back(second[...].astype(F32), grad)).astype(BF16)
    to_all(g_out, *scratch[9:11])
    plane.finish(0)
    plane.finish(1)
    up_grad[...] = total_of(up_buf)


def backward(terms, second, g_third, up_term, packet):
    return pl.pallas_call(
        backward_kernel,
        out_shape=[
            jax.ShapeDtypeStruct((4, 2, 128, 1024), BF16),
            jax.ShapeDtypeStruct((64, 512), F32),
            gathered(packet),
        ],
        in_specs=[VM] * 5,
        out_specs=[VM] * 3,
        scratch_shapes=[pltpu.VMEM((16, 64, 512), BF16), *PAIR_SCRATCH],
        compiler_params=params(6),
        name="backward_exchange",
    )(terms, second, g_third, up_term, packet)


PACKET = 512 + 1024 + 1024 + 128 + 128


def head_kernel(
    length, label, hidden_sum, second_sum, down_t, head, per_token_out, pulled_out, packet_out, parts, send, recv
):
    me, y, c, up, dn, op, oc = ring_places()
    slot = y * 2 + c
    peers = [(k, e) for k in (0, 1, 3, 2) for e in range(2) if (k, e) != (0, 0)]

    def device(k, e):
        return dict(y=add_mod(y, k, 4), c=add_mod(c, e, 2))

    for k, e in peers:
        signal(device(4 - k if k else 0, e))
    pl.semaphore_wait(pltpu.get_barrier_semaphore(), 7)
    contract = (((1,), (1,)), ((), ()))
    pushed = lax.dot_general(thirds(hidden_sum[...]), down_t[...], contract, preferred_element_type=F32)
    parts[slot] = second_sum[...] + jnp.sum(pushed, axis=0, keepdims=True)
    steps = [
        remote(parts.at[slot], parts.at[slot], send.at[k, e], recv.at[k, e], device(k, e)) for k, e in peers
    ]
    for step in steps:
        step.start()
    for step in steps:
        step.wait()
    pooled = parts[0]
    for s in range(1, 8):
        pooled = pooled + parts[s]
    count = length[0].astype(F32)
    pooled = pooled / count
    final = normalize(pooled)
    logits = jnp.sum(jnp.dot(thirds(final), head[...], preferred_element_type=F32), axis=0, keepdims=True)
    top = jnp.max(logits, axis=-1, keepdims=True)
    total = jnp.log(jnp.sum(jnp.exp(logits - top), axis=-1, keepdims=True)) + top
    labels = (lax.broadcasted_iota(jnp.int32, logits.shape, 1) == label[0]).astype(F32)
    loss = total - jnp.sum(logits * labels, axis=-1, keepdims=True)
    g_logits = (jnp.exp(logits - total) - labels) / 16.0
    g_final = lax.dot_general(thirds(g_logits), head[...], contract, preferred_element_type=F32)
    g_final = jnp.sum(g_final, axis=0, keepdims=True)
    per_token = normalize_back(pooled, g_final) / count
    rounded = per_token.astype(BF16)
    per_token_out[...] = per_token
    pulled_out[...] = jnp.dot(rounded, down_t[...], preferred_element_type=F32)
    packet_out[:, 0:512] = hidden_sum[...]
    packet_out[:, 512:1536] = rounded.astype(F32)
    packet_out[:, 1536:2560] = final
    packet_out[:, 2560:2688] = g_logits
    packet_out[:, 2688:2816] = jnp.broadcast_to(loss, (1, 128))


def classify(length, label, hidden_sum, second_sum, down_t, head):
    return pl.pallas_call(
        head_kernel,
        out_shape=[
            jax.ShapeDtypeStruct((1, 1024), F32),
            jax.ShapeDtypeStruct((1, 512), F32),
            jax.ShapeDtypeStruct((1, PACKET), F32),
        ],
        in_specs=[SM, SM, VM, VM, VM, VM],
        out_specs=[VM, VM, VM],
        scratch_shapes=[
            pltpu.VMEM((8, 1, 1024), F32),
            pltpu.SemaphoreType.DMA((4, 2)),
            pltpu.SemaphoreType.DMA((4, 2)),
        ],
        compiler_params=params(7),
        name="classify",
    )(length, label, hidden_sum, second_sum, down_t, head)


SCALE = 0.125
WIDE = 256


def head_rows(value, head):
    rows = lax.broadcasted_iota(jnp.int32, value.shape, 0)
    return jnp.where((rows >= 64) == (head == 1), value, jnp.zeros_like(value))


def head_cols(value, head):
    cols = lax.broadcasted_iota(jnp.int32, value.shape, 1)
    return jnp.where((cols >= 64) == (head == 1), value, jnp.zeros_like(value))


def attend_kernel(length, qkv, context, context_t, probs_t):
    keys = qkv[:, 128:256]
    query_t = qkv[:, 0:128].T
    values_t = qkv[:, 256:384].T
    seen = lax.broadcasted_iota(jnp.int32, (1024, WIDE), 0) < length[0]
    for block in range(1024 // WIDE):
        cols = slice(block * WIDE, (block + 1) * WIDE)
        for head in range(2):
            scores = jnp.dot(keys, head_rows(query_t[:, cols], head), preferred_element_type=F32) * SCALE
            scores = jnp.where(seen, scores, -1e30)
            expo = jnp.exp(scores - jnp.max(scores, axis=0, keepdims=True))
            probs = (expo * (1.0 / jnp.sum(expo, axis=0, keepdims=True))).astype(BF16)
            probs_t[head, :, cols] = probs
            rows = slice(head * 64, head * 64 + 64)
            context_t[rows, cols] = jnp.dot(values_t[rows], probs, preferred_element_type=F32).astype(BF16)
    context[...] = context_t[...].T


def attend(length, qkv):
    return pl.pallas_call(
        attend_kernel,
        out_shape=[
            jax.ShapeDtypeStruct((1024, 128), BF16),
            jax.ShapeDtypeStruct((128, 1024), BF16),
            jax.ShapeDtypeStruct((2, 1024, 1024), BF16),
        ],
        in_specs=[SM, VM],
        out_specs=[VM, VM, VM],
        compiler_params=pltpu.CompilerParams(vmem_limit_bytes=48 * 2**20),
        name="attend",
    )(length, qkv)


def attend_back_kernel(qkv, probs_t, context_t, grad, out, grad_q, grad_k, grad_v):
    query = qkv[:, 0:128]
    keys_t = qkv[:, 128:256].T
    values = qkv[:, 256:384]
    grad_t = grad[...].T
    product = grad_t * context_t[...].astype(F32)
    for block in range(1024 // WIDE):
        cols = slice(block * WIDE, (block + 1) * WIDE)
        for head in range(2):
            rows = slice(head * 64, head * 64 + 64)
            probs = probs_t[head, :, cols]
            delta = jnp.sum(product[rows, cols], axis=0, keepdims=True)
            pulled = jnp.dot(values, head_rows(grad_t[:, cols], head).astype(BF16), preferred_element_type=F32)
            g_scores = (probs.astype(F32) * (pulled - delta) * SCALE).astype(BF16)
            grad_q[rows, cols] = jnp.dot(keys_t[rows], g_scores, preferred_element_type=F32)
            g_keys = jnp.dot(g_scores, head_cols(query[cols], head), preferred_element_type=F32)
            g_vals = jnp.dot(probs, head_cols(grad[cols], head).astype(BF16), preferred_element_type=F32)
            if block == 0 and head == 0:
                grad_k[...] = g_keys
                grad_v[...] = g_vals
            else:
                grad_k[...] += g_keys
                grad_v[...] += g_vals
    out[:, 0:128] = grad_q[...].T.astype(BF16)
    out[:, 128:256] = grad_k[...].astype(BF16)
    out[:, 256:384] = grad_v[...].astype(BF16)


def attend_back(qkv, probs_t, context_t, grad):
    return pl.pallas_call(
        attend_back_kernel,
        out_shape=jax.ShapeDtypeStruct((1024, 384), BF16),
        in_specs=[VM, VM, VM, VM],
        out_specs=VM,
        scratch_shapes=[
            pltpu.VMEM((128, 1024), F32),
            pltpu.VMEM((1024, 128), F32),
            pltpu.VMEM((1024, 128), F32),
        ],
        compiler_params=pltpu.CompilerParams(vmem_limit_bytes=48 * 2**20),
        name="attend_back",
    )(qkv, probs_t, context_t, grad)


def gelu(values):
    inner = jnp.tanh(0.7978845608028654 * (values + 0.044715 * values * values * values))
    return 0.5 * values * (1.0 + inner)


def gelu_slope(values):
    inner = jnp.tanh(0.7978845608028654 * (values + 0.044715 * values * values * values))
    return 0.5 * (1.0 + inner) + 0.5 * values * (1.0 - inner * inner) * 0.7978845608028654 * (
        1.0 + 3.0 * 0.044715 * values * values
    )


def per_device(token_ids, lengths, teacher_bins, table, qkv_shard, out_shard, up_shard, down_shard, head_shard):
    me = where_am_i()
    vocab = table.shape[0]

    packet = jnp.concatenate(
        [
            token_ids,
            jnp.broadcast_to(lengths[:, None], (1, 128)),
            jnp.broadcast_to(teacher_bins[:, None], (1, 128)),
            jnp.zeros((5, 128), jnp.int32),
        ],
        axis=0,
    )
    got = spread_ids(packet)
    length = got[0, 0, 1, 0:1]
    label = got[0, 0, 2, 0:1]
    shifted = got[:, :, 0, :] - (me["y"] * 2 + me["xh"]) * vocab
    inside = (shifted >= 0) & (shifted < vocab)
    rows = jnp.take(table, jnp.clip(shifted, 0, vocab - 1), axis=0)
    rows = jnp.where(inside[..., None], rows, jnp.zeros_like(rows))
    first, normed, qkv_w, out_w, head_w = embed(rows, [qkv_shard.reshape(64, 384), out_shard.T, head_shard])
    qkv_w = qkv_w.reshape(1024, 384)
    out_w = out_w.reshape(1024, 128)
    head_w = head_w.reshape(1024, 128)
    normed = normed.reshape(1024, 1024)
    qkv = jnp.dot(normed, qkv_w, preferred_element_type=F32).astype(BF16)
    context, context_t, probs_t = attend(length, qkv)
    terms = jnp.einsum("ph,dh->pd", context, out_w, preferred_element_type=F32).astype(BF16)
    second, normed_two, up_w, down_w = residual(terms.reshape(4, 2, 128, 1024), first, [up_shard, down_shard.T])
    up_w = up_w.reshape(1024, 512)
    down_w = down_w.reshape(1024, 512)
    normed_two = normed_two.reshape(1024, 1024)
    hidden = jnp.dot(normed_two, up_w, preferred_element_type=F32)
    live = (jnp.arange(1024, dtype=jnp.int32)[:, None] < length[0]).astype(F32)
    own = (me["y"] * 2 + me["c"]) * 128 + jnp.arange(128, dtype=jnp.int32)[:, None]
    live_own = (own < length[0]).astype(F32)
    hidden_sum = jnp.sum(gelu(hidden).astype(BF16).astype(F32) * live, axis=0, keepdims=True)
    second_sum = jnp.sum(second.astype(F32) * live_own, axis=0, keepdims=True)
    per_token, pulled, packet = classify(length, label, hidden_sum, second_sum, down_w, head_w)
    g_pre = (gelu_slope(hidden) * (pulled * live)).astype(BF16)
    up_term = jnp.einsum("pd,pf->df", normed_two, g_pre, preferred_element_type=F32).astype(BF16)
    terms = jnp.einsum("pf,df->pd", g_pre, up_w, preferred_element_type=F32).astype(BF16)
    g_second, up_grad, packets = backward(
        terms.reshape(4, 2, 128, 1024), second, per_token * live_own, up_term.reshape(16, 64, 512), packet
    )
    g_second = g_second.reshape(1024, 1024)
    out_term = jnp.einsum("pd,ph->dh", g_second, context, preferred_element_type=F32).astype(BF16)
    g_context = jnp.einsum("pd,dh->ph", g_second, out_w, preferred_element_type=F32)
    g_qkv = attend_back(qkv, probs_t, context_t, g_context)
    qkv_term = jnp.einsum("pd,pr->dr", normed, g_qkv, preferred_element_type=F32).astype(BF16)
    out_grad, qkv_grad, down_grad, head_grad, loss = collect(
        packets.reshape(16, PACKET), out_term.reshape(16, 64, 128), qkv_term.reshape(16, 64, 384)
    )
    return loss[0, 0], qkv_grad.reshape(64, 3, 128), out_grad.T, up_grad, down_grad, head_grad


def solution(mesh):
    fine = Mesh(mesh.devices.reshape(2, 4, 2, 4, 2), ("xl", "z", "c", "y", "xh"))
    dp, tensor = ("xl", "z", "c"), ("y", "xh")
    return jax.shard_map(
        per_device,
        mesh=fine,
        in_specs=(
            P(dp, tensor),
            P(dp),
            P(dp),
            P(tensor, None),
            P(dp, None, tensor),
            P(tensor, dp),
            P(dp, tensor),
            P(tensor, dp),
            P(dp, None),
        ),
        out_specs=(
            P(),
            P(dp, None, tensor),
            P(tensor, dp),
            P(dp, tensor),
            P(tensor, dp),
            P(dp, None),
        ),
        check_vma=False,
    )
```

```python
import functools

import jax
import jax.numpy as jnp
from jax import lax
from jax.experimental import pallas as pl
from jax.experimental.pallas import tpu as pltpu
from jax.sharding import Mesh
from jax.sharding import PartitionSpec as P

MESH = pl.DeviceIdType.MESH
EPS = 1e-05
F32 = jnp.float32
BF16 = jnp.bfloat16
HIGH = lax.Precision.HIGHEST
VM = pl.BlockSpec(memory_space=pltpu.VMEM)
SM = pl.BlockSpec(memory_space=pltpu.SMEM)


def where_am_i():
    return {name: lax.axis_index(name) for name in ("xl", "z", "c", "y", "xh")}


def add_mod(value, step, size):
    return lax.rem(value + step, size)


def params(number):
    return pltpu.CompilerParams(collective_id=number, has_side_effects=True)


def remote(src, dst, send, recv, device):
    return pltpu.make_async_remote_copy(
        src_ref=src, dst_ref=dst, send_sem=send, recv_sem=recv, device_id=device, device_id_type=MESH
    )


def signal(device):
    pl.semaphore_signal(pltpu.get_barrier_semaphore(), inc=1, device_id=device, device_id_type=MESH)


def normalize(values):
    mean = jnp.mean(values, axis=-1, keepdims=True)
    centered = values - mean
    return centered * lax.rsqrt(jnp.mean(centered * centered, axis=-1, keepdims=True) + EPS)


def normalize_back(values, grad):
    mean = jnp.mean(values, axis=-1, keepdims=True)
    centered = values - mean
    scale = lax.rsqrt(jnp.mean(centered * centered, axis=-1, keepdims=True) + EPS)
    normed = centered * scale
    return scale * (
        grad
        - jnp.mean(grad, axis=-1, keepdims=True)
        - normed * jnp.mean(grad * normed, axis=-1, keepdims=True)
    )


def spread_ids_kernel(src, out, send, recv):
    me = where_am_i()
    xl, z, c, y, xh = (me[n] for n in ("xl", "z", "c", "y", "xh"))
    here = xh == c

    for role in range(2):
        for k in range(4):
            source = dict(
                xl=add_mod(xl, role, 2), c=add_mod(xh, role, 2), xh=c, y=add_mod(y, 4 - k, 4), z=z
            )
            if role == 0 and k == 0:

                @pl.when(jnp.logical_not(here))
                def _(source=source):
                    signal(source)
            else:
                signal(source)
    pl.semaphore_wait(pltpu.get_barrier_semaphore(), jnp.where(here, 7, 8))

    def copy(role, k):
        return remote(
            src,
            out.at[role, y],
            send.at[role, k],
            recv.at[role, k],
            dict(xl=add_mod(xl, role, 2), c=xh, xh=add_mod(c, role, 2), y=add_mod(y, k, 4), z=z),
        )

    for role in range(2):
        for k in range(4):
            if role == 0 and k == 0:

                @pl.when(jnp.logical_not(here))
                def _():
                    copy(0, 0).start()

                @pl.when(here)
                def _():
                    pltpu.make_async_copy(src, out.at[0, y], recv.at[0, 0]).start()
            else:
                copy(role, k).start()
    for role in range(2):
        for k in range(4):
            if role == 0 and k == 0:

                @pl.when(jnp.logical_not(here))
                def _():
                    copy(0, 0).wait_send()
            else:
                copy(role, k).wait_send()
            pltpu.make_async_copy(src, out.at[role, add_mod(y, 4 - k, 4)], recv.at[role, k]).wait()


def spread_ids(packet):
    return pl.pallas_call(
        spread_ids_kernel,
        out_shape=jax.ShapeDtypeStruct((2, 4, 8, 128), jnp.int32),
        in_specs=[VM],
        out_specs=VM,
        scratch_shapes=[pltpu.SemaphoreType.DMA((2, 4)), pltpu.SemaphoreType.DMA((2, 4))],
        compiler_params=params(1),
        name="spread_ids",
    )(packet)


class Plane:
    def __init__(self, srcs, dsts, send, recv, collect):
        self.srcs, self.dsts, self.send, self.recv, self.collect = srcs, dsts, send, recv, collect
        self.me = where_am_i()
        c, xh = self.me["c"], self.me["xh"]
        self.here = xh == c
        self.mine, self.other = (xh, c) if collect else (c, xh)
        self.slot = (self.me["xl"] * 4 + self.me["z"]) * 2 + self.mine
        self.places = [(a, k, e) for k in (2, 1, 3, 0) for a in (1, 0) for e in range(2)]

    def target(self, a, k, e):
        me = self.me
        swapped = dict(c=e, xh=me["c"]) if self.collect else dict(c=me["xh"], xh=e)
        return dict(xl=add_mod(me["xl"], a, 2), z=add_mod(me["z"], k, 4), y=me["y"], **swapped)

    def origin(self, a, k, e):
        me = self.me
        swapped = dict(c=me["xh"], xh=e) if self.collect else dict(c=e, xh=me["c"])
        return dict(xl=add_mod(me["xl"], a, 2), z=add_mod(me["z"], 4 - k, 4), y=me["y"], **swapped)

    def number(self, a, k, e, back):
        me = self.me
        return (add_mod(me["xl"], a, 2) * 4 + add_mod(me["z"], 4 - k if back else k, 4)) * 2 + e

    def block(self, i, a, k, e):
        if self.collect and len(self.srcs[i].shape) == 3 and self.srcs[i].shape[0] == 16:
            return self.srcs[i].at[self.number(a, k, e, False)]
        return self.srcs[i]

    def copy(self, i, a, k, e):
        return remote(
            self.block(i, a, k, e),
            self.dsts[i].at[self.slot],
            self.send.at[i, a, k, e],
            self.recv.at[i, a, k, self.mine],
            self.target(a, k, e),
        )

    def greet(self):
        for a, k, e in self.places:
            if a == 0 and k == 0:

                @pl.when(jnp.logical_not(jnp.logical_and(self.here, e == self.mine)))
                def _(a=a, k=k, e=e):
                    signal(self.origin(a, k, e))
            else:
                signal(self.origin(a, k, e))
        return jnp.where(self.here, 15, 16)

    def is_self(self, e):
        return jnp.logical_and(self.here, e == self.other)

    def start(self, i):
        for a, k, e in self.places:
            if a == 0 and k == 0:

                @pl.when(jnp.logical_not(self.is_self(e)))
                def _(a=a, k=k, e=e):
                    self.copy(i, a, k, e).start()

                @pl.when(self.is_self(e))
                def _(a=a, k=k, e=e):
                    pltpu.make_async_copy(
                        self.block(i, a, k, e), self.dsts[i].at[self.slot], self.recv.at[i, a, k, self.mine]
                    ).start()
            else:
                self.copy(i, a, k, e).start()

    def finish(self, i):
        for a, k, e in self.places:
            if a == 0 and k == 0:

                @pl.when(jnp.logical_not(self.is_self(e)))
                def _(a=a, k=k, e=e):
                    self.copy(i, a, k, e).wait_send()
            else:
                self.copy(i, a, k, e).wait_send()
            pltpu.make_async_copy(
                self.block(i, 0, 0, 0), self.dsts[i].at[self.number(a, k, e, True)], self.recv.at[i, a, k, e]
            ).wait()


def plane_sems(count):
    return [pltpu.SemaphoreType.DMA((count, 2, 4, 2))] * 2


def gathered(shard):
    return jax.ShapeDtypeStruct((16, *shard.shape), shard.dtype)


def total_of(buf):
    total = buf[0].astype(F32)
    for s in range(1, 16):
        total = total + buf[s].astype(F32)
    return total


def thirds(row):
    high = row.astype(BF16).astype(F32)
    middle = (row - high).astype(BF16).astype(F32)
    low = row - high - middle
    index = lax.broadcasted_iota(jnp.int32, (8, row.shape[1]), 0)
    rows = jnp.where(index == 0, high, jnp.where(index == 1, middle, jnp.where(index == 2, low, 0.0)))
    return rows.astype(BF16)


def picked(values, start):
    rows = lax.broadcasted_iota(jnp.int32, (values.shape[1], 64), 0)
    cols = lax.broadcasted_iota(jnp.int32, (values.shape[1], 64), 1)
    chosen = (rows == cols + start).astype(F32)
    return jnp.dot(values, chosen, precision=HIGH, preferred_element_type=F32)


def collect_kernel(packets, out_term, qkv_term, out_grad, qkv_grad, down_grad, head_grad, loss, out_buf, qkv_buf, send, recv):
    plane = Plane([out_term, qkv_term], [out_buf, qkv_buf], send, recv, True)
    pl.semaphore_wait(pltpu.get_barrier_semaphore(), plane.greet())
    plane.start(0)
    plane.start(1)
    me = plane.me
    start = ((me["xl"] * 4 + me["z"]) * 2 + me["c"]) * 64
    over = (((0,), (0,)), ((), ()))
    down_grad[...] = lax.dot_general(
        packets[:, 0:512], picked(packets[:, 512:1536], start), over, precision=HIGH, preferred_element_type=F32
    )
    head_grad[...] = lax.dot_general(
        picked(packets[:, 1536:2560], start), packets[:, 2560:2688], over, precision=HIGH, preferred_element_type=F32
    )
    loss[...] = jnp.sum(packets[:, 2688:2816], axis=0, keepdims=True) / 16.0
    plane.finish(0)
    out_grad[...] = total_of(out_buf)
    plane.finish(1)
    total = total_of(qkv_buf)
    for piece in range(3):
        qkv_grad[:, piece] = total[:, piece * 128 : piece * 128 + 128]


def collect(packets, out_term, qkv_term):
    return pl.pallas_call(
        collect_kernel,
        out_shape=[
            jax.ShapeDtypeStruct((64, 128), F32),
            jax.ShapeDtypeStruct((64, 3, 128), F32),
            jax.ShapeDtypeStruct((512, 64), F32),
            jax.ShapeDtypeStruct((64, 128), F32),
            jax.ShapeDtypeStruct((1, 128), F32),
        ],
        in_specs=[VM] * 3,
        out_specs=[VM] * 5,
        scratch_shapes=[pltpu.VMEM((16, 64, 128), BF16), pltpu.VMEM((16, 64, 384), BF16), *plane_sems(2)],
        compiler_params=params(3),
        name="collect_gradients",
    )(packets, out_term, qkv_term)


def ring_places():
    me = where_am_i()
    y, c = me["y"], me["c"]
    return me, y, c, add_mod(y, 1, 4), add_mod(y, 3, 4), add_mod(y, 2, 4), 1 - c


HALVES = (pl.ds(0, 64), pl.ds(64, 64))


def to_owner(blocks, stage, far, near, send, recv, meanwhile=None):
    me, y, c, up, dn, op, oc = ring_places()
    first = [
        remote(blocks(op).at[HALVES[0]], far.at[0], send.at[0], recv.at[0], dict(y=up)),
        remote(blocks(op).at[HALVES[1]], far.at[1], send.at[1], recv.at[1], dict(y=dn)),
    ]
    for step in first:
        step.start()
    if meanwhile is not None:
        meanwhile()

    def second(side):
        return remote(
            stage.at[side], near.at[side], send.at[2 + side], recv.at[2 + side], dict(y=(up, dn)[side])
        )

    stage[0, 64:128] = blocks(up)[64:128]
    stage[1, 0:64] = blocks(dn)[0:64]
    first[0].wait_recv()
    stage[0, 0:64] = (blocks(up)[0:64].astype(F32) + far[0].astype(F32)).astype(BF16)
    second(0).start()
    first[1].wait_recv()
    stage[1, 64:128] = (blocks(dn)[64:128].astype(F32) + far[1].astype(F32)).astype(BF16)
    second(1).start()

    def finish():
        for step in first:
            step.wait_send()
        second(0).wait()
        second(1).wait()
        return blocks(y)[...].astype(F32) + near[0].astype(F32) + near[1].astype(F32)

    return finish


def to_all(out, send, recv):
    me, y, c, up, dn, op, oc = ring_places()

    def go(k, row, col, part, device):
        ref = out.at[row, col] if part is None else out.at[row, col, HALVES[part]]
        return remote(ref, ref, send.at[k], recv.at[k], device)

    begin = [
        go(0, y, c, None, dict(y=up)),
        go(1, y, c, None, dict(y=dn)),
        go(2, y, c, None, dict(c=oc)),
    ]
    for step in begin:
        step.start()
    begin[0].wait_recv()
    later = [go(3, dn, c, 0, dict(y=up)), go(4, dn, c, None, dict(c=oc))]
    for step in later:
        step.start()
    begin[1].wait_recv()
    later += [go(5, up, c, 1, dict(y=dn)), go(6, up, c, None, dict(c=oc))]
    for step in later[2:]:
        step.start()
    later[0].wait_recv()
    last = [go(7, op, c, 0, dict(c=oc)), go(8, op, c, 1, dict(c=oc))]
    last[0].start()
    later[2].wait_recv()
    last[1].start()
    begin[2].wait_recv()
    later[1].wait_recv()
    later[3].wait_recv()
    last[0].wait_recv()
    last[1].wait_recv()
    for step in begin + later + last:
        step.wait_send()


def embed_kernel(
    rows, qkv_s, out_s, head_s, first_out, normed_out, qkv_w, out_w, head_w,
    stage, far, near, other, total, rsend, rrecv, asend, arecv, psend, precv,
):
    me, y, c, up, dn, op, oc = ring_places()
    plane = Plane([qkv_s, out_s, head_s], [qkv_w, out_w, head_w], psend, precv, False)
    partner = dict(xl=1 - me["xl"], xh=1 - me["xh"])
    for device in (dict(y=up), dict(y=dn), dict(c=oc), partner):
        signal(device)
    pl.semaphore_wait(pltpu.get_barrier_semaphore(), plane.greet() + 4)
    done = [
        to_owner(
            lambda b, role=role: rows.at[role, b],
            stage.at[role],
            far.at[role],
            near.at[role],
            rsend.at[role],
            rrecv.at[role],
            (lambda: [plane.start(i) for i in range(3)]) if role == 1 else None,
        )
        for role in (1, 0)
    ]
    total[...] = done[0]().astype(BF16)
    cross = remote(total, other, rsend.at[2, 0], rrecv.at[2, 0], partner)
    cross.start()
    mine = done[1]()
    cross.wait()
    first = mine + other[...].astype(F32)
    first_out[...] = first.astype(BF16)
    normed_out[y, c] = normalize(first).astype(BF16)
    to_all(normed_out, asend, arecv)
    for i in range(3):
        plane.finish(i)


def embed(rows, shards):
    return pl.pallas_call(
        embed_kernel,
        out_shape=[
            jax.ShapeDtypeStruct((128, 1024), BF16),
            jax.ShapeDtypeStruct((4, 2, 128, 1024), BF16),
            *map(gathered, shards),
        ],
        in_specs=[VM] * 4,
        out_specs=[VM] * 5,
        scratch_shapes=[
            pltpu.VMEM((2, 2, 128, 1024), BF16),
            pltpu.VMEM((2, 2, 64, 1024), BF16),
            pltpu.VMEM((2, 2, 128, 1024), BF16),
            pltpu.VMEM((128, 1024), BF16),
            pltpu.VMEM((128, 1024), BF16),
            pltpu.SemaphoreType.DMA((3, 4)),
            pltpu.SemaphoreType.DMA((3, 4)),
            pltpu.SemaphoreType.DMA((9,)),
            pltpu.SemaphoreType.DMA((9,)),
            *plane_sems(3),
        ],
        compiler_params=params(4),
        name="embed_exchange",
    )(rows, *shards)


def pair_sum_to_owner(plane, terms, pair, summed, stage, far, near, psend, precv, rsend, rrecv):
    me, y, c, up, dn, op, oc = ring_places()
    order = (op, up, dn, y)
    for device in (dict(y=up), dict(y=dn), dict(c=oc)):
        signal(device)
    pl.semaphore_wait(pltpu.get_barrier_semaphore(), plane.greet() + 3)
    steps = [
        remote(terms.at[b, oc], pair.at[b], psend.at[i], precv.at[i], dict(c=oc))
        for i, b in enumerate(order)
    ]
    for step in steps:
        step.start()
    for i in range(len(plane.srcs)):
        plane.start(i)
    for i, b in enumerate(order):
        steps[i].wait_recv()
        summed[b] = (terms[b, c].astype(F32) + pair[b].astype(F32)).astype(BF16)
    total = to_owner(lambda b: summed.at[b], stage, far, near, rsend, rrecv)()
    for step in steps:
        step.wait_send()
    return total


PAIR_SCRATCH = [
    pltpu.VMEM((4, 128, 1024), BF16),
    pltpu.VMEM((4, 128, 1024), BF16),
    pltpu.VMEM((2, 128, 1024), BF16),
    pltpu.VMEM((2, 64, 1024), BF16),
    pltpu.VMEM((2, 128, 1024), BF16),
    pltpu.SemaphoreType.DMA((4,)),
    pltpu.SemaphoreType.DMA((4,)),
    pltpu.SemaphoreType.DMA((4,)),
    pltpu.SemaphoreType.DMA((4,)),
    pltpu.SemaphoreType.DMA((9,)),
    pltpu.SemaphoreType.DMA((9,)),
    *plane_sems(2),
]


def residual_kernel(terms, first, up_s, down_s, second_out, normed_out, up_w, down_w, *scratch):
    me, y, c, up, dn, op, oc = ring_places()
    plane = Plane([up_s, down_s], [up_w, down_w], *scratch[11:], False)
    attn = pair_sum_to_owner(plane, terms, *scratch[:9])
    second = (first[...].astype(F32) + attn).astype(BF16)
    second_out[...] = second
    normed_out[y, c] = normalize(second.astype(F32)).astype(BF16)
    to_all(normed_out, *scratch[9:11])
    plane.finish(0)
    plane.finish(1)


def residual(terms, first, shards):
    return pl.pallas_call(
        residual_kernel,
        out_shape=[
            jax.ShapeDtypeStruct((128, 1024), BF16),
            jax.ShapeDtypeStruct((4, 2, 128, 1024), BF16),
            *map(gathered, shards),
        ],
        in_specs=[VM] * 4,
        out_specs=[VM] * 4,
        scratch_shapes=PAIR_SCRATCH,
        compiler_params=params(5),
        name="residual_exchange",
    )(terms, first, *shards)


def backward_kernel(length, terms, second, per_token, up_term, packet, g_out, up_grad, packets, up_buf, *scratch):
    me, y, c, up, dn, op, oc = ring_places()
    plane = Plane([packet, up_term], [packets, up_buf], *scratch[11:], True)
    grad = pair_sum_to_owner(plane, terms, *scratch[:9])
    live = (y * 2 + c) * 128 + lax.broadcasted_iota(jnp.int32, (128, 1), 0) < length[0]
    g_third = jnp.where(live, per_token[...], 0.0)
    g_out[y, c] = (g_third + normalize_back(second[...].astype(F32), grad)).astype(BF16)
    to_all(g_out, *scratch[9:11])
    plane.finish(0)
    plane.finish(1)
    up_grad[...] = total_of(up_buf)


def backward(length, terms, second, per_token, up_term, packet):
    return pl.pallas_call(
        backward_kernel,
        out_shape=[
            jax.ShapeDtypeStruct((4, 2, 128, 1024), BF16),
            jax.ShapeDtypeStruct((64, 512), F32),
            gathered(packet),
        ],
        in_specs=[SM] + [VM] * 5,
        out_specs=[VM] * 3,
        scratch_shapes=[pltpu.VMEM((16, 64, 512), BF16), *PAIR_SCRATCH],
        compiler_params=params(6),
        name="backward_exchange",
    )(length, terms, second, per_token, up_term, packet)


PACKET = 512 + 1024 + 1024 + 128 + 128
ROWS = 256
LHS_T = (((0,), (0,)), ((), ()))
RHS_T = (((1,), (1,)), ((), ()))


def ffn_kernel(
    length, label, normed, second, up_w, down_w, head_w, per_token_out, packet_out, terms, up_term,
    slope, g_pre, parts, send, recv,
):
    me, y, c, up, dn, op, oc = ring_places()
    slot = y * 2 + c
    peers = [(k, e) for k in (2, 1, 3, 0) for e in range(2) if (k, e) != (0, 0)]

    def device(k, e):
        return dict(y=add_mod(y, k, 4), c=add_mod(c, e, 2))

    for k, e in peers:
        signal(device(4 - k if k else 0, e))

    def live(start, size):
        return start + lax.broadcasted_iota(jnp.int32, (size, 1), 0) < length[0]

    hidden_sum = jnp.zeros((1, 512), F32)
    for block in range(1024 // ROWS):
        rows = pl.ds(block * ROWS, ROWS)
        hidden = jnp.dot(normed[rows], up_w[...], preferred_element_type=F32)
        square = hidden * hidden
        inner = jnp.tanh(0.7978845608028654 * hidden * (1.0 + 0.044715 * square))
        half = 0.5 * (1.0 + inner)
        acted = (hidden * half).astype(BF16).astype(F32)
        slope[rows] = half + 0.5 * hidden * (1.0 - inner * inner) * (
            0.7978845608028654 + (0.7978845608028654 * 3.0 * 0.044715) * square
        )
        hidden_sum += jnp.sum(jnp.where(live(block * ROWS, ROWS), acted, 0.0), axis=0, keepdims=True)
    own = jnp.where(live(slot * 128, 128), second[...].astype(F32), 0.0)
    pushed = lax.dot_general(thirds(hidden_sum), down_w[...], RHS_T, preferred_element_type=F32)
    parts[slot] = jnp.sum(own, axis=0, keepdims=True) + jnp.sum(pushed, axis=0, keepdims=True)
    pl.semaphore_wait(pltpu.get_barrier_semaphore(), 7)
    steps = [
        remote(parts.at[slot], parts.at[slot], send.at[k, e], recv.at[k, e], device(k, e)) for k, e in peers
    ]
    for step in steps:
        step.start()
    for step in steps:
        step.wait()
    pooled = parts[0]
    for s in range(1, 8):
        pooled = pooled + parts[s]
    count = length[0].astype(F32)
    pooled = pooled / count
    final = normalize(pooled)
    logits = jnp.sum(jnp.dot(thirds(final), head_w[...], preferred_element_type=F32), axis=0, keepdims=True)
    top = jnp.max(logits, axis=-1, keepdims=True)
    total = jnp.log(jnp.sum(jnp.exp(logits - top), axis=-1, keepdims=True)) + top
    labels = (lax.broadcasted_iota(jnp.int32, logits.shape, 1) == label[0]).astype(F32)
    loss = total - jnp.sum(logits * labels, axis=-1, keepdims=True)
    g_logits = (jnp.exp(logits - total) - labels) / 16.0
    g_final = lax.dot_general(thirds(g_logits), head_w[...], RHS_T, preferred_element_type=F32)
    g_final = jnp.sum(g_final, axis=0, keepdims=True)
    per_token = normalize_back(pooled, g_final) / count
    rounded = per_token.astype(BF16)
    pulled = jnp.dot(rounded, down_w[...], preferred_element_type=F32)
    for block in range(1024 // ROWS):
        rows = pl.ds(block * ROWS, ROWS)
        grad = jnp.where(live(block * ROWS, ROWS), slope[rows] * pulled, 0.0).astype(BF16)
        g_pre[rows] = grad
        terms[rows] = lax.dot_general(grad, up_w[...], RHS_T, preferred_element_type=F32).astype(BF16)
    for block in range(1024 // ROWS):
        cols = pl.ds(block * ROWS, ROWS)
        up_term[cols] = lax.dot_general(
            normed[:, cols], g_pre[...], LHS_T, preferred_element_type=F32
        ).astype(BF16)
    per_token_out[...] = per_token
    packet_out[:, 0:512] = hidden_sum
    packet_out[:, 512:1536] = rounded.astype(F32)
    packet_out[:, 1536:2560] = final
    packet_out[:, 2560:2688] = g_logits
    packet_out[:, 2688:2816] = jnp.broadcast_to(loss, (1, 128))


def ffn(length, label, normed, second, up_w, down_w, head_w):
    return pl.pallas_call(
        ffn_kernel,
        out_shape=[
            jax.ShapeDtypeStruct((1, 1024), F32),
            jax.ShapeDtypeStruct((1, PACKET), F32),
            jax.ShapeDtypeStruct((1024, 1024), BF16),
            jax.ShapeDtypeStruct((1024, 512), BF16),
        ],
        in_specs=[SM, SM, VM, VM, VM, VM, VM],
        out_specs=[VM, VM, VM, VM],
        scratch_shapes=[
            pltpu.VMEM((1024, 512), F32),
            pltpu.VMEM((1024, 512), BF16),
            pltpu.VMEM((8, 1, 1024), F32),
            pltpu.SemaphoreType.DMA((4, 2)),
            pltpu.SemaphoreType.DMA((4, 2)),
        ],
        compiler_params=params(7),
        name="ffn",
    )(length, label, normed, second, up_w, down_w, head_w)


SCALE = 0.125
WIDE = 256


def head_rows(value, head):
    rows = lax.broadcasted_iota(jnp.int32, value.shape, 0)
    return jnp.where((rows >= 64) == (head == 1), value, jnp.zeros_like(value))


def head_cols(value, head):
    cols = lax.broadcasted_iota(jnp.int32, value.shape, 1)
    return jnp.where((cols >= 64) == (head == 1), value, jnp.zeros_like(value))


def attend_kernel(length, normed, qkv_w, out_w, qkv, context_t, probs_t, terms):
    for block in range(4):
        rows = pl.ds(block * 256, 256)
        qkv[rows] = jnp.dot(normed[rows], qkv_w[...], preferred_element_type=F32).astype(BF16)
    keys = qkv[:, 128:256]
    query_t = (qkv[:, 0:128] * SCALE).T
    values_t = qkv[:, 256:384].T
    out_t = out_w[...].T
    seen = lax.broadcasted_iota(jnp.int32, (1024, WIDE), 0) < length[0]
    for block in range(1024 // WIDE):
        cols = slice(block * WIDE, (block + 1) * WIDE)
        for head in range(2):
            scores = jnp.dot(keys, head_rows(query_t[:, cols], head), preferred_element_type=F32)
            scores = jnp.where(seen, scores, -1e30)
            expo = jnp.exp(scores - jnp.max(scores, axis=0, keepdims=True))
            probs = (expo * (1.0 / jnp.sum(expo, axis=0, keepdims=True))).astype(BF16)
            probs_t[head, :, cols] = probs
            rows = slice(head * 64, head * 64 + 64)
            context_t[rows, cols] = jnp.dot(values_t[rows], probs, preferred_element_type=F32).astype(BF16)
        terms[cols] = jnp.dot(context_t[:, cols].T, out_t, preferred_element_type=F32).astype(BF16)


def attend(length, normed, qkv_w, out_w):
    return pl.pallas_call(
        attend_kernel,
        out_shape=[
            jax.ShapeDtypeStruct((1024, 384), BF16),
            jax.ShapeDtypeStruct((128, 1024), BF16),
            jax.ShapeDtypeStruct((2, 1024, 1024), BF16),
            jax.ShapeDtypeStruct((1024, 1024), BF16),
        ],
        in_specs=[SM, VM, VM, VM],
        out_specs=[VM] * 4,
        compiler_params=pltpu.CompilerParams(vmem_limit_bytes=48 * 2**20),
        name="attend",
    )(length, normed, qkv_w, out_w)


def attend_back_kernel(
    g_second, normed, out_w, qkv, probs_t, context_t, out_term, qkv_term, grad, grad_t, grad_q, grad_k, grad_v
):
    out_term[...] = jnp.dot(context_t[...], g_second[...], preferred_element_type=F32).T.astype(BF16)
    for block in range(4):
        rows = pl.ds(block * 256, 256)
        part = jnp.dot(g_second[rows], out_w[...], preferred_element_type=F32)
        grad[rows] = part.astype(BF16)
        grad_t[:, block * 256 : block * 256 + 256] = part.T
    query = qkv[:, 0:128] * SCALE
    keys_t = (qkv[:, 128:256] * SCALE).T
    values = qkv[:, 256:384]
    product = grad_t[...] * context_t[...].astype(F32)
    for block in range(1024 // WIDE):
        cols = slice(block * WIDE, (block + 1) * WIDE)
        for head in range(2):
            rows = slice(head * 64, head * 64 + 64)
            probs = probs_t[head, :, cols]
            delta = jnp.sum(product[rows, cols], axis=0, keepdims=True)
            pulled = jnp.dot(values, head_rows(grad_t[:, cols], head).astype(BF16), preferred_element_type=F32)
            g_scores = (probs.astype(F32) * (pulled - delta)).astype(BF16)
            grad_q[rows, cols] = jnp.dot(keys_t[rows], g_scores, preferred_element_type=F32).astype(BF16)
            g_keys = jnp.dot(g_scores, head_cols(query[cols], head), preferred_element_type=F32)
            g_vals = jnp.dot(probs, head_cols(grad[cols], head), preferred_element_type=F32)
            if block == 0 and head == 0:
                grad_k[...] = g_keys
                grad_v[...] = g_vals
            else:
                grad_k[...] += g_keys
                grad_v[...] += g_vals
    for piece, value in enumerate((None, grad_k, grad_v)):
        left = grad_q[...] if value is None else value[...].T.astype(BF16)
        part = jnp.dot(left, normed[...], preferred_element_type=F32)
        qkv_term[:, piece * 128 : piece * 128 + 128] = part.T.astype(BF16)


def attend_back(g_second, normed, out_w, qkv, probs_t, context_t):
    return pl.pallas_call(
        attend_back_kernel,
        out_shape=[
            jax.ShapeDtypeStruct((1024, 128), BF16),
            jax.ShapeDtypeStruct((1024, 384), BF16),
        ],
        in_specs=[VM] * 6,
        out_specs=[VM] * 2,
        scratch_shapes=[
            pltpu.VMEM((1024, 128), BF16),
            pltpu.VMEM((128, 1024), F32),
            pltpu.VMEM((128, 1024), BF16),
            pltpu.VMEM((1024, 128), F32),
            pltpu.VMEM((1024, 128), F32),
        ],
        compiler_params=pltpu.CompilerParams(vmem_limit_bytes=48 * 2**20),
        name="attend_back",
    )(g_second, normed, out_w, qkv, probs_t, context_t)


def per_device(token_ids, lengths, teacher_bins, table, qkv_shard, out_shard, up_shard, down_shard, head_shard):
    me = where_am_i()
    vocab = table.shape[0]

    packet = jnp.concatenate(
        [
            token_ids,
            jnp.broadcast_to(lengths[:, None], (1, 128)),
            jnp.broadcast_to(teacher_bins[:, None], (1, 128)),
            jnp.zeros((5, 128), jnp.int32),
        ],
        axis=0,
    )
    got = spread_ids(packet)
    length = got[0, 0, 1, 0:1]
    label = got[0, 0, 2, 0:1]
    shifted = got[:, :, 0, :] - (me["y"] * 2 + me["xh"]) * vocab
    inside = (shifted >= 0) & (shifted < vocab)
    rows = jnp.take(table, jnp.clip(shifted, 0, vocab - 1), axis=0)
    rows = jnp.where(inside[..., None], rows, jnp.zeros_like(rows))
    first, normed, qkv_w, out_w, head_w = embed(rows, [qkv_shard.reshape(64, 384), out_shard.T, head_shard])
    qkv_w = qkv_w.reshape(1024, 384)
    out_w = out_w.reshape(1024, 128)
    head_w = head_w.reshape(1024, 128)
    normed = normed.reshape(1024, 1024)
    qkv, context_t, probs_t, terms = attend(length, normed, qkv_w, out_w)
    second, normed_two, up_w, down_w = residual(terms.reshape(4, 2, 128, 1024), first, [up_shard, down_shard.T])
    up_w = up_w.reshape(1024, 512)
    down_w = down_w.reshape(1024, 512)
    per_token, packet, terms, up_term = ffn(
        length, label, normed_two.reshape(1024, 1024), second, up_w, down_w, head_w
    )
    g_second, up_grad, packets = backward(
        length, terms.reshape(4, 2, 128, 1024), second, per_token, up_term.reshape(16, 64, 512), packet
    )
    out_term, qkv_term = attend_back(g_second.reshape(1024, 1024), normed, out_w, qkv, probs_t, context_t)
    out_grad, qkv_grad, down_grad, head_grad, loss = collect(
        packets.reshape(16, PACKET), out_term.reshape(16, 64, 128), qkv_term.reshape(16, 64, 384)
    )
    return loss[0, 0], qkv_grad, out_grad.T, up_grad, down_grad, head_grad


def solution(mesh):
    fine = Mesh(mesh.devices.reshape(2, 4, 2, 4, 2), ("xl", "z", "c", "y", "xh"))
    dp, tensor = ("xl", "z", "c"), ("y", "xh")
    return jax.shard_map(
        per_device,
        mesh=fine,
        in_specs=(
            P(dp, tensor),
            P(dp),
            P(dp),
            P(tensor, None),
            P(dp, None, tensor),
            P(tensor, dp),
            P(dp, tensor),
            P(tensor, dp),
            P(dp, None),
        ),
        out_specs=(
            P(),
            P(dp, None, tensor),
            P(tensor, dp),
            P(dp, tensor),
            P(tensor, dp),
            P(dp, None),
        ),
        check_vma=False,
    )
```

```python
import functools

import jax
import jax.numpy as jnp
from jax import lax
from jax.experimental import pallas as pl
from jax.experimental.pallas import tpu as pltpu
from jax.sharding import Mesh
from jax.sharding import PartitionSpec as P

MESH = pl.DeviceIdType.MESH
EPS = 1e-05
F32 = jnp.float32
BF16 = jnp.bfloat16
HIGH = lax.Precision.HIGHEST
VM = pl.BlockSpec(memory_space=pltpu.VMEM)
SM = pl.BlockSpec(memory_space=pltpu.SMEM)


def where_am_i():
    return {name: lax.axis_index(name) for name in ("xl", "z", "c", "y", "xh")}


def add_mod(value, step, size):
    return lax.rem(value + step, size)


def params(number, mebibytes):
    return pltpu.CompilerParams(
        collective_id=number, has_side_effects=True, vmem_limit_bytes=mebibytes * 2**20
    )


def remote(src, dst, send, recv, device):
    return pltpu.make_async_remote_copy(
        src_ref=src, dst_ref=dst, send_sem=send, recv_sem=recv, device_id=device, device_id_type=MESH
    )


def signal(device):
    pl.semaphore_signal(pltpu.get_barrier_semaphore(), inc=1, device_id=device, device_id_type=MESH)


def normalize(values):
    mean = jnp.mean(values, axis=-1, keepdims=True)
    centered = values - mean
    return centered * lax.rsqrt(jnp.mean(centered * centered, axis=-1, keepdims=True) + EPS)


def normalize_back(values, grad):
    mean = jnp.mean(values, axis=-1, keepdims=True)
    centered = values - mean
    scale = lax.rsqrt(jnp.mean(centered * centered, axis=-1, keepdims=True) + EPS)
    normed = centered * scale
    return scale * (
        grad
        - jnp.mean(grad, axis=-1, keepdims=True)
        - normed * jnp.mean(grad * normed, axis=-1, keepdims=True)
    )


class Ids:
    def __init__(self, src, out, send, recv):
        self.src, self.out, self.send, self.recv = src, out, send, recv
        self.me = where_am_i()
        self.here = self.me["xh"] == self.me["c"]

    def greet(self):
        me = self.me
        for role in range(2):
            for k in range(4):
                source = dict(
                    xl=add_mod(me["xl"], role, 2),
                    c=add_mod(me["xh"], role, 2),
                    xh=me["c"],
                    y=add_mod(me["y"], 4 - k, 4),
                    z=me["z"],
                )
                if role == 0 and k == 0:

                    @pl.when(jnp.logical_not(self.here))
                    def _(source=source):
                        signal(source)
                else:
                    signal(source)
        return jnp.where(self.here, 7, 8)

    def copy(self, role, k):
        me = self.me
        return remote(
            self.src,
            self.out.at[role, me["y"]],
            self.send.at[role, k],
            self.recv.at[role, k],
            dict(
                xl=add_mod(me["xl"], role, 2),
                c=me["xh"],
                xh=add_mod(me["c"], role, 2),
                y=add_mod(me["y"], k, 4),
                z=me["z"],
            ),
        )

    def local(self):
        return pltpu.make_async_copy(self.src, self.out.at[0, self.me["y"]], self.recv.at[0, 0])

    def start(self):
        for role in (1, 0):
            for k in (2, 1, 3, 0):
                if role == 0 and k == 0:

                    @pl.when(jnp.logical_not(self.here))
                    def _():
                        self.copy(0, 0).start()

                    @pl.when(self.here)
                    def _():
                        self.local().start()
                else:
                    self.copy(role, k).start()

    def arrive(self, role):
        for k in range(4):
            place = add_mod(self.me["y"], 4 - k, 4)
            pltpu.make_async_copy(self.src, self.out.at[role, place], self.recv.at[role, k]).wait()

    def sent(self):
        for role in range(2):
            for k in range(4):
                if role == 0 and k == 0:

                    @pl.when(jnp.logical_not(self.here))
                    def _():
                        self.copy(0, 0).wait_send()
                else:
                    self.copy(role, k).wait_send()


class Plane:
    def __init__(self, srcs, dsts, send, recv, collect):
        self.srcs, self.dsts, self.send, self.recv, self.collect = srcs, dsts, send, recv, collect
        self.me = where_am_i()
        c, xh = self.me["c"], self.me["xh"]
        self.here = xh == c
        self.mine, self.other = (xh, c) if collect else (c, xh)
        self.slot = (self.me["xl"] * 4 + self.me["z"]) * 2 + self.mine
        self.places = [(a, k, e) for k in (2, 1, 3, 0) for a in (1, 0) for e in range(2)]

    def target(self, a, k, e):
        me = self.me
        swapped = dict(c=e, xh=me["c"]) if self.collect else dict(c=me["xh"], xh=e)
        return dict(xl=add_mod(me["xl"], a, 2), z=add_mod(me["z"], k, 4), y=me["y"], **swapped)

    def origin(self, a, k, e):
        me = self.me
        swapped = dict(c=me["xh"], xh=e) if self.collect else dict(c=e, xh=me["c"])
        return dict(xl=add_mod(me["xl"], a, 2), z=add_mod(me["z"], 4 - k, 4), y=me["y"], **swapped)

    def number(self, a, k, e, back):
        me = self.me
        return (add_mod(me["xl"], a, 2) * 4 + add_mod(me["z"], 4 - k if back else k, 4)) * 2 + e

    def block(self, i, a, k, e):
        if self.collect and len(self.srcs[i].shape) == 3 and self.srcs[i].shape[0] == 16:
            return self.srcs[i].at[self.number(a, k, e, False)]
        return self.srcs[i]

    def copy(self, i, a, k, e):
        return remote(
            self.block(i, a, k, e),
            self.dsts[i].at[self.slot],
            self.send.at[i, a, k, e],
            self.recv.at[i, a, k, self.mine],
            self.target(a, k, e),
        )

    def greet(self):
        for a, k, e in self.places:
            if a == 0 and k == 0:

                @pl.when(jnp.logical_not(jnp.logical_and(self.here, e == self.mine)))
                def _(a=a, k=k, e=e):
                    signal(self.origin(a, k, e))
            else:
                signal(self.origin(a, k, e))
        return jnp.where(self.here, 15, 16)

    def is_self(self, e):
        return jnp.logical_and(self.here, e == self.other)

    def start(self, i):
        for a, k, e in self.places:
            if a == 0 and k == 0:

                @pl.when(jnp.logical_not(self.is_self(e)))
                def _(a=a, k=k, e=e):
                    self.copy(i, a, k, e).start()

                @pl.when(self.is_self(e))
                def _(a=a, k=k, e=e):
                    pltpu.make_async_copy(
                        self.block(i, a, k, e), self.dsts[i].at[self.slot], self.recv.at[i, a, k, self.mine]
                    ).start()
            else:
                self.copy(i, a, k, e).start()

    def finish(self, i):
        for a, k, e in self.places:
            if a == 0 and k == 0:

                @pl.when(jnp.logical_not(self.is_self(e)))
                def _(a=a, k=k, e=e):
                    self.copy(i, a, k, e).wait_send()
            else:
                self.copy(i, a, k, e).wait_send()
            pltpu.make_async_copy(
                self.block(i, 0, 0, 0), self.dsts[i].at[self.number(a, k, e, True)], self.recv.at[i, a, k, e]
            ).wait()


def plane_sems(count):
    return [pltpu.SemaphoreType.DMA((count, 2, 4, 2))] * 2


def gathered(shard):
    return jax.ShapeDtypeStruct((16, *shard.shape), shard.dtype)


def total_of(buf):
    total = buf[0].astype(F32)
    for s in range(1, 16):
        total = total + buf[s].astype(F32)
    return total


def thirds(row):
    high = row.astype(BF16).astype(F32)
    middle = (row - high).astype(BF16).astype(F32)
    low = row - high - middle
    index = lax.broadcasted_iota(jnp.int32, (8, row.shape[1]), 0)
    rows = jnp.where(index == 0, high, jnp.where(index == 1, middle, jnp.where(index == 2, low, 0.0)))
    return rows.astype(BF16)


def picked(values, start):
    rows = lax.broadcasted_iota(jnp.int32, (values.shape[1], 64), 0)
    cols = lax.broadcasted_iota(jnp.int32, (values.shape[1], 64), 1)
    chosen = (rows == cols + start).astype(F32)
    return jnp.dot(values, chosen, precision=HIGH, preferred_element_type=F32)


def collect_kernel(packets, out_term, qkv_term, out_grad, qkv_grad, down_grad, head_grad, loss, out_buf, qkv_buf, send, recv):
    plane = Plane([out_term, qkv_term], [out_buf, qkv_buf], send, recv, True)
    pl.semaphore_wait(pltpu.get_barrier_semaphore(), plane.greet())
    plane.start(0)
    plane.start(1)
    me = plane.me
    start = ((me["xl"] * 4 + me["z"]) * 2 + me["c"]) * 64
    over = (((0,), (0,)), ((), ()))
    down_grad[...] = lax.dot_general(
        packets[:, 0:512], picked(packets[:, 512:1536], start), over, precision=HIGH, preferred_element_type=F32
    )
    head_grad[...] = lax.dot_general(
        picked(packets[:, 1536:2560], start), packets[:, 2560:2688], over, precision=HIGH, preferred_element_type=F32
    )
    loss[...] = jnp.sum(packets[:, 2688:2816], axis=0, keepdims=True) / 16.0
    plane.finish(0)
    out_grad[...] = total_of(out_buf)
    plane.finish(1)
    total = total_of(qkv_buf)
    for piece in range(3):
        qkv_grad[:, piece] = total[:, piece * 128 : piece * 128 + 128]


def collect(packets, out_term, qkv_term):
    return pl.pallas_call(
        collect_kernel,
        out_shape=[
            jax.ShapeDtypeStruct((64, 128), F32),
            jax.ShapeDtypeStruct((64, 3, 128), F32),
            jax.ShapeDtypeStruct((512, 64), F32),
            jax.ShapeDtypeStruct((64, 128), F32),
            jax.ShapeDtypeStruct((1, 128), F32),
        ],
        in_specs=[VM] * 3,
        out_specs=[VM] * 5,
        scratch_shapes=[pltpu.VMEM((16, 64, 128), BF16), pltpu.VMEM((16, 64, 384), BF16), *plane_sems(2)],
        compiler_params=params(3, 16),
        name="collect_gradients",
    )(packets, out_term, qkv_term)


def ring_places():
    me = where_am_i()
    y, c = me["y"], me["c"]
    return me, y, c, add_mod(y, 1, 4), add_mod(y, 3, 4), add_mod(y, 2, 4), 1 - c


HALVES = (pl.ds(0, 64), pl.ds(64, 64))


def to_owner(blocks, stage, far, near, send, recv):
    me, y, c, up, dn, op, oc = ring_places()
    first = [
        remote(blocks(op).at[HALVES[0]], far.at[0], send.at[0], recv.at[0], dict(y=up)),
        remote(blocks(op).at[HALVES[1]], far.at[1], send.at[1], recv.at[1], dict(y=dn)),
    ]

    def second(side):
        return remote(
            stage.at[side], near.at[side], send.at[2 + side], recv.at[2 + side], dict(y=(up, dn)[side])
        )

    def begin():
        for step in first:
            step.start()

    def relay():
        stage[0, 64:128] = blocks(up)[64:128]
        stage[1, 0:64] = blocks(dn)[0:64]
        first[0].wait_recv()
        stage[0, 0:64] = (blocks(up)[0:64].astype(F32) + far[0].astype(F32)).astype(BF16)
        second(0).start()
        first[1].wait_recv()
        stage[1, 64:128] = (blocks(dn)[64:128].astype(F32) + far[1].astype(F32)).astype(BF16)
        second(1).start()

    def finish():
        for step in first:
            step.wait_send()
        second(0).wait()
        second(1).wait()
        return blocks(y)[...].astype(F32) + near[0].astype(F32) + near[1].astype(F32)

    return begin, relay, finish


def to_all(out, send, recv):
    me, y, c, up, dn, op, oc = ring_places()

    def go(k, row, col, part, device):
        ref = out.at[row, col] if part is None else out.at[row, col, HALVES[part]]
        return remote(ref, ref, send.at[k], recv.at[k], device)

    begin = [
        go(0, y, c, None, dict(y=up)),
        go(1, y, c, None, dict(y=dn)),
        go(2, y, c, None, dict(c=oc)),
    ]
    for step in begin:
        step.start()
    begin[0].wait_recv()
    later = [go(3, dn, c, 0, dict(y=up)), go(4, dn, c, None, dict(c=oc))]
    for step in later:
        step.start()
    begin[1].wait_recv()
    later += [go(5, up, c, 1, dict(y=dn)), go(6, up, c, None, dict(c=oc))]
    for step in later[2:]:
        step.start()
    later[0].wait_recv()
    last = [go(7, op, c, 0, dict(c=oc)), go(8, op, c, 1, dict(c=oc))]
    last[0].start()
    later[2].wait_recv()
    last[1].start()
    begin[2].wait_recv()
    later[1].wait_recv()
    later[3].wait_recv()
    last[0].wait_recv()
    last[1].wait_recv()
    for step in begin + later + last:
        step.wait_send()


def embed_kernel(
    count, label, ids, table, qkv_s, out_s, head_s, info, first_out, normed_out, qkv_w, out_w, head_w,
    packet, got, shard, chosen, rows, stage, far, near, other, total,
    load, isend, irecv, rsend, rrecv, asend, arecv, psend, precv,
):
    me, y, c, up, dn, op, oc = ring_places()
    vocab = table.shape[0]
    padded = shard.shape[0]
    fetch = pltpu.make_async_copy(table, shard.at[pl.ds(0, vocab)], load)
    fetch.start()
    tokens = Ids(packet, got, isend, irecv)
    plane = Plane([qkv_s, out_s, head_s], [qkv_w, out_w, head_w], psend, precv, False)
    partner = dict(xl=1 - me["xl"], xh=1 - me["xh"])
    for device in (dict(y=up), dict(y=dn), dict(c=oc), partner):
        signal(device)
    greeted = tokens.greet() + plane.greet() + 4
    line = lax.broadcasted_iota(jnp.int32, (8, 128), 0)
    packet[...] = jnp.where(line == 0, ids[...], jnp.where(line == 1, count[0], label[0]))
    if padded > vocab:
        shard[vocab:padded] = jnp.zeros((padded - vocab, shard.shape[1]), BF16)
    pl.semaphore_wait(pltpu.get_barrier_semaphore(), greeted)
    tokens.start()
    for i in range(3):
        plane.start(i)
    base = (y * 2 + me["xh"]) * vocab
    lanes = lax.broadcasted_iota(jnp.int32, (128, 128), 1)

    def look_up(role):
        tokens.arrive(role)
        for b in range(4):
            wanted = jnp.broadcast_to(got[role, b, 0:1, :], (128, 128)).T - base
            for tile in range(padded // 128):
                chosen[b * 128 : b * 128 + 128, tile * 128 : tile * 128 + 128] = jnp.where(
                    wanted == lanes + tile * 128, 1.0, 0.0
                ).astype(BF16)
        if role == 1:
            fetch.wait()
        for part in range(4):
            cols = slice(part * 256, part * 256 + 256)
            found = jnp.dot(chosen[...], shard[:, cols], preferred_element_type=F32).astype(BF16)
            for b in range(4):
                rows[role, b, :, cols] = found[b * 128 : b * 128 + 128]

    owner = [
        to_owner(
            lambda b, role=role: rows.at[role, b],
            stage.at[role],
            far.at[role],
            near.at[role],
            rsend.at[role],
            rrecv.at[role],
        )
        for role in range(2)
    ]
    look_up(1)
    owner[1][0]()
    look_up(0)
    owner[0][0]()
    info[...] = got[0, 0]
    owner[1][1]()
    owner[0][1]()
    total[...] = owner[1][2]().astype(BF16)
    cross = remote(total, other, rsend.at[2, 0], rrecv.at[2, 0], partner)
    cross.start()
    mine = owner[0][2]()
    cross.wait()
    first = mine + other[...].astype(F32)
    first_out[...] = first.astype(BF16)
    normed_out[y, c] = normalize(first).astype(BF16)
    to_all(normed_out, asend, arecv)
    for i in range(3):
        plane.finish(i)
    tokens.sent()


def embed(count, label, ids, table, shards):
    padded = -(-table.shape[0] // 256) * 256
    return pl.pallas_call(
        embed_kernel,
        out_shape=[
            jax.ShapeDtypeStruct((8, 128), jnp.int32),
            jax.ShapeDtypeStruct((128, 1024), BF16),
            jax.ShapeDtypeStruct((4, 2, 128, 1024), BF16),
            *map(gathered, shards),
        ],
        in_specs=[SM, SM, VM, pl.BlockSpec(memory_space=pl.ANY), VM, VM, VM],
        out_specs=[VM] * 6,
        scratch_shapes=[
            pltpu.VMEM((8, 128), jnp.int32),
            pltpu.VMEM((2, 4, 8, 128), jnp.int32),
            pltpu.VMEM((padded, 1024), BF16),
            pltpu.VMEM((512, padded), BF16),
            pltpu.VMEM((2, 4, 128, 1024), BF16),
            pltpu.VMEM((2, 2, 128, 1024), BF16),
            pltpu.VMEM((2, 2, 64, 1024), BF16),
            pltpu.VMEM((2, 2, 128, 1024), BF16),
            pltpu.VMEM((128, 1024), BF16),
            pltpu.VMEM((128, 1024), BF16),
            pltpu.SemaphoreType.DMA,
            pltpu.SemaphoreType.DMA((2, 4)),
            pltpu.SemaphoreType.DMA((2, 4)),
            pltpu.SemaphoreType.DMA((3, 4)),
            pltpu.SemaphoreType.DMA((3, 4)),
            pltpu.SemaphoreType.DMA((9,)),
            pltpu.SemaphoreType.DMA((9,)),
            *plane_sems(3),
        ],
        compiler_params=params(4, 40),
        name="embed_exchange",
    )(count, label, ids, table, *shards)


def pair_sum_to_owner(plane, terms, pair, summed, stage, far, near, psend, precv, rsend, rrecv):
    me, y, c, up, dn, op, oc = ring_places()
    order = (op, up, dn, y)
    for device in (dict(y=up), dict(y=dn), dict(c=oc)):
        signal(device)
    pl.semaphore_wait(pltpu.get_barrier_semaphore(), plane.greet() + 3)
    steps = [
        remote(terms.at[b, oc], pair.at[b], psend.at[i], precv.at[i], dict(c=oc))
        for i, b in enumerate(order)
    ]
    for step in steps:
        step.start()
    for i in range(len(plane.srcs)):
        plane.start(i)
    begin, relay, finish = to_owner(lambda b: summed.at[b], stage, far, near, rsend, rrecv)
    for i, b in enumerate(order):
        steps[i].wait_recv()
        summed[b] = (terms[b, c].astype(F32) + pair[b].astype(F32)).astype(BF16)
        if i == 0:
            begin()
    relay()
    total = finish()
    for step in steps:
        step.wait_send()
    return total


PAIR_SCRATCH = [
    pltpu.VMEM((4, 128, 1024), BF16),
    pltpu.VMEM((4, 128, 1024), BF16),
    pltpu.VMEM((2, 128, 1024), BF16),
    pltpu.VMEM((2, 64, 1024), BF16),
    pltpu.VMEM((2, 128, 1024), BF16),
    pltpu.SemaphoreType.DMA((4,)),
    pltpu.SemaphoreType.DMA((4,)),
    pltpu.SemaphoreType.DMA((4,)),
    pltpu.SemaphoreType.DMA((4,)),
    pltpu.SemaphoreType.DMA((9,)),
    pltpu.SemaphoreType.DMA((9,)),
    *plane_sems(2),
]


def residual_kernel(terms, first, up_s, down_s, second_out, normed_out, up_w, down_w, *scratch):
    me, y, c, up, dn, op, oc = ring_places()
    plane = Plane([up_s, down_s], [up_w, down_w], *scratch[11:], False)
    attn = pair_sum_to_owner(plane, terms, *scratch[:9])
    second = (first[...].astype(F32) + attn).astype(BF16)
    second_out[...] = second
    normed_out[y, c] = normalize(second.astype(F32)).astype(BF16)
    to_all(normed_out, *scratch[9:11])
    plane.finish(0)
    plane.finish(1)


def residual(terms, first, shards):
    return pl.pallas_call(
        residual_kernel,
        out_shape=[
            jax.ShapeDtypeStruct((128, 1024), BF16),
            jax.ShapeDtypeStruct((4, 2, 128, 1024), BF16),
            *map(gathered, shards),
        ],
        in_specs=[VM] * 4,
        out_specs=[VM] * 4,
        scratch_shapes=PAIR_SCRATCH,
        compiler_params=params(5, 24),
        name="residual_exchange",
    )(terms, first, *shards)


def backward_kernel(info, terms, second, per_token, up_term, packet, g_out, up_grad, packets, up_buf, *scratch):
    me, y, c, up, dn, op, oc = ring_places()
    plane = Plane([packet, up_term], [packets, up_buf], *scratch[11:], True)
    grad = pair_sum_to_owner(plane, terms, *scratch[:9])
    live = (y * 2 + c) * 128 + lax.broadcasted_iota(jnp.int32, (128, 1), 0) < info[1:2, 0:1]
    g_third = jnp.where(live, per_token[...], 0.0)
    g_out[y, c] = (g_third + normalize_back(second[...].astype(F32), grad)).astype(BF16)
    to_all(g_out, *scratch[9:11])
    plane.finish(0)
    plane.finish(1)
    up_grad[...] = total_of(up_buf)


def backward(info, terms, second, per_token, up_term, packet):
    return pl.pallas_call(
        backward_kernel,
        out_shape=[
            jax.ShapeDtypeStruct((4, 2, 128, 1024), BF16),
            jax.ShapeDtypeStruct((64, 512), F32),
            gathered(packet),
        ],
        in_specs=[VM] * 6,
        out_specs=[VM] * 3,
        scratch_shapes=[pltpu.VMEM((16, 64, 512), BF16), *PAIR_SCRATCH],
        compiler_params=params(6, 24),
        name="backward_exchange",
    )(info, terms, second, per_token, up_term, packet)


PACKET = 512 + 1024 + 1024 + 128 + 128
ROWS = 256
LHS_T = (((0,), (0,)), ((), ()))
RHS_T = (((1,), (1,)), ((), ()))


def ffn_kernel(
    info, normed, second, up_w, down_w, head_w, per_token_out, packet_out, terms, up_term,
    slope, g_pre, parts, send, recv,
):
    me, y, c, up, dn, op, oc = ring_places()
    slot = y * 2 + c
    peers = [(k, e) for k in (2, 1, 3, 0) for e in range(2) if (k, e) != (0, 0)]

    def device(k, e):
        return dict(y=add_mod(y, k, 4), c=add_mod(c, e, 2))

    for k, e in peers:
        signal(device(4 - k if k else 0, e))

    length, label = info[1:2, 0:1], info[2:3, 0:1]

    def live(start, size):
        return start + lax.broadcasted_iota(jnp.int32, (size, 1), 0) < length

    hidden_sum = jnp.zeros((1, 512), F32)
    for block in range(1024 // ROWS):
        rows = pl.ds(block * ROWS, ROWS)
        hidden = jnp.dot(normed[rows], up_w[...], preferred_element_type=F32)
        square = hidden * hidden
        inner = jnp.tanh(0.7978845608028654 * hidden * (1.0 + 0.044715 * square))
        half = 0.5 * (1.0 + inner)
        acted = (hidden * half).astype(BF16).astype(F32)
        slope[rows] = half + 0.5 * hidden * (1.0 - inner * inner) * (
            0.7978845608028654 + (0.7978845608028654 * 3.0 * 0.044715) * square
        )
        hidden_sum += jnp.sum(jnp.where(live(block * ROWS, ROWS), acted, 0.0), axis=0, keepdims=True)
    own = jnp.where(live(slot * 128, 128), second[...].astype(F32), 0.0)
    pushed = lax.dot_general(thirds(hidden_sum), down_w[...], RHS_T, preferred_element_type=F32)
    parts[slot] = jnp.sum(own, axis=0, keepdims=True) + jnp.sum(pushed, axis=0, keepdims=True)
    pl.semaphore_wait(pltpu.get_barrier_semaphore(), 7)
    steps = [
        remote(parts.at[slot], parts.at[slot], send.at[k, e], recv.at[k, e], device(k, e)) for k, e in peers
    ]
    for step in steps:
        step.start()
    for step in steps:
        step.wait()
    pooled = parts[0]
    for s in range(1, 8):
        pooled = pooled + parts[s]
    count = length.astype(F32)
    pooled = pooled / count
    final = normalize(pooled)
    logits = jnp.sum(jnp.dot(thirds(final), head_w[...], preferred_element_type=F32), axis=0, keepdims=True)
    top = jnp.max(logits, axis=-1, keepdims=True)
    total = jnp.log(jnp.sum(jnp.exp(logits - top), axis=-1, keepdims=True)) + top
    labels = (lax.broadcasted_iota(jnp.int32, logits.shape, 1) == label).astype(F32)
    loss = total - jnp.sum(logits * labels, axis=-1, keepdims=True)
    g_logits = (jnp.exp(logits - total) - labels) / 16.0
    g_final = lax.dot_general(thirds(g_logits), head_w[...], RHS_T, preferred_element_type=F32)
    g_final = jnp.sum(g_final, axis=0, keepdims=True)
    per_token = normalize_back(pooled, g_final) / count
    rounded = per_token.astype(BF16)
    pulled = jnp.dot(rounded, down_w[...], preferred_element_type=F32)
    for block in range(1024 // ROWS):
        rows = pl.ds(block * ROWS, ROWS)
        grad = jnp.where(live(block * ROWS, ROWS), slope[rows] * pulled, 0.0).astype(BF16)
        g_pre[rows] = grad
        terms[rows] = lax.dot_general(grad, up_w[...], RHS_T, preferred_element_type=F32).astype(BF16)
    for block in range(1024 // ROWS):
        cols = pl.ds(block * ROWS, ROWS)
        up_term[cols] = lax.dot_general(
            normed[:, cols], g_pre[...], LHS_T, preferred_element_type=F32
        ).astype(BF16)
    per_token_out[...] = per_token
    packet_out[:, 0:512] = hidden_sum
    packet_out[:, 512:1536] = rounded.astype(F32)
    packet_out[:, 1536:2560] = final
    packet_out[:, 2560:2688] = g_logits
    packet_out[:, 2688:2816] = jnp.broadcast_to(loss, (1, 128))


def ffn(info, normed, second, up_w, down_w, head_w):
    return pl.pallas_call(
        ffn_kernel,
        out_shape=[
            jax.ShapeDtypeStruct((1, 1024), F32),
            jax.ShapeDtypeStruct((1, PACKET), F32),
            jax.ShapeDtypeStruct((1024, 1024), BF16),
            jax.ShapeDtypeStruct((1024, 512), BF16),
        ],
        in_specs=[VM] * 6,
        out_specs=[VM, VM, VM, VM],
        scratch_shapes=[
            pltpu.VMEM((1024, 512), F32),
            pltpu.VMEM((1024, 512), BF16),
            pltpu.VMEM((8, 1, 1024), F32),
            pltpu.SemaphoreType.DMA((4, 2)),
            pltpu.SemaphoreType.DMA((4, 2)),
        ],
        compiler_params=params(7, 32),
        name="ffn",
    )(info, normed, second, up_w, down_w, head_w)


SCALE = 0.125
WIDE = 256


def head_rows(value, head):
    rows = lax.broadcasted_iota(jnp.int32, value.shape, 0)
    return jnp.where((rows >= 64) == (head == 1), value, jnp.zeros_like(value))


def head_cols(value, head):
    cols = lax.broadcasted_iota(jnp.int32, value.shape, 1)
    return jnp.where((cols >= 64) == (head == 1), value, jnp.zeros_like(value))


def attend_kernel(info, normed, qkv_w, out_w, qkv, context_t, probs_t, terms):
    for block in range(4):
        rows = pl.ds(block * 256, 256)
        qkv[rows] = jnp.dot(normed[rows], qkv_w[...], preferred_element_type=F32).astype(BF16)
    keys = qkv[:, 128:256]
    query_t = (qkv[:, 0:128] * SCALE).T
    values_t = qkv[:, 256:384].T
    out_t = out_w[...].T
    seen = lax.broadcasted_iota(jnp.int32, (1024, WIDE), 0) < info[1:2, 0:1]
    for block in range(1024 // WIDE):
        cols = slice(block * WIDE, (block + 1) * WIDE)
        for head in range(2):
            scores = jnp.dot(keys, head_rows(query_t[:, cols], head), preferred_element_type=F32)
            scores = jnp.where(seen, scores, -1e30)
            expo = jnp.exp(scores - jnp.max(scores, axis=0, keepdims=True))
            probs = (expo * (1.0 / jnp.sum(expo, axis=0, keepdims=True))).astype(BF16)
            probs_t[head, :, cols] = probs
            rows = slice(head * 64, head * 64 + 64)
            context_t[rows, cols] = jnp.dot(values_t[rows], probs, preferred_element_type=F32).astype(BF16)
        terms[cols] = jnp.dot(context_t[:, cols].T, out_t, preferred_element_type=F32).astype(BF16)


def attend(info, normed, qkv_w, out_w):
    return pl.pallas_call(
        attend_kernel,
        out_shape=[
            jax.ShapeDtypeStruct((1024, 384), BF16),
            jax.ShapeDtypeStruct((128, 1024), BF16),
            jax.ShapeDtypeStruct((2, 1024, 1024), BF16),
            jax.ShapeDtypeStruct((1024, 1024), BF16),
        ],
        in_specs=[VM] * 4,
        out_specs=[VM] * 4,
        compiler_params=pltpu.CompilerParams(vmem_limit_bytes=32 * 2**20),
        name="attend",
    )(info, normed, qkv_w, out_w)


def attend_back_kernel(
    g_second, normed, out_w, qkv, probs_t, context_t, out_term, qkv_term, grad, grad_t, grad_q, grad_k, grad_v
):
    out_term[...] = jnp.dot(context_t[...], g_second[...], preferred_element_type=F32).T.astype(BF16)
    for block in range(4):
        rows = pl.ds(block * 256, 256)
        part = jnp.dot(g_second[rows], out_w[...], preferred_element_type=F32)
        grad[rows] = part.astype(BF16)
        grad_t[:, block * 256 : block * 256 + 256] = part.T
    query = qkv[:, 0:128] * SCALE
    keys_t = (qkv[:, 128:256] * SCALE).T
    values = qkv[:, 256:384]
    product = grad_t[...] * context_t[...].astype(F32)
    for block in range(1024 // WIDE):
        cols = slice(block * WIDE, (block + 1) * WIDE)
        for head in range(2):
            rows = slice(head * 64, head * 64 + 64)
            probs = probs_t[head, :, cols]
            delta = jnp.sum(product[rows, cols], axis=0, keepdims=True)
            pulled = jnp.dot(values, head_rows(grad_t[:, cols], head).astype(BF16), preferred_element_type=F32)
            g_scores = (probs.astype(F32) * (pulled - delta)).astype(BF16)
            grad_q[rows, cols] = jnp.dot(keys_t[rows], g_scores, preferred_element_type=F32).astype(BF16)
            g_keys = jnp.dot(g_scores, head_cols(query[cols], head), preferred_element_type=F32)
            g_vals = jnp.dot(probs, head_cols(grad[cols], head), preferred_element_type=F32)
            if block == 0 and head == 0:
                grad_k[...] = g_keys
                grad_v[...] = g_vals
            else:
                grad_k[...] += g_keys
                grad_v[...] += g_vals
    for piece, value in enumerate((None, grad_k, grad_v)):
        left = grad_q[...] if value is None else value[...].T.astype(BF16)
        part = jnp.dot(left, normed[...], preferred_element_type=F32)
        qkv_term[:, piece * 128 : piece * 128 + 128] = part.T.astype(BF16)


def attend_back(g_second, normed, out_w, qkv, probs_t, context_t):
    return pl.pallas_call(
        attend_back_kernel,
        out_shape=[
            jax.ShapeDtypeStruct((1024, 128), BF16),
            jax.ShapeDtypeStruct((1024, 384), BF16),
        ],
        in_specs=[VM] * 6,
        out_specs=[VM] * 2,
        scratch_shapes=[
            pltpu.VMEM((1024, 128), BF16),
            pltpu.VMEM((128, 1024), F32),
            pltpu.VMEM((128, 1024), BF16),
            pltpu.VMEM((1024, 128), F32),
            pltpu.VMEM((1024, 128), F32),
        ],
        compiler_params=pltpu.CompilerParams(vmem_limit_bytes=32 * 2**20),
        name="attend_back",
    )(g_second, normed, out_w, qkv, probs_t, context_t)


def per_device(token_ids, lengths, teacher_bins, table, qkv_shard, out_shard, up_shard, down_shard, head_shard):
    info, first, normed, qkv_w, out_w, head_w = embed(
        lengths, teacher_bins, token_ids, table, [qkv_shard.reshape(64, 384), out_shard.T, head_shard]
    )
    normed = normed.reshape(1024, 1024)
    qkv_w = qkv_w.reshape(1024, 384)
    out_w = out_w.reshape(1024, 128)
    head_w = head_w.reshape(1024, 128)
    qkv, context_t, probs_t, terms = attend(info, normed, qkv_w, out_w)
    second, normed_two, up_w, down_w = residual(terms.reshape(4, 2, 128, 1024), first, [up_shard, down_shard.T])
    up_w = up_w.reshape(1024, 512)
    down_w = down_w.reshape(1024, 512)
    per_token, packet, terms, up_term = ffn(
        info, normed_two.reshape(1024, 1024), second, up_w, down_w, head_w
    )
    g_second, up_grad, packets = backward(
        info, terms.reshape(4, 2, 128, 1024), second, per_token, up_term.reshape(16, 64, 512), packet
    )
    out_term, qkv_term = attend_back(g_second.reshape(1024, 1024), normed, out_w, qkv, probs_t, context_t)
    out_grad, qkv_grad, down_grad, head_grad, loss = collect(
        packets.reshape(16, PACKET), out_term.reshape(16, 64, 128), qkv_term.reshape(16, 64, 384)
    )
    return loss[0, 0], qkv_grad, out_grad.T, up_grad, down_grad, head_grad


def solution(mesh):
    fine = Mesh(mesh.devices.reshape(2, 4, 2, 4, 2), ("xl", "z", "c", "y", "xh"))
    dp, tensor = ("xl", "z", "c"), ("y", "xh")
    return jax.shard_map(
        per_device,
        mesh=fine,
        in_specs=(
            P(dp, tensor),
            P(dp),
            P(dp),
            P(tensor, None),
            P(dp, None, tensor),
            P(tensor, dp),
            P(dp, tensor),
            P(tensor, dp),
            P(dp, None),
        ),
        out_specs=(
            P(),
            P(dp, None, tensor),
            P(tensor, dp),
            P(dp, tensor),
            P(tensor, dp),
            P(dp, None),
        ),
        check_vma=False,
    )
```

```python
import functools
import types

import jax
import jax.numpy as jnp
from jax import lax
from jax.experimental import pallas as pl
from jax.experimental.pallas import tpu as pltpu
from jax.sharding import Mesh
from jax.sharding import PartitionSpec as P

MESH = pl.DeviceIdType.MESH
EPS = 1e-05
F32 = jnp.float32
BF16 = jnp.bfloat16
HIGH = lax.Precision.HIGHEST
VM = pl.BlockSpec(memory_space=pltpu.VMEM)
SM = pl.BlockSpec(memory_space=pltpu.SMEM)


def where_am_i():
    return {name: lax.axis_index(name) for name in ("xl", "z", "c", "y", "xh")}


def add_mod(value, step, size):
    return lax.rem(value + step, size)


def params(number, mebibytes):
    return pltpu.CompilerParams(
        collective_id=number, has_side_effects=True, vmem_limit_bytes=mebibytes * 2**20
    )


def remote(src, dst, send, recv, device):
    return pltpu.make_async_remote_copy(
        src_ref=src, dst_ref=dst, send_sem=send, recv_sem=recv, device_id=device, device_id_type=MESH
    )


def signal(device):
    pl.semaphore_signal(pltpu.get_barrier_semaphore(), inc=1, device_id=device, device_id_type=MESH)


def normalize(values):
    mean = jnp.mean(values, axis=-1, keepdims=True)
    centered = values - mean
    return centered * lax.rsqrt(jnp.mean(centered * centered, axis=-1, keepdims=True) + EPS)


def normalize_back(values, grad):
    mean = jnp.mean(values, axis=-1, keepdims=True)
    centered = values - mean
    scale = lax.rsqrt(jnp.mean(centered * centered, axis=-1, keepdims=True) + EPS)
    normed = centered * scale
    return scale * (
        grad
        - jnp.mean(grad, axis=-1, keepdims=True)
        - normed * jnp.mean(grad * normed, axis=-1, keepdims=True)
    )


class Ids:
    def __init__(self, src, out, send, recv):
        self.src, self.out, self.send, self.recv = src, out, send, recv
        self.me = where_am_i()
        self.here = self.me["xh"] == self.me["c"]

    def greet(self):
        me = self.me
        for role in range(2):
            for k in range(4):
                source = dict(
                    xl=add_mod(me["xl"], role, 2),
                    c=add_mod(me["xh"], role, 2),
                    xh=me["c"],
                    y=add_mod(me["y"], 4 - k, 4),
                    z=me["z"],
                )
                if role == 0 and k == 0:

                    @pl.when(jnp.logical_not(self.here))
                    def _(source=source):
                        signal(source)
                else:
                    signal(source)
        return jnp.where(self.here, 7, 8)

    def copy(self, role, k):
        me = self.me
        return remote(
            self.src,
            self.out.at[role, me["y"]],
            self.send.at[role, k],
            self.recv.at[role, k],
            dict(
                xl=add_mod(me["xl"], role, 2),
                c=me["xh"],
                xh=add_mod(me["c"], role, 2),
                y=add_mod(me["y"], k, 4),
                z=me["z"],
            ),
        )

    def local(self):
        return pltpu.make_async_copy(self.src, self.out.at[0, self.me["y"]], self.recv.at[0, 0])

    def start(self):
        for role in (1, 0):
            for k in (2, 1, 3, 0):
                if role == 0 and k == 0:

                    @pl.when(jnp.logical_not(self.here))
                    def _():
                        self.copy(0, 0).start()

                    @pl.when(self.here)
                    def _():
                        self.local().start()
                else:
                    self.copy(role, k).start()

    def arrive(self, role):
        for k in range(4):
            place = add_mod(self.me["y"], 4 - k, 4)
            pltpu.make_async_copy(self.src, self.out.at[role, place], self.recv.at[role, k]).wait()

    def sent(self):
        for role in range(2):
            for k in range(4):
                if role == 0 and k == 0:

                    @pl.when(jnp.logical_not(self.here))
                    def _():
                        self.copy(0, 0).wait_send()
                else:
                    self.copy(role, k).wait_send()


class Plane:
    def __init__(self, items, send, recv, collect):
        self.items, self.send, self.recv, self.collect = items, send, recv, collect
        self.me = where_am_i()
        c, xh = self.me["c"], self.me["xh"]
        self.here = xh == c
        self.mine, self.other = (xh, c) if collect else (c, xh)
        self.slot = (self.me["xl"] * 4 + self.me["z"]) * 2 + self.mine
        self.places = [(a, k, e) for k in (2, 1, 3, 0) for a in (1, 0) for e in range(2)]

    def target(self, a, k, e):
        me = self.me
        swapped = dict(c=e, xh=me["c"]) if self.collect else dict(c=me["xh"], xh=e)
        return dict(xl=add_mod(me["xl"], a, 2), z=add_mod(me["z"], k, 4), y=me["y"], **swapped)

    def origin(self, a, k, e):
        me = self.me
        swapped = dict(c=me["xh"], xh=e) if self.collect else dict(c=e, xh=me["c"])
        return dict(xl=add_mod(me["xl"], a, 2), z=add_mod(me["z"], 4 - k, 4), y=me["y"], **swapped)

    def number(self, a, k, e):
        return (add_mod(self.me["xl"], a, 2) * 4 + add_mod(self.me["z"], k, 4)) * 2 + e

    def greet(self):
        for a, k, e in self.places:
            if a == 0 and k == 0:

                @pl.when(jnp.logical_not(jnp.logical_and(self.here, e == self.mine)))
                def _(a=a, k=k, e=e):
                    signal(self.origin(a, k, e))
            else:
                signal(self.origin(a, k, e))
        return jnp.where(self.here, 15, 16)

    def start(self, i):
        block, place = self.items[i][:2]

        def copy(a, k, e):
            return remote(
                block(self.number(a, k, e)), place(self.slot), self.send.at[i], self.recv.at[i], self.target(a, k, e)
            )

        for a, k, e in self.places:
            if a == 0 and k == 0:
                is_self = jnp.logical_and(self.here, e == self.other)

                @pl.when(jnp.logical_not(is_self))
                def _(a=a, k=k, e=e):
                    copy(a, k, e).start()

                @pl.when(is_self)
                def _(a=a, k=k, e=e):
                    pltpu.make_async_copy(
                        block(self.number(a, k, e)), place(self.slot), self.recv.at[i]
                    ).start()
            else:
                copy(a, k, e).start()

    def arrive(self, i):
        whole = self.items[i][2]
        pltpu.make_async_copy(whole, whole, self.recv.at[i]).wait()

    def sent(self, i):
        whole, but_one = self.items[i][2:]

        @pl.when(self.here)
        def _():
            pltpu.make_async_copy(but_one, but_one, self.send.at[i]).wait()

        @pl.when(jnp.logical_not(self.here))
        def _():
            pltpu.make_async_copy(whole, whole, self.send.at[i]).wait()


def rows64(number):
    return pl.ds(pl.multiple_of(number * 64, 64), 64)


def spread_item(shard, target, cols=None):
    cols = pl.ds(0, target.shape[1]) if cols is None else cols
    return (
        lambda number: shard,
        lambda slot: target.at[rows64(slot), cols],
        target.at[:, cols],
        target.at[pl.ds(0, 960), cols],
    )


def collect_item(source, buf):
    return (
        lambda number: source.at[rows64(number)],
        lambda slot: buf.at[slot],
        buf,
        buf.at[pl.ds(0, 15)],
    )


def total_of(buf):
    total = buf[0].astype(F32)
    for s in range(1, 16):
        total = total + buf[s].astype(F32)
    return total


def thirds(row):
    high = row.astype(BF16).astype(F32)
    middle = (row - high).astype(BF16).astype(F32)
    low = row - high - middle
    index = lax.broadcasted_iota(jnp.int32, (8, row.shape[1]), 0)
    rows = jnp.where(index == 0, high, jnp.where(index == 1, middle, jnp.where(index == 2, low, 0.0)))
    return rows.astype(BF16)


def picked(values, start):
    rows = lax.broadcasted_iota(jnp.int32, (64, values.shape[1]), 0)
    cols = lax.broadcasted_iota(jnp.int32, (64, values.shape[1]), 1)
    chosen = (cols == rows + start).astype(F32)
    return lax.dot_general(chosen, values, RHS_T, precision=HIGH, preferred_element_type=F32)


def ring_places():
    me = where_am_i()
    y, c = me["y"], me["c"]
    return me, y, c, add_mod(y, 1, 4), add_mod(y, 3, 4), add_mod(y, 2, 4), 1 - c


class Owner:
    def __init__(self, blocks, stage, far, near, send, recv):
        self.blocks, self.stage, self.far, self.near, self.send, self.recv = blocks, stage, far, near, send, recv
        _, self.y, _, self.up, self.dn, op, _ = ring_places()
        self.first = [
            remote(blocks(op).at[pl.ds(0, 32)], far.at[0], send.at[0], recv.at[0], dict(y=self.up)),
            remote(blocks(op).at[pl.ds(32, 32)], far.at[1], send.at[1], recv.at[1], dict(y=self.dn)),
        ]
        self.second = [
            remote(stage.at[i], near.at[i], send.at[2 + i], recv.at[2 + i], dict(y=(self.up, self.dn)[i]))
            for i in range(2)
        ]

    def begin(self):
        for step in self.first:
            step.start()

    def relay(self):
        blocks, stage, far = self.blocks, self.stage, self.far
        stage[0, 32:64] = blocks(self.up)[32:64]
        stage[1, 0:32] = blocks(self.dn)[0:32]
        self.first[0].wait_recv()
        stage[0, 0:32] = (blocks(self.up)[0:32].astype(F32) + far[0].astype(F32)).astype(BF16)
        self.second[0].start()
        self.first[1].wait_recv()
        stage[1, 32:64] = (blocks(self.dn)[32:64].astype(F32) + far[1].astype(F32)).astype(BF16)
        self.second[1].start()

    def finish(self):
        for step in self.second:
            step.wait_recv()
        return self.blocks(self.y)[...].astype(F32) + self.near[0].astype(F32) + self.near[1].astype(F32)

    def sent(self):
        for step in self.first + self.second:
            step.wait_send()


class Gather:
    def __init__(self, out, chunk, send, recv):
        self.out, self.chunk, self.send, self.recv = out, chunk, send, recv
        _, y, c, up, dn, op, oc = ring_places()
        moves = [
            (y, c, None, dict(y=up)),
            (y, c, None, dict(y=dn)),
            (y, c, None, dict(c=oc)),
            (dn, c, 0, dict(y=up)),
            (dn, c, None, dict(c=oc)),
            (up, c, 1, dict(y=dn)),
            (up, c, None, dict(c=oc)),
            (op, c, 0, dict(c=oc)),
            (op, c, 1, dict(c=oc)),
        ]
        self.steps = []
        for k, (row, col, half, device) in enumerate(moves):
            start = (row * 2 + col) * 128 + chunk * 64
            if half is None:
                ref = out.at[pl.ds(pl.multiple_of(start, 64), 64)]
            else:
                ref = out.at[pl.ds(pl.multiple_of(start + half * 32, 32), 32)]
            self.steps.append(remote(ref, ref, send.at[k], recv.at[k], device))

    def begin(self):
        for k in (0, 1, 2):
            self.steps[k].start()

    def sides(self):
        self.steps[0].wait_recv()
        self.steps[3].start()
        self.steps[4].start()
        self.steps[1].wait_recv()
        self.steps[5].start()
        self.steps[6].start()

    def far(self):
        self.steps[3].wait_recv()
        self.steps[7].start()
        self.steps[5].wait_recv()
        self.steps[8].start()

    def pair_own(self):
        self.steps[2].wait_recv()

    def pair_sides(self):
        self.steps[4].wait_recv()
        self.steps[6].wait_recv()

    def pair_far(self):
        self.steps[7].wait_recv()
        self.steps[8].wait_recv()

    def sent(self):
        for step in self.steps:
            step.wait_send()


def gather_beside(gathers, block_work):
    _, y, c, up, dn, op, oc = ring_places()
    for g in gathers:
        g.pair_own()
    block_work(y)
    for g in gathers:
        g.sides()
    for g in gathers:
        g.pair_sides()
    block_work(up)
    for g in gathers:
        g.far()
    block_work(dn)
    for g in gathers:
        g.pair_far()
    block_work(op)


class PairOwner:
    def __init__(self, terms, r, name):
        self.terms = terms
        get = lambda part: getattr(r, name + part)
        _, y, self.c, self.up, self.dn, self.op, oc = ring_places()
        self.pair, self.summed = get("_pair"), get("_summed")
        self.order = (self.op, self.up, self.dn, y)
        self.steps = [
            remote(
                terms.at[self.rows(b, oc)], self.pair.at[b], get("_psend").at[i], get("_precv").at[i], dict(c=oc)
            )
            for i, b in enumerate(self.order)
        ]
        self.owners = [
            Owner(
                lambda b, ch=ch: self.summed.at[b, pl.ds(ch * 64, 64)],
                get("_stage").at[ch],
                get("_far").at[ch],
                get("_near").at[ch],
                get("_rsend").at[ch],
                get("_rrecv").at[ch],
            )
            for ch in range(2)
        ]

    def rows(self, b, c):
        return pl.ds(pl.multiple_of((b * 2 + c) * 128, 128), 128)

    def push(self, i):
        self.steps[i].start()

    def pull(self, i):
        b = self.order[i]
        self.steps[i].wait_recv()
        self.summed[b] = (self.terms[self.rows(b, self.c)].astype(F32) + self.pair[b].astype(F32)).astype(BF16)

    def sent(self):
        for step in self.steps:
            step.wait_send()
        for owner in self.owners:
            owner.sent()


def pair_owner_scratch(name):
    return {
        name + "_pair": pltpu.VMEM((4, 128, 1024), BF16),
        name + "_summed": pltpu.VMEM((4, 128, 1024), BF16),
        name + "_stage": pltpu.VMEM((2, 2, 64, 1024), BF16),
        name + "_far": pltpu.VMEM((2, 2, 32, 1024), BF16),
        name + "_near": pltpu.VMEM((2, 2, 64, 1024), BF16),
        name + "_psend": pltpu.SemaphoreType.DMA((4,)),
        name + "_precv": pltpu.SemaphoreType.DMA((4,)),
        name + "_rsend": pltpu.SemaphoreType.DMA((2, 4)),
        name + "_rrecv": pltpu.SemaphoreType.DMA((2, 4)),
        name + "_asend": pltpu.SemaphoreType.DMA((2, 9)),
        name + "_arecv": pltpu.SemaphoreType.DMA((2, 9)),
    }


SCALE = 0.125
PACKET = 512 + 1024 + 1024 + 128 + 128
LHS_T = (((0,), (0,)), ((), ()))
RHS_T = (((1,), (1,)), ((), ()))


def rows256(b):
    return pl.ds(pl.multiple_of(b * 256, 256), 256)


def of_head(value, head, axis):
    index = lax.broadcasted_iota(jnp.int32, value.shape, axis)
    return jnp.where((index >= 64) == (head == 1), value, jnp.zeros_like(value))


def step_kernel(names, *refs):
    r = types.SimpleNamespace(**dict(zip(names, refs, strict=True)))
    me, y, c, up, dn, op, oc = ring_places()
    slot = y * 2 + c
    vocab, padded = r.table.shape[0], r.shard.shape[0]

    fetch = pltpu.make_async_copy(r.table, r.shard.at[pl.ds(0, vocab)], r.load.at[0])
    fetch_ids = pltpu.make_async_copy(r.ids, r.ids_here, r.load.at[1])
    fetch_ids.start()
    fetch.start()
    tokens = Ids(r.packet_in, r.got, r.isend, r.irecv)
    spread = Plane(
        [spread_item(r.qkv_s.at[i], r.qkv_w, pl.ds(i * 128, 128)) for i in range(3)]
        + [
            spread_item(r.out_s, r.out_w),
            spread_item(r.up_s, r.up_w),
            spread_item(r.head_s, r.head_w),
            spread_item(r.down_s, r.down_w),
        ],
        r.ssend,
        r.srecv,
        False,
    )
    collect = Plane(
        [
            (lambda number: r.packet, lambda slot: r.packets.at[slot], r.packets, r.packets.at[pl.ds(0, 15)]),
            collect_item(r.up_term, r.up_buf),
            collect_item(r.out_term, r.out_buf),
        ]
        + [collect_item(r.qkv_term.at[i], r.qkv_buf.at[i]) for i in range(3)],
        r.csend,
        r.crecv,
        True,
    )
    partner = dict(xl=1 - me["xl"], xh=1 - me["xh"])
    peers = [(k, e) for k in (2, 1, 3, 0) for e in range(2) if (k, e) != (0, 0)]
    for device in (dict(y=up), dict(y=dn), dict(c=oc), partner):
        signal(device)
    for k, e in peers:
        signal(dict(y=add_mod(y, (4 - k) % 4, 4), c=add_mod(c, e, 2)))
    greeted = tokens.greet() + spread.greet() + collect.greet() + 11
    if padded > vocab:
        r.shard[vocab:padded] = jnp.zeros((padded - vocab, 1024), BF16)
    fetch_ids.wait()
    line = lax.broadcasted_iota(jnp.int32, (8, 128), 0)
    r.packet_in[...] = jnp.where(line == 0, r.ids_here[...], jnp.where(line == 1, r.count[0], r.label[0]))
    pl.semaphore_wait(pltpu.get_barrier_semaphore(), greeted)
    tokens.start()
    for i in range(4):
        spread.start(i)

    base = (y * 2 + me["xh"]) * vocab
    lanes = lax.broadcasted_iota(jnp.int32, (64, 128), 1)

    def look_up(role, ch):
        for b in range(4):
            wanted = jnp.broadcast_to(r.got[role, b, 0:1, :], (128, 128)).T[ch * 64 : ch * 64 + 64] - base
            for tile in range(padded // 128):
                r.chosen[b * 64 : b * 64 + 64, tile * 128 : tile * 128 + 128] = jnp.where(
                    wanted == lanes + tile * 128, 1.0, 0.0
                ).astype(BF16)
        if role == 1 and ch == 0:
            fetch.wait()
        for part in range(4):
            cols = slice(part * 256, part * 256 + 256)
            found = jnp.dot(r.chosen[...], r.shard[:, cols], preferred_element_type=F32).astype(BF16)
            for b in range(4):
                r.rows[role, ch, b, :, cols] = found[b * 64 : b * 64 + 64]

    own = {
        (role, ch): Owner(
            lambda b, role=role, ch=ch: r.rows.at[role, ch, b],
            r.e_stage.at[role, ch],
            r.e_far.at[role, ch],
            r.e_near.at[role, ch],
            r.e_rsend.at[role, ch],
            r.e_rrecv.at[role, ch],
        )
        for role in range(2)
        for ch in range(2)
    }
    cross = [
        remote(r.total.at[ch], r.theirs.at[ch], r.xsend.at[ch], r.xrecv.at[ch], partner) for ch in range(2)
    ]
    tokens.arrive(1)
    look_up(1, 0)
    own[1, 0].begin()
    look_up(1, 1)
    own[1, 1].begin()
    own[1, 0].relay()
    tokens.arrive(0)
    look_up(0, 0)
    own[0, 0].begin()
    own[1, 1].relay()
    r.total[0] = own[1, 0].finish().astype(BF16)
    cross[0].start()
    look_up(0, 1)
    own[0, 1].begin()
    own[0, 0].relay()
    r.total[1] = own[1, 1].finish().astype(BF16)
    cross[1].start()
    for i in range(4, 7):
        spread.start(i)
    own[0, 1].relay()
    length, label = r.got[0, 0, 1:2, 0:1], r.got[0, 0, 2:3, 0:1]
    gathers = [Gather(r.normed, ch, r.e_asend.at[ch], r.e_arecv.at[ch]) for ch in range(2)]
    first = []

    def own_rows(ch):
        return pl.ds(pl.multiple_of(slot * 128 + ch * 64, 64), 64)

    for ch in range(2):
        mine = own[0, ch].finish()
        cross[ch].wait_recv()
        value = mine + r.theirs[ch].astype(F32)
        first.append(value)
        r.normed[own_rows(ch)] = normalize(value).astype(BF16)
        gathers[ch].begin()
    for ch in range(2):
        r.first[ch * 64 : ch * 64 + 64] = first[ch]
    for i in range(4):
        spread.arrive(i)

    def project(b):
        r.qkv[rows256(b)] = jnp.dot(r.normed[rows256(b)], r.qkv_w[...], preferred_element_type=F32).astype(BF16)

    gather_beside(gathers, project)

    r.query_t[...] = (r.qkv[:, 0:128] * SCALE).T
    r.values_t[...] = r.qkv[:, 256:384].T
    r.out_t[...] = r.out_w[...].T
    seen = lax.broadcasted_iota(jnp.int32, (1024, 256), 0) < length

    def attend(b):
        cols = rows256(b)
        for head in range(2):
            scores = jnp.dot(
                r.qkv[:, 128:256], of_head(r.query_t[:, cols], head, 0), preferred_element_type=F32
            )
            scores = jnp.where(seen, scores, -1e30)
            expo = jnp.exp(scores - jnp.max(scores, axis=0, keepdims=True))
            probs = (expo * (1.0 / jnp.sum(expo, axis=0, keepdims=True))).astype(BF16)
            r.probs_t[head, :, cols] = probs
            rows = slice(head * 64, head * 64 + 64)
            r.context_t[rows, cols] = jnp.dot(
                r.values_t[rows], probs, preferred_element_type=F32
            ).astype(BF16)
        r.terms[cols] = jnp.dot(r.context_t[:, cols].T, r.out_t[...], preferred_element_type=F32).astype(BF16)

    summed = PairOwner(r.terms, r, "a")
    attend(op)
    summed.push(0)
    attend(up)
    summed.push(1)
    summed.pull(0)
    for owner in summed.owners:
        owner.begin()
    attend(dn)
    summed.push(2)
    summed.pull(1)
    attend(y)
    summed.push(3)
    summed.pull(2)
    for owner in summed.owners:
        owner.relay()
    summed.pull(3)
    more = [Gather(r.normed_two, ch, r.a_asend.at[ch], r.a_arecv.at[ch]) for ch in range(2)]
    for ch in range(2):
        second = (r.first[ch * 64 : ch * 64 + 64] + summed.owners[ch].finish()).astype(BF16)
        r.second[ch * 64 : ch * 64 + 64] = second
        r.normed_two[own_rows(ch)] = normalize(second.astype(F32)).astype(BF16)
        more[ch].begin()

    def live(start, size):
        return start + lax.broadcasted_iota(jnp.int32, (size, 1), 0) < length

    r.hidden_sum[...] = jnp.zeros((1, 512), F32)
    spread.arrive(4)

    def hidden_block(b):
        hidden = jnp.dot(r.normed_two[rows256(b)], r.up_w[...], preferred_element_type=F32)
        square = hidden * hidden
        inner = jnp.tanh(0.7978845608028654 * hidden * (1.0 + 0.044715 * square))
        half = 0.5 * (1.0 + inner)
        acted = (hidden * half).astype(BF16).astype(F32)
        r.slope[rows256(b)] = half + 0.5 * hidden * (1.0 - inner * inner) * (
            0.7978845608028654 + (0.7978845608028654 * 3.0 * 0.044715) * square
        )
        r.hidden_sum[...] += jnp.sum(jnp.where(live(b * 256, 256), acted, 0.0), axis=0, keepdims=True)

    gather_beside(more, hidden_block)

    spread.arrive(5)
    spread.arrive(6)
    hidden_sum = r.hidden_sum[...]
    own_sum = jnp.sum(jnp.where(live(slot * 128, 128), r.second[...].astype(F32), 0.0), axis=0, keepdims=True)
    pushed = lax.dot_general(thirds(hidden_sum), r.down_w[...], RHS_T, preferred_element_type=F32)
    r.parts[slot] = own_sum + jnp.sum(pushed, axis=0, keepdims=True)
    small = [
        remote(
            r.parts.at[slot],
            r.parts.at[slot],
            r.hsend.at[k, e],
            r.hrecv.at[k, e],
            dict(y=add_mod(y, k, 4), c=add_mod(c, e, 2)),
        )
        for k, e in peers
    ]
    for step in small:
        step.start()
    for step in small:
        step.wait()
    pooled = r.parts[0]
    for s in range(1, 8):
        pooled = pooled + r.parts[s]
    count = length.astype(F32)
    pooled = pooled / count
    final = normalize(pooled)
    logits = jnp.sum(jnp.dot(thirds(final), r.head_w[...], preferred_element_type=F32), axis=0, keepdims=True)
    top = jnp.max(logits, axis=-1, keepdims=True)
    total = jnp.log(jnp.sum(jnp.exp(logits - top), axis=-1, keepdims=True)) + top
    labels = (lax.broadcasted_iota(jnp.int32, logits.shape, 1) == label).astype(F32)
    loss = total - jnp.sum(logits * labels, axis=-1, keepdims=True)
    g_logits = (jnp.exp(logits - total) - labels) / 16.0
    g_final = lax.dot_general(thirds(g_logits), r.head_w[...], RHS_T, preferred_element_type=F32)
    per_token = normalize_back(pooled, jnp.sum(g_final, axis=0, keepdims=True)) / count
    rounded = per_token.astype(BF16)
    pulled = jnp.dot(rounded, r.down_w[...], preferred_element_type=F32)

    back = PairOwner(r.terms_back, r, "b")
    for i, b in enumerate(back.order):
        rows = rows256(b)
        grad = jnp.where(live(b * 256, 256), r.slope[rows] * pulled, 0.0).astype(BF16)
        r.g_pre[rows] = grad
        r.terms_back[rows] = lax.dot_general(
            grad, r.up_w[...], RHS_T, preferred_element_type=F32
        ).astype(BF16)
        back.push(i)
    back.pull(0)
    for owner in back.owners:
        owner.begin()
    for i in range(1, 4):
        back.pull(i)
    for block in range(4):
        cols = pl.ds(block * 256, 256)
        r.up_term[cols] = lax.dot_general(
            r.normed_two[:, cols], r.g_pre[...], LHS_T, preferred_element_type=F32
        ).astype(BF16)
    for owner in back.owners:
        owner.relay()
    r.packet[:, 0:512] = hidden_sum
    r.packet[:, 512:1536] = rounded.astype(F32)
    r.packet[:, 1536:2560] = final
    r.packet[:, 2560:2688] = g_logits
    r.packet[:, 2688:2816] = jnp.broadcast_to(loss, (1, 128))
    collect.start(1)
    collect.start(0)
    last = [Gather(r.g_second, ch, r.b_asend.at[ch], r.b_arecv.at[ch]) for ch in range(2)]
    for ch in range(2):
        grad = normalize_back(r.second[ch * 64 : ch * 64 + 64].astype(F32), back.owners[ch].finish())
        grad += jnp.where(live(slot * 128 + ch * 64, 64), per_token, 0.0)
        r.g_second[own_rows(ch)] = grad.astype(BF16)
        last[ch].begin()

    r.keys_t[...] = (r.qkv[:, 128:256] * SCALE).T
    r.grad_k[...] = jnp.zeros((1024, 128), F32)
    r.grad_v[...] = jnp.zeros((1024, 128), F32)

    def attend_back(b):
        cols = rows256(b)
        g_context = jnp.dot(r.g_second[cols], r.out_w[...], preferred_element_type=F32)
        g_context_t = g_context.T
        g_context = g_context.astype(BF16)
        product = g_context_t * r.context_t[:, cols].astype(F32)
        query = r.qkv[cols, 0:128] * SCALE
        for head in range(2):
            rows = slice(head * 64, head * 64 + 64)
            probs = r.probs_t[head, :, cols]
            delta = jnp.sum(product[rows], axis=0, keepdims=True)
            moved = jnp.dot(
                r.qkv[:, 256:384], of_head(g_context_t, head, 0).astype(BF16), preferred_element_type=F32
            )
            g_scores = (probs.astype(F32) * (moved - delta)).astype(BF16)
            r.grad_q[rows, cols] = jnp.dot(
                r.keys_t[rows], g_scores, preferred_element_type=F32
            ).astype(BF16)
            r.grad_k[...] += jnp.dot(g_scores, of_head(query, head, 1), preferred_element_type=F32)
            r.grad_v[...] += jnp.dot(probs, of_head(g_context, head, 1), preferred_element_type=F32)

    gather_beside(last, attend_back)
    r.out_term[...] = jnp.dot(r.context_t[...], r.g_second[...], preferred_element_type=F32).T.astype(BF16)
    collect.start(2)
    for piece in range(3):
        left = r.grad_q[...] if piece == 0 else (r.grad_k, r.grad_v)[piece - 1][...].T.astype(BF16)
        r.qkv_term[piece] = jnp.dot(left, r.normed[...], preferred_element_type=F32).T.astype(BF16)
        collect.start(3 + piece)

    collect.arrive(0)
    begin = ((me["xl"] * 4 + me["z"]) * 2 + me["c"]) * 64
    packets = jnp.concatenate([r.packets[s] for s in range(16)], axis=0)
    r.down_grad[...] = jnp.dot(
        picked(packets[:, 512:1536], begin), packets[:, 0:512], precision=HIGH, preferred_element_type=F32
    )
    r.head_grad[...] = jnp.dot(
        picked(packets[:, 1536:2560], begin), packets[:, 2560:2688], precision=HIGH, preferred_element_type=F32
    )
    r.loss[...] = jnp.sum(packets[:, 2688:2816], axis=0, keepdims=True) / 16.0
    collect.arrive(1)
    r.up_grad[...] = total_of(r.up_buf)

    tokens.sent()
    for i in range(7):
        spread.sent(i)
    for owner in own.values():
        owner.sent()
    for step in cross:
        step.wait_send()
    for g in gathers + more + last:
        g.sent()
    summed.sent()
    back.sent()
    for i in range(6):
        collect.sent(i)
    for i in range(2, 6):
        collect.arrive(i)


HBM = pl.BlockSpec(memory_space=pltpu.HBM)


def step(count, label, ids, table, qkv_s, out_s, up_s, down_s, head_s):
    padded = -(-table.shape[0] // 256) * 256
    inputs = dict(
        count=SM, label=SM, ids=HBM, table=HBM, qkv_s=HBM, out_s=HBM, up_s=HBM, down_s=HBM, head_s=HBM
    )
    outputs = dict(
        up_grad=jax.ShapeDtypeStruct((64, 512), F32),
        down_grad=jax.ShapeDtypeStruct((64, 512), F32),
        head_grad=jax.ShapeDtypeStruct((64, 128), F32),
        loss=jax.ShapeDtypeStruct((1, 128), F32),
        out_buf=jax.ShapeDtypeStruct((16, 64, 128), BF16),
        qkv_buf=jax.ShapeDtypeStruct((3, 16, 64, 128), BF16),
    )
    dma = pltpu.SemaphoreType.DMA
    vm = pltpu.VMEM
    scratch = dict(
        load=dma((2,)),
        ids_here=vm((1, 128), jnp.int32),
        packet_in=vm((8, 128), jnp.int32),
        got=vm((2, 4, 8, 128), jnp.int32),
        isend=dma((2, 4)),
        irecv=dma((2, 4)),
        ssend=dma((7,)),
        srecv=dma((7,)),
        csend=dma((6,)),
        crecv=dma((6,)),
        shard=vm((padded, 1024), BF16),
        chosen=vm((256, padded), BF16),
        rows=vm((2, 2, 4, 64, 1024), BF16),
        e_stage=vm((2, 2, 2, 64, 1024), BF16),
        e_far=vm((2, 2, 2, 32, 1024), BF16),
        e_near=vm((2, 2, 2, 64, 1024), BF16),
        e_rsend=dma((2, 2, 4)),
        e_rrecv=dma((2, 2, 4)),
        e_asend=dma((2, 9)),
        e_arecv=dma((2, 9)),
        total=vm((2, 64, 1024), BF16),
        theirs=vm((2, 64, 1024), BF16),
        xsend=dma((2,)),
        xrecv=dma((2,)),
        first=vm((128, 1024), F32),
        normed=vm((1024, 1024), BF16),
        qkv_w=vm((1024, 384), BF16),
        out_w=vm((1024, 128), BF16),
        up_w=vm((1024, 512), BF16),
        down_w=vm((1024, 512), BF16),
        head_w=vm((1024, 128), BF16),
        qkv=vm((1024, 384), BF16),
        query_t=vm((128, 1024), BF16),
        values_t=vm((128, 1024), BF16),
        keys_t=vm((128, 1024), BF16),
        out_t=vm((128, 1024), BF16),
        probs_t=vm((2, 1024, 1024), BF16),
        context_t=vm((128, 1024), BF16),
        terms=vm((1024, 1024), BF16),
        **pair_owner_scratch("a"),
        second=vm((128, 1024), BF16),
        normed_two=vm((1024, 1024), BF16),
        hidden_sum=vm((1, 512), F32),
        slope=vm((1024, 512), F32),
        parts=vm((8, 1, 1024), F32),
        hsend=dma((4, 2)),
        hrecv=dma((4, 2)),
        g_pre=vm((1024, 512), BF16),
        terms_back=vm((1024, 1024), BF16),
        **pair_owner_scratch("b"),
        up_term=vm((1024, 512), BF16),
        up_buf=vm((16, 64, 512), BF16),
        packet=vm((1, PACKET), F32),
        packets=vm((16, 1, PACKET), F32),
        g_second=vm((1024, 1024), BF16),
        grad_q=vm((128, 1024), BF16),
        grad_k=vm((1024, 128), F32),
        grad_v=vm((1024, 128), F32),
        out_term=vm((1024, 128), BF16),
        qkv_term=vm((3, 1024, 128), BF16),
    )
    return pl.pallas_call(
        functools.partial(step_kernel, (*inputs, *outputs, *scratch)),
        out_shape=list(outputs.values()),
        in_specs=list(inputs.values()),
        out_specs=[VM] * len(outputs),
        scratch_shapes=list(scratch.values()),
        compiler_params=params(1, 61),
        name="step",
    )(count, label, ids, table, qkv_s, out_s, up_s, down_s, head_s)


def results_kernel(up, down, head, out_buf, qkv_buf, up_grad, down_grad, head_grad, out_grad, qkv_grad):
    up_grad[...] = up[...]
    down_grad[...] = down[...]
    head_grad[...] = head[...]
    out_grad[...] = total_of(out_buf)
    for i in range(3):
        qkv_grad[i] = total_of(qkv_buf.at[i])


def results(*arrays):
    return pl.pallas_call(
        results_kernel,
        out_shape=[
            jax.ShapeDtypeStruct((64, 512), F32),
            jax.ShapeDtypeStruct((64, 512), F32),
            jax.ShapeDtypeStruct((64, 128), F32),
            jax.ShapeDtypeStruct((64, 128), F32),
            jax.ShapeDtypeStruct((3, 64, 128), F32),
        ],
        in_specs=[VM] * 5,
        out_specs=[VM] * 5,
        compiler_params=pltpu.CompilerParams(vmem_limit_bytes=8 * 2**20),
        name="results",
    )(*arrays)


def per_device(token_ids, lengths, teacher_bins, table, qkv_shard, out_shard, up_shard, down_shard, head_shard):
    up_grad, down_grad, head_grad, loss, out_buf, qkv_buf = step(
        lengths,
        teacher_bins,
        token_ids,
        table,
        jnp.transpose(qkv_shard, (1, 0, 2)),
        out_shard.T,
        up_shard,
        down_shard.T,
        head_shard,
    )
    up_grad, down_grad, head_grad, out_grad, qkv_grad = results(up_grad, down_grad, head_grad, out_buf, qkv_buf)
    return loss[0, 0], jnp.transpose(qkv_grad, (1, 0, 2)), out_grad.T, up_grad, down_grad.T, head_grad


def solution(mesh):
    fine = Mesh(mesh.devices.reshape(2, 4, 2, 4, 2), ("xl", "z", "c", "y", "xh"))
    dp, tensor = ("xl", "z", "c"), ("y", "xh")
    return jax.shard_map(
        per_device,
        mesh=fine,
        in_specs=(
            P(dp, tensor),
            P(dp),
            P(dp),
            P(tensor, None),
            P(dp, None, tensor),
            P(tensor, dp),
            P(dp, tensor),
            P(tensor, dp),
            P(dp, None),
        ),
        out_specs=(
            P(),
            P(dp, None, tensor),
            P(tensor, dp),
            P(dp, tensor),
            P(tensor, dp),
            P(dp, None),
        ),
        check_vma=False,
    )
```

```python
import functools
import types

import jax
import jax.numpy as jnp
from jax import lax
from jax.experimental import pallas as pl
from jax.experimental.pallas import tpu as pltpu
from jax.sharding import Mesh
from jax.sharding import PartitionSpec as P

MESH = pl.DeviceIdType.MESH
EPS = 1e-05
F32 = jnp.float32
BF16 = jnp.bfloat16
HIGH = lax.Precision.HIGHEST
VM = pl.BlockSpec(memory_space=pltpu.VMEM)
SM = pl.BlockSpec(memory_space=pltpu.SMEM)


def where_am_i():
    return {name: lax.axis_index(name) for name in ("xl", "z", "c", "y", "xh")}


def add_mod(value, step, size):
    return lax.rem(value + step, size)


def params(number, mebibytes):
    return pltpu.CompilerParams(
        collective_id=number, has_side_effects=True, vmem_limit_bytes=mebibytes * 2**20
    )


def remote(src, dst, send, recv, device):
    return pltpu.make_async_remote_copy(
        src_ref=src, dst_ref=dst, send_sem=send, recv_sem=recv, device_id=device, device_id_type=MESH
    )


def signal(device):
    pl.semaphore_signal(pltpu.get_barrier_semaphore(), inc=1, device_id=device, device_id_type=MESH)


def normalize(values):
    mean = jnp.mean(values, axis=-1, keepdims=True)
    centered = values - mean
    return centered * lax.rsqrt(jnp.mean(centered * centered, axis=-1, keepdims=True) + EPS)


def normalize_back(values, grad):
    mean = jnp.mean(values, axis=-1, keepdims=True)
    centered = values - mean
    scale = lax.rsqrt(jnp.mean(centered * centered, axis=-1, keepdims=True) + EPS)
    normed = centered * scale
    return scale * (
        grad
        - jnp.mean(grad, axis=-1, keepdims=True)
        - normed * jnp.mean(grad * normed, axis=-1, keepdims=True)
    )


class Ids:
    def __init__(self, src, out, send, recv):
        self.src, self.out, self.send, self.recv = src, out, send, recv
        self.me = where_am_i()
        self.here = self.me["xh"] == self.me["c"]

    def greet(self):
        me = self.me
        for role in range(2):
            for k in range(4):
                source = dict(
                    xl=add_mod(me["xl"], role, 2),
                    c=add_mod(me["xh"], role, 2),
                    xh=me["c"],
                    y=add_mod(me["y"], 4 - k, 4),
                    z=me["z"],
                )
                if role == 0 and k == 0:

                    @pl.when(jnp.logical_not(self.here))
                    def _(source=source):
                        signal(source)
                else:
                    signal(source)
        return jnp.where(self.here, 7, 8)

    def copy(self, role, k):
        me = self.me
        return remote(
            self.src,
            self.out.at[role, me["y"]],
            self.send.at[role, k],
            self.recv.at[role, k],
            dict(
                xl=add_mod(me["xl"], role, 2),
                c=me["xh"],
                xh=add_mod(me["c"], role, 2),
                y=add_mod(me["y"], k, 4),
                z=me["z"],
            ),
        )

    def local(self):
        return pltpu.make_async_copy(self.src, self.out.at[0, self.me["y"]], self.recv.at[0, 0])

    def start(self):
        for role in (1, 0):
            for k in (2, 1, 3, 0):
                if role == 0 and k == 0:

                    @pl.when(jnp.logical_not(self.here))
                    def _():
                        self.copy(0, 0).start()

                    @pl.when(self.here)
                    def _():
                        self.local().start()
                else:
                    self.copy(role, k).start()

    def arrive(self, role):
        for k in range(4):
            place = add_mod(self.me["y"], 4 - k, 4)
            pltpu.make_async_copy(self.src, self.out.at[role, place], self.recv.at[role, k]).wait()

    def sent(self):
        for role in range(2):
            for k in range(4):
                if role == 0 and k == 0:

                    @pl.when(jnp.logical_not(self.here))
                    def _():
                        self.copy(0, 0).wait_send()
                else:
                    self.copy(role, k).wait_send()


class Plane:
    def __init__(self, items, send, recv, collect):
        self.items, self.send, self.recv, self.collect = items, send, recv, collect
        self.me = where_am_i()
        c, xh = self.me["c"], self.me["xh"]
        self.here = xh == c
        self.mine, self.other = (xh, c) if collect else (c, xh)
        self.slot = (self.me["xl"] * 4 + self.me["z"]) * 2 + self.mine
        self.places = [(a, k, e) for k in (2, 1, 3, 0) for a in (1, 0) for e in range(2)]

    def target(self, a, k, e):
        me = self.me
        swapped = dict(c=e, xh=me["c"]) if self.collect else dict(c=me["xh"], xh=e)
        return dict(xl=add_mod(me["xl"], a, 2), z=add_mod(me["z"], k, 4), y=me["y"], **swapped)

    def origin(self, a, k, e):
        me = self.me
        swapped = dict(c=me["xh"], xh=e) if self.collect else dict(c=e, xh=me["c"])
        return dict(xl=add_mod(me["xl"], a, 2), z=add_mod(me["z"], 4 - k, 4), y=me["y"], **swapped)

    def number(self, a, k, e):
        return (add_mod(self.me["xl"], a, 2) * 4 + add_mod(self.me["z"], k, 4)) * 2 + e

    def greet(self):
        for a, k, e in self.places:
            if a == 0 and k == 0:

                @pl.when(jnp.logical_not(jnp.logical_and(self.here, e == self.mine)))
                def _(a=a, k=k, e=e):
                    signal(self.origin(a, k, e))
            else:
                signal(self.origin(a, k, e))
        return jnp.where(self.here, 15, 16)

    def start(self, i):
        block, place = self.items[i][:2]

        def copy(a, k, e):
            return remote(
                block(self.number(a, k, e)), place(self.slot), self.send.at[i], self.recv.at[i], self.target(a, k, e)
            )

        for a, k, e in self.places:
            if a == 0 and k == 0:
                is_self = jnp.logical_and(self.here, e == self.other)

                @pl.when(jnp.logical_not(is_self))
                def _(a=a, k=k, e=e):
                    copy(a, k, e).start()

                @pl.when(is_self)
                def _(a=a, k=k, e=e):
                    pltpu.make_async_copy(
                        block(self.number(a, k, e)), place(self.slot), self.recv.at[i]
                    ).start()
            else:
                copy(a, k, e).start()

    def arrive(self, i):
        whole = self.items[i][2]
        pltpu.make_async_copy(whole, whole, self.recv.at[i]).wait()

    def sent(self, i):
        whole, but_one = self.items[i][2:]

        @pl.when(self.here)
        def _():
            pltpu.make_async_copy(but_one, but_one, self.send.at[i]).wait()

        @pl.when(jnp.logical_not(self.here))
        def _():
            pltpu.make_async_copy(whole, whole, self.send.at[i]).wait()


def rows64(number):
    return pl.ds(pl.multiple_of(number * 64, 64), 64)


def spread_item(shard, target, cols=None):
    cols = pl.ds(0, target.shape[1]) if cols is None else cols
    return (
        lambda number: shard,
        lambda slot: target.at[rows64(slot), cols],
        target.at[:, cols],
        target.at[pl.ds(0, 960), cols],
    )


def collect_item(source, buf):
    return (
        lambda number: source.at[rows64(number)],
        lambda slot: buf.at[slot],
        buf,
        buf.at[pl.ds(0, 15)],
    )


def total_of(buf):
    total = buf[0].astype(F32)
    for s in range(1, 16):
        total = total + buf[s].astype(F32)
    return total


def thirds(row):
    high = row.astype(BF16).astype(F32)
    middle = (row - high).astype(BF16).astype(F32)
    low = row - high - middle
    index = lax.broadcasted_iota(jnp.int32, (8, row.shape[1]), 0)
    rows = jnp.where(index == 0, high, jnp.where(index == 1, middle, jnp.where(index == 2, low, 0.0)))
    return rows.astype(BF16)


def picked(values, start):
    rows = lax.broadcasted_iota(jnp.int32, (64, values.shape[1]), 0)
    cols = lax.broadcasted_iota(jnp.int32, (64, values.shape[1]), 1)
    chosen = (cols == rows + start).astype(F32)
    return lax.dot_general(chosen, values, RHS_T, precision=HIGH, preferred_element_type=F32)


def ring_places():
    me = where_am_i()
    y, c = me["y"], me["c"]
    return me, y, c, add_mod(y, 1, 4), add_mod(y, 3, 4), add_mod(y, 2, 4), 1 - c


class Owner:
    def __init__(self, blocks, stage, far, near, send, recv):
        self.blocks, self.stage, self.far, self.near = blocks, stage, far, near
        _, self.y, _, self.up, self.dn, op, _ = ring_places()
        self.ways = (self.up, self.dn)
        self.parts = (pl.ds(0, 32), pl.ds(32, 32))

        def go(k, source, target, side):
            return remote(source, target, send.at[k], recv.at[k], dict(y=self.ways[side]))

        self.first = [go(i, blocks(op).at[self.parts[i]], far.at[i], i) for i in range(2)]
        self.second = [
            go(2 + i, blocks(self.ways[i]).at[self.parts[1 - i]], near.at[i, self.parts[1 - i]], i)
            for i in range(2)
        ]
        self.third = [go(4 + i, stage.at[i], near.at[i, self.parts[i]], i) for i in range(2)]

    def begin(self):
        for step in self.first:
            step.start()

    def early(self, sides=(0, 1)):
        for i in sides:
            self.second[i].start()

    def relay(self):
        for i in range(2):
            self.first[i].wait_recv()
            mine = self.blocks(self.ways[i])[self.parts[i]]
            self.stage[i] = (mine.astype(F32) + self.far[i].astype(F32)).astype(BF16)
            self.third[i].start()

    def finish(self):
        for step in self.second + self.third:
            step.wait_recv()
        return self.blocks(self.y)[...].astype(F32) + self.near[0].astype(F32) + self.near[1].astype(F32)

    def sent(self):
        for step in self.first + self.second + self.third:
            step.wait_send()


class Gather:
    def __init__(self, out, chunk, send, recv):
        self.out, self.chunk, self.send, self.recv = out, chunk, send, recv
        _, y, c, up, dn, op, oc = ring_places()
        moves = [
            (y, c, None, dict(y=up)),
            (y, c, None, dict(y=dn)),
            (y, c, None, dict(c=oc)),
            (dn, c, 0, dict(y=up)),
            (dn, c, None, dict(c=oc)),
            (up, c, 1, dict(y=dn)),
            (up, c, None, dict(c=oc)),
            (op, c, 0, dict(c=oc)),
            (op, c, 1, dict(c=oc)),
        ]
        self.steps = []
        for k, (row, col, half, device) in enumerate(moves):
            start = (row * 2 + col) * 128 + chunk * 64
            if half is None:
                ref = out.at[pl.ds(pl.multiple_of(start, 64), 64)]
            else:
                ref = out.at[pl.ds(pl.multiple_of(start + half * 32, 32), 32)]
            self.steps.append(remote(ref, ref, send.at[k], recv.at[k], device))

    def begin(self):
        for k in (0, 1, 2):
            self.steps[k].start()

    def sides(self):
        self.steps[0].wait_recv()
        self.steps[3].start()
        self.steps[4].start()
        self.steps[1].wait_recv()
        self.steps[5].start()
        self.steps[6].start()

    def far(self):
        self.steps[3].wait_recv()
        self.steps[7].start()
        self.steps[5].wait_recv()
        self.steps[8].start()

    def pair_own(self):
        self.steps[2].wait_recv()

    def pair_sides(self):
        self.steps[4].wait_recv()
        self.steps[6].wait_recv()

    def pair_far(self):
        self.steps[7].wait_recv()
        self.steps[8].wait_recv()

    def sent(self):
        for step in self.steps:
            step.wait_send()


def gather_beside(gathers, block_work, last_work=None):
    _, y, c, up, dn, op, oc = ring_places()
    for g in gathers:
        g.pair_own()
    block_work(y)
    for g in gathers:
        g.sides()
    for g in gathers:
        g.pair_sides()
    block_work(up)
    for g in gathers:
        g.far()
    block_work(dn)
    for g in gathers:
        g.pair_far()
    (last_work or block_work)(op)


class PairOwner:
    def __init__(self, terms, r, name):
        self.terms = terms
        get = lambda part: getattr(r, name + part)
        _, y, self.c, self.up, self.dn, self.op, oc = ring_places()
        self.pair, self.summed = get("_pair"), get("_summed")
        self.order = (self.op, self.up, self.dn, y)
        self.steps = [
            remote(
                terms.at[self.rows(b, oc)], self.pair.at[b], get("_psend").at[i], get("_precv").at[i], dict(c=oc)
            )
            for i, b in enumerate(self.order)
        ]
        self.owners = [
            Owner(
                lambda b, ch=ch: self.summed.at[b, pl.ds(ch * 64, 64)],
                get("_stage").at[ch],
                get("_far").at[ch],
                get("_near").at[ch],
                get("_rsend").at[ch],
                get("_rrecv").at[ch],
            )
            for ch in range(2)
        ]

    def rows(self, b, c):
        return pl.ds(pl.multiple_of((b * 2 + c) * 128, 128), 128)

    def push(self, i):
        self.steps[i].start()

    def pull(self, i):
        b = self.order[i]
        self.steps[i].wait_recv()
        self.summed[b] = (self.terms[self.rows(b, self.c)].astype(F32) + self.pair[b].astype(F32)).astype(BF16)

    def sent(self):
        for step in self.steps:
            step.wait_send()
        for owner in self.owners:
            owner.sent()


def pair_owner_scratch(name):
    return {
        name + "_pair": pltpu.VMEM((4, 128, 1024), BF16),
        name + "_summed": pltpu.VMEM((4, 128, 1024), BF16),
        name + "_stage": pltpu.VMEM((2, 2, 32, 1024), BF16),
        name + "_far": pltpu.VMEM((2, 2, 32, 1024), BF16),
        name + "_near": pltpu.VMEM((2, 2, 64, 1024), BF16),
        name + "_psend": pltpu.SemaphoreType.DMA((4,)),
        name + "_precv": pltpu.SemaphoreType.DMA((4,)),
        name + "_rsend": pltpu.SemaphoreType.DMA((2, 6)),
        name + "_rrecv": pltpu.SemaphoreType.DMA((2, 6)),
        name + "_asend": pltpu.SemaphoreType.DMA((2, 9)),
        name + "_arecv": pltpu.SemaphoreType.DMA((2, 9)),
    }


SCALE = 0.125
PACKET = 512 + 1024 + 1024 + 128 + 128
LHS_T = (((0,), (0,)), ((), ()))
RHS_T = (((1,), (1,)), ((), ()))


def rows256(b):
    return pl.ds(pl.multiple_of(b * 256, 256), 256)


def of_head(value, head, axis):
    index = lax.broadcasted_iota(jnp.int32, value.shape, axis)
    return jnp.where((index >= 64) == (head == 1), value, jnp.zeros_like(value))


def step_kernel(names, *refs):
    r = types.SimpleNamespace(**dict(zip(names, refs, strict=True)))
    me, y, c, up, dn, op, oc = ring_places()
    slot = y * 2 + c
    vocab, padded = r.table.shape[0], r.shard.shape[0]

    fetch = pltpu.make_async_copy(r.table, r.shard.at[pl.ds(0, vocab)], r.load.at[0])
    fetch_ids = pltpu.make_async_copy(r.ids, r.ids_here, r.load.at[1])
    fetch_ids.start()
    fetch.start()
    tokens = Ids(r.packet_in, r.got, r.isend, r.irecv)
    spread = Plane(
        [spread_item(r.qkv_s.at[i], r.qkv_w, pl.ds(i * 128, 128)) for i in range(3)]
        + [
            spread_item(r.out_s, r.out_w),
            spread_item(r.up_s, r.up_w),
            spread_item(r.head_s, r.head_w),
            spread_item(r.down_s, r.down_w),
        ],
        r.ssend,
        r.srecv,
        False,
    )
    collect = Plane(
        [
            (lambda number: r.packet, lambda slot: r.packets.at[slot], r.packets, r.packets.at[pl.ds(0, 15)]),
            collect_item(r.up_term, r.up_buf),
            collect_item(r.out_term, r.out_buf),
        ]
        + [collect_item(r.qkv_term.at[i], r.qkv_buf.at[i]) for i in range(3)],
        r.csend,
        r.crecv,
        True,
    )
    partner = dict(xl=1 - me["xl"], xh=1 - me["xh"])
    peers = [(k, e) for k in (2, 1, 3, 0) for e in range(2) if (k, e) != (0, 0)]
    for device in (dict(y=up), dict(y=dn), dict(c=oc), partner):
        signal(device)
    for k, e in peers:
        signal(dict(y=add_mod(y, (4 - k) % 4, 4), c=add_mod(c, e, 2)))
    greeted = tokens.greet() + spread.greet() + collect.greet() + 11
    if padded > vocab:
        r.shard[vocab:padded] = jnp.zeros((padded - vocab, 1024), BF16)
    fetch_ids.wait()
    line = lax.broadcasted_iota(jnp.int32, (8, 128), 0)
    r.packet_in[...] = jnp.where(line == 0, r.ids_here[...], jnp.where(line == 1, r.count[0], r.label[0]))
    pl.semaphore_wait(pltpu.get_barrier_semaphore(), greeted)
    tokens.start()
    for i in range(3):
        spread.start(i)

    base = (y * 2 + me["xh"]) * vocab
    lanes = lax.broadcasted_iota(jnp.int32, (64, 128), 1)

    def look_up(role, ch):
        for b in range(4):
            wanted = jnp.broadcast_to(r.got[role, b, 0:1, :], (128, 128)).T[ch * 64 : ch * 64 + 64] - base
            for tile in range(padded // 128):
                r.chosen[b * 64 : b * 64 + 64, tile * 128 : tile * 128 + 128] = jnp.where(
                    wanted == lanes + tile * 128, 1.0, 0.0
                ).astype(BF16)
        if role == 1 and ch == 0:
            fetch.wait()
        for part in range(4):
            cols = slice(part * 256, part * 256 + 256)
            found = jnp.dot(r.chosen[...], r.shard[:, cols], preferred_element_type=F32).astype(BF16)
            for b in range(4):
                r.rows[role, ch, b, :, cols] = found[b * 64 : b * 64 + 64]

    own = {
        (role, ch): Owner(
            lambda b, role=role, ch=ch: r.rows.at[role, ch, b],
            r.e_stage.at[role, ch],
            r.e_far.at[role, ch],
            r.e_near.at[role, ch],
            r.e_rsend.at[role, ch],
            r.e_rrecv.at[role, ch],
        )
        for role in range(2)
        for ch in range(2)
    }
    cross = [
        remote(r.total.at[ch], r.theirs.at[ch], r.xsend.at[ch], r.xrecv.at[ch], partner) for ch in range(2)
    ]
    tokens.arrive(1)
    look_up(1, 0)
    own[1, 0].begin()
    own[1, 0].early()
    look_up(1, 1)
    own[1, 1].begin()
    own[1, 1].early()
    own[1, 0].relay()
    tokens.arrive(0)
    look_up(0, 0)
    own[0, 0].begin()
    own[0, 0].early()
    own[1, 1].relay()
    r.total[0] = own[1, 0].finish().astype(BF16)
    cross[0].start()
    look_up(0, 1)
    own[0, 1].begin()
    own[0, 1].early()
    own[0, 0].relay()
    r.total[1] = own[1, 1].finish().astype(BF16)
    cross[1].start()
    for i in range(3, 7):
        spread.start(i)
    own[0, 1].relay()
    length, label = r.got[0, 0, 1:2, 0:1], r.got[0, 0, 2:3, 0:1]
    gathers = [Gather(r.normed, ch, r.e_asend.at[ch], r.e_arecv.at[ch]) for ch in range(2)]
    first = []

    def own_rows(ch):
        return pl.ds(pl.multiple_of(slot * 128 + ch * 64, 64), 64)

    for ch in range(2):
        mine = own[0, ch].finish()
        cross[ch].wait_recv()
        value = mine + r.theirs[ch].astype(F32)
        first.append(value)
        r.normed[own_rows(ch)] = normalize(value).astype(BF16)
        gathers[ch].begin()
    for ch in range(2):
        r.first[ch * 64 : ch * 64 + 64] = first[ch]
    for i in range(3):
        spread.arrive(i)

    def project(b):
        r.qkv[rows256(b)] = jnp.dot(r.normed[rows256(b)], r.qkv_w[...], preferred_element_type=F32).astype(BF16)

    gather_beside(gathers, project)

    r.query_t[...] = (r.qkv[:, 0:128] * SCALE).T
    r.values_t[...] = r.qkv[:, 256:384].T
    spread.arrive(3)
    r.out_t[...] = r.out_w[...].T
    seen = lax.broadcasted_iota(jnp.int32, (1024, 256), 0) < length

    def attend(b, head):
        cols = rows256(b)
        scores = jnp.dot(r.qkv[:, 128:256], of_head(r.query_t[:, cols], head, 0), preferred_element_type=F32)
        scores = jnp.where(seen, scores, -1e30)
        expo = jnp.exp(scores - jnp.max(scores, axis=0, keepdims=True))
        probs = (expo * (1.0 / jnp.sum(expo, axis=0, keepdims=True))).astype(BF16)
        r.probs_t[head, :, cols] = probs
        rows = slice(head * 64, head * 64 + 64)
        r.context_t[rows, cols] = jnp.dot(r.values_t[rows], probs, preferred_element_type=F32).astype(BF16)

    def put_out(b):
        cols = rows256(b)
        r.terms[cols] = jnp.dot(r.context_t[:, cols].T, r.out_t[...], preferred_element_type=F32).astype(BF16)

    summed = PairOwner(r.terms, r, "a")
    for i, b in enumerate(summed.order):
        attend(b, 0)
        if i > 0:
            summed.pull(i - 1)
            for owner in summed.owners:
                if i == 1:
                    owner.begin()
                else:
                    owner.early((i - 2,))
        if i == 3:
            summed.owners[0].relay()
        attend(b, 1)
        put_out(b)
        summed.push(i)
    summed.owners[1].relay()
    summed.pull(3)
    more = [Gather(r.normed_two, ch, r.a_asend.at[ch], r.a_arecv.at[ch]) for ch in range(2)]
    for ch in range(2):
        second = (r.first[ch * 64 : ch * 64 + 64] + summed.owners[ch].finish()).astype(BF16)
        r.second[ch * 64 : ch * 64 + 64] = second
        r.normed_two[own_rows(ch)] = normalize(second.astype(F32)).astype(BF16)
        more[ch].begin()

    def live(start, size):
        return start + lax.broadcasted_iota(jnp.int32, (size, 1), 0) < length

    r.hidden_sum[...] = jnp.zeros((1, 512), F32)
    spread.arrive(4)

    def hidden_block(b):
        hidden = jnp.dot(r.normed_two[rows256(b)], r.up_w[...], preferred_element_type=F32)
        square = hidden * hidden
        inner = jnp.tanh(0.7978845608028654 * hidden * (1.0 + 0.044715 * square))
        half = 0.5 * (1.0 + inner)
        acted = (hidden * half).astype(BF16).astype(F32)
        r.slope[rows256(b)] = half + 0.5 * hidden * (1.0 - inner * inner) * (
            0.7978845608028654 + (0.7978845608028654 * 3.0 * 0.044715) * square
        )
        r.hidden_sum[...] += jnp.sum(jnp.where(live(b * 256, 256), acted, 0.0), axis=0, keepdims=True)

    gather_beside(more, hidden_block)

    spread.arrive(5)
    spread.arrive(6)
    hidden_sum = r.hidden_sum[...]
    own_sum = jnp.sum(jnp.where(live(slot * 128, 128), r.second[...].astype(F32), 0.0), axis=0, keepdims=True)
    pushed = lax.dot_general(thirds(hidden_sum), r.down_w[...], RHS_T, preferred_element_type=F32)
    r.parts[slot] = own_sum + jnp.sum(pushed, axis=0, keepdims=True)
    small = [
        remote(
            r.parts.at[slot],
            r.parts.at[slot],
            r.hsend.at[k, e],
            r.hrecv.at[k, e],
            dict(y=add_mod(y, k, 4), c=add_mod(c, e, 2)),
        )
        for k, e in peers
    ]
    for step in small:
        step.start()
    for step in small:
        step.wait()
    pooled = r.parts[0]
    for s in range(1, 8):
        pooled = pooled + r.parts[s]
    count = length.astype(F32)
    pooled = pooled / count
    final = normalize(pooled)
    logits = jnp.sum(jnp.dot(thirds(final), r.head_w[...], preferred_element_type=F32), axis=0, keepdims=True)
    top = jnp.max(logits, axis=-1, keepdims=True)
    total = jnp.log(jnp.sum(jnp.exp(logits - top), axis=-1, keepdims=True)) + top
    labels = (lax.broadcasted_iota(jnp.int32, logits.shape, 1) == label).astype(F32)
    loss = total - jnp.sum(logits * labels, axis=-1, keepdims=True)
    g_logits = (jnp.exp(logits - total) - labels) / 16.0
    g_final = lax.dot_general(thirds(g_logits), r.head_w[...], RHS_T, preferred_element_type=F32)
    per_token = normalize_back(pooled, jnp.sum(g_final, axis=0, keepdims=True)) / count
    rounded = per_token.astype(BF16)
    pulled = jnp.dot(rounded, r.down_w[...], preferred_element_type=F32)

    back = PairOwner(r.terms_back, r, "b")
    for i, b in enumerate(back.order):
        rows = rows256(b)
        grad = jnp.where(live(b * 256, 256), r.slope[rows] * pulled, 0.0).astype(BF16)
        r.g_pre[rows] = grad
        r.terms_back[rows] = lax.dot_general(
            grad, r.up_w[...], RHS_T, preferred_element_type=F32
        ).astype(BF16)
        back.push(i)
    back.pull(0)
    for owner in back.owners:
        owner.begin()
    for i in range(1, 4):
        back.pull(i)
        if i < 3:
            for owner in back.owners:
                owner.early((i - 1,))
    for block in range(4):
        cols = pl.ds(block * 256, 256)
        r.up_term[cols] = lax.dot_general(
            r.normed_two[:, cols], r.g_pre[...], LHS_T, preferred_element_type=F32
        ).astype(BF16)
    for owner in back.owners:
        owner.relay()
    r.packet[:, 0:512] = hidden_sum
    r.packet[:, 512:1536] = rounded.astype(F32)
    r.packet[:, 1536:2560] = final
    r.packet[:, 2560:2688] = g_logits
    r.packet[:, 2688:2816] = jnp.broadcast_to(loss, (1, 128))
    collect.start(1)
    collect.start(0)
    last = [Gather(r.g_second, ch, r.b_asend.at[ch], r.b_arecv.at[ch]) for ch in range(2)]
    for ch in range(2):
        grad = normalize_back(r.second[ch * 64 : ch * 64 + 64].astype(F32), back.owners[ch].finish())
        grad += jnp.where(live(slot * 128 + ch * 64, 64), per_token, 0.0)
        r.g_second[own_rows(ch)] = grad.astype(BF16)
        last[ch].begin()

    r.keys_t[...] = (r.qkv[:, 128:256] * SCALE).T
    r.grad_k[...] = jnp.zeros((1024, 128), F32)
    r.grad_v[...] = jnp.zeros((1024, 128), F32)

    def back_values(b):
        cols = rows256(b)
        g_context = jnp.dot(r.g_second[cols], r.out_w[...], preferred_element_type=F32)
        g_context_t = g_context.T
        g_context = g_context.astype(BF16)
        for head in range(2):
            r.grad_v[...] += jnp.dot(
                r.probs_t[head, :, cols], of_head(g_context, head, 1), preferred_element_type=F32
            )
        return g_context_t

    def back_scores(b, g_context_t):
        cols = rows256(b)
        product = g_context_t * r.context_t[:, cols].astype(F32)
        query = r.qkv[cols, 0:128] * SCALE
        for head in range(2):
            rows = slice(head * 64, head * 64 + 64)
            delta = jnp.sum(product[rows], axis=0, keepdims=True)
            moved = jnp.dot(
                r.qkv[:, 256:384], of_head(g_context_t, head, 0).astype(BF16), preferred_element_type=F32
            )
            g_scores = (r.probs_t[head, :, cols].astype(F32) * (moved - delta)).astype(BF16)
            r.grad_q[rows, cols] = jnp.dot(
                r.keys_t[rows], g_scores, preferred_element_type=F32
            ).astype(BF16)
            r.grad_k[...] += jnp.dot(g_scores, of_head(query, head, 1), preferred_element_type=F32)

    def send_term(piece, left):
        r.qkv_term[piece] = jnp.dot(left, r.normed[...], preferred_element_type=F32).T.astype(BF16)
        collect.start(3 + piece)

    def attend_back(b):
        back_scores(b, back_values(b))

    def attend_back_last(b):
        r.out_term[...] = jnp.dot(
            r.context_t[...], r.g_second[...], preferred_element_type=F32
        ).T.astype(BF16)
        collect.start(2)
        g_context_t = back_values(b)
        send_term(2, r.grad_v[...].T.astype(BF16))
        back_scores(b, g_context_t)
        send_term(0, r.grad_q[...])
        send_term(1, r.grad_k[...].T.astype(BF16))

    gather_beside(last, attend_back, attend_back_last)

    collect.arrive(0)
    begin = ((me["xl"] * 4 + me["z"]) * 2 + me["c"]) * 64
    packets = jnp.concatenate([r.packets[s] for s in range(16)], axis=0)
    r.down_grad[...] = jnp.dot(
        picked(packets[:, 512:1536], begin), packets[:, 0:512], precision=HIGH, preferred_element_type=F32
    )
    r.head_grad[...] = jnp.dot(
        picked(packets[:, 1536:2560], begin), packets[:, 2560:2688], precision=HIGH, preferred_element_type=F32
    )
    r.loss[...] = jnp.sum(packets[:, 2688:2816], axis=0, keepdims=True) / 16.0
    collect.arrive(1)
    r.up_grad[...] = total_of(r.up_buf)

    tokens.sent()
    for i in range(7):
        spread.sent(i)
    for owner in own.values():
        owner.sent()
    for step in cross:
        step.wait_send()
    for g in gathers + more + last:
        g.sent()
    summed.sent()
    back.sent()
    for i in range(6):
        collect.sent(i)
    for i in range(2, 6):
        collect.arrive(i)


HBM = pl.BlockSpec(memory_space=pltpu.HBM)


def step(count, label, ids, table, qkv_s, out_s, up_s, down_s, head_s):
    padded = -(-table.shape[0] // 256) * 256
    inputs = dict(
        count=SM, label=SM, ids=HBM, table=HBM, qkv_s=HBM, out_s=HBM, up_s=HBM, down_s=HBM, head_s=HBM
    )
    outputs = dict(
        up_grad=jax.ShapeDtypeStruct((64, 512), F32),
        down_grad=jax.ShapeDtypeStruct((64, 512), F32),
        head_grad=jax.ShapeDtypeStruct((64, 128), F32),
        loss=jax.ShapeDtypeStruct((1, 128), F32),
        out_buf=jax.ShapeDtypeStruct((16, 64, 128), BF16),
        qkv_buf=jax.ShapeDtypeStruct((3, 16, 64, 128), BF16),
    )
    dma = pltpu.SemaphoreType.DMA
    vm = pltpu.VMEM
    scratch = dict(
        load=dma((2,)),
        ids_here=vm((1, 128), jnp.int32),
        packet_in=vm((8, 128), jnp.int32),
        got=vm((2, 4, 8, 128), jnp.int32),
        isend=dma((2, 4)),
        irecv=dma((2, 4)),
        ssend=dma((7,)),
        srecv=dma((7,)),
        csend=dma((6,)),
        crecv=dma((6,)),
        shard=vm((padded, 1024), BF16),
        chosen=vm((256, padded), BF16),
        rows=vm((2, 2, 4, 64, 1024), BF16),
        e_stage=vm((2, 2, 2, 32, 1024), BF16),
        e_far=vm((2, 2, 2, 32, 1024), BF16),
        e_near=vm((2, 2, 2, 64, 1024), BF16),
        e_rsend=dma((2, 2, 6)),
        e_rrecv=dma((2, 2, 6)),
        e_asend=dma((2, 9)),
        e_arecv=dma((2, 9)),
        total=vm((2, 64, 1024), BF16),
        theirs=vm((2, 64, 1024), BF16),
        xsend=dma((2,)),
        xrecv=dma((2,)),
        first=vm((128, 1024), F32),
        normed=vm((1024, 1024), BF16),
        qkv_w=vm((1024, 384), BF16),
        out_w=vm((1024, 128), BF16),
        up_w=vm((1024, 512), BF16),
        down_w=vm((1024, 512), BF16),
        head_w=vm((1024, 128), BF16),
        qkv=vm((1024, 384), BF16),
        query_t=vm((128, 1024), BF16),
        values_t=vm((128, 1024), BF16),
        keys_t=vm((128, 1024), BF16),
        out_t=vm((128, 1024), BF16),
        probs_t=vm((2, 1024, 1024), BF16),
        context_t=vm((128, 1024), BF16),
        terms=vm((1024, 1024), BF16),
        **pair_owner_scratch("a"),
        second=vm((128, 1024), BF16),
        normed_two=vm((1024, 1024), BF16),
        hidden_sum=vm((1, 512), F32),
        slope=vm((1024, 512), F32),
        parts=vm((8, 1, 1024), F32),
        hsend=dma((4, 2)),
        hrecv=dma((4, 2)),
        g_pre=vm((1024, 512), BF16),
        terms_back=vm((1024, 1024), BF16),
        **pair_owner_scratch("b"),
        up_term=vm((1024, 512), BF16),
        up_buf=vm((16, 64, 512), BF16),
        packet=vm((1, PACKET), F32),
        packets=vm((16, 1, PACKET), F32),
        g_second=vm((1024, 1024), BF16),
        grad_q=vm((128, 1024), BF16),
        grad_k=vm((1024, 128), F32),
        grad_v=vm((1024, 128), F32),
        out_term=vm((1024, 128), BF16),
        qkv_term=vm((3, 1024, 128), BF16),
    )
    return pl.pallas_call(
        functools.partial(step_kernel, (*inputs, *outputs, *scratch)),
        out_shape=list(outputs.values()),
        in_specs=list(inputs.values()),
        out_specs=[VM] * len(outputs),
        scratch_shapes=list(scratch.values()),
        compiler_params=params(1, 54),
        name="step",
    )(count, label, ids, table, qkv_s, out_s, up_s, down_s, head_s)


def results_kernel(up, down, head, out_buf, qkv_buf, up_grad, down_grad, head_grad, out_grad, qkv_grad):
    up_grad[...] = up[...]
    down_grad[...] = down[...]
    head_grad[...] = head[...]
    out_grad[...] = total_of(out_buf)
    for i in range(3):
        qkv_grad[i] = total_of(qkv_buf.at[i])


def results(*arrays):
    return pl.pallas_call(
        results_kernel,
        out_shape=[
            jax.ShapeDtypeStruct((64, 512), F32),
            jax.ShapeDtypeStruct((64, 512), F32),
            jax.ShapeDtypeStruct((64, 128), F32),
            jax.ShapeDtypeStruct((64, 128), F32),
            jax.ShapeDtypeStruct((3, 64, 128), F32),
        ],
        in_specs=[VM] * 5,
        out_specs=[VM] * 5,
        compiler_params=pltpu.CompilerParams(vmem_limit_bytes=8 * 2**20),
        name="results",
    )(*arrays)


def per_device(token_ids, lengths, teacher_bins, table, qkv_shard, out_shard, up_shard, down_shard, head_shard):
    up_grad, down_grad, head_grad, loss, out_buf, qkv_buf = step(
        lengths,
        teacher_bins,
        token_ids,
        table,
        jnp.transpose(qkv_shard, (1, 0, 2)),
        out_shard.T,
        up_shard,
        down_shard.T,
        head_shard,
    )
    up_grad, down_grad, head_grad, out_grad, qkv_grad = results(up_grad, down_grad, head_grad, out_buf, qkv_buf)
    return loss[0, 0], jnp.transpose(qkv_grad, (1, 0, 2)), out_grad.T, up_grad, down_grad.T, head_grad


def solution(mesh):
    fine = Mesh(mesh.devices.reshape(2, 4, 2, 4, 2), ("xl", "z", "c", "y", "xh"))
    dp, tensor = ("xl", "z", "c"), ("y", "xh")
    return jax.shard_map(
        per_device,
        mesh=fine,
        in_specs=(
            P(dp, tensor),
            P(dp),
            P(dp),
            P(tensor, None),
            P(dp, None, tensor),
            P(tensor, dp),
            P(dp, tensor),
            P(tensor, dp),
            P(dp, None),
        ),
        out_specs=(
            P(),
            P(dp, None, tensor),
            P(tensor, dp),
            P(dp, tensor),
            P(tensor, dp),
            P(dp, None),
        ),
        check_vma=False,
    )
```

```python
import functools
import types

import jax
import jax.numpy as jnp
from jax import lax
from jax.experimental import pallas as pl
from jax.experimental.pallas import tpu as pltpu
from jax.sharding import Mesh
from jax.sharding import PartitionSpec as P

MESH = pl.DeviceIdType.MESH
EPS = 1e-05
F32 = jnp.float32
BF16 = jnp.bfloat16
HIGH = lax.Precision.HIGHEST
VM = pl.BlockSpec(memory_space=pltpu.VMEM)
SM = pl.BlockSpec(memory_space=pltpu.SMEM)


def where_am_i():
    return {name: lax.axis_index(name) for name in ("xl", "z", "c", "y", "xh")}


def add_mod(value, step, size):
    return lax.rem(value + step, size)


def params(number, mebibytes):
    return pltpu.CompilerParams(
        collective_id=number, has_side_effects=True, vmem_limit_bytes=mebibytes * 2**20
    )


def remote(src, dst, send, recv, device):
    return pltpu.make_async_remote_copy(
        src_ref=src, dst_ref=dst, send_sem=send, recv_sem=recv, device_id=device, device_id_type=MESH
    )


def signal(device):
    pl.semaphore_signal(pltpu.get_barrier_semaphore(), inc=1, device_id=device, device_id_type=MESH)


def normalize(values):
    mean = jnp.mean(values, axis=-1, keepdims=True)
    centered = values - mean
    return centered * lax.rsqrt(jnp.mean(centered * centered, axis=-1, keepdims=True) + EPS)


def normalize_back(values, grad):
    mean = jnp.mean(values, axis=-1, keepdims=True)
    centered = values - mean
    scale = lax.rsqrt(jnp.mean(centered * centered, axis=-1, keepdims=True) + EPS)
    normed = centered * scale
    return scale * (
        grad
        - jnp.mean(grad, axis=-1, keepdims=True)
        - normed * jnp.mean(grad * normed, axis=-1, keepdims=True)
    )


class Ids:
    def __init__(self, src, out, send, recv):
        self.src, self.out, self.send, self.recv = src, out, send, recv
        self.me = where_am_i()
        self.here = self.me["xh"] == self.me["c"]

    def greet(self):
        me = self.me
        for role in range(2):
            for k in range(4):
                source = dict(
                    xl=add_mod(me["xl"], role, 2),
                    c=add_mod(me["xh"], role, 2),
                    xh=me["c"],
                    y=add_mod(me["y"], 4 - k, 4),
                    z=me["z"],
                )
                if role == 0 and k == 0:

                    @pl.when(jnp.logical_not(self.here))
                    def _(source=source):
                        signal(source)
                else:
                    signal(source)
        return jnp.where(self.here, 7, 8)

    def copy(self, role, k):
        me = self.me
        return remote(
            self.src,
            self.out.at[role, me["y"]],
            self.send.at[role, k],
            self.recv.at[role, k],
            dict(
                xl=add_mod(me["xl"], role, 2),
                c=me["xh"],
                xh=add_mod(me["c"], role, 2),
                y=add_mod(me["y"], k, 4),
                z=me["z"],
            ),
        )

    def local(self):
        return pltpu.make_async_copy(self.src, self.out.at[0, self.me["y"]], self.recv.at[0, 0])

    def start(self):
        for role in (1, 0):
            for k in (2, 1, 3, 0):
                if role == 0 and k == 0:

                    @pl.when(jnp.logical_not(self.here))
                    def _():
                        self.copy(0, 0).start()

                    @pl.when(self.here)
                    def _():
                        self.local().start()
                else:
                    self.copy(role, k).start()

    def arrive(self, role):
        for k in range(4):
            place = add_mod(self.me["y"], 4 - k, 4)
            pltpu.make_async_copy(self.src, self.out.at[role, place], self.recv.at[role, k]).wait()

    def sent(self):
        for role in range(2):
            for k in range(4):
                if role == 0 and k == 0:

                    @pl.when(jnp.logical_not(self.here))
                    def _():
                        self.copy(0, 0).wait_send()
                else:
                    self.copy(role, k).wait_send()


class Plane:
    def __init__(self, items, send, recv, collect):
        self.items, self.send, self.recv, self.collect = items, send, recv, collect
        self.me = where_am_i()
        c, xh = self.me["c"], self.me["xh"]
        self.here = xh == c
        self.mine, self.other = (xh, c) if collect else (c, xh)
        self.slot = (self.me["xl"] * 4 + self.me["z"]) * 2 + self.mine
        self.places = [(a, k, e) for k in (2, 1, 3, 0) for a in (1, 0) for e in range(2)]

    def target(self, a, k, e):
        me = self.me
        swapped = dict(c=e, xh=me["c"]) if self.collect else dict(c=me["xh"], xh=e)
        return dict(xl=add_mod(me["xl"], a, 2), z=add_mod(me["z"], k, 4), y=me["y"], **swapped)

    def origin(self, a, k, e):
        me = self.me
        swapped = dict(c=me["xh"], xh=e) if self.collect else dict(c=e, xh=me["c"])
        return dict(xl=add_mod(me["xl"], a, 2), z=add_mod(me["z"], 4 - k, 4), y=me["y"], **swapped)

    def number(self, a, k, e):
        return (add_mod(self.me["xl"], a, 2) * 4 + add_mod(self.me["z"], k, 4)) * 2 + e

    def greet(self):
        for a, k, e in self.places:
            if a == 0 and k == 0:

                @pl.when(jnp.logical_not(jnp.logical_and(self.here, e == self.mine)))
                def _(a=a, k=k, e=e):
                    signal(self.origin(a, k, e))
            else:
                signal(self.origin(a, k, e))
        return jnp.where(self.here, 15, 16)

    def start(self, i):
        block, place = self.items[i][:2]

        def copy(a, k, e):
            return remote(
                block(self.number(a, k, e)), place(self.slot), self.send.at[i], self.recv.at[i], self.target(a, k, e)
            )

        for a, k, e in self.places:
            if a == 0 and k == 0:
                is_self = jnp.logical_and(self.here, e == self.other)

                @pl.when(jnp.logical_not(is_self))
                def _(a=a, k=k, e=e):
                    copy(a, k, e).start()

                @pl.when(is_self)
                def _(a=a, k=k, e=e):
                    pltpu.make_async_copy(
                        block(self.number(a, k, e)), place(self.slot), self.recv.at[i]
                    ).start()
            else:
                copy(a, k, e).start()

    def arrive(self, i):
        whole = self.items[i][2]
        pltpu.make_async_copy(whole, whole, self.recv.at[i]).wait()

    def sent(self, i):
        whole, but_one = self.items[i][2:]

        @pl.when(self.here)
        def _():
            pltpu.make_async_copy(but_one, but_one, self.send.at[i]).wait()

        @pl.when(jnp.logical_not(self.here))
        def _():
            pltpu.make_async_copy(whole, whole, self.send.at[i]).wait()


def rows64(number):
    return pl.ds(pl.multiple_of(number * 64, 64), 64)


def spread_item(shard, target, cols=None):
    cols = pl.ds(0, target.shape[1]) if cols is None else cols
    return (
        lambda number: shard,
        lambda slot: target.at[rows64(slot), cols],
        target.at[:, cols],
        target.at[pl.ds(0, 960), cols],
    )


def collect_item(source, buf):
    return (
        lambda number: source.at[rows64(number)],
        lambda slot: buf.at[slot],
        buf,
        buf.at[pl.ds(0, 15)],
    )


def total_of(buf):
    total = buf[0].astype(F32)
    for s in range(1, 16):
        total = total + buf[s].astype(F32)
    return total


def thirds(row):
    high = row.astype(BF16).astype(F32)
    middle = (row - high).astype(BF16).astype(F32)
    low = row - high - middle
    index = lax.broadcasted_iota(jnp.int32, (8, row.shape[1]), 0)
    rows = jnp.where(index == 0, high, jnp.where(index == 1, middle, jnp.where(index == 2, low, 0.0)))
    return rows.astype(BF16)


def picked(values, start):
    rows = lax.broadcasted_iota(jnp.int32, (64, values.shape[1]), 0)
    cols = lax.broadcasted_iota(jnp.int32, (64, values.shape[1]), 1)
    chosen = (cols == rows + start).astype(F32)
    return lax.dot_general(chosen, values, RHS_T, precision=HIGH, preferred_element_type=F32)


def ring_places():
    me = where_am_i()
    y, c = me["y"], me["c"]
    return me, y, c, add_mod(y, 1, 4), add_mod(y, 3, 4), add_mod(y, 2, 4), 1 - c


class Owner:
    def __init__(self, blocks, stage, far, near, send, recv):
        self.blocks, self.stage, self.far, self.near = blocks, stage, far, near
        _, self.y, _, self.up, self.dn, op, _ = ring_places()
        self.ways = (self.up, self.dn)
        self.parts = (pl.ds(0, 32), pl.ds(32, 32))

        def go(k, source, target, side):
            return remote(source, target, send.at[k], recv.at[k], dict(y=self.ways[side]))

        self.first = [go(i, blocks(op).at[self.parts[i]], far.at[i], i) for i in range(2)]
        self.second = [
            go(2 + i, blocks(self.ways[i]).at[self.parts[1 - i]], near.at[i, self.parts[1 - i]], i)
            for i in range(2)
        ]
        self.third = [go(4 + i, stage.at[i], near.at[i, self.parts[i]], i) for i in range(2)]

    def begin(self):
        for step in self.first:
            step.start()

    def early(self, sides=(0, 1)):
        for i in sides:
            self.second[i].start()

    def relay(self):
        for i in range(2):
            self.first[i].wait_recv()
            mine = self.blocks(self.ways[i])[self.parts[i]]
            self.stage[i] = (mine.astype(F32) + self.far[i].astype(F32)).astype(BF16)
            self.third[i].start()

    def finish(self):
        for step in self.second + self.third:
            step.wait_recv()
        return self.blocks(self.y)[...].astype(F32) + self.near[0].astype(F32) + self.near[1].astype(F32)

    def sent(self):
        for step in self.first + self.second + self.third:
            step.wait_send()


class Gather:
    def __init__(self, out, chunk, send, recv):
        self.out, self.chunk, self.send, self.recv = out, chunk, send, recv
        _, y, c, up, dn, op, oc = ring_places()
        moves = [
            (y, c, None, dict(y=up)),
            (y, c, None, dict(y=dn)),
            (y, c, None, dict(c=oc)),
            (dn, c, 0, dict(y=up)),
            (dn, c, None, dict(c=oc)),
            (up, c, 1, dict(y=dn)),
            (up, c, None, dict(c=oc)),
            (op, c, 0, dict(c=oc)),
            (op, c, 1, dict(c=oc)),
        ]
        self.steps = []
        for k, (row, col, half, device) in enumerate(moves):
            start = (row * 2 + col) * 128 + chunk * 64
            if half is None:
                ref = out.at[pl.ds(pl.multiple_of(start, 64), 64)]
            else:
                ref = out.at[pl.ds(pl.multiple_of(start + half * 32, 32), 32)]
            self.steps.append(remote(ref, ref, send.at[k], recv.at[k], device))

    def begin(self):
        for k in (0, 1, 2):
            self.steps[k].start()

    def sides(self):
        self.steps[0].wait_recv()
        self.steps[3].start()
        self.steps[4].start()
        self.steps[1].wait_recv()
        self.steps[5].start()
        self.steps[6].start()

    def far(self):
        self.steps[3].wait_recv()
        self.steps[7].start()
        self.steps[5].wait_recv()
        self.steps[8].start()

    def pair_own(self):
        self.steps[2].wait_recv()

    def pair_sides(self):
        self.steps[4].wait_recv()
        self.steps[6].wait_recv()

    def pair_far(self):
        self.steps[7].wait_recv()
        self.steps[8].wait_recv()

    def sent(self):
        for step in self.steps:
            step.wait_send()


def gather_beside(gathers, block_work, last_work=None, after_sides=None):
    _, y, c, up, dn, op, oc = ring_places()
    for g in gathers:
        g.pair_own()
    block_work(y)
    for g in gathers:
        g.sides()
    if after_sides is not None:
        after_sides()
    for g in gathers:
        g.pair_sides()
    block_work(up)
    for g in gathers:
        g.far()
    block_work(dn)
    for g in gathers:
        g.pair_far()
    (last_work or block_work)(op)


class PairOwner:
    def __init__(self, terms, r, name):
        self.terms = terms
        get = lambda part: getattr(r, name + part)
        _, y, self.c, self.up, self.dn, self.op, oc = ring_places()
        self.pair, self.summed = get("_pair"), get("_summed")
        self.order = (self.op, self.up, self.dn, y)
        self.steps = [
            remote(
                terms.at[self.rows(b, oc)], self.pair.at[b], get("_psend").at[i], get("_precv").at[i], dict(c=oc)
            )
            for i, b in enumerate(self.order)
        ]
        self.owners = [
            Owner(
                lambda b, ch=ch: self.summed.at[b, pl.ds(ch * 64, 64)],
                get("_stage").at[ch],
                get("_far").at[ch],
                get("_near").at[ch],
                get("_rsend").at[ch],
                get("_rrecv").at[ch],
            )
            for ch in range(2)
        ]

    def rows(self, b, c):
        return pl.ds(pl.multiple_of((b * 2 + c) * 128, 128), 128)

    def push(self, i):
        self.steps[i].start()

    def pull(self, i):
        b = self.order[i]
        self.steps[i].wait_recv()
        self.summed[b] = (self.terms[self.rows(b, self.c)].astype(F32) + self.pair[b].astype(F32)).astype(BF16)

    def sent(self):
        for step in self.steps:
            step.wait_send()
        for owner in self.owners:
            owner.sent()


def pair_owner_scratch(name):
    return {
        name + "_pair": pltpu.VMEM((4, 128, 1024), BF16),
        name + "_summed": pltpu.VMEM((4, 128, 1024), BF16),
        name + "_stage": pltpu.VMEM((2, 2, 32, 1024), BF16),
        name + "_far": pltpu.VMEM((2, 2, 32, 1024), BF16),
        name + "_near": pltpu.VMEM((2, 2, 64, 1024), BF16),
        name + "_psend": pltpu.SemaphoreType.DMA((4,)),
        name + "_precv": pltpu.SemaphoreType.DMA((4,)),
        name + "_rsend": pltpu.SemaphoreType.DMA((2, 6)),
        name + "_rrecv": pltpu.SemaphoreType.DMA((2, 6)),
        name + "_asend": pltpu.SemaphoreType.DMA((2, 9)),
        name + "_arecv": pltpu.SemaphoreType.DMA((2, 9)),
    }


SCALE = 0.125
PACKET = 512 + 1024 + 1024 + 128 + 128
LHS_T = (((0,), (0,)), ((), ()))
RHS_T = (((1,), (1,)), ((), ()))


def rows256(b):
    return pl.ds(pl.multiple_of(b * 256, 256), 256)


def of_head(value, head, axis):
    index = lax.broadcasted_iota(jnp.int32, value.shape, axis)
    return jnp.where((index >= 64) == (head == 1), value, jnp.zeros_like(value))


def step_kernel(names, *refs):
    r = types.SimpleNamespace(**dict(zip(names, refs, strict=True)))
    me, y, c, up, dn, op, oc = ring_places()
    slot = y * 2 + c
    vocab, padded = r.table.shape[0], r.shard.shape[0]

    fetch = pltpu.make_async_copy(r.table, r.shard.at[pl.ds(0, vocab)], r.load.at[0])
    fetch_ids = pltpu.make_async_copy(r.ids, r.ids_here, r.load.at[1])
    fetch_ids.start()
    fetch.start()
    tokens = Ids(r.packet_in, r.got, r.isend, r.irecv)
    spread = Plane(
        [spread_item(r.qkv_s.at[i], r.qkv_w, pl.ds(i * 128, 128)) for i in range(3)]
        + [
            spread_item(r.out_s, r.out_w),
            spread_item(r.up_s, r.up_w),
            spread_item(r.head_s, r.head_w),
            spread_item(r.down_s, r.down_w),
        ],
        r.ssend,
        r.srecv,
        False,
    )
    collect = Plane(
        [
            (lambda number: r.packet, lambda slot: r.packets.at[slot], r.packets, r.packets.at[pl.ds(0, 15)]),
            collect_item(r.up_term, r.up_buf),
            collect_item(r.out_term, r.out_buf),
        ]
        + [collect_item(r.qkv_term.at[i], r.qkv_buf.at[i]) for i in range(3)],
        r.csend,
        r.crecv,
        True,
    )
    partner = dict(xl=1 - me["xl"], xh=1 - me["xh"])
    peers = [(k, e) for k in (2, 1, 3, 0) for e in range(2) if (k, e) != (0, 0)]
    for device in (dict(y=up), dict(y=dn), dict(c=oc), partner):
        signal(device)
    for k, e in peers:
        signal(dict(y=add_mod(y, (4 - k) % 4, 4), c=add_mod(c, e, 2)))
    greeted = tokens.greet() + spread.greet() + collect.greet() + 11
    if padded > vocab:
        r.shard[vocab:padded] = jnp.zeros((padded - vocab, 1024), BF16)
    fetch_ids.wait()
    line = lax.broadcasted_iota(jnp.int32, (8, 128), 0)
    r.packet_in[...] = jnp.where(line == 0, r.ids_here[...], jnp.where(line == 1, r.count[0], r.label[0]))
    pl.semaphore_wait(pltpu.get_barrier_semaphore(), greeted)
    tokens.start()
    for i in range(3):
        spread.start(i)

    base = (y * 2 + me["xh"]) * vocab
    lanes = lax.broadcasted_iota(jnp.int32, (64, 128), 1)

    def look_up(role, ch):
        for b in range(4):
            wanted = jnp.broadcast_to(r.got[role, b, 0:1, :], (128, 128)).T[ch * 64 : ch * 64 + 64] - base
            for tile in range(padded // 128):
                r.chosen[b * 64 : b * 64 + 64, tile * 128 : tile * 128 + 128] = jnp.where(
                    wanted == lanes + tile * 128, 1.0, 0.0
                ).astype(BF16)
        if role == 1 and ch == 0:
            fetch.wait()
        for part in range(4):
            cols = slice(part * 256, part * 256 + 256)
            found = jnp.dot(r.chosen[...], r.shard[:, cols], preferred_element_type=F32).astype(BF16)
            for b in range(4):
                r.rows[role, ch, b, :, cols] = found[b * 64 : b * 64 + 64]

    own = {
        (role, ch): Owner(
            lambda b, role=role, ch=ch: r.rows.at[role, ch, b],
            r.e_stage.at[role, ch],
            r.e_far.at[role, ch],
            r.e_near.at[role, ch],
            r.e_rsend.at[role, ch],
            r.e_rrecv.at[role, ch],
        )
        for role in range(2)
        for ch in range(2)
    }
    cross = [
        remote(r.total.at[ch], r.theirs.at[ch], r.xsend.at[ch], r.xrecv.at[ch], partner) for ch in range(2)
    ]
    tokens.arrive(1)
    look_up(1, 0)
    own[1, 0].begin()
    own[1, 0].early()
    look_up(1, 1)
    own[1, 1].begin()
    own[1, 1].early()
    own[1, 0].relay()
    tokens.arrive(0)
    look_up(0, 0)
    own[0, 0].begin()
    own[0, 0].early()
    own[1, 1].relay()
    r.total[0] = own[1, 0].finish().astype(BF16)
    cross[0].start()
    look_up(0, 1)
    own[0, 1].begin()
    own[0, 1].early()
    own[0, 0].relay()
    r.total[1] = own[1, 1].finish().astype(BF16)
    cross[1].start()
    for i in range(3, 7):
        spread.start(i)
    own[0, 1].relay()
    length, label = r.got[0, 0, 1:2, 0:1], r.got[0, 0, 2:3, 0:1]
    gathers = [Gather(r.normed, ch, r.e_asend.at[ch], r.e_arecv.at[ch]) for ch in range(2)]
    first = []

    def own_rows(ch):
        return pl.ds(pl.multiple_of(slot * 128 + ch * 64, 64), 64)

    for ch in range(2):
        mine = own[0, ch].finish()
        cross[ch].wait_recv()
        value = mine + r.theirs[ch].astype(F32)
        first.append(value)
        r.normed[own_rows(ch)] = normalize(value).astype(BF16)
        gathers[ch].begin()
    for ch in range(2):
        r.first[ch * 64 : ch * 64 + 64] = first[ch]
    for i in range(3):
        spread.arrive(i)

    def project(b):
        r.qkv[rows256(b)] = jnp.dot(r.normed[rows256(b)], r.qkv_w[...], preferred_element_type=F32).astype(BF16)

    wide = [Gather(r.out_full, ch, r.wsend.at[ch], r.wrecv.at[ch]) for ch in range(2)]

    def widen():
        spread.arrive(3)
        r.out_full[pl.ds(pl.multiple_of(slot * 128, 128), 128)] = r.out_w[...].T
        for g in wide:
            g.begin()

    gather_beside(gathers, project, after_sides=widen)

    r.query_t[...] = (r.qkv[:, 0:128] * SCALE).T
    r.values_t[...] = r.qkv[:, 256:384].T
    seen = lax.broadcasted_iota(jnp.int32, (1024, 256), 0) < length

    def attend(b, head):
        cols = rows256(b)
        scores = jnp.dot(r.qkv[:, 128:256], of_head(r.query_t[:, cols], head, 0), preferred_element_type=F32)
        scores = jnp.where(seen, scores, -1e30)
        expo = jnp.exp(scores - jnp.max(scores, axis=0, keepdims=True))
        probs = (expo * (1.0 / jnp.sum(expo, axis=0, keepdims=True))).astype(BF16)
        r.probs_t[head, :, cols] = probs
        rows = slice(head * 64, head * 64 + 64)
        r.context_t[rows, cols] = jnp.dot(r.values_t[rows], probs, preferred_element_type=F32).astype(BF16)

    order = (op, up, dn, y)
    here128 = pl.ds(pl.multiple_of(slot * 128, 128), 128)

    def piece(i, e):
        return r.context.at[pl.ds(pl.multiple_of((order[i] * 2 + add_mod(c, e, 2)) * 128, 128), 128)]

    pieces = {
        (i, e): remote(
            piece(i, e),
            r.context_own.at[:, here128],
            r.tsend.at[i, e],
            r.trecv.at[i, e],
            dict(y=order[i], c=add_mod(c, e, 2)),
        )
        for i in range(4)
        for e in range(2)
        if (i, e) != (3, 0)
    }

    def hand_over(i):
        r.context[rows256(order[i])] = r.context_t[:, rows256(order[i])].T
        for e in range(2):
            if (i, e) in pieces:
                pieces[i, e].start()
            else:
                r.context_own[:, here128] = r.context[here128]

    for i, b in enumerate(order):
        attend(b, 0)
        attend(b, 1)
        hand_over(i)
        if i == 1:
            for g in wide:
                g.sides()
        if i == 2:
            for g in wide:
                g.far()
    for step in pieces.values():
        step.wait_recv()
    for g in wide:
        g.pair_own()
        g.pair_sides()
        g.pair_far()
    attn = jnp.dot(r.context_own[...], r.out_full[...], preferred_element_type=F32)
    more = [Gather(r.normed_two, ch, r.a_asend.at[ch], r.a_arecv.at[ch]) for ch in range(2)]
    for ch in range(2):
        second = (r.first[ch * 64 : ch * 64 + 64] + attn[ch * 64 : ch * 64 + 64]).astype(BF16)
        r.second[ch * 64 : ch * 64 + 64] = second
        r.normed_two[own_rows(ch)] = normalize(second.astype(F32)).astype(BF16)
        more[ch].begin()

    def live(start, size):
        return start + lax.broadcasted_iota(jnp.int32, (size, 1), 0) < length

    r.hidden_sum[...] = jnp.zeros((1, 512), F32)
    spread.arrive(4)

    def hidden_block(b):
        hidden = jnp.dot(r.normed_two[rows256(b)], r.up_w[...], preferred_element_type=F32)
        square = hidden * hidden
        inner = jnp.tanh(0.7978845608028654 * hidden * (1.0 + 0.044715 * square))
        half = 0.5 * (1.0 + inner)
        acted = (hidden * half).astype(BF16).astype(F32)
        r.slope[rows256(b)] = half + 0.5 * hidden * (1.0 - inner * inner) * (
            0.7978845608028654 + (0.7978845608028654 * 3.0 * 0.044715) * square
        )
        r.hidden_sum[...] += jnp.sum(jnp.where(live(b * 256, 256), acted, 0.0), axis=0, keepdims=True)

    gather_beside(more, hidden_block)

    spread.arrive(5)
    spread.arrive(6)
    hidden_sum = r.hidden_sum[...]
    own_sum = jnp.sum(jnp.where(live(slot * 128, 128), r.second[...].astype(F32), 0.0), axis=0, keepdims=True)
    pushed = lax.dot_general(thirds(hidden_sum), r.down_w[...], RHS_T, preferred_element_type=F32)
    r.parts[slot] = own_sum + jnp.sum(pushed, axis=0, keepdims=True)
    small = [
        remote(
            r.parts.at[slot],
            r.parts.at[slot],
            r.hsend.at[k, e],
            r.hrecv.at[k, e],
            dict(y=add_mod(y, k, 4), c=add_mod(c, e, 2)),
        )
        for k, e in peers
    ]
    for step in small:
        step.start()
    for step in small:
        step.wait()
    pooled = r.parts[0]
    for s in range(1, 8):
        pooled = pooled + r.parts[s]
    count = length.astype(F32)
    pooled = pooled / count
    final = normalize(pooled)
    logits = jnp.sum(jnp.dot(thirds(final), r.head_w[...], preferred_element_type=F32), axis=0, keepdims=True)
    top = jnp.max(logits, axis=-1, keepdims=True)
    total = jnp.log(jnp.sum(jnp.exp(logits - top), axis=-1, keepdims=True)) + top
    labels = (lax.broadcasted_iota(jnp.int32, logits.shape, 1) == label).astype(F32)
    loss = total - jnp.sum(logits * labels, axis=-1, keepdims=True)
    g_logits = (jnp.exp(logits - total) - labels) / 16.0
    g_final = lax.dot_general(thirds(g_logits), r.head_w[...], RHS_T, preferred_element_type=F32)
    per_token = normalize_back(pooled, jnp.sum(g_final, axis=0, keepdims=True)) / count
    rounded = per_token.astype(BF16)
    pulled = jnp.dot(rounded, r.down_w[...], preferred_element_type=F32)

    back = PairOwner(r.terms_back, r, "b")
    for i, b in enumerate(back.order):
        rows = rows256(b)
        grad = jnp.where(live(b * 256, 256), r.slope[rows] * pulled, 0.0).astype(BF16)
        r.g_pre[rows] = grad
        r.terms_back[rows] = lax.dot_general(
            grad, r.up_w[...], RHS_T, preferred_element_type=F32
        ).astype(BF16)
        back.push(i)
    back.pull(0)
    for owner in back.owners:
        owner.begin()
    for i in range(1, 4):
        back.pull(i)
        if i < 3:
            for owner in back.owners:
                owner.early((i - 1,))
    for block in range(4):
        cols = pl.ds(block * 256, 256)
        r.up_term[cols] = lax.dot_general(
            r.normed_two[:, cols], r.g_pre[...], LHS_T, preferred_element_type=F32
        ).astype(BF16)
    for owner in back.owners:
        owner.relay()
    r.packet[:, 0:512] = hidden_sum
    r.packet[:, 512:1536] = rounded.astype(F32)
    r.packet[:, 1536:2560] = final
    r.packet[:, 2560:2688] = g_logits
    r.packet[:, 2688:2816] = jnp.broadcast_to(loss, (1, 128))
    collect.start(1)
    collect.start(0)
    last = [Gather(r.g_second, ch, r.b_asend.at[ch], r.b_arecv.at[ch]) for ch in range(2)]
    for ch in range(2):
        grad = normalize_back(r.second[ch * 64 : ch * 64 + 64].astype(F32), back.owners[ch].finish())
        grad += jnp.where(live(slot * 128 + ch * 64, 64), per_token, 0.0)
        r.g_second[own_rows(ch)] = grad.astype(BF16)
        last[ch].begin()

    r.keys_t[...] = (r.qkv[:, 128:256] * SCALE).T
    r.grad_k[...] = jnp.zeros((1024, 128), F32)
    r.grad_v[...] = jnp.zeros((1024, 128), F32)

    def back_values(b):
        cols = rows256(b)
        g_context = jnp.dot(r.g_second[cols], r.out_w[...], preferred_element_type=F32)
        g_context_t = g_context.T
        g_context = g_context.astype(BF16)
        for head in range(2):
            r.grad_v[...] += jnp.dot(
                r.probs_t[head, :, cols], of_head(g_context, head, 1), preferred_element_type=F32
            )
        return g_context_t

    def back_scores(b, g_context_t):
        cols = rows256(b)
        product = g_context_t * r.context_t[:, cols].astype(F32)
        query = r.qkv[cols, 0:128] * SCALE
        for head in range(2):
            rows = slice(head * 64, head * 64 + 64)
            delta = jnp.sum(product[rows], axis=0, keepdims=True)
            moved = jnp.dot(
                r.qkv[:, 256:384], of_head(g_context_t, head, 0).astype(BF16), preferred_element_type=F32
            )
            g_scores = (r.probs_t[head, :, cols].astype(F32) * (moved - delta)).astype(BF16)
            r.grad_q[rows, cols] = jnp.dot(
                r.keys_t[rows], g_scores, preferred_element_type=F32
            ).astype(BF16)
            r.grad_k[...] += jnp.dot(g_scores, of_head(query, head, 1), preferred_element_type=F32)

    def send_term(piece, left):
        r.qkv_term[piece] = jnp.dot(left, r.normed[...], preferred_element_type=F32).T.astype(BF16)
        collect.start(3 + piece)

    def attend_back(b):
        back_scores(b, back_values(b))

    def attend_back_last(b):
        r.out_term[...] = jnp.dot(
            r.context_t[...], r.g_second[...], preferred_element_type=F32
        ).T.astype(BF16)
        collect.start(2)
        g_context_t = back_values(b)
        send_term(2, r.grad_v[...].T.astype(BF16))
        back_scores(b, g_context_t)
        send_term(0, r.grad_q[...])
        send_term(1, r.grad_k[...].T.astype(BF16))

    gather_beside(last, attend_back, attend_back_last)

    collect.arrive(0)
    begin = ((me["xl"] * 4 + me["z"]) * 2 + me["c"]) * 64
    packets = jnp.concatenate([r.packets[s] for s in range(16)], axis=0)
    r.down_grad[...] = jnp.dot(
        picked(packets[:, 512:1536], begin), packets[:, 0:512], precision=HIGH, preferred_element_type=F32
    )
    r.head_grad[...] = jnp.dot(
        picked(packets[:, 1536:2560], begin), packets[:, 2560:2688], precision=HIGH, preferred_element_type=F32
    )
    r.loss[...] = jnp.sum(packets[:, 2688:2816], axis=0, keepdims=True) / 16.0
    collect.arrive(1)
    r.up_grad[...] = total_of(r.up_buf)

    tokens.sent()
    for i in range(7):
        spread.sent(i)
    for owner in own.values():
        owner.sent()
    for step in cross:
        step.wait_send()
    for g in gathers + wide + more + last:
        g.sent()
    for step in pieces.values():
        step.wait_send()
    back.sent()
    for i in range(6):
        collect.sent(i)
    for i in range(2, 6):
        collect.arrive(i)


HBM = pl.BlockSpec(memory_space=pltpu.HBM)


def step(count, label, ids, table, qkv_s, out_s, up_s, down_s, head_s):
    padded = -(-table.shape[0] // 256) * 256
    inputs = dict(
        count=SM, label=SM, ids=HBM, table=HBM, qkv_s=HBM, out_s=HBM, up_s=HBM, down_s=HBM, head_s=HBM
    )
    outputs = dict(
        up_grad=jax.ShapeDtypeStruct((64, 512), F32),
        down_grad=jax.ShapeDtypeStruct((64, 512), F32),
        head_grad=jax.ShapeDtypeStruct((64, 128), F32),
        loss=jax.ShapeDtypeStruct((1, 128), F32),
        out_buf=jax.ShapeDtypeStruct((16, 64, 128), BF16),
        qkv_buf=jax.ShapeDtypeStruct((3, 16, 64, 128), BF16),
    )
    dma = pltpu.SemaphoreType.DMA
    vm = pltpu.VMEM
    scratch = dict(
        load=dma((2,)),
        ids_here=vm((1, 128), jnp.int32),
        packet_in=vm((8, 128), jnp.int32),
        got=vm((2, 4, 8, 128), jnp.int32),
        isend=dma((2, 4)),
        irecv=dma((2, 4)),
        ssend=dma((7,)),
        srecv=dma((7,)),
        csend=dma((6,)),
        crecv=dma((6,)),
        shard=vm((padded, 1024), BF16),
        chosen=vm((256, padded), BF16),
        rows=vm((2, 2, 4, 64, 1024), BF16),
        e_stage=vm((2, 2, 2, 32, 1024), BF16),
        e_far=vm((2, 2, 2, 32, 1024), BF16),
        e_near=vm((2, 2, 2, 64, 1024), BF16),
        e_rsend=dma((2, 2, 6)),
        e_rrecv=dma((2, 2, 6)),
        e_asend=dma((2, 9)),
        e_arecv=dma((2, 9)),
        total=vm((2, 64, 1024), BF16),
        theirs=vm((2, 64, 1024), BF16),
        xsend=dma((2,)),
        xrecv=dma((2,)),
        first=vm((128, 1024), F32),
        normed=vm((1024, 1024), BF16),
        qkv_w=vm((1024, 384), BF16),
        out_w=vm((1024, 128), BF16),
        up_w=vm((1024, 512), BF16),
        down_w=vm((1024, 512), BF16),
        head_w=vm((1024, 128), BF16),
        qkv=vm((1024, 384), BF16),
        query_t=vm((128, 1024), BF16),
        values_t=vm((128, 1024), BF16),
        keys_t=vm((128, 1024), BF16),
        out_full=vm((1024, 1024), BF16),
        wsend=dma((2, 9)),
        wrecv=dma((2, 9)),
        context=vm((1024, 128), BF16),
        context_own=vm((128, 1024), BF16),
        tsend=dma((4, 2)),
        trecv=dma((4, 2)),
        a_asend=dma((2, 9)),
        a_arecv=dma((2, 9)),
        probs_t=vm((2, 1024, 1024), BF16),
        context_t=vm((128, 1024), BF16),
        second=vm((128, 1024), BF16),
        normed_two=vm((1024, 1024), BF16),
        hidden_sum=vm((1, 512), F32),
        slope=vm((1024, 512), F32),
        parts=vm((8, 1, 1024), F32),
        hsend=dma((4, 2)),
        hrecv=dma((4, 2)),
        g_pre=vm((1024, 512), BF16),
        terms_back=vm((1024, 1024), BF16),
        **pair_owner_scratch("b"),
        up_term=vm((1024, 512), BF16),
        up_buf=vm((16, 64, 512), BF16),
        packet=vm((1, PACKET), F32),
        packets=vm((16, 1, PACKET), F32),
        g_second=vm((1024, 1024), BF16),
        grad_q=vm((128, 1024), BF16),
        grad_k=vm((1024, 128), F32),
        grad_v=vm((1024, 128), F32),
        out_term=vm((1024, 128), BF16),
        qkv_term=vm((3, 1024, 128), BF16),
    )
    return pl.pallas_call(
        functools.partial(step_kernel, (*inputs, *outputs, *scratch)),
        out_shape=list(outputs.values()),
        in_specs=list(inputs.values()),
        out_specs=[VM] * len(outputs),
        scratch_shapes=list(scratch.values()),
        compiler_params=params(1, 54),
        name="step",
    )(count, label, ids, table, qkv_s, out_s, up_s, down_s, head_s)


def results_kernel(*refs):
    sources, targets, here, sems = refs[:5], refs[5:10], refs[10:15], refs[15]
    steps = [pltpu.make_async_copy(sources[i], here[i], sems.at[i]) for i in range(5)]
    for step in steps:
        step.start()
    for i in range(5):
        steps[i].wait()
        if i < 3:
            targets[i][...] = here[i][...]
        elif i == 3:
            targets[i][...] = total_of(here[i])
        else:
            for piece in range(3):
                targets[i][piece] = total_of(here[i].at[piece])


def results(*arrays):
    return pl.pallas_call(
        results_kernel,
        out_shape=[
            jax.ShapeDtypeStruct((64, 512), F32),
            jax.ShapeDtypeStruct((64, 512), F32),
            jax.ShapeDtypeStruct((64, 128), F32),
            jax.ShapeDtypeStruct((64, 128), F32),
            jax.ShapeDtypeStruct((3, 64, 128), F32),
        ],
        in_specs=[HBM] * 5,
        out_specs=[VM] * 5,
        scratch_shapes=[pltpu.VMEM(a.shape, a.dtype) for a in arrays] + [pltpu.SemaphoreType.DMA((5,))],
        compiler_params=pltpu.CompilerParams(vmem_limit_bytes=67043328),
        name="results",
    )(*arrays)


def per_device(token_ids, lengths, teacher_bins, table, qkv_shard, out_shard, up_shard, down_shard, head_shard):
    up_grad, down_grad, head_grad, loss, out_buf, qkv_buf = step(
        lengths,
        teacher_bins,
        token_ids,
        table,
        jnp.transpose(qkv_shard, (1, 0, 2)),
        out_shard.T,
        up_shard,
        down_shard.T,
        head_shard,
    )
    up_grad, down_grad, head_grad, out_grad, qkv_grad = results(up_grad, down_grad, head_grad, out_buf, qkv_buf)
    return loss[0, 0], jnp.transpose(qkv_grad, (1, 0, 2)), out_grad.T, up_grad, down_grad.T, head_grad


def solution(mesh):
    fine = Mesh(mesh.devices.reshape(2, 4, 2, 4, 2), ("xl", "z", "c", "y", "xh"))
    dp, tensor = ("xl", "z", "c"), ("y", "xh")
    return jax.shard_map(
        per_device,
        mesh=fine,
        in_specs=(
            P(dp, tensor),
            P(dp),
            P(dp),
            P(tensor, None),
            P(dp, None, tensor),
            P(tensor, dp),
            P(dp, tensor),
            P(tensor, dp),
            P(dp, None),
        ),
        out_specs=(
            P(),
            P(dp, None, tensor),
            P(tensor, dp),
            P(dp, tensor),
            P(tensor, dp),
            P(dp, None),
        ),
        check_vma=False,
    )
```

```python
import functools
import types

import jax
import jax.numpy as jnp
from jax import lax
from jax.experimental import pallas as pl
from jax.experimental.pallas import tpu as pltpu
from jax.sharding import Mesh
from jax.sharding import PartitionSpec as P

MESH = pl.DeviceIdType.MESH
EPS = 1e-05
F32 = jnp.float32
BF16 = jnp.bfloat16
HIGH = lax.Precision.HIGHEST
VM = pl.BlockSpec(memory_space=pltpu.VMEM)
SM = pl.BlockSpec(memory_space=pltpu.SMEM)


def where_am_i():
    return {name: lax.axis_index(name) for name in ("xl", "z", "c", "y", "xh")}


def add_mod(value, step, size):
    return lax.rem(value + step, size)


def params(number, mebibytes):
    return pltpu.CompilerParams(
        collective_id=number, has_side_effects=True, vmem_limit_bytes=mebibytes * 2**20
    )


def remote(src, dst, send, recv, device):
    return pltpu.make_async_remote_copy(
        src_ref=src, dst_ref=dst, send_sem=send, recv_sem=recv, device_id=device, device_id_type=MESH
    )


def signal(device):
    pl.semaphore_signal(pltpu.get_barrier_semaphore(), inc=1, device_id=device, device_id_type=MESH)


def normalize(values):
    mean = jnp.mean(values, axis=-1, keepdims=True)
    centered = values - mean
    return centered * lax.rsqrt(jnp.mean(centered * centered, axis=-1, keepdims=True) + EPS)


def normalize_back(values, grad):
    mean = jnp.mean(values, axis=-1, keepdims=True)
    centered = values - mean
    scale = lax.rsqrt(jnp.mean(centered * centered, axis=-1, keepdims=True) + EPS)
    normed = centered * scale
    return scale * (
        grad
        - jnp.mean(grad, axis=-1, keepdims=True)
        - normed * jnp.mean(grad * normed, axis=-1, keepdims=True)
    )


class Ids:
    def __init__(self, src, out, send, recv):
        self.src, self.out, self.send, self.recv = src, out, send, recv
        self.me = where_am_i()
        self.here = self.me["xh"] == self.me["c"]

    def greet(self):
        me = self.me
        for role in range(2):
            for k in range(4):
                source = dict(
                    xl=add_mod(me["xl"], role, 2),
                    c=add_mod(me["xh"], role, 2),
                    xh=me["c"],
                    y=add_mod(me["y"], 4 - k, 4),
                    z=me["z"],
                )
                if role == 0 and k == 0:

                    @pl.when(jnp.logical_not(self.here))
                    def _(source=source):
                        signal(source)
                else:
                    signal(source)
        return jnp.where(self.here, 7, 8)

    def copy(self, role, k):
        me = self.me
        return remote(
            self.src,
            self.out.at[role, me["y"]],
            self.send.at[role, k],
            self.recv.at[role, k],
            dict(
                xl=add_mod(me["xl"], role, 2),
                c=me["xh"],
                xh=add_mod(me["c"], role, 2),
                y=add_mod(me["y"], k, 4),
                z=me["z"],
            ),
        )

    def local(self):
        return pltpu.make_async_copy(self.src, self.out.at[0, self.me["y"]], self.recv.at[0, 0])

    def start(self):
        for role in (1, 0):
            for k in (2, 1, 3, 0):
                if role == 0 and k == 0:

                    @pl.when(jnp.logical_not(self.here))
                    def _():
                        self.copy(0, 0).start()

                    @pl.when(self.here)
                    def _():
                        self.local().start()
                else:
                    self.copy(role, k).start()

    def arrive(self, role):
        for k in range(4):
            place = add_mod(self.me["y"], 4 - k, 4)
            pltpu.make_async_copy(self.src, self.out.at[role, place], self.recv.at[role, k]).wait()

    def sent(self):
        for role in range(2):
            for k in range(4):
                if role == 0 and k == 0:

                    @pl.when(jnp.logical_not(self.here))
                    def _():
                        self.copy(0, 0).wait_send()
                else:
                    self.copy(role, k).wait_send()


class Plane:
    def __init__(self, items, send, recv, collect):
        self.items, self.send, self.recv, self.collect = items, send, recv, collect
        self.me = where_am_i()
        c, xh = self.me["c"], self.me["xh"]
        self.here = xh == c
        self.mine, self.other = (xh, c) if collect else (c, xh)
        self.slot = (self.me["xl"] * 4 + self.me["z"]) * 2 + self.mine
        self.places = [(a, k, e) for k in (2, 1, 3, 0) for a in (1, 0) for e in range(2)]

    def target(self, a, k, e):
        me = self.me
        swapped = dict(c=e, xh=me["c"]) if self.collect else dict(c=me["xh"], xh=e)
        return dict(xl=add_mod(me["xl"], a, 2), z=add_mod(me["z"], k, 4), y=me["y"], **swapped)

    def origin(self, a, k, e):
        me = self.me
        swapped = dict(c=me["xh"], xh=e) if self.collect else dict(c=e, xh=me["c"])
        return dict(xl=add_mod(me["xl"], a, 2), z=add_mod(me["z"], 4 - k, 4), y=me["y"], **swapped)

    def number(self, a, k, e):
        return (add_mod(self.me["xl"], a, 2) * 4 + add_mod(self.me["z"], k, 4)) * 2 + e

    def greet(self):
        for a, k, e in self.places:
            if a == 0 and k == 0:

                @pl.when(jnp.logical_not(jnp.logical_and(self.here, e == self.mine)))
                def _(a=a, k=k, e=e):
                    signal(self.origin(a, k, e))
            else:
                signal(self.origin(a, k, e))
        return jnp.where(self.here, 15, 16)

    def start(self, i):
        block, place = self.items[i][:2]

        def copy(a, k, e):
            return remote(
                block(self.number(a, k, e)), place(self.slot), self.send.at[i], self.recv.at[i], self.target(a, k, e)
            )

        for a, k, e in self.places:
            if a == 0 and k == 0:
                is_self = jnp.logical_and(self.here, e == self.other)

                @pl.when(jnp.logical_not(is_self))
                def _(a=a, k=k, e=e):
                    copy(a, k, e).start()

                @pl.when(is_self)
                def _(a=a, k=k, e=e):
                    pltpu.make_async_copy(
                        block(self.number(a, k, e)), place(self.slot), self.recv.at[i]
                    ).start()
            else:
                copy(a, k, e).start()

    def arrive(self, i):
        whole = self.items[i][2]
        pltpu.make_async_copy(whole, whole, self.recv.at[i]).wait()

    def sent(self, i):
        whole, but_one = self.items[i][2:]

        @pl.when(self.here)
        def _():
            pltpu.make_async_copy(but_one, but_one, self.send.at[i]).wait()

        @pl.when(jnp.logical_not(self.here))
        def _():
            pltpu.make_async_copy(whole, whole, self.send.at[i]).wait()


def rows64(number):
    return pl.ds(pl.multiple_of(number * 64, 64), 64)


def spread_item(shard, target, cols=None):
    cols = pl.ds(0, target.shape[1]) if cols is None else cols
    return (
        lambda number: shard,
        lambda slot: target.at[rows64(slot), cols],
        target.at[:, cols],
        target.at[pl.ds(0, 960), cols],
    )


def collect_item(source, buf):
    return (
        lambda number: source.at[rows64(number)],
        lambda slot: buf.at[slot],
        buf,
        buf.at[pl.ds(0, 15)],
    )


def total_of(buf):
    total = buf[0].astype(F32)
    for s in range(1, 16):
        total = total + buf[s].astype(F32)
    return total


def thirds(row):
    high = row.astype(BF16).astype(F32)
    middle = (row - high).astype(BF16).astype(F32)
    low = row - high - middle
    index = lax.broadcasted_iota(jnp.int32, (8, row.shape[1]), 0)
    rows = jnp.where(index == 0, high, jnp.where(index == 1, middle, jnp.where(index == 2, low, 0.0)))
    return rows.astype(BF16)


def picked(values, start):
    rows = lax.broadcasted_iota(jnp.int32, (64, values.shape[1]), 0)
    cols = lax.broadcasted_iota(jnp.int32, (64, values.shape[1]), 1)
    chosen = (cols == rows + start).astype(F32)
    return lax.dot_general(chosen, values, RHS_T, precision=HIGH, preferred_element_type=F32)


def ring_places():
    me = where_am_i()
    y, c = me["y"], me["c"]
    return me, y, c, add_mod(y, 1, 4), add_mod(y, 3, 4), add_mod(y, 2, 4), 1 - c


class Owner:
    def __init__(self, blocks, stage, far, near, send, recv):
        self.blocks, self.stage, self.far, self.near = blocks, stage, far, near
        _, self.y, _, self.up, self.dn, op, _ = ring_places()
        self.ways = (self.up, self.dn)
        self.parts = (pl.ds(0, 32), pl.ds(32, 32))

        def go(k, source, target, side):
            return remote(source, target, send.at[k], recv.at[k], dict(y=self.ways[side]))

        self.first = [go(i, blocks(op).at[self.parts[i]], far.at[i], i) for i in range(2)]
        self.second = [
            go(2 + i, blocks(self.ways[i]).at[self.parts[1 - i]], near.at[i, self.parts[1 - i]], i)
            for i in range(2)
        ]
        self.third = [go(4 + i, stage.at[i], near.at[i, self.parts[i]], i) for i in range(2)]

    def begin(self):
        for step in self.first:
            step.start()

    def early(self, sides=(0, 1)):
        for i in sides:
            self.second[i].start()

    def relay(self):
        for i in range(2):
            self.first[i].wait_recv()
            mine = self.blocks(self.ways[i])[self.parts[i]]
            self.stage[i] = (mine.astype(F32) + self.far[i].astype(F32)).astype(BF16)
            self.third[i].start()

    def finish(self):
        for step in self.second + self.third:
            step.wait_recv()
        return self.blocks(self.y)[...].astype(F32) + self.near[0].astype(F32) + self.near[1].astype(F32)

    def sent(self):
        for step in self.first + self.second + self.third:
            step.wait_send()


class Gather:
    def __init__(self, out, chunk, send, recv):
        self.out, self.chunk, self.send, self.recv = out, chunk, send, recv
        _, y, c, up, dn, op, oc = ring_places()
        moves = [
            (y, c, None, dict(y=up)),
            (y, c, None, dict(y=dn)),
            (y, c, None, dict(c=oc)),
            (dn, c, 0, dict(y=up)),
            (dn, c, None, dict(c=oc)),
            (up, c, 1, dict(y=dn)),
            (up, c, None, dict(c=oc)),
            (op, c, 0, dict(c=oc)),
            (op, c, 1, dict(c=oc)),
        ]
        self.steps = []
        for k, (row, col, half, device) in enumerate(moves):
            start = (row * 2 + col) * 128 + chunk * 64
            if half is None:
                ref = out.at[pl.ds(pl.multiple_of(start, 64), 64)]
            else:
                ref = out.at[pl.ds(pl.multiple_of(start + half * 32, 32), 32)]
            self.steps.append(remote(ref, ref, send.at[k], recv.at[k], device))

    def begin(self):
        for k in (0, 1, 2):
            self.steps[k].start()

    def sides(self):
        self.steps[0].wait_recv()
        self.steps[3].start()
        self.steps[4].start()
        self.steps[1].wait_recv()
        self.steps[5].start()
        self.steps[6].start()

    def far(self):
        self.steps[3].wait_recv()
        self.steps[7].start()
        self.steps[5].wait_recv()
        self.steps[8].start()

    def pair_own(self):
        self.steps[2].wait_recv()

    def pair_sides(self):
        self.steps[4].wait_recv()
        self.steps[6].wait_recv()

    def pair_far(self):
        self.steps[7].wait_recv()
        self.steps[8].wait_recv()

    def sent(self):
        for step in self.steps:
            step.wait_send()


def gather_beside(gathers, block_work, last_work=None, after_sides=None):
    _, y, c, up, dn, op, oc = ring_places()
    for g in gathers:
        g.pair_own()
    block_work(y)
    for g in gathers:
        g.sides()
    if after_sides is not None:
        after_sides()
    for g in gathers:
        g.pair_sides()
    block_work(up)
    for g in gathers:
        g.far()
    block_work(dn)
    for g in gathers:
        g.pair_far()
    (last_work or block_work)(op)


class PairOwner:
    def __init__(self, terms, r, name):
        self.terms = terms
        get = lambda part: getattr(r, name + part)
        _, y, self.c, self.up, self.dn, self.op, oc = ring_places()
        self.pair, self.summed = get("_pair"), get("_summed")
        self.order = (self.op, self.up, self.dn, y)
        self.steps = [
            remote(
                terms.at[self.rows(b, oc)], self.pair.at[b], get("_psend").at[i], get("_precv").at[i], dict(c=oc)
            )
            for i, b in enumerate(self.order)
        ]
        self.owners = [
            Owner(
                lambda b, ch=ch: self.summed.at[b, pl.ds(ch * 64, 64)],
                get("_stage").at[ch],
                get("_far").at[ch],
                get("_near").at[ch],
                get("_rsend").at[ch],
                get("_rrecv").at[ch],
            )
            for ch in range(2)
        ]

    def rows(self, b, c):
        return pl.ds(pl.multiple_of((b * 2 + c) * 128, 128), 128)

    def push(self, i):
        self.steps[i].start()

    def pull(self, i):
        b = self.order[i]
        self.steps[i].wait_recv()
        self.summed[b] = (self.terms[self.rows(b, self.c)].astype(F32) + self.pair[b].astype(F32)).astype(BF16)

    def sent(self):
        for step in self.steps:
            step.wait_send()
        for owner in self.owners:
            owner.sent()


def pair_owner_scratch(name):
    return {
        name + "_pair": pltpu.VMEM((4, 128, 1024), BF16),
        name + "_summed": pltpu.VMEM((4, 128, 1024), BF16),
        name + "_stage": pltpu.VMEM((2, 2, 32, 1024), BF16),
        name + "_far": pltpu.VMEM((2, 2, 32, 1024), BF16),
        name + "_near": pltpu.VMEM((2, 2, 64, 1024), BF16),
        name + "_psend": pltpu.SemaphoreType.DMA((4,)),
        name + "_precv": pltpu.SemaphoreType.DMA((4,)),
        name + "_rsend": pltpu.SemaphoreType.DMA((2, 6)),
        name + "_rrecv": pltpu.SemaphoreType.DMA((2, 6)),
        name + "_asend": pltpu.SemaphoreType.DMA((2, 9)),
        name + "_arecv": pltpu.SemaphoreType.DMA((2, 9)),
    }


SCALE = 0.125
PACKET = 512 + 1024 + 1024 + 128 + 128
LHS_T = (((0,), (0,)), ((), ()))
RHS_T = (((1,), (1,)), ((), ()))


def rows256(b):
    return pl.ds(pl.multiple_of(b * 256, 256), 256)


def of_head(value, head, axis):
    index = lax.broadcasted_iota(jnp.int32, value.shape, axis)
    return jnp.where((index >= 64) == (head == 1), value, jnp.zeros_like(value))


def step_kernel(names, *refs):
    r = types.SimpleNamespace(**dict(zip(names, refs, strict=True)))
    me, y, c, up, dn, op, oc = ring_places()
    slot = y * 2 + c
    vocab, padded = r.table.shape[0], r.shard.shape[0]

    fetch = pltpu.make_async_copy(r.table, r.shard.at[pl.ds(0, vocab)], r.load.at[0])
    fetch_ids = pltpu.make_async_copy(r.ids, r.ids_here, r.load.at[1])
    fetch_ids.start()
    fetch.start()
    tokens = Ids(r.packet_in, r.got, r.isend, r.irecv)
    spread = Plane(
        [spread_item(r.qkv_s.at[i], r.qkv_w, pl.ds(i * 128, 128)) for i in range(3)]
        + [
            spread_item(r.out_s, r.out_w),
            spread_item(r.up_s, r.up_w),
            spread_item(r.head_s, r.head_w),
            spread_item(r.down_s, r.down_w),
        ],
        r.ssend,
        r.srecv,
        False,
    )
    collect = Plane(
        [
            (lambda number: r.packet, lambda slot: r.packets.at[slot], r.packets, r.packets.at[pl.ds(0, 15)]),
            collect_item(r.up_term, r.up_buf),
            collect_item(r.out_term, r.out_buf),
        ]
        + [collect_item(r.qkv_term.at[i], r.qkv_buf.at[i]) for i in range(3)],
        r.csend,
        r.crecv,
        True,
    )
    partner = dict(xl=1 - me["xl"], xh=1 - me["xh"])
    peers = [(k, e) for k in (2, 1, 3, 0) for e in range(2) if (k, e) != (0, 0)]
    for device in (dict(y=up), dict(y=dn), dict(c=oc), partner):
        signal(device)
    for k, e in peers:
        signal(dict(y=add_mod(y, (4 - k) % 4, 4), c=add_mod(c, e, 2)))
    greeted = tokens.greet() + spread.greet() + collect.greet() + 11
    if padded > vocab:
        r.shard[vocab:padded] = jnp.zeros((padded - vocab, 1024), BF16)
    fetch_ids.wait()
    line = lax.broadcasted_iota(jnp.int32, (8, 128), 0)
    r.packet_in[...] = jnp.where(line == 0, r.ids_here[...], jnp.where(line == 1, r.count[0], r.label[0]))
    pl.semaphore_wait(pltpu.get_barrier_semaphore(), greeted)
    tokens.start()
    for i in range(3):
        spread.start(i)

    base = (y * 2 + me["xh"]) * vocab
    lanes = lax.broadcasted_iota(jnp.int32, (64, 128), 1)

    def look_up(role, ch):
        for b in range(4):
            wanted = jnp.broadcast_to(r.got[role, b, 0:1, :], (128, 128)).T[ch * 64 : ch * 64 + 64] - base
            for tile in range(padded // 128):
                r.chosen[b * 64 : b * 64 + 64, tile * 128 : tile * 128 + 128] = jnp.where(
                    wanted == lanes + tile * 128, 1.0, 0.0
                ).astype(BF16)
        if role == 1 and ch == 0:
            fetch.wait()
        for part in range(4):
            cols = slice(part * 256, part * 256 + 256)
            found = jnp.dot(r.chosen[...], r.shard[:, cols], preferred_element_type=F32).astype(BF16)
            for b in range(4):
                r.rows[role, ch, b, :, cols] = found[b * 64 : b * 64 + 64]

    own = {
        (role, ch): Owner(
            lambda b, role=role, ch=ch: r.rows.at[role, ch, b],
            r.e_stage.at[role, ch],
            r.e_far.at[role, ch],
            r.e_near.at[role, ch],
            r.e_rsend.at[role, ch],
            r.e_rrecv.at[role, ch],
        )
        for role in range(2)
        for ch in range(2)
    }
    cross = [
        remote(r.total.at[ch], r.theirs.at[ch], r.xsend.at[ch], r.xrecv.at[ch], partner) for ch in range(2)
    ]
    tokens.arrive(1)
    look_up(1, 0)
    own[1, 0].begin()
    own[1, 0].early()
    look_up(1, 1)
    own[1, 1].begin()
    own[1, 1].early()
    own[1, 0].relay()
    tokens.arrive(0)
    look_up(0, 0)
    own[0, 0].begin()
    own[0, 0].early()
    own[1, 1].relay()
    r.total[0] = own[1, 0].finish().astype(BF16)
    cross[0].start()
    look_up(0, 1)
    own[0, 1].begin()
    own[0, 1].early()
    own[0, 0].relay()
    r.total[1] = own[1, 1].finish().astype(BF16)
    cross[1].start()
    for i in range(3, 7):
        spread.start(i)
    own[0, 1].relay()
    length, label = r.got[0, 0, 1:2, 0:1], r.got[0, 0, 2:3, 0:1]
    gathers = [Gather(r.normed, ch, r.e_asend.at[ch], r.e_arecv.at[ch]) for ch in range(2)]
    first = []

    def own_rows(ch):
        return pl.ds(pl.multiple_of(slot * 128 + ch * 64, 64), 64)

    for ch in range(2):
        mine = own[0, ch].finish()
        cross[ch].wait_recv()
        value = mine + r.theirs[ch].astype(F32)
        first.append(value)
        r.normed[own_rows(ch)] = normalize(value).astype(BF16)
        gathers[ch].begin()
    for ch in range(2):
        r.first[ch * 64 : ch * 64 + 64] = first[ch]
    for i in range(3):
        spread.arrive(i)

    def project(b):
        r.qkv[rows256(b)] = jnp.dot(r.normed[rows256(b)], r.qkv_w[...], preferred_element_type=F32).astype(BF16)

    wide = [Gather(r.out_full, ch, r.wsend.at[ch], r.wrecv.at[ch]) for ch in range(2)]

    def widen():
        spread.arrive(3)
        r.out_full[pl.ds(pl.multiple_of(slot * 128, 128), 128)] = r.out_w[...].T
        for g in wide:
            g.begin()

    gather_beside(gathers, project, after_sides=widen)

    r.query_t[...] = (r.qkv[:, 0:128] * SCALE).T
    r.values_t[...] = r.qkv[:, 256:384].T
    seen = lax.broadcasted_iota(jnp.int32, (1024, 256), 0) < length

    def attend(b, head):
        cols = rows256(b)
        scores = jnp.dot(r.qkv[:, 128:256], of_head(r.query_t[:, cols], head, 0), preferred_element_type=F32)
        scores = jnp.where(seen, scores, -1e30)
        expo = jnp.exp(scores - jnp.max(scores, axis=0, keepdims=True))
        probs = (expo * (1.0 / jnp.sum(expo, axis=0, keepdims=True))).astype(BF16)
        r.probs_t[head, :, cols] = probs
        rows = slice(head * 64, head * 64 + 64)
        r.context_t[rows, cols] = jnp.dot(r.values_t[rows], probs, preferred_element_type=F32).astype(BF16)

    order = (op, up, dn, y)
    here128 = pl.ds(pl.multiple_of(slot * 128, 128), 128)

    def piece(i, e):
        return r.context.at[pl.ds(pl.multiple_of((order[i] * 2 + add_mod(c, e, 2)) * 128, 128), 128)]

    pieces = {
        (i, e): remote(
            piece(i, e),
            r.context_own.at[:, here128],
            r.tsend.at[i, e],
            r.trecv.at[i, e],
            dict(y=order[i], c=add_mod(c, e, 2)),
        )
        for i in range(4)
        for e in range(2)
        if (i, e) != (3, 0)
    }

    def hand_over(i):
        r.context[rows256(order[i])] = r.context_t[:, rows256(order[i])].T
        for e in range(2):
            if (i, e) in pieces:
                pieces[i, e].start()
            else:
                r.context_own[:, here128] = r.context[here128]

    for i, b in enumerate(order):
        attend(b, 0)
        attend(b, 1)
        hand_over(i)
        if i == 0:
            for g in wide:
                g.sides()
    for g in wide:
        g.far()
    for step in pieces.values():
        step.wait_recv()
    for g in wide:
        g.pair_own()
        g.pair_sides()
        g.pair_far()
    attn = jnp.dot(r.context_own[...], r.out_full[...], preferred_element_type=F32)
    more = [Gather(r.normed_two, ch, r.a_asend.at[ch], r.a_arecv.at[ch]) for ch in range(2)]
    for ch in range(2):
        second = (r.first[ch * 64 : ch * 64 + 64] + attn[ch * 64 : ch * 64 + 64]).astype(BF16)
        r.second[ch * 64 : ch * 64 + 64] = second
        r.normed_two[own_rows(ch)] = normalize(second.astype(F32)).astype(BF16)
        more[ch].begin()

    def live(start, size):
        return start + lax.broadcasted_iota(jnp.int32, (size, 1), 0) < length

    r.hidden_sum[...] = jnp.zeros((1, 512), F32)
    spread.arrive(4)

    def hidden_block(b):
        hidden = jnp.dot(r.normed_two[rows256(b)], r.up_w[...], preferred_element_type=F32)
        square = hidden * hidden
        inner = jnp.tanh(0.7978845608028654 * hidden * (1.0 + 0.044715 * square))
        half = 0.5 * (1.0 + inner)
        acted = (hidden * half).astype(BF16).astype(F32)
        r.slope[rows256(b)] = half + 0.5 * hidden * (1.0 - inner * inner) * (
            0.7978845608028654 + (0.7978845608028654 * 3.0 * 0.044715) * square
        )
        r.hidden_sum[...] += jnp.sum(jnp.where(live(b * 256, 256), acted, 0.0), axis=0, keepdims=True)

    gather_beside(more, hidden_block)

    spread.arrive(5)
    spread.arrive(6)
    hidden_sum = r.hidden_sum[...]
    own_sum = jnp.sum(jnp.where(live(slot * 128, 128), r.second[...].astype(F32), 0.0), axis=0, keepdims=True)
    pushed = lax.dot_general(thirds(hidden_sum), r.down_w[...], RHS_T, preferred_element_type=F32)
    r.parts[slot] = own_sum + jnp.sum(pushed, axis=0, keepdims=True)
    small = [
        remote(
            r.parts.at[slot],
            r.parts.at[slot],
            r.hsend.at[k, e],
            r.hrecv.at[k, e],
            dict(y=add_mod(y, k, 4), c=add_mod(c, e, 2)),
        )
        for k, e in peers
    ]
    for step in small:
        step.start()
    for step in small:
        step.wait()
    pooled = r.parts[0]
    for s in range(1, 8):
        pooled = pooled + r.parts[s]
    count = length.astype(F32)
    pooled = pooled / count
    final = normalize(pooled)
    logits = jnp.sum(jnp.dot(thirds(final), r.head_w[...], preferred_element_type=F32), axis=0, keepdims=True)
    top = jnp.max(logits, axis=-1, keepdims=True)
    total = jnp.log(jnp.sum(jnp.exp(logits - top), axis=-1, keepdims=True)) + top
    labels = (lax.broadcasted_iota(jnp.int32, logits.shape, 1) == label).astype(F32)
    loss = total - jnp.sum(logits * labels, axis=-1, keepdims=True)
    g_logits = (jnp.exp(logits - total) - labels) / 16.0
    g_final = lax.dot_general(thirds(g_logits), r.head_w[...], RHS_T, preferred_element_type=F32)
    per_token = normalize_back(pooled, jnp.sum(g_final, axis=0, keepdims=True)) / count
    rounded = per_token.astype(BF16)
    pulled = jnp.dot(rounded, r.down_w[...], preferred_element_type=F32)

    back = PairOwner(r.terms_back, r, "b")
    for i, b in enumerate(back.order):
        rows = rows256(b)
        grad = jnp.where(live(b * 256, 256), r.slope[rows] * pulled, 0.0).astype(BF16)
        r.g_pre[rows] = grad
        r.terms_back[rows] = lax.dot_general(
            grad, r.up_w[...], RHS_T, preferred_element_type=F32
        ).astype(BF16)
        back.push(i)
        if i == 2:
            back.pull(0)
            for owner in back.owners:
                owner.begin()
    for i in range(1, 4):
        back.pull(i)
        if i < 3:
            for owner in back.owners:
                owner.early((i - 1,))
    for block in range(4):
        cols = pl.ds(block * 256, 256)
        r.up_term[cols] = lax.dot_general(
            r.normed_two[:, cols], r.g_pre[...], LHS_T, preferred_element_type=F32
        ).astype(BF16)
    for owner in back.owners:
        owner.relay()
    r.packet[:, 0:512] = hidden_sum
    r.packet[:, 512:1536] = rounded.astype(F32)
    r.packet[:, 1536:2560] = final
    r.packet[:, 2560:2688] = g_logits
    r.packet[:, 2688:2816] = jnp.broadcast_to(loss, (1, 128))
    collect.start(1)
    collect.start(0)
    last = [Gather(r.g_second, ch, r.b_asend.at[ch], r.b_arecv.at[ch]) for ch in range(2)]
    for ch in range(2):
        grad = normalize_back(r.second[ch * 64 : ch * 64 + 64].astype(F32), back.owners[ch].finish())
        grad += jnp.where(live(slot * 128 + ch * 64, 64), per_token, 0.0)
        r.g_second[own_rows(ch)] = grad.astype(BF16)
        last[ch].begin()

    r.keys_t[...] = (r.qkv[:, 128:256] * SCALE).T
    r.grad_k[...] = jnp.zeros((1024, 128), F32)
    r.grad_v[...] = jnp.zeros((1024, 128), F32)

    def back_values(b):
        cols = rows256(b)
        g_context = jnp.dot(r.g_second[cols], r.out_w[...], preferred_element_type=F32)
        g_context_t = g_context.T
        g_context = g_context.astype(BF16)
        for head in range(2):
            r.grad_v[...] += jnp.dot(
                r.probs_t[head, :, cols], of_head(g_context, head, 1), preferred_element_type=F32
            )
        return g_context_t

    def back_scores(b, g_context_t):
        cols = rows256(b)
        product = g_context_t * r.context_t[:, cols].astype(F32)
        query = r.qkv[cols, 0:128] * SCALE
        for head in range(2):
            rows = slice(head * 64, head * 64 + 64)
            delta = jnp.sum(product[rows], axis=0, keepdims=True)
            moved = jnp.dot(
                r.qkv[:, 256:384], of_head(g_context_t, head, 0).astype(BF16), preferred_element_type=F32
            )
            g_scores = (r.probs_t[head, :, cols].astype(F32) * (moved - delta)).astype(BF16)
            r.grad_q[rows, cols] = jnp.dot(
                r.keys_t[rows], g_scores, preferred_element_type=F32
            ).astype(BF16)
            r.grad_k[...] += jnp.dot(g_scores, of_head(query, head, 1), preferred_element_type=F32)

    def send_term(piece, left):
        r.qkv_term[piece] = jnp.dot(left, r.normed[...], preferred_element_type=F32).T.astype(BF16)
        collect.start(3 + piece)

    def attend_back(b):
        back_scores(b, back_values(b))

    def attend_back_last(b):
        r.out_term[...] = jnp.dot(
            r.context_t[...], r.g_second[...], preferred_element_type=F32
        ).T.astype(BF16)
        collect.start(2)
        g_context_t = back_values(b)
        send_term(2, r.grad_v[...].T.astype(BF16))
        back_scores(b, g_context_t)
        send_term(0, r.grad_q[...])
        send_term(1, r.grad_k[...].T.astype(BF16))

    gather_beside(last, attend_back, attend_back_last)

    collect.arrive(0)
    begin = ((me["xl"] * 4 + me["z"]) * 2 + me["c"]) * 64
    packets = jnp.concatenate([r.packets[s] for s in range(16)], axis=0)
    r.down_grad[...] = jnp.dot(
        picked(packets[:, 512:1536], begin), packets[:, 0:512], precision=HIGH, preferred_element_type=F32
    )
    r.head_grad[...] = jnp.dot(
        picked(packets[:, 1536:2560], begin), packets[:, 2560:2688], precision=HIGH, preferred_element_type=F32
    )
    r.loss[...] = jnp.sum(packets[:, 2688:2816], axis=0, keepdims=True) / 16.0
    collect.arrive(1)
    r.up_grad[...] = total_of(r.up_buf)

    tokens.sent()
    for i in range(7):
        spread.sent(i)
    for owner in own.values():
        owner.sent()
    for step in cross:
        step.wait_send()
    for g in gathers + wide + more + last:
        g.sent()
    for step in pieces.values():
        step.wait_send()
    back.sent()
    for i in range(6):
        collect.sent(i)
    for i in range(2, 6):
        collect.arrive(i)


HBM = pl.BlockSpec(memory_space=pltpu.HBM)


def step(count, label, ids, table, qkv_s, out_s, up_s, down_s, head_s):
    padded = -(-table.shape[0] // 256) * 256
    inputs = dict(
        count=SM, label=SM, ids=HBM, table=HBM, qkv_s=HBM, out_s=HBM, up_s=HBM, down_s=HBM, head_s=HBM
    )
    outputs = dict(
        up_grad=jax.ShapeDtypeStruct((64, 512), F32),
        down_grad=jax.ShapeDtypeStruct((64, 512), F32),
        head_grad=jax.ShapeDtypeStruct((64, 128), F32),
        loss=jax.ShapeDtypeStruct((1, 128), F32),
        out_buf=jax.ShapeDtypeStruct((16, 64, 128), BF16),
        qkv_buf=jax.ShapeDtypeStruct((3, 16, 64, 128), BF16),
    )
    dma = pltpu.SemaphoreType.DMA
    vm = pltpu.VMEM
    scratch = dict(
        load=dma((2,)),
        ids_here=vm((1, 128), jnp.int32),
        packet_in=vm((8, 128), jnp.int32),
        got=vm((2, 4, 8, 128), jnp.int32),
        isend=dma((2, 4)),
        irecv=dma((2, 4)),
        ssend=dma((7,)),
        srecv=dma((7,)),
        csend=dma((6,)),
        crecv=dma((6,)),
        shard=vm((padded, 1024), BF16),
        chosen=vm((256, padded), BF16),
        rows=vm((2, 2, 4, 64, 1024), BF16),
        e_stage=vm((2, 2, 2, 32, 1024), BF16),
        e_far=vm((2, 2, 2, 32, 1024), BF16),
        e_near=vm((2, 2, 2, 64, 1024), BF16),
        e_rsend=dma((2, 2, 6)),
        e_rrecv=dma((2, 2, 6)),
        e_asend=dma((2, 9)),
        e_arecv=dma((2, 9)),
        total=vm((2, 64, 1024), BF16),
        theirs=vm((2, 64, 1024), BF16),
        xsend=dma((2,)),
        xrecv=dma((2,)),
        first=vm((128, 1024), F32),
        normed=vm((1024, 1024), BF16),
        qkv_w=vm((1024, 384), BF16),
        out_w=vm((1024, 128), BF16),
        up_w=vm((1024, 512), BF16),
        down_w=vm((1024, 512), BF16),
        head_w=vm((1024, 128), BF16),
        qkv=vm((1024, 384), BF16),
        query_t=vm((128, 1024), BF16),
        values_t=vm((128, 1024), BF16),
        keys_t=vm((128, 1024), BF16),
        out_full=vm((1024, 1024), BF16),
        wsend=dma((2, 9)),
        wrecv=dma((2, 9)),
        context=vm((1024, 128), BF16),
        context_own=vm((128, 1024), BF16),
        tsend=dma((4, 2)),
        trecv=dma((4, 2)),
        a_asend=dma((2, 9)),
        a_arecv=dma((2, 9)),
        probs_t=vm((2, 1024, 1024), BF16),
        context_t=vm((128, 1024), BF16),
        second=vm((128, 1024), BF16),
        normed_two=vm((1024, 1024), BF16),
        hidden_sum=vm((1, 512), F32),
        slope=vm((1024, 512), F32),
        parts=vm((8, 1, 1024), F32),
        hsend=dma((4, 2)),
        hrecv=dma((4, 2)),
        g_pre=vm((1024, 512), BF16),
        terms_back=vm((1024, 1024), BF16),
        **pair_owner_scratch("b"),
        up_term=vm((1024, 512), BF16),
        up_buf=vm((16, 64, 512), BF16),
        packet=vm((1, PACKET), F32),
        packets=vm((16, 1, PACKET), F32),
        g_second=vm((1024, 1024), BF16),
        grad_q=vm((128, 1024), BF16),
        grad_k=vm((1024, 128), F32),
        grad_v=vm((1024, 128), F32),
        out_term=vm((1024, 128), BF16),
        qkv_term=vm((3, 1024, 128), BF16),
    )
    return pl.pallas_call(
        functools.partial(step_kernel, (*inputs, *outputs, *scratch)),
        out_shape=list(outputs.values()),
        in_specs=list(inputs.values()),
        out_specs=[VM] * len(outputs),
        scratch_shapes=list(scratch.values()),
        compiler_params=params(1, 54),
        name="step",
    )(count, label, ids, table, qkv_s, out_s, up_s, down_s, head_s)


def results_kernel(*refs):
    sources, targets, here, sems = refs[:5], refs[5:10], refs[10:15], refs[15]
    steps = [pltpu.make_async_copy(sources[i], here[i], sems.at[i]) for i in range(5)]
    for step in steps:
        step.start()
    for i in range(5):
        steps[i].wait()
        if i < 3:
            targets[i][...] = here[i][...]
        elif i == 3:
            targets[i][...] = total_of(here[i])
        else:
            for piece in range(3):
                targets[i][piece] = total_of(here[i].at[piece])


def results(*arrays):
    return pl.pallas_call(
        results_kernel,
        out_shape=[
            jax.ShapeDtypeStruct((64, 512), F32),
            jax.ShapeDtypeStruct((64, 512), F32),
            jax.ShapeDtypeStruct((64, 128), F32),
            jax.ShapeDtypeStruct((64, 128), F32),
            jax.ShapeDtypeStruct((3, 64, 128), F32),
        ],
        in_specs=[HBM] * 5,
        out_specs=[VM] * 5,
        scratch_shapes=[pltpu.VMEM(a.shape, a.dtype) for a in arrays] + [pltpu.SemaphoreType.DMA((5,))],
        compiler_params=pltpu.CompilerParams(vmem_limit_bytes=67043328),
        name="results",
    )(*arrays)


def per_device(token_ids, lengths, teacher_bins, table, qkv_shard, out_shard, up_shard, down_shard, head_shard):
    up_grad, down_grad, head_grad, loss, out_buf, qkv_buf = step(
        lengths,
        teacher_bins,
        token_ids,
        table,
        jnp.transpose(qkv_shard, (1, 0, 2)),
        out_shard.T,
        up_shard,
        down_shard.T,
        head_shard,
    )
    up_grad, down_grad, head_grad, out_grad, qkv_grad = results(up_grad, down_grad, head_grad, out_buf, qkv_buf)
    return loss[0, 0], jnp.transpose(qkv_grad, (1, 0, 2)), out_grad.T, up_grad, down_grad.T, head_grad


def solution(mesh):
    fine = Mesh(mesh.devices.reshape(2, 4, 2, 4, 2), ("xl", "z", "c", "y", "xh"))
    dp, tensor = ("xl", "z", "c"), ("y", "xh")
    return jax.shard_map(
        per_device,
        mesh=fine,
        in_specs=(
            P(dp, tensor),
            P(dp),
            P(dp),
            P(tensor, None),
            P(dp, None, tensor),
            P(tensor, dp),
            P(dp, tensor),
            P(tensor, dp),
            P(dp, None),
        ),
        out_specs=(
            P(),
            P(dp, None, tensor),
            P(tensor, dp),
            P(dp, tensor),
            P(tensor, dp),
            P(dp, None),
        ),
        check_vma=False,
    )
```

```python
import functools
import types

import jax
import jax.numpy as jnp
from jax import lax
from jax.experimental import pallas as pl
from jax.experimental.pallas import tpu as pltpu
from jax.sharding import Mesh
from jax.sharding import PartitionSpec as P

MESH = pl.DeviceIdType.MESH
EPS = 1e-05
F32 = jnp.float32
BF16 = jnp.bfloat16
HIGH = lax.Precision.HIGHEST
VM = pl.BlockSpec(memory_space=pltpu.VMEM)
SM = pl.BlockSpec(memory_space=pltpu.SMEM)


def where_am_i():
    return {name: lax.axis_index(name) for name in ("xl", "z", "c", "y", "xh")}


def add_mod(value, step, size):
    return lax.rem(value + step, size)


def params(number, mebibytes):
    return pltpu.CompilerParams(
        collective_id=number, has_side_effects=True, vmem_limit_bytes=mebibytes * 2**20
    )


def remote(src, dst, send, recv, device):
    return pltpu.make_async_remote_copy(
        src_ref=src, dst_ref=dst, send_sem=send, recv_sem=recv, device_id=device, device_id_type=MESH
    )


def signal(device):
    pl.semaphore_signal(pltpu.get_barrier_semaphore(), inc=1, device_id=device, device_id_type=MESH)


def normalize(values):
    mean = jnp.mean(values, axis=-1, keepdims=True)
    centered = values - mean
    return centered * lax.rsqrt(jnp.mean(centered * centered, axis=-1, keepdims=True) + EPS)


def normalize_back(values, grad):
    mean = jnp.mean(values, axis=-1, keepdims=True)
    centered = values - mean
    scale = lax.rsqrt(jnp.mean(centered * centered, axis=-1, keepdims=True) + EPS)
    normed = centered * scale
    return scale * (
        grad
        - jnp.mean(grad, axis=-1, keepdims=True)
        - normed * jnp.mean(grad * normed, axis=-1, keepdims=True)
    )


class Ids:
    def __init__(self, src, out, send, recv):
        self.src, self.out, self.send, self.recv = src, out, send, recv
        self.me = where_am_i()
        self.here = self.me["xh"] == self.me["c"]

    def greet(self):
        me = self.me
        for role in range(2):
            for k in range(4):
                source = dict(
                    xl=add_mod(me["xl"], role, 2),
                    c=add_mod(me["xh"], role, 2),
                    xh=me["c"],
                    y=add_mod(me["y"], 4 - k, 4),
                    z=me["z"],
                )
                if role == 0 and k == 0:

                    @pl.when(jnp.logical_not(self.here))
                    def _(source=source):
                        signal(source)
                else:
                    signal(source)
        return jnp.where(self.here, 7, 8)

    def copy(self, role, k):
        me = self.me
        return remote(
            self.src,
            self.out.at[role, me["y"]],
            self.send.at[role, k],
            self.recv.at[role, k],
            dict(
                xl=add_mod(me["xl"], role, 2),
                c=me["xh"],
                xh=add_mod(me["c"], role, 2),
                y=add_mod(me["y"], k, 4),
                z=me["z"],
            ),
        )

    def local(self):
        return pltpu.make_async_copy(self.src, self.out.at[0, self.me["y"]], self.recv.at[0, 0])

    def start(self):
        for role in (1, 0):
            for k in (2, 1, 3, 0):
                if role == 0 and k == 0:

                    @pl.when(jnp.logical_not(self.here))
                    def _():
                        self.copy(0, 0).start()

                    @pl.when(self.here)
                    def _():
                        self.local().start()
                else:
                    self.copy(role, k).start()

    def arrive(self, role):
        for k in range(4):
            place = add_mod(self.me["y"], 4 - k, 4)
            pltpu.make_async_copy(self.src, self.out.at[role, place], self.recv.at[role, k]).wait()

    def sent(self):
        for role in range(2):
            for k in range(4):
                if role == 0 and k == 0:

                    @pl.when(jnp.logical_not(self.here))
                    def _():
                        self.copy(0, 0).wait_send()
                else:
                    self.copy(role, k).wait_send()


class Plane:
    def __init__(self, items, send, recv, collect):
        self.items, self.send, self.recv, self.collect = items, send, recv, collect
        self.me = where_am_i()
        c, xh = self.me["c"], self.me["xh"]
        self.here = xh == c
        self.mine, self.other = (xh, c) if collect else (c, xh)
        self.slot = (self.me["xl"] * 4 + self.me["z"]) * 2 + self.mine
        self.places = [(a, k, e) for k in (2, 1, 3, 0) for a in (1, 0) for e in range(2)]

    def target(self, a, k, e):
        me = self.me
        swapped = dict(c=e, xh=me["c"]) if self.collect else dict(c=me["xh"], xh=e)
        return dict(xl=add_mod(me["xl"], a, 2), z=add_mod(me["z"], k, 4), y=me["y"], **swapped)

    def origin(self, a, k, e):
        me = self.me
        swapped = dict(c=me["xh"], xh=e) if self.collect else dict(c=e, xh=me["c"])
        return dict(xl=add_mod(me["xl"], a, 2), z=add_mod(me["z"], 4 - k, 4), y=me["y"], **swapped)

    def number(self, a, k, e):
        return (add_mod(self.me["xl"], a, 2) * 4 + add_mod(self.me["z"], k, 4)) * 2 + e

    def greet(self):
        for a, k, e in self.places:
            if a == 0 and k == 0:

                @pl.when(jnp.logical_not(jnp.logical_and(self.here, e == self.mine)))
                def _(a=a, k=k, e=e):
                    signal(self.origin(a, k, e))
            else:
                signal(self.origin(a, k, e))
        return jnp.where(self.here, 15, 16)

    def start(self, i):
        block, place = self.items[i][:2]

        def copy(a, k, e):
            return remote(
                block(self.number(a, k, e)), place(self.slot), self.send.at[i], self.recv.at[i], self.target(a, k, e)
            )

        for a, k, e in self.places:
            if a == 0 and k == 0:
                is_self = jnp.logical_and(self.here, e == self.other)

                @pl.when(jnp.logical_not(is_self))
                def _(a=a, k=k, e=e):
                    copy(a, k, e).start()

                @pl.when(is_self)
                def _(a=a, k=k, e=e):
                    pltpu.make_async_copy(
                        block(self.number(a, k, e)), place(self.slot), self.recv.at[i]
                    ).start()
            else:
                copy(a, k, e).start()


    def across(self, x):
        x = lax.rem(x, 4)
        high = jnp.where(x >= 2, 1, 0)
        return dict(xh=high, xl=x - 2 * high)

    def greet_relays(self):
        me = self.me
        xl, z, c, xh, y = me["xl"], me["z"], me["c"], me["xh"], me["y"]
        way = 1 - 2 * c
        behind = add_mod(z, 4 - way, 4)
        signal(dict(xl=xl, xh=xh, z=behind, c=xh, y=y))
        for high in range(2):
            signal(dict(xl=1 - xl, xh=high, z=behind, c=xh, y=y))
        ends = self.across(2 * xh + xl + 4 + way)
        for k in (0, 1, 3, 2):
            place = behind if k == 2 else add_mod(z, 4 - k, 4)
            signal(dict(xl=ends["xl"], xh=1 - ends["xh"], z=place, c=ends["xh"], y=y))
        before = self.across(2 * xh + xl + 4 - way)
        signal(dict(z=behind))
        signal(dict(z=z, **before))
        signal(dict(z=behind, **before))
        return jnp.where(self.here, 4, 10) + 3

    def start_relayed(self, i, j, buf, arrive):
        me = self.me
        xl, z, c, xh, y = me["xl"], me["z"], me["c"], me["xh"], me["y"]
        block, place = self.items[i][:2]

        def send(number, target, recv, device):
            remote(block(number), target, self.send.at[i], recv, device).start()

        for a, k in ((0, 2), (1, 2), (0, 1), (0, 3), (0, 0), (1, 1), (1, 3), (1, 0)):
            for e in range(2):
                way = 1 - 2 * e
                number = self.number(a, k, e)
                hop = 2 - way if k == 2 else k

                def direct(a=a, k=k, e=e, number=number):
                    send(number, place(self.slot), self.recv.at[i], self.target(a, k, e))

                def on_z(index, a=a, e=e, number=number, hop=hop):
                    device = dict(xl=add_mod(xl, a, 2), xh=c, z=add_mod(z, hop, 4), c=e, y=y)
                    send(number, buf.at[j, index], arrive.at[j, index], device)

                def on_x(index, e=e, number=number, hop=hop, way=way):
                    device = dict(z=add_mod(z, hop, 4), c=e, y=y, **self.across(2 * c + xl + 4 - way))
                    send(number, buf.at[j, index], arrive.at[j, index], device)

                if a == 1:
                    if k == 2:
                        on_z(1 + xh)
                    else:
                        direct()
                    continue

                @pl.when(jnp.logical_not(self.here))
                def _(k=k, on_x=on_x):
                    on_x({0: 3, 1: 4, 3: 5, 2: 6}[k])

                if k == 2:

                    @pl.when(self.here)
                    def _(on_z=on_z):
                        on_z(0)
                elif k:

                    @pl.when(self.here)
                    def _(direct=direct):
                        direct()
                else:
                    is_self = jnp.logical_and(self.here, e == self.other)

                    @pl.when(jnp.logical_and(self.here, e != self.other))
                    def _(direct=direct):
                        direct()

                    @pl.when(is_self)
                    def _(number=number):
                        pltpu.make_async_copy(block(number), place(self.slot), self.recv.at[i]).start()

    def forward(self, i, j, buf, arrive, leave):
        me = self.me
        xl, z, c, xh = me["xl"], me["z"], me["c"], me["xh"]
        place = self.items[i][1]
        way = 1 - 2 * c
        behind, ahead = add_mod(z, 4 - way, 4), add_mod(z, 4 + way, 4)
        ends = self.across(2 * xh + xl + 4 + way)

        def go(index, slot, device):
            pltpu.make_async_copy(buf.at[j, index], buf.at[j, index], arrive.at[j, index]).wait()
            remote(buf.at[j, index], place(slot), leave.at[j], self.recv.at[i], device).start()

        go(0, (xl * 4 + behind) * 2 + xh, dict(z=ahead))
        for high in range(2):
            go(1 + high, ((1 - xl) * 4 + behind) * 2 + high, dict(z=ahead))
        for index, k in ((6, 2), (4, 1), (5, 3), (3, 0)):
            source = behind if k == 2 else add_mod(z, 4 - k, 4)
            slot = (ends["xl"] * 4 + source) * 2 + 1 - ends["xh"]
            go(index, slot, dict(z=ahead if k == 2 else z, **ends))

    def arrive(self, i):
        whole = self.items[i][2]
        pltpu.make_async_copy(whole, whole, self.recv.at[i]).wait()

    def sent(self, i):
        whole, but_one = self.items[i][2:]

        @pl.when(self.here)
        def _():
            pltpu.make_async_copy(but_one, but_one, self.send.at[i]).wait()

        @pl.when(jnp.logical_not(self.here))
        def _():
            pltpu.make_async_copy(whole, whole, self.send.at[i]).wait()


def rows64(number):
    return pl.ds(pl.multiple_of(number * 64, 64), 64)


def spread_item(shard, target, cols=None):
    cols = pl.ds(0, target.shape[1]) if cols is None else cols
    return (
        lambda number: shard,
        lambda slot: target.at[rows64(slot), cols],
        target.at[:, cols],
        target.at[pl.ds(0, 960), cols],
    )


def collect_item(source, buf):
    return (
        lambda number: source.at[rows64(number)],
        lambda slot: buf.at[slot],
        buf,
        buf.at[pl.ds(0, 15)],
    )


def total_of(buf):
    total = buf[0].astype(F32)
    for s in range(1, 16):
        total = total + buf[s].astype(F32)
    return total


def thirds(row):
    high = row.astype(BF16).astype(F32)
    middle = (row - high).astype(BF16).astype(F32)
    low = row - high - middle
    index = lax.broadcasted_iota(jnp.int32, (8, row.shape[1]), 0)
    rows = jnp.where(index == 0, high, jnp.where(index == 1, middle, jnp.where(index == 2, low, 0.0)))
    return rows.astype(BF16)


def picked(values, start):
    rows = lax.broadcasted_iota(jnp.int32, (64, values.shape[1]), 0)
    cols = lax.broadcasted_iota(jnp.int32, (64, values.shape[1]), 1)
    chosen = (cols == rows + start).astype(F32)
    return lax.dot_general(chosen, values, RHS_T, precision=HIGH, preferred_element_type=F32)


def ring_places():
    me = where_am_i()
    y, c = me["y"], me["c"]
    return me, y, c, add_mod(y, 1, 4), add_mod(y, 3, 4), add_mod(y, 2, 4), 1 - c


class Owner:
    def __init__(self, blocks, stage, far, near, send, recv):
        self.blocks, self.stage, self.far, self.near = blocks, stage, far, near
        _, self.y, _, self.up, self.dn, op, _ = ring_places()
        self.ways = (self.up, self.dn)
        self.parts = (pl.ds(0, 32), pl.ds(32, 32))

        def go(k, source, target, side):
            return remote(source, target, send.at[k], recv.at[k], dict(y=self.ways[side]))

        self.first = [go(i, blocks(op).at[self.parts[i]], far.at[i], i) for i in range(2)]
        self.second = [
            go(2 + i, blocks(self.ways[i]).at[self.parts[1 - i]], near.at[i, self.parts[1 - i]], i)
            for i in range(2)
        ]
        self.third = [go(4 + i, stage.at[i], near.at[i, self.parts[i]], i) for i in range(2)]

    def begin(self):
        for step in self.first:
            step.start()

    def early(self, sides=(0, 1)):
        for i in sides:
            self.second[i].start()

    def relay(self):
        for i in range(2):
            self.first[i].wait_recv()
            mine = self.blocks(self.ways[i])[self.parts[i]]
            self.stage[i] = (mine.astype(F32) + self.far[i].astype(F32)).astype(BF16)
            self.third[i].start()

    def finish(self):
        for step in self.second + self.third:
            step.wait_recv()
        return self.blocks(self.y)[...].astype(F32) + self.near[0].astype(F32) + self.near[1].astype(F32)

    def sent(self):
        for step in self.first + self.second + self.third:
            step.wait_send()


class Gather:
    def __init__(self, out, chunk, send, recv):
        self.out, self.chunk, self.send, self.recv = out, chunk, send, recv
        _, y, c, up, dn, op, oc = ring_places()
        moves = [
            (y, c, None, dict(y=up)),
            (y, c, None, dict(y=dn)),
            (y, c, None, dict(c=oc)),
            (dn, c, 0, dict(y=up)),
            (dn, c, None, dict(c=oc)),
            (up, c, 1, dict(y=dn)),
            (up, c, None, dict(c=oc)),
            (op, c, 0, dict(c=oc)),
            (op, c, 1, dict(c=oc)),
        ]
        self.steps = []
        for k, (row, col, half, device) in enumerate(moves):
            start = (row * 2 + col) * 128 + chunk * 64
            if half is None:
                ref = out.at[pl.ds(pl.multiple_of(start, 64), 64)]
            else:
                ref = out.at[pl.ds(pl.multiple_of(start + half * 32, 32), 32)]
            self.steps.append(remote(ref, ref, send.at[k], recv.at[k], device))

    def begin(self):
        for k in (0, 1, 2):
            self.steps[k].start()

    def sides(self):
        self.steps[0].wait_recv()
        self.steps[3].start()
        self.steps[4].start()
        self.steps[1].wait_recv()
        self.steps[5].start()
        self.steps[6].start()

    def far(self):
        self.steps[3].wait_recv()
        self.steps[7].start()
        self.steps[5].wait_recv()
        self.steps[8].start()

    def pair_own(self):
        self.steps[2].wait_recv()

    def pair_sides(self):
        self.steps[4].wait_recv()
        self.steps[6].wait_recv()

    def pair_far(self):
        self.steps[7].wait_recv()
        self.steps[8].wait_recv()

    def sent(self):
        for step in self.steps:
            step.wait_send()


def gather_beside(gathers, block_work, last_work=None, after_sides=None):
    _, y, c, up, dn, op, oc = ring_places()
    for g in gathers:
        g.pair_own()
    block_work(y)
    for g in gathers:
        g.sides()
    if after_sides is not None:
        after_sides()
    for g in gathers:
        g.pair_sides()
    block_work(up)
    for g in gathers:
        g.far()
    block_work(dn)
    for g in gathers:
        g.pair_far()
    (last_work or block_work)(op)


class PairOwner:
    def __init__(self, terms, r, name):
        self.terms = terms
        get = lambda part: getattr(r, name + part)
        _, y, self.c, self.up, self.dn, self.op, oc = ring_places()
        self.pair, self.summed = get("_pair"), get("_summed")
        self.order = (self.op, self.up, self.dn, y)
        self.steps = [
            remote(
                terms.at[self.rows(b, oc)], self.pair.at[b], get("_psend").at[i], get("_precv").at[i], dict(c=oc)
            )
            for i, b in enumerate(self.order)
        ]
        self.owners = [
            Owner(
                lambda b, ch=ch: self.summed.at[b, pl.ds(ch * 64, 64)],
                get("_stage").at[ch],
                get("_far").at[ch],
                get("_near").at[ch],
                get("_rsend").at[ch],
                get("_rrecv").at[ch],
            )
            for ch in range(2)
        ]

    def rows(self, b, c):
        return pl.ds(pl.multiple_of((b * 2 + c) * 128, 128), 128)

    def push(self, i):
        self.steps[i].start()

    def pull(self, i):
        b = self.order[i]
        self.steps[i].wait_recv()
        self.summed[b] = (self.terms[self.rows(b, self.c)].astype(F32) + self.pair[b].astype(F32)).astype(BF16)

    def sent(self):
        for step in self.steps:
            step.wait_send()
        for owner in self.owners:
            owner.sent()


def pair_owner_scratch(name):
    return {
        name + "_pair": pltpu.VMEM((4, 128, 1024), BF16),
        name + "_summed": pltpu.VMEM((4, 128, 1024), BF16),
        name + "_stage": pltpu.VMEM((2, 2, 32, 1024), BF16),
        name + "_far": pltpu.VMEM((2, 2, 32, 1024), BF16),
        name + "_near": pltpu.VMEM((2, 2, 64, 1024), BF16),
        name + "_psend": pltpu.SemaphoreType.DMA((4,)),
        name + "_precv": pltpu.SemaphoreType.DMA((4,)),
        name + "_rsend": pltpu.SemaphoreType.DMA((2, 6)),
        name + "_rrecv": pltpu.SemaphoreType.DMA((2, 6)),
        name + "_asend": pltpu.SemaphoreType.DMA((2, 9)),
        name + "_arecv": pltpu.SemaphoreType.DMA((2, 9)),
    }


SCALE = 0.125
PACKET = 512 + 1024 + 1024 + 128 + 128
LHS_T = (((0,), (0,)), ((), ()))
RHS_T = (((1,), (1,)), ((), ()))


def rows256(b):
    return pl.ds(pl.multiple_of(b * 256, 256), 256)


def of_head(value, head, axis):
    index = lax.broadcasted_iota(jnp.int32, value.shape, axis)
    return jnp.where((index >= 64) == (head == 1), value, jnp.zeros_like(value))


def step_kernel(names, *refs):
    r = types.SimpleNamespace(**dict(zip(names, refs, strict=True)))
    me, y, c, up, dn, op, oc = ring_places()
    slot = y * 2 + c
    vocab, padded = r.table.shape[0], r.shard.shape[0]

    fetch = pltpu.make_async_copy(r.table, r.shard.at[pl.ds(0, vocab)], r.load.at[0])
    fetch_ids = pltpu.make_async_copy(r.ids, r.ids_here, r.load.at[1])
    fetch_ids.start()
    fetch.start()
    tokens = Ids(r.packet_in, r.got, r.isend, r.irecv)
    spread = Plane(
        [spread_item(r.qkv_s.at[i], r.qkv_w, pl.ds(i * 128, 128)) for i in range(3)]
        + [
            spread_item(r.out_s, r.out_w),
            spread_item(r.up_s, r.up_w),
            spread_item(r.head_s, r.head_w),
            spread_item(r.down_s, r.down_w),
        ],
        r.ssend,
        r.srecv,
        False,
    )
    collect = Plane(
        [
            (lambda number: r.packet, lambda slot: r.packets.at[slot], r.packets, r.packets.at[pl.ds(0, 15)]),
            collect_item(r.up_term, r.up_buf),
            collect_item(r.out_term, r.out_buf),
        ]
        + [collect_item(r.qkv_term.at[i], r.qkv_buf.at[i]) for i in range(3)],
        r.csend,
        r.crecv,
        True,
    )
    partner = dict(xl=1 - me["xl"], xh=1 - me["xh"])
    peers = [(k, e) for k in (2, 1, 3, 0) for e in range(2) if (k, e) != (0, 0)]
    for device in (dict(y=up), dict(y=dn), dict(c=oc), partner):
        signal(device)
    for k, e in peers:
        signal(dict(y=add_mod(y, (4 - k) % 4, 4), c=add_mod(c, e, 2)))
    greeted = tokens.greet() + spread.greet() + collect.greet() + collect.greet_relays() + 11
    if padded > vocab:
        r.shard[vocab:padded] = jnp.zeros((padded - vocab, 1024), BF16)
    fetch_ids.wait()
    line = lax.broadcasted_iota(jnp.int32, (8, 128), 0)
    r.packet_in[...] = jnp.where(line == 0, r.ids_here[...], jnp.where(line == 1, r.count[0], r.label[0]))
    pl.semaphore_wait(pltpu.get_barrier_semaphore(), greeted)
    tokens.start()
    for i in range(3):
        spread.start(i)

    base = (y * 2 + me["xh"]) * vocab
    lanes = lax.broadcasted_iota(jnp.int32, (64, 128), 1)

    def look_up(role, ch):
        for b in range(4):
            wanted = jnp.broadcast_to(r.got[role, b, 0:1, :], (128, 128)).T[ch * 64 : ch * 64 + 64] - base
            for tile in range(padded // 128):
                r.chosen[b * 64 : b * 64 + 64, tile * 128 : tile * 128 + 128] = jnp.where(
                    wanted == lanes + tile * 128, 1.0, 0.0
                ).astype(BF16)
        if role == 1 and ch == 0:
            fetch.wait()
        for part in range(4):
            cols = slice(part * 256, part * 256 + 256)
            found = jnp.dot(r.chosen[...], r.shard[:, cols], preferred_element_type=F32).astype(BF16)
            for b in range(4):
                r.rows[role, ch, b, :, cols] = found[b * 64 : b * 64 + 64]

    own = {
        (role, ch): Owner(
            lambda b, role=role, ch=ch: r.rows.at[role, ch, b],
            r.e_stage.at[role, ch],
            r.e_far.at[role, ch],
            r.e_near.at[role, ch],
            r.e_rsend.at[role, ch],
            r.e_rrecv.at[role, ch],
        )
        for role in range(2)
        for ch in range(2)
    }
    cross = [
        remote(r.total.at[ch], r.theirs.at[ch], r.xsend.at[ch], r.xrecv.at[ch], partner) for ch in range(2)
    ]
    tokens.arrive(1)
    look_up(1, 0)
    own[1, 0].begin()
    own[1, 0].early()
    look_up(1, 1)
    own[1, 1].begin()
    own[1, 1].early()
    own[1, 0].relay()
    tokens.arrive(0)
    look_up(0, 0)
    own[0, 0].begin()
    own[0, 0].early()
    own[1, 1].relay()
    r.total[0] = own[1, 0].finish().astype(BF16)
    cross[0].start()
    look_up(0, 1)
    own[0, 1].begin()
    own[0, 1].early()
    own[0, 0].relay()
    r.total[1] = own[1, 1].finish().astype(BF16)
    cross[1].start()
    for i in range(3, 7):
        spread.start(i)
    own[0, 1].relay()
    length, label = r.got[0, 0, 1:2, 0:1], r.got[0, 0, 2:3, 0:1]
    gathers = [Gather(r.normed, ch, r.e_asend.at[ch], r.e_arecv.at[ch]) for ch in range(2)]
    first = []

    def own_rows(ch):
        return pl.ds(pl.multiple_of(slot * 128 + ch * 64, 64), 64)

    for ch in range(2):
        mine = own[0, ch].finish()
        cross[ch].wait_recv()
        value = mine + r.theirs[ch].astype(F32)
        first.append(value)
        r.normed[own_rows(ch)] = normalize(value).astype(BF16)
        gathers[ch].begin()
    for ch in range(2):
        r.first[ch * 64 : ch * 64 + 64] = first[ch]
    for i in range(3):
        spread.arrive(i)

    def project(b):
        r.qkv[rows256(b)] = jnp.dot(r.normed[rows256(b)], r.qkv_w[...], preferred_element_type=F32).astype(BF16)

    wide = [Gather(r.out_full, ch, r.wsend.at[ch], r.wrecv.at[ch]) for ch in range(2)]

    def widen():
        spread.arrive(3)
        r.out_full[pl.ds(pl.multiple_of(slot * 128, 128), 128)] = r.out_w[...].T
        for g in wide:
            g.begin()

    gather_beside(gathers, project, after_sides=widen)

    r.query_t[...] = (r.qkv[:, 0:128] * SCALE).T
    r.values_t[...] = r.qkv[:, 256:384].T
    seen = lax.broadcasted_iota(jnp.int32, (1024, 256), 0) < length

    def attend(b, head):
        cols = rows256(b)
        scores = jnp.dot(r.qkv[:, 128:256], of_head(r.query_t[:, cols], head, 0), preferred_element_type=F32)
        scores = jnp.where(seen, scores, -1e30)
        expo = jnp.exp(scores - jnp.max(scores, axis=0, keepdims=True))
        probs = (expo * (1.0 / jnp.sum(expo, axis=0, keepdims=True))).astype(BF16)
        r.probs_t[head, :, cols] = probs
        rows = slice(head * 64, head * 64 + 64)
        r.context_t[rows, cols] = jnp.dot(r.values_t[rows], probs, preferred_element_type=F32).astype(BF16)

    order = (op, up, dn, y)
    here128 = pl.ds(pl.multiple_of(slot * 128, 128), 128)

    def piece(i, e):
        return r.context.at[pl.ds(pl.multiple_of((order[i] * 2 + add_mod(c, e, 2)) * 128, 128), 128)]

    pieces = {
        (i, e): remote(
            piece(i, e),
            r.context_own.at[:, here128],
            r.tsend.at[i, e],
            r.trecv.at[i, e],
            dict(y=order[i], c=add_mod(c, e, 2)),
        )
        for i in range(4)
        for e in range(2)
        if (i, e) != (3, 0)
    }

    def hand_over(i):
        r.context[rows256(order[i])] = r.context_t[:, rows256(order[i])].T
        for e in range(2):
            if (i, e) in pieces:
                pieces[i, e].start()
            else:
                r.context_own[:, here128] = r.context[here128]

    for i, b in enumerate(order):
        attend(b, 0)
        attend(b, 1)
        hand_over(i)
        if i == 0:
            for g in wide:
                g.sides()
    for g in wide:
        g.far()
    for step in pieces.values():
        step.wait_recv()
    for g in wide:
        g.pair_own()
        g.pair_sides()
        g.pair_far()
    attn = jnp.dot(r.context_own[...], r.out_full[...], preferred_element_type=F32)
    more = [Gather(r.normed_two, ch, r.a_asend.at[ch], r.a_arecv.at[ch]) for ch in range(2)]
    for ch in range(2):
        second = (r.first[ch * 64 : ch * 64 + 64] + attn[ch * 64 : ch * 64 + 64]).astype(BF16)
        r.second[ch * 64 : ch * 64 + 64] = second
        r.normed_two[own_rows(ch)] = normalize(second.astype(F32)).astype(BF16)
        more[ch].begin()

    def live(start, size):
        return start + lax.broadcasted_iota(jnp.int32, (size, 1), 0) < length

    r.hidden_sum[...] = jnp.zeros((1, 512), F32)
    spread.arrive(4)

    def hidden_block(b):
        hidden = jnp.dot(r.normed_two[rows256(b)], r.up_w[...], preferred_element_type=F32)
        square = hidden * hidden
        inner = jnp.tanh(0.7978845608028654 * hidden * (1.0 + 0.044715 * square))
        half = 0.5 * (1.0 + inner)
        acted = (hidden * half).astype(BF16).astype(F32)
        r.slope[rows256(b)] = half + 0.5 * hidden * (1.0 - inner * inner) * (
            0.7978845608028654 + (0.7978845608028654 * 3.0 * 0.044715) * square
        )
        r.hidden_sum[...] += jnp.sum(jnp.where(live(b * 256, 256), acted, 0.0), axis=0, keepdims=True)

    gather_beside(more, hidden_block)

    spread.arrive(5)
    spread.arrive(6)
    hidden_sum = r.hidden_sum[...]
    own_sum = jnp.sum(jnp.where(live(slot * 128, 128), r.second[...].astype(F32), 0.0), axis=0, keepdims=True)
    pushed = lax.dot_general(thirds(hidden_sum), r.down_w[...], RHS_T, preferred_element_type=F32)
    r.parts[slot] = own_sum + jnp.sum(pushed, axis=0, keepdims=True)
    small = [
        remote(
            r.parts.at[slot],
            r.parts.at[slot],
            r.hsend.at[k, e],
            r.hrecv.at[k, e],
            dict(y=add_mod(y, k, 4), c=add_mod(c, e, 2)),
        )
        for k, e in peers
    ]
    for step in small:
        step.start()
    for step in small:
        step.wait()
    pooled = r.parts[0]
    for s in range(1, 8):
        pooled = pooled + r.parts[s]
    count = length.astype(F32)
    pooled = pooled / count
    final = normalize(pooled)
    logits = jnp.sum(jnp.dot(thirds(final), r.head_w[...], preferred_element_type=F32), axis=0, keepdims=True)
    top = jnp.max(logits, axis=-1, keepdims=True)
    total = jnp.log(jnp.sum(jnp.exp(logits - top), axis=-1, keepdims=True)) + top
    labels = (lax.broadcasted_iota(jnp.int32, logits.shape, 1) == label).astype(F32)
    loss = total - jnp.sum(logits * labels, axis=-1, keepdims=True)
    g_logits = (jnp.exp(logits - total) - labels) / 16.0
    g_final = lax.dot_general(thirds(g_logits), r.head_w[...], RHS_T, preferred_element_type=F32)
    per_token = normalize_back(pooled, jnp.sum(g_final, axis=0, keepdims=True)) / count
    rounded = per_token.astype(BF16)
    pulled = jnp.dot(rounded, r.down_w[...], preferred_element_type=F32)

    back = PairOwner(r.terms_back, r, "b")
    for i, b in enumerate(back.order):
        rows = rows256(b)
        grad = jnp.where(live(b * 256, 256), r.slope[rows] * pulled, 0.0).astype(BF16)
        r.g_pre[rows] = grad
        r.terms_back[rows] = lax.dot_general(
            grad, r.up_w[...], RHS_T, preferred_element_type=F32
        ).astype(BF16)
        back.push(i)
        if i == 2:
            back.pull(0)
            for owner in back.owners:
                owner.begin()
    for i in range(1, 4):
        back.pull(i)
        if i < 3:
            for owner in back.owners:
                owner.early((i - 1,))
    for block in range(4):
        cols = pl.ds(block * 256, 256)
        r.up_term[cols] = lax.dot_general(
            r.normed_two[:, cols], r.g_pre[...], LHS_T, preferred_element_type=F32
        ).astype(BF16)
    for owner in back.owners:
        owner.relay()
    r.packet[:, 0:512] = hidden_sum
    r.packet[:, 512:1536] = rounded.astype(F32)
    r.packet[:, 1536:2560] = final
    r.packet[:, 2560:2688] = g_logits
    r.packet[:, 2688:2816] = jnp.broadcast_to(loss, (1, 128))
    collect.start(1)
    collect.start(0)
    last = [Gather(r.g_second, ch, r.b_asend.at[ch], r.b_arecv.at[ch]) for ch in range(2)]
    for ch in range(2):
        grad = normalize_back(r.second[ch * 64 : ch * 64 + 64].astype(F32), back.owners[ch].finish())
        grad += jnp.where(live(slot * 128 + ch * 64, 64), per_token, 0.0)
        r.g_second[own_rows(ch)] = grad.astype(BF16)
        last[ch].begin()

    r.keys_t[...] = (r.qkv[:, 128:256] * SCALE).T
    r.grad_k[...] = jnp.zeros((1024, 128), F32)
    r.grad_v[...] = jnp.zeros((1024, 128), F32)

    def back_values(b):
        cols = rows256(b)
        g_context = jnp.dot(r.g_second[cols], r.out_w[...], preferred_element_type=F32)
        g_context_t = g_context.T
        g_context = g_context.astype(BF16)
        for head in range(2):
            r.grad_v[...] += jnp.dot(
                r.probs_t[head, :, cols], of_head(g_context, head, 1), preferred_element_type=F32
            )
        return g_context_t

    def back_scores(b, g_context_t):
        cols = rows256(b)
        product = g_context_t * r.context_t[:, cols].astype(F32)
        query = r.qkv[cols, 0:128] * SCALE
        for head in range(2):
            rows = slice(head * 64, head * 64 + 64)
            delta = jnp.sum(product[rows], axis=0, keepdims=True)
            moved = jnp.dot(
                r.qkv[:, 256:384], of_head(g_context_t, head, 0).astype(BF16), preferred_element_type=F32
            )
            g_scores = (r.probs_t[head, :, cols].astype(F32) * (moved - delta)).astype(BF16)
            r.grad_q[rows, cols] = jnp.dot(
                r.keys_t[rows], g_scores, preferred_element_type=F32
            ).astype(BF16)
            r.grad_k[...] += jnp.dot(g_scores, of_head(query, head, 1), preferred_element_type=F32)

    def send_term(piece, left):
        r.qkv_term[piece] = jnp.dot(left, r.normed[...], preferred_element_type=F32).T.astype(BF16)
        collect.start_relayed(3 + piece, 1 + piece, r.relay_buf, r.relay_in)

    def pass_on(j):
        collect.forward(2 + j, j, r.relay_buf, r.relay_in, r.relay_out)

    def attend_back(b):
        back_scores(b, back_values(b))

    def attend_back_last(b):
        r.out_term[...] = jnp.dot(
            r.context_t[...], r.g_second[...], preferred_element_type=F32
        ).T.astype(BF16)
        collect.start_relayed(2, 0, r.relay_buf, r.relay_in)
        g_context_t = back_values(b)
        send_term(2, r.grad_v[...].T.astype(BF16))
        back_scores(b, g_context_t)
        send_term(0, r.grad_q[...])
        pass_on(0)
        send_term(1, r.grad_k[...].T.astype(BF16))
        pass_on(3)

    gather_beside(last, attend_back, attend_back_last)

    collect.arrive(0)
    begin = ((me["xl"] * 4 + me["z"]) * 2 + me["c"]) * 64
    packets = jnp.concatenate([r.packets[s] for s in range(16)], axis=0)
    r.down_grad[...] = jnp.dot(
        picked(packets[:, 512:1536], begin), packets[:, 0:512], precision=HIGH, preferred_element_type=F32
    )
    r.head_grad[...] = jnp.dot(
        picked(packets[:, 1536:2560], begin), packets[:, 2560:2688], precision=HIGH, preferred_element_type=F32
    )
    r.loss[...] = jnp.sum(packets[:, 2688:2816], axis=0, keepdims=True) / 16.0
    pass_on(1)
    pass_on(2)
    collect.arrive(1)
    r.up_grad[...] = total_of(r.up_buf)

    tokens.sent()
    for i in range(7):
        spread.sent(i)
    for owner in own.values():
        owner.sent()
    for step in cross:
        step.wait_send()
    for g in gathers + wide + more + last:
        g.sent()
    for step in pieces.values():
        step.wait_send()
    back.sent()
    for i in range(6):
        collect.sent(i)
    for j in range(4):
        pltpu.make_async_copy(r.relay_buf.at[j], r.relay_buf.at[j], r.relay_out.at[j]).wait()
    for i in range(2, 6):
        collect.arrive(i)


HBM = pl.BlockSpec(memory_space=pltpu.HBM)


def step(count, label, ids, table, qkv_s, out_s, up_s, down_s, head_s):
    padded = -(-table.shape[0] // 256) * 256
    inputs = dict(
        count=SM, label=SM, ids=HBM, table=HBM, qkv_s=HBM, out_s=HBM, up_s=HBM, down_s=HBM, head_s=HBM
    )
    outputs = dict(
        up_grad=jax.ShapeDtypeStruct((64, 512), F32),
        down_grad=jax.ShapeDtypeStruct((64, 512), F32),
        head_grad=jax.ShapeDtypeStruct((64, 128), F32),
        loss=jax.ShapeDtypeStruct((1, 128), F32),
        out_buf=jax.ShapeDtypeStruct((16, 64, 128), BF16),
        qkv_buf=jax.ShapeDtypeStruct((3, 16, 64, 128), BF16),
    )
    dma = pltpu.SemaphoreType.DMA
    vm = pltpu.VMEM
    scratch = dict(
        load=dma((2,)),
        ids_here=vm((1, 128), jnp.int32),
        packet_in=vm((8, 128), jnp.int32),
        got=vm((2, 4, 8, 128), jnp.int32),
        isend=dma((2, 4)),
        irecv=dma((2, 4)),
        ssend=dma((7,)),
        srecv=dma((7,)),
        csend=dma((6,)),
        crecv=dma((6,)),
        relay_buf=vm((4, 7, 64, 128), BF16),
        relay_in=dma((4, 7)),
        relay_out=dma((4,)),
        shard=vm((padded, 1024), BF16),
        chosen=vm((256, padded), BF16),
        rows=vm((2, 2, 4, 64, 1024), BF16),
        e_stage=vm((2, 2, 2, 32, 1024), BF16),
        e_far=vm((2, 2, 2, 32, 1024), BF16),
        e_near=vm((2, 2, 2, 64, 1024), BF16),
        e_rsend=dma((2, 2, 6)),
        e_rrecv=dma((2, 2, 6)),
        e_asend=dma((2, 9)),
        e_arecv=dma((2, 9)),
        total=vm((2, 64, 1024), BF16),
        theirs=vm((2, 64, 1024), BF16),
        xsend=dma((2,)),
        xrecv=dma((2,)),
        first=vm((128, 1024), F32),
        normed=vm((1024, 1024), BF16),
        qkv_w=vm((1024, 384), BF16),
        out_w=vm((1024, 128), BF16),
        up_w=vm((1024, 512), BF16),
        down_w=vm((1024, 512), BF16),
        head_w=vm((1024, 128), BF16),
        qkv=vm((1024, 384), BF16),
        query_t=vm((128, 1024), BF16),
        values_t=vm((128, 1024), BF16),
        keys_t=vm((128, 1024), BF16),
        out_full=vm((1024, 1024), BF16),
        wsend=dma((2, 9)),
        wrecv=dma((2, 9)),
        context=vm((1024, 128), BF16),
        context_own=vm((128, 1024), BF16),
        tsend=dma((4, 2)),
        trecv=dma((4, 2)),
        a_asend=dma((2, 9)),
        a_arecv=dma((2, 9)),
        probs_t=vm((2, 1024, 1024), BF16),
        context_t=vm((128, 1024), BF16),
        second=vm((128, 1024), BF16),
        normed_two=vm((1024, 1024), BF16),
        hidden_sum=vm((1, 512), F32),
        slope=vm((1024, 512), F32),
        parts=vm((8, 1, 1024), F32),
        hsend=dma((4, 2)),
        hrecv=dma((4, 2)),
        g_pre=vm((1024, 512), BF16),
        terms_back=vm((1024, 1024), BF16),
        **pair_owner_scratch("b"),
        up_term=vm((1024, 512), BF16),
        up_buf=vm((16, 64, 512), BF16),
        packet=vm((1, PACKET), F32),
        packets=vm((16, 1, PACKET), F32),
        g_second=vm((1024, 1024), BF16),
        grad_q=vm((128, 1024), BF16),
        grad_k=vm((1024, 128), F32),
        grad_v=vm((1024, 128), F32),
        out_term=vm((1024, 128), BF16),
        qkv_term=vm((3, 1024, 128), BF16),
    )
    return pl.pallas_call(
        functools.partial(step_kernel, (*inputs, *outputs, *scratch)),
        out_shape=list(outputs.values()),
        in_specs=list(inputs.values()),
        out_specs=[VM] * len(outputs),
        scratch_shapes=list(scratch.values()),
        compiler_params=params(1, 54),
        name="step",
    )(count, label, ids, table, qkv_s, out_s, up_s, down_s, head_s)


def results_kernel(*refs):
    sources, targets, here, sems = refs[:5], refs[5:10], refs[10:15], refs[15]
    steps = [pltpu.make_async_copy(sources[i], here[i], sems.at[i]) for i in range(5)]
    for step in steps:
        step.start()
    for i in range(5):
        steps[i].wait()
        if i < 3:
            targets[i][...] = here[i][...]
        elif i == 3:
            targets[i][...] = total_of(here[i])
        else:
            for piece in range(3):
                targets[i][piece] = total_of(here[i].at[piece])


def results(*arrays):
    return pl.pallas_call(
        results_kernel,
        out_shape=[
            jax.ShapeDtypeStruct((64, 512), F32),
            jax.ShapeDtypeStruct((64, 512), F32),
            jax.ShapeDtypeStruct((64, 128), F32),
            jax.ShapeDtypeStruct((64, 128), F32),
            jax.ShapeDtypeStruct((3, 64, 128), F32),
        ],
        in_specs=[HBM] * 5,
        out_specs=[VM] * 5,
        scratch_shapes=[pltpu.VMEM(a.shape, a.dtype) for a in arrays] + [pltpu.SemaphoreType.DMA((5,))],
        compiler_params=pltpu.CompilerParams(vmem_limit_bytes=67043328),
        name="results",
    )(*arrays)


def per_device(token_ids, lengths, teacher_bins, table, qkv_shard, out_shard, up_shard, down_shard, head_shard):
    up_grad, down_grad, head_grad, loss, out_buf, qkv_buf = step(
        lengths,
        teacher_bins,
        token_ids,
        table,
        jnp.transpose(qkv_shard, (1, 0, 2)),
        out_shard.T,
        up_shard,
        down_shard.T,
        head_shard,
    )
    up_grad, down_grad, head_grad, out_grad, qkv_grad = results(up_grad, down_grad, head_grad, out_buf, qkv_buf)
    return loss[0, 0], jnp.transpose(qkv_grad, (1, 0, 2)), out_grad.T, up_grad, down_grad.T, head_grad


def solution(mesh):
    fine = Mesh(mesh.devices.reshape(2, 4, 2, 4, 2), ("xl", "z", "c", "y", "xh"))
    dp, tensor = ("xl", "z", "c"), ("y", "xh")
    return jax.shard_map(
        per_device,
        mesh=fine,
        in_specs=(
            P(dp, tensor),
            P(dp),
            P(dp),
            P(tensor, None),
            P(dp, None, tensor),
            P(tensor, dp),
            P(dp, tensor),
            P(tensor, dp),
            P(dp, None),
        ),
        out_specs=(
            P(),
            P(dp, None, tensor),
            P(tensor, dp),
            P(dp, tensor),
            P(tensor, dp),
            P(dp, None),
        ),
        check_vma=False,
    )
```

```python
import functools
import types

import jax
import jax.numpy as jnp
from jax import lax
from jax.experimental import pallas as pl
from jax.experimental.pallas import tpu as pltpu
from jax.sharding import Mesh
from jax.sharding import PartitionSpec as P

MESH = pl.DeviceIdType.MESH
EPS = 1e-05
F32 = jnp.float32
BF16 = jnp.bfloat16
HIGH = lax.Precision.HIGHEST
VM = pl.BlockSpec(memory_space=pltpu.VMEM)
SM = pl.BlockSpec(memory_space=pltpu.SMEM)


def where_am_i():
    return {name: lax.axis_index(name) for name in ("xl", "z", "c", "y", "xh")}


def add_mod(value, step, size):
    return lax.rem(value + step, size)


def params(number, mebibytes):
    return pltpu.CompilerParams(
        collective_id=number, has_side_effects=True, vmem_limit_bytes=mebibytes * 2**20
    )


def remote(src, dst, send, recv, device):
    return pltpu.make_async_remote_copy(
        src_ref=src, dst_ref=dst, send_sem=send, recv_sem=recv, device_id=device, device_id_type=MESH
    )


def signal(device):
    pl.semaphore_signal(pltpu.get_barrier_semaphore(), inc=1, device_id=device, device_id_type=MESH)


def normalize(values):
    mean = jnp.mean(values, axis=-1, keepdims=True)
    centered = values - mean
    return centered * lax.rsqrt(jnp.mean(centered * centered, axis=-1, keepdims=True) + EPS)


def normalize_back(values, grad):
    mean = jnp.mean(values, axis=-1, keepdims=True)
    centered = values - mean
    scale = lax.rsqrt(jnp.mean(centered * centered, axis=-1, keepdims=True) + EPS)
    normed = centered * scale
    return scale * (
        grad
        - jnp.mean(grad, axis=-1, keepdims=True)
        - normed * jnp.mean(grad * normed, axis=-1, keepdims=True)
    )


class Ids:
    def __init__(self, src, out, send, recv):
        self.src, self.out, self.send, self.recv = src, out, send, recv
        self.me = where_am_i()
        self.here = self.me["xh"] == self.me["c"]

    def greet(self):
        me = self.me
        for role in range(2):
            for k in range(4):
                source = dict(
                    xl=add_mod(me["xl"], role, 2),
                    c=add_mod(me["xh"], role, 2),
                    xh=me["c"],
                    y=add_mod(me["y"], 4 - k, 4),
                    z=me["z"],
                )
                if role == 0 and k == 0:

                    @pl.when(jnp.logical_not(self.here))
                    def _(source=source):
                        signal(source)
                else:
                    signal(source)
        return jnp.where(self.here, 7, 8)

    def copy(self, role, k):
        me = self.me
        return remote(
            self.src,
            self.out.at[role, me["y"]],
            self.send.at[role, k],
            self.recv.at[role, k],
            dict(
                xl=add_mod(me["xl"], role, 2),
                c=me["xh"],
                xh=add_mod(me["c"], role, 2),
                y=add_mod(me["y"], k, 4),
                z=me["z"],
            ),
        )

    def local(self):
        return pltpu.make_async_copy(self.src, self.out.at[0, self.me["y"]], self.recv.at[0, 0])

    def start(self):
        for role in (1, 0):
            for k in (2, 1, 3, 0):
                if role == 0 and k == 0:

                    @pl.when(jnp.logical_not(self.here))
                    def _():
                        self.copy(0, 0).start()

                    @pl.when(self.here)
                    def _():
                        self.local().start()
                else:
                    self.copy(role, k).start()

    def arrive(self, role):
        for k in range(4):
            place = add_mod(self.me["y"], 4 - k, 4)
            pltpu.make_async_copy(self.src, self.out.at[role, place], self.recv.at[role, k]).wait()

    def sent(self):
        for role in range(2):
            for k in range(4):
                if role == 0 and k == 0:

                    @pl.when(jnp.logical_not(self.here))
                    def _():
                        self.copy(0, 0).wait_send()
                else:
                    self.copy(role, k).wait_send()


class Plane:
    def __init__(self, items, send, recv, collect):
        self.items, self.send, self.recv, self.collect = items, send, recv, collect
        self.me = where_am_i()
        c, xh = self.me["c"], self.me["xh"]
        self.here = xh == c
        self.mine, self.other = (xh, c) if collect else (c, xh)
        self.slot = (self.me["xl"] * 4 + self.me["z"]) * 2 + self.mine
        self.places = [(a, k, e) for k in (2, 1, 3, 0) for a in (1, 0) for e in range(2)]

    def target(self, a, k, e):
        me = self.me
        swapped = dict(c=e, xh=me["c"]) if self.collect else dict(c=me["xh"], xh=e)
        return dict(xl=add_mod(me["xl"], a, 2), z=add_mod(me["z"], k, 4), y=me["y"], **swapped)

    def origin(self, a, k, e):
        me = self.me
        swapped = dict(c=me["xh"], xh=e) if self.collect else dict(c=e, xh=me["c"])
        return dict(xl=add_mod(me["xl"], a, 2), z=add_mod(me["z"], 4 - k, 4), y=me["y"], **swapped)

    def number(self, a, k, e):
        return (add_mod(self.me["xl"], a, 2) * 4 + add_mod(self.me["z"], k, 4)) * 2 + e

    def greet(self):
        for a, k, e in self.places:
            if a == 0 and k == 0:

                @pl.when(jnp.logical_not(jnp.logical_and(self.here, e == self.mine)))
                def _(a=a, k=k, e=e):
                    signal(self.origin(a, k, e))
            else:
                signal(self.origin(a, k, e))
        return jnp.where(self.here, 15, 16)

    def start(self, i):
        block, place = self.items[i][:2]

        def copy(a, k, e):
            return remote(
                block(self.number(a, k, e)), place(self.slot), self.send.at[i], self.recv.at[i], self.target(a, k, e)
            )

        for a, k, e in self.places:
            if a == 0 and k == 0:
                is_self = jnp.logical_and(self.here, e == self.other)

                @pl.when(jnp.logical_not(is_self))
                def _(a=a, k=k, e=e):
                    copy(a, k, e).start()

                @pl.when(is_self)
                def _(a=a, k=k, e=e):
                    pltpu.make_async_copy(
                        block(self.number(a, k, e)), place(self.slot), self.recv.at[i]
                    ).start()
            else:
                copy(a, k, e).start()

    def arrive(self, i):
        whole = self.items[i][2]
        pltpu.make_async_copy(whole, whole, self.recv.at[i]).wait()

    def sent(self, i):
        whole, but_one = self.items[i][2:]

        @pl.when(self.here)
        def _():
            pltpu.make_async_copy(but_one, but_one, self.send.at[i]).wait()

        @pl.when(jnp.logical_not(self.here))
        def _():
            pltpu.make_async_copy(whole, whole, self.send.at[i]).wait()


def rows64(number):
    return pl.ds(pl.multiple_of(number * 64, 64), 64)


def spread_item(shard, target, cols=None):
    cols = pl.ds(0, target.shape[1]) if cols is None else cols
    return (
        lambda number: shard,
        lambda slot: target.at[rows64(slot), cols],
        target.at[:, cols],
        target.at[pl.ds(0, 960), cols],
    )


def collect_item(source, buf):
    return (
        lambda number: source.at[rows64(number)],
        lambda slot: buf.at[slot],
        buf,
        buf.at[pl.ds(0, 15)],
    )


def total_of(buf):
    total = buf[0].astype(F32)
    for s in range(1, 16):
        total = total + buf[s].astype(F32)
    return total


def thirds(row):
    high = row.astype(BF16).astype(F32)
    middle = (row - high).astype(BF16).astype(F32)
    low = row - high - middle
    index = lax.broadcasted_iota(jnp.int32, (8, row.shape[1]), 0)
    rows = jnp.where(index == 0, high, jnp.where(index == 1, middle, jnp.where(index == 2, low, 0.0)))
    return rows.astype(BF16)


def picked(values, start):
    rows = lax.broadcasted_iota(jnp.int32, (64, values.shape[1]), 0)
    cols = lax.broadcasted_iota(jnp.int32, (64, values.shape[1]), 1)
    chosen = (cols == rows + start).astype(F32)
    return lax.dot_general(chosen, values, RHS_T, precision=HIGH, preferred_element_type=F32)


def ring_places():
    me = where_am_i()
    y, c = me["y"], me["c"]
    return me, y, c, add_mod(y, 1, 4), add_mod(y, 3, 4), add_mod(y, 2, 4), 1 - c


class Owner:
    def __init__(self, blocks, stage, far, near, send, recv):
        self.blocks, self.stage, self.far, self.near = blocks, stage, far, near
        _, self.y, _, self.up, self.dn, op, _ = ring_places()
        self.ways = (self.up, self.dn)
        self.parts = (pl.ds(0, 32), pl.ds(32, 32))

        def go(k, source, target, side):
            return remote(source, target, send.at[k], recv.at[k], dict(y=self.ways[side]))

        self.first = [go(i, blocks(op).at[self.parts[i]], far.at[i], i) for i in range(2)]
        self.second = [
            go(2 + i, blocks(self.ways[i]).at[self.parts[1 - i]], near.at[i, self.parts[1 - i]], i)
            for i in range(2)
        ]
        self.third = [go(4 + i, stage.at[i], near.at[i, self.parts[i]], i) for i in range(2)]

    def begin(self):
        for step in self.first:
            step.start()

    def early(self, sides=(0, 1)):
        for i in sides:
            self.second[i].start()

    def relay(self):
        for i in range(2):
            self.first[i].wait_recv()
            mine = self.blocks(self.ways[i])[self.parts[i]]
            self.stage[i] = (mine.astype(F32) + self.far[i].astype(F32)).astype(BF16)
            self.third[i].start()

    def finish(self):
        for step in self.second + self.third:
            step.wait_recv()
        return self.blocks(self.y)[...].astype(F32) + self.near[0].astype(F32) + self.near[1].astype(F32)

    def sent(self):
        for step in self.first + self.second + self.third:
            step.wait_send()


class Gather:
    def __init__(self, out, chunk, send, recv):
        self.out, self.chunk, self.send, self.recv = out, chunk, send, recv
        _, y, c, up, dn, op, oc = ring_places()
        moves = [
            (y, c, None, dict(y=up)),
            (y, c, None, dict(y=dn)),
            (y, c, None, dict(c=oc)),
            (dn, c, 0, dict(y=up)),
            (dn, c, None, dict(c=oc)),
            (up, c, 1, dict(y=dn)),
            (up, c, None, dict(c=oc)),
            (op, c, 0, dict(c=oc)),
            (op, c, 1, dict(c=oc)),
        ]
        self.steps = []
        for k, (row, col, half, device) in enumerate(moves):
            start = (row * 2 + col) * 128 + chunk * 64
            if half is None:
                ref = out.at[pl.ds(pl.multiple_of(start, 64), 64)]
            else:
                ref = out.at[pl.ds(pl.multiple_of(start + half * 32, 32), 32)]
            self.steps.append(remote(ref, ref, send.at[k], recv.at[k], device))

    def begin(self):
        for k in (0, 1, 2):
            self.steps[k].start()

    def sides(self):
        self.steps[0].wait_recv()
        self.steps[3].start()
        self.steps[4].start()
        self.steps[1].wait_recv()
        self.steps[5].start()
        self.steps[6].start()

    def far(self):
        self.steps[3].wait_recv()
        self.steps[7].start()
        self.steps[5].wait_recv()
        self.steps[8].start()

    def pair_own(self):
        self.steps[2].wait_recv()

    def pair_sides(self):
        self.steps[4].wait_recv()
        self.steps[6].wait_recv()

    def pair_far(self):
        self.steps[7].wait_recv()
        self.steps[8].wait_recv()

    def sent(self):
        for step in self.steps:
            step.wait_send()


def gather_beside(gathers, block_work, last_work=None, after_sides=None):
    _, y, c, up, dn, op, oc = ring_places()
    for g in gathers:
        g.pair_own()
    block_work(y)
    for g in gathers:
        g.sides()
    if after_sides is not None:
        after_sides()
    for g in gathers:
        g.pair_sides()
    block_work(up)
    for g in gathers:
        g.far()
    block_work(dn)
    for g in gathers:
        g.pair_far()
    (last_work or block_work)(op)


class PairOwner:
    def __init__(self, terms, r, name):
        self.terms = terms
        get = lambda part: getattr(r, name + part)
        _, y, self.c, self.up, self.dn, self.op, oc = ring_places()
        self.pair, self.summed = get("_pair"), get("_summed")
        self.order = (self.op, self.up, self.dn, y)
        self.steps = [
            remote(
                terms.at[self.rows(b, oc)], self.pair.at[b], get("_psend").at[i], get("_precv").at[i], dict(c=oc)
            )
            for i, b in enumerate(self.order)
        ]
        self.owners = [
            Owner(
                lambda b, ch=ch: self.summed.at[b, pl.ds(ch * 64, 64)],
                get("_stage").at[ch],
                get("_far").at[ch],
                get("_near").at[ch],
                get("_rsend").at[ch],
                get("_rrecv").at[ch],
            )
            for ch in range(2)
        ]

    def rows(self, b, c):
        return pl.ds(pl.multiple_of((b * 2 + c) * 128, 128), 128)

    def push(self, i):
        self.steps[i].start()

    def pull(self, i):
        b = self.order[i]
        self.steps[i].wait_recv()
        self.summed[b] = (self.terms[self.rows(b, self.c)].astype(F32) + self.pair[b].astype(F32)).astype(BF16)

    def sent(self):
        for step in self.steps:
            step.wait_send()
        for owner in self.owners:
            owner.sent()


def pair_owner_scratch(name):
    return {
        name + "_pair": pltpu.VMEM((4, 128, 1024), BF16),
        name + "_summed": pltpu.VMEM((4, 128, 1024), BF16),
        name + "_stage": pltpu.VMEM((2, 2, 32, 1024), BF16),
        name + "_far": pltpu.VMEM((2, 2, 32, 1024), BF16),
        name + "_near": pltpu.VMEM((2, 2, 64, 1024), BF16),
        name + "_psend": pltpu.SemaphoreType.DMA((4,)),
        name + "_precv": pltpu.SemaphoreType.DMA((4,)),
        name + "_rsend": pltpu.SemaphoreType.DMA((2, 6)),
        name + "_rrecv": pltpu.SemaphoreType.DMA((2, 6)),
        name + "_asend": pltpu.SemaphoreType.DMA((2, 9)),
        name + "_arecv": pltpu.SemaphoreType.DMA((2, 9)),
    }


SCALE = 0.125
PACKET = 512 + 1024 + 1024 + 128 + 128
LHS_T = (((0,), (0,)), ((), ()))
RHS_T = (((1,), (1,)), ((), ()))


def rows256(b):
    return pl.ds(pl.multiple_of(b * 256, 256), 256)


def of_head(value, head, axis):
    index = lax.broadcasted_iota(jnp.int32, value.shape, axis)
    return jnp.where((index >= 64) == (head == 1), value, jnp.zeros_like(value))


def step_kernel(names, *refs):
    r = types.SimpleNamespace(**dict(zip(names, refs, strict=True)))
    me, y, c, up, dn, op, oc = ring_places()
    slot = y * 2 + c
    vocab, padded = r.table.shape[0], r.shard.shape[0]

    fetch = pltpu.make_async_copy(r.table, r.shard.at[pl.ds(0, vocab)], r.load.at[0])
    fetch_ids = pltpu.make_async_copy(r.ids, r.ids_here, r.load.at[1])
    fetch_ids.start()
    fetch.start()
    tokens = Ids(r.packet_in, r.got, r.isend, r.irecv)
    spread = Plane(
        [spread_item(r.qkv_s.at[i], r.qkv_w, pl.ds(i * 128, 128)) for i in range(3)]
        + [
            spread_item(r.out_s, r.out_w),
            spread_item(r.up_s, r.up_w),
            spread_item(r.head_s, r.head_w),
            spread_item(r.down_s, r.down_w),
        ],
        r.ssend,
        r.srecv,
        False,
    )
    collect = Plane(
        [
            (lambda number: r.packet, lambda slot: r.packets.at[slot], r.packets, r.packets.at[pl.ds(0, 15)]),
            collect_item(r.up_term, r.up_buf),
            collect_item(r.out_term, r.out_buf),
        ]
        + [collect_item(r.qkv_term.at[i], r.qkv_buf.at[i]) for i in range(3)],
        r.csend,
        r.crecv,
        True,
    )
    partner = dict(xl=1 - me["xl"], xh=1 - me["xh"])
    peers = [(k, e) for k in (2, 1, 3, 0) for e in range(2) if (k, e) != (0, 0)]
    for device in (dict(y=up), dict(y=dn), dict(c=oc), partner):
        signal(device)
    for k, e in peers:
        signal(dict(y=add_mod(y, (4 - k) % 4, 4), c=add_mod(c, e, 2)))
    greeted = tokens.greet() + spread.greet() + collect.greet() + 11
    if padded > vocab:
        r.shard[vocab:padded] = jnp.zeros((padded - vocab, 1024), BF16)
    fetch_ids.wait()
    line = lax.broadcasted_iota(jnp.int32, (8, 128), 0)
    r.packet_in[...] = jnp.where(line == 0, r.ids_here[...], jnp.where(line == 1, r.count[0], r.label[0]))
    pl.semaphore_wait(pltpu.get_barrier_semaphore(), greeted)
    tokens.start()
    for i in range(3):
        spread.start(i)

    base = (y * 2 + me["xh"]) * vocab
    lanes = lax.broadcasted_iota(jnp.int32, (64, 128), 1)

    def look_up(role, ch):
        for b in range(4):
            wanted = jnp.broadcast_to(r.got[role, b, 0:1, :], (128, 128)).T[ch * 64 : ch * 64 + 64] - base
            for tile in range(padded // 128):
                r.chosen[b * 64 : b * 64 + 64, tile * 128 : tile * 128 + 128] = jnp.where(
                    wanted == lanes + tile * 128, 1.0, 0.0
                ).astype(BF16)
        if role == 1 and ch == 0:
            fetch.wait()
        for part in range(4):
            cols = slice(part * 256, part * 256 + 256)
            found = jnp.dot(r.chosen[...], r.shard[:, cols], preferred_element_type=F32).astype(BF16)
            for b in range(4):
                r.rows[role, ch, b, :, cols] = found[b * 64 : b * 64 + 64]

    own = {
        (role, ch): Owner(
            lambda b, role=role, ch=ch: r.rows.at[role, ch, b],
            r.e_stage.at[role, ch],
            r.e_far.at[role, ch],
            r.e_near.at[role, ch],
            r.e_rsend.at[role, ch],
            r.e_rrecv.at[role, ch],
        )
        for role in range(2)
        for ch in range(2)
    }
    cross = [
        remote(r.total.at[ch], r.theirs.at[ch], r.xsend.at[ch], r.xrecv.at[ch], partner) for ch in range(2)
    ]
    tokens.arrive(1)
    look_up(1, 0)
    own[1, 0].begin()
    own[1, 0].early()
    look_up(1, 1)
    own[1, 1].begin()
    own[1, 1].early()
    own[1, 0].relay()
    tokens.arrive(0)
    look_up(0, 0)
    own[0, 0].begin()
    own[0, 0].early()
    own[1, 1].relay()
    r.total[0] = own[1, 0].finish().astype(BF16)
    cross[0].start()
    look_up(0, 1)
    own[0, 1].begin()
    own[0, 1].early()
    own[0, 0].relay()
    r.total[1] = own[1, 1].finish().astype(BF16)
    cross[1].start()
    spread.start(3)
    own[0, 1].relay()
    length, label = r.got[0, 0, 1:2, 0:1], r.got[0, 0, 2:3, 0:1]
    gathers = [Gather(r.normed, ch, r.e_asend.at[ch], r.e_arecv.at[ch]) for ch in range(2)]
    first = []

    def own_rows(ch):
        return pl.ds(pl.multiple_of(slot * 128 + ch * 64, 64), 64)

    for ch in range(2):
        mine = own[0, ch].finish()
        cross[ch].wait_recv()
        value = mine + r.theirs[ch].astype(F32)
        first.append(value)
        r.normed[own_rows(ch)] = normalize(value).astype(BF16)
        gathers[ch].begin()
    for i in range(4, 7):
        spread.start(i)
    for ch in range(2):
        r.first[ch * 64 : ch * 64 + 64] = first[ch]
    for i in range(3):
        spread.arrive(i)

    def project(b):
        r.qkv[rows256(b)] = jnp.dot(r.normed[rows256(b)], r.qkv_w[...], preferred_element_type=F32).astype(BF16)

    wide = [Gather(r.out_full, ch, r.wsend.at[ch], r.wrecv.at[ch]) for ch in range(2)]

    def widen():
        spread.arrive(3)
        r.out_full[pl.ds(pl.multiple_of(slot * 128, 128), 128)] = r.out_w[...].T
        for g in wide:
            g.begin()

    gather_beside(gathers, project, after_sides=widen)

    r.query_t[...] = (r.qkv[:, 0:128] * SCALE).T
    r.values_t[...] = r.qkv[:, 256:384].T
    seen = lax.broadcasted_iota(jnp.int32, (1024, 256), 0) < length

    def attend(b, head):
        cols = rows256(b)
        scores = jnp.dot(r.qkv[:, 128:256], of_head(r.query_t[:, cols], head, 0), preferred_element_type=F32)
        scores = jnp.where(seen, scores, -1e30)
        expo = jnp.exp(scores - jnp.max(scores, axis=0, keepdims=True))
        probs = (expo * (1.0 / jnp.sum(expo, axis=0, keepdims=True))).astype(BF16)
        r.probs_t[head, :, cols] = probs
        rows = slice(head * 64, head * 64 + 64)
        r.context_t[rows, cols] = jnp.dot(r.values_t[rows], probs, preferred_element_type=F32).astype(BF16)

    order = (op, up, dn, y)
    here128 = pl.ds(pl.multiple_of(slot * 128, 128), 128)

    def piece(i, e):
        return r.context.at[pl.ds(pl.multiple_of((order[i] * 2 + add_mod(c, e, 2)) * 128, 128), 128)]

    pieces = {
        (i, e): remote(
            piece(i, e),
            r.context_own.at[:, here128],
            r.tsend.at[i, e],
            r.trecv.at[i, e],
            dict(y=order[i], c=add_mod(c, e, 2)),
        )
        for i in range(4)
        for e in range(2)
        if (i, e) != (3, 0)
    }

    def hand_over(i):
        r.context[rows256(order[i])] = r.context_t[:, rows256(order[i])].T
        for e in range(2):
            if (i, e) in pieces:
                pieces[i, e].start()
            else:
                r.context_own[:, here128] = r.context[here128]

    for i, b in enumerate(order):
        attend(b, 0)
        attend(b, 1)
        hand_over(i)
        if i == 0:
            for g in wide:
                g.sides()
    for g in wide:
        g.far()
    for step in pieces.values():
        step.wait_recv()
    for g in wide:
        g.pair_own()
        g.pair_sides()
        g.pair_far()
    attn = jnp.dot(r.context_own[...], r.out_full[...], preferred_element_type=F32)
    more = [Gather(r.normed_two, ch, r.a_asend.at[ch], r.a_arecv.at[ch]) for ch in range(2)]
    for ch in range(2):
        second = (r.first[ch * 64 : ch * 64 + 64] + attn[ch * 64 : ch * 64 + 64]).astype(BF16)
        r.second[ch * 64 : ch * 64 + 64] = second
        r.normed_two[own_rows(ch)] = normalize(second.astype(F32)).astype(BF16)
        more[ch].begin()

    def live(start, size):
        return start + lax.broadcasted_iota(jnp.int32, (size, 1), 0) < length

    r.hidden_sum[...] = jnp.zeros((1, 512), F32)
    spread.arrive(4)

    def hidden_block(b):
        hidden = jnp.dot(r.normed_two[rows256(b)], r.up_w[...], preferred_element_type=F32)
        square = hidden * hidden
        inner = jnp.tanh(0.7978845608028654 * hidden * (1.0 + 0.044715 * square))
        half = 0.5 * (1.0 + inner)
        acted = (hidden * half).astype(BF16).astype(F32)
        r.slope[rows256(b)] = half + 0.5 * hidden * (1.0 - inner * inner) * (
            0.7978845608028654 + (0.7978845608028654 * 3.0 * 0.044715) * square
        )
        r.hidden_sum[...] += jnp.sum(jnp.where(live(b * 256, 256), acted, 0.0), axis=0, keepdims=True)

    gather_beside(more, hidden_block)

    spread.arrive(5)
    spread.arrive(6)
    hidden_sum = r.hidden_sum[...]
    own_sum = jnp.sum(jnp.where(live(slot * 128, 128), r.second[...].astype(F32), 0.0), axis=0, keepdims=True)
    pushed = lax.dot_general(thirds(hidden_sum), r.down_w[...], RHS_T, preferred_element_type=F32)
    r.parts[slot] = own_sum + jnp.sum(pushed, axis=0, keepdims=True)
    small = [
        remote(
            r.parts.at[slot],
            r.parts.at[slot],
            r.hsend.at[k, e],
            r.hrecv.at[k, e],
            dict(y=add_mod(y, k, 4), c=add_mod(c, e, 2)),
        )
        for k, e in peers
    ]
    for step in small:
        step.start()
    for step in small:
        step.wait()
    pooled = r.parts[0]
    for s in range(1, 8):
        pooled = pooled + r.parts[s]
    count = length.astype(F32)
    pooled = pooled / count
    final = normalize(pooled)
    logits = jnp.sum(jnp.dot(thirds(final), r.head_w[...], preferred_element_type=F32), axis=0, keepdims=True)
    top = jnp.max(logits, axis=-1, keepdims=True)
    total = jnp.log(jnp.sum(jnp.exp(logits - top), axis=-1, keepdims=True)) + top
    labels = (lax.broadcasted_iota(jnp.int32, logits.shape, 1) == label).astype(F32)
    loss = total - jnp.sum(logits * labels, axis=-1, keepdims=True)
    g_logits = (jnp.exp(logits - total) - labels) / 16.0
    g_final = lax.dot_general(thirds(g_logits), r.head_w[...], RHS_T, preferred_element_type=F32)
    per_token = normalize_back(pooled, jnp.sum(g_final, axis=0, keepdims=True)) / count
    rounded = per_token.astype(BF16)
    pulled = jnp.dot(rounded, r.down_w[...], preferred_element_type=F32)

    back = PairOwner(r.terms_back, r, "b")
    for i, b in enumerate(back.order):
        rows = rows256(b)
        grad = jnp.where(live(b * 256, 256), r.slope[rows] * pulled, 0.0).astype(BF16)
        r.g_pre[rows] = grad
        r.terms_back[rows] = lax.dot_general(
            grad, r.up_w[...], RHS_T, preferred_element_type=F32
        ).astype(BF16)
        back.push(i)
        if i == 2:
            back.pull(0)
            for owner in back.owners:
                owner.begin()
    for i in range(1, 4):
        back.pull(i)
        if i < 3:
            for owner in back.owners:
                owner.early((i - 1,))
    for block in range(4):
        cols = pl.ds(block * 256, 256)
        r.up_term[cols] = lax.dot_general(
            r.normed_two[:, cols], r.g_pre[...], LHS_T, preferred_element_type=F32
        ).astype(BF16)
    for owner in back.owners:
        owner.relay()
    r.packet[:, 0:512] = hidden_sum
    r.packet[:, 512:1536] = rounded.astype(F32)
    r.packet[:, 1536:2560] = final
    r.packet[:, 2560:2688] = g_logits
    r.packet[:, 2688:2816] = jnp.broadcast_to(loss, (1, 128))
    collect.start(1)
    collect.start(0)
    last = [Gather(r.g_second, ch, r.b_asend.at[ch], r.b_arecv.at[ch]) for ch in range(2)]
    for ch in range(2):
        grad = normalize_back(r.second[ch * 64 : ch * 64 + 64].astype(F32), back.owners[ch].finish())
        grad += jnp.where(live(slot * 128 + ch * 64, 64), per_token, 0.0)
        r.g_second[own_rows(ch)] = grad.astype(BF16)
        last[ch].begin()

    r.keys_t[...] = (r.qkv[:, 128:256] * SCALE).T
    r.grad_k[...] = jnp.zeros((1024, 128), F32)
    r.grad_v[...] = jnp.zeros((1024, 128), F32)

    def back_values(b):
        cols = rows256(b)
        g_context = jnp.dot(r.g_second[cols], r.out_w[...], preferred_element_type=F32)
        g_context_t = g_context.T
        g_context = g_context.astype(BF16)
        for head in range(2):
            r.grad_v[...] += jnp.dot(
                r.probs_t[head, :, cols], of_head(g_context, head, 1), preferred_element_type=F32
            )
        return g_context_t

    def back_scores(b, g_context_t):
        cols = rows256(b)
        product = g_context_t * r.context_t[:, cols].astype(F32)
        query = r.qkv[cols, 0:128] * SCALE
        for head in range(2):
            rows = slice(head * 64, head * 64 + 64)
            delta = jnp.sum(product[rows], axis=0, keepdims=True)
            moved = jnp.dot(
                r.qkv[:, 256:384], of_head(g_context_t, head, 0).astype(BF16), preferred_element_type=F32
            )
            g_scores = (r.probs_t[head, :, cols].astype(F32) * (moved - delta)).astype(BF16)
            r.grad_q[rows, cols] = jnp.dot(
                r.keys_t[rows], g_scores, preferred_element_type=F32
            ).astype(BF16)
            r.grad_k[...] += jnp.dot(g_scores, of_head(query, head, 1), preferred_element_type=F32)

    def send_term(piece, left):
        r.qkv_term[piece] = jnp.dot(left, r.normed[...], preferred_element_type=F32).T.astype(BF16)
        collect.start(3 + piece)

    def attend_back(b):
        back_scores(b, back_values(b))

    def attend_back_last(b):
        r.out_term[...] = jnp.dot(
            r.context_t[...], r.g_second[...], preferred_element_type=F32
        ).T.astype(BF16)
        collect.start(2)
        g_context_t = back_values(b)
        send_term(2, r.grad_v[...].T.astype(BF16))
        back_scores(b, g_context_t)
        send_term(0, r.grad_q[...])
        send_term(1, r.grad_k[...].T.astype(BF16))

    gather_beside(last, attend_back, attend_back_last)

    collect.arrive(0)
    begin = ((me["xl"] * 4 + me["z"]) * 2 + me["c"]) * 64
    packets = jnp.concatenate([r.packets[s] for s in range(16)], axis=0)
    r.down_grad[...] = jnp.dot(
        picked(packets[:, 512:1536], begin), packets[:, 0:512], precision=HIGH, preferred_element_type=F32
    )
    r.head_grad[...] = jnp.dot(
        picked(packets[:, 1536:2560], begin), packets[:, 2560:2688], precision=HIGH, preferred_element_type=F32
    )
    r.loss[...] = jnp.sum(packets[:, 2688:2816], axis=0, keepdims=True) / 16.0
    collect.arrive(1)
    r.up_grad[...] = total_of(r.up_buf)

    tokens.sent()
    for i in range(7):
        spread.sent(i)
    for owner in own.values():
        owner.sent()
    for step in cross:
        step.wait_send()
    for g in gathers + wide + more + last:
        g.sent()
    for step in pieces.values():
        step.wait_send()
    back.sent()
    for i in range(6):
        collect.sent(i)
    collect.arrive(2)
    r.out_grad[...] = total_of(r.out_buf)
    for piece in (2, 0, 1):
        collect.arrive(3 + piece)
        r.qkv_grad[piece] = total_of(r.qkv_buf.at[piece])


HBM = pl.BlockSpec(memory_space=pltpu.HBM)


def step(count, label, ids, table, qkv_s, out_s, up_s, down_s, head_s):
    padded = -(-table.shape[0] // 256) * 256
    inputs = dict(
        count=SM, label=SM, ids=HBM, table=HBM, qkv_s=HBM, out_s=HBM, up_s=HBM, down_s=HBM, head_s=HBM
    )
    outputs = dict(
        up_grad=jax.ShapeDtypeStruct((64, 512), F32),
        down_grad=jax.ShapeDtypeStruct((64, 512), F32),
        head_grad=jax.ShapeDtypeStruct((64, 128), F32),
        loss=jax.ShapeDtypeStruct((1, 128), F32),
        out_grad=jax.ShapeDtypeStruct((64, 128), F32),
        qkv_grad=jax.ShapeDtypeStruct((3, 64, 128), F32),
    )
    dma = pltpu.SemaphoreType.DMA
    vm = pltpu.VMEM
    scratch = dict(
        load=dma((2,)),
        ids_here=vm((1, 128), jnp.int32),
        packet_in=vm((8, 128), jnp.int32),
        got=vm((2, 4, 8, 128), jnp.int32),
        isend=dma((2, 4)),
        irecv=dma((2, 4)),
        ssend=dma((7,)),
        srecv=dma((7,)),
        csend=dma((6,)),
        crecv=dma((6,)),
        shard=vm((padded, 1024), BF16),
        chosen=vm((256, padded), BF16),
        rows=vm((2, 2, 4, 64, 1024), BF16),
        e_stage=vm((2, 2, 2, 32, 1024), BF16),
        e_far=vm((2, 2, 2, 32, 1024), BF16),
        e_near=vm((2, 2, 2, 64, 1024), BF16),
        e_rsend=dma((2, 2, 6)),
        e_rrecv=dma((2, 2, 6)),
        e_asend=dma((2, 9)),
        e_arecv=dma((2, 9)),
        total=vm((2, 64, 1024), BF16),
        theirs=vm((2, 64, 1024), BF16),
        xsend=dma((2,)),
        xrecv=dma((2,)),
        first=vm((128, 1024), F32),
        normed=vm((1024, 1024), BF16),
        qkv_w=vm((1024, 384), BF16),
        out_w=vm((1024, 128), BF16),
        up_w=vm((1024, 512), BF16),
        down_w=vm((1024, 512), BF16),
        head_w=vm((1024, 128), BF16),
        qkv=vm((1024, 384), BF16),
        query_t=vm((128, 1024), BF16),
        values_t=vm((128, 1024), BF16),
        keys_t=vm((128, 1024), BF16),
        out_full=vm((1024, 1024), BF16),
        wsend=dma((2, 9)),
        wrecv=dma((2, 9)),
        context=vm((1024, 128), BF16),
        context_own=vm((128, 1024), BF16),
        tsend=dma((4, 2)),
        trecv=dma((4, 2)),
        a_asend=dma((2, 9)),
        a_arecv=dma((2, 9)),
        probs_t=vm((2, 1024, 1024), BF16),
        context_t=vm((128, 1024), BF16),
        second=vm((128, 1024), BF16),
        normed_two=vm((1024, 1024), BF16),
        hidden_sum=vm((1, 512), F32),
        slope=vm((1024, 512), F32),
        parts=vm((8, 1, 1024), F32),
        hsend=dma((4, 2)),
        hrecv=dma((4, 2)),
        g_pre=vm((1024, 512), BF16),
        terms_back=vm((1024, 1024), BF16),
        **pair_owner_scratch("b"),
        up_term=vm((1024, 512), BF16),
        up_buf=vm((16, 64, 512), BF16),
        packet=vm((1, PACKET), F32),
        packets=vm((16, 1, PACKET), F32),
        g_second=vm((1024, 1024), BF16),
        grad_q=vm((128, 1024), BF16),
        grad_k=vm((1024, 128), F32),
        grad_v=vm((1024, 128), F32),
        out_term=vm((1024, 128), BF16),
        qkv_term=vm((3, 1024, 128), BF16),
        out_buf=vm((16, 64, 128), BF16),
        qkv_buf=vm((3, 16, 64, 128), BF16),
    )
    return pl.pallas_call(
        functools.partial(step_kernel, (*inputs, *outputs, *scratch)),
        out_shape=list(outputs.values()),
        in_specs=list(inputs.values()),
        out_specs=[VM] * len(outputs),
        scratch_shapes=list(scratch.values()),
        compiler_params=params(1, 54),
        name="step",
    )(count, label, ids, table, qkv_s, out_s, up_s, down_s, head_s)


def results_kernel(*refs):
    sources, targets, here, sems = refs[:5], refs[5:10], refs[10:15], refs[15]
    steps = [pltpu.make_async_copy(sources[i], here[i], sems.at[i]) for i in range(5)]
    for step in steps:
        step.start()
    for i in range(5):
        steps[i].wait()
        targets[i][...] = here[i][...]


def results(*arrays):
    return pl.pallas_call(
        results_kernel,
        out_shape=[
            jax.ShapeDtypeStruct((64, 512), F32),
            jax.ShapeDtypeStruct((64, 512), F32),
            jax.ShapeDtypeStruct((64, 128), F32),
            jax.ShapeDtypeStruct((64, 128), F32),
            jax.ShapeDtypeStruct((3, 64, 128), F32),
        ],
        in_specs=[HBM] * 5,
        out_specs=[VM] * 5,
        scratch_shapes=[pltpu.VMEM(a.shape, a.dtype) for a in arrays] + [pltpu.SemaphoreType.DMA((5,))],
        compiler_params=pltpu.CompilerParams(vmem_limit_bytes=67043328),
        name="results",
    )(*arrays)


def per_device(token_ids, lengths, teacher_bins, table, qkv_shard, out_shard, up_shard, down_shard, head_shard):
    up_grad, down_grad, head_grad, loss, out_grad, qkv_grad = step(
        lengths,
        teacher_bins,
        token_ids,
        table,
        jnp.transpose(qkv_shard, (1, 0, 2)),
        out_shard.T,
        up_shard,
        down_shard.T,
        head_shard,
    )
    up_grad, down_grad, head_grad, out_grad, qkv_grad = results(up_grad, down_grad, head_grad, out_grad, qkv_grad)
    return loss[0, 0], jnp.transpose(qkv_grad, (1, 0, 2)), out_grad.T, up_grad, down_grad.T, head_grad


def solution(mesh):
    fine = Mesh(mesh.devices.reshape(2, 4, 2, 4, 2), ("xl", "z", "c", "y", "xh"))
    dp, tensor = ("xl", "z", "c"), ("y", "xh")
    return jax.shard_map(
        per_device,
        mesh=fine,
        in_specs=(
            P(dp, tensor),
            P(dp),
            P(dp),
            P(tensor, None),
            P(dp, None, tensor),
            P(tensor, dp),
            P(dp, tensor),
            P(tensor, dp),
            P(dp, None),
        ),
        out_specs=(
            P(),
            P(dp, None, tensor),
            P(tensor, dp),
            P(dp, tensor),
            P(tensor, dp),
            P(dp, None),
        ),
        check_vma=False,
    )
```

```python
import functools
import types

import jax
import jax.numpy as jnp
from jax import lax
from jax.experimental import pallas as pl
from jax.experimental.pallas import tpu as pltpu
from jax.sharding import Mesh
from jax.sharding import PartitionSpec as P

MESH = pl.DeviceIdType.MESH
EPS = 1e-05
F32 = jnp.float32
BF16 = jnp.bfloat16
HIGH = lax.Precision.HIGHEST
VM = pl.BlockSpec(memory_space=pltpu.VMEM)
SM = pl.BlockSpec(memory_space=pltpu.SMEM)


def where_am_i():
    return {name: lax.axis_index(name) for name in ("xl", "z", "c", "y", "xh")}


def add_mod(value, step, size):
    return lax.rem(value + step, size)


def params(number, mebibytes):
    return pltpu.CompilerParams(
        collective_id=number, has_side_effects=True, vmem_limit_bytes=mebibytes * 2**20
    )


def remote(src, dst, send, recv, device):
    return pltpu.make_async_remote_copy(
        src_ref=src, dst_ref=dst, send_sem=send, recv_sem=recv, device_id=device, device_id_type=MESH
    )


def signal(device):
    pl.semaphore_signal(pltpu.get_barrier_semaphore(), inc=1, device_id=device, device_id_type=MESH)


def normalize(values):
    mean = jnp.mean(values, axis=-1, keepdims=True)
    centered = values - mean
    return centered * lax.rsqrt(jnp.mean(centered * centered, axis=-1, keepdims=True) + EPS)


def normalize_back(values, grad):
    mean = jnp.mean(values, axis=-1, keepdims=True)
    centered = values - mean
    scale = lax.rsqrt(jnp.mean(centered * centered, axis=-1, keepdims=True) + EPS)
    normed = centered * scale
    return scale * (
        grad
        - jnp.mean(grad, axis=-1, keepdims=True)
        - normed * jnp.mean(grad * normed, axis=-1, keepdims=True)
    )


class Ids:
    def __init__(self, src, out, send, recv):
        self.src, self.out, self.send, self.recv = src, out, send, recv
        self.me = where_am_i()
        self.here = self.me["xh"] == self.me["c"]

    def greet(self):
        me = self.me
        for role in range(2):
            for k in range(4):
                source = dict(
                    xl=add_mod(me["xl"], role, 2),
                    c=add_mod(me["xh"], role, 2),
                    xh=me["c"],
                    y=add_mod(me["y"], 4 - k, 4),
                    z=me["z"],
                )
                if role == 0 and k == 0:

                    @pl.when(jnp.logical_not(self.here))
                    def _(source=source):
                        signal(source)
                else:
                    signal(source)
        return jnp.where(self.here, 7, 8)

    def copy(self, role, k):
        me = self.me
        return remote(
            self.src,
            self.out.at[role, me["y"]],
            self.send.at[role, k],
            self.recv.at[role, k],
            dict(
                xl=add_mod(me["xl"], role, 2),
                c=me["xh"],
                xh=add_mod(me["c"], role, 2),
                y=add_mod(me["y"], k, 4),
                z=me["z"],
            ),
        )

    def local(self):
        return pltpu.make_async_copy(self.src, self.out.at[0, self.me["y"]], self.recv.at[0, 0])

    def start(self):
        for role in (1, 0):
            for k in (2, 1, 3, 0):
                if role == 0 and k == 0:

                    @pl.when(jnp.logical_not(self.here))
                    def _():
                        self.copy(0, 0).start()

                    @pl.when(self.here)
                    def _():
                        self.local().start()
                else:
                    self.copy(role, k).start()

    def arrive(self, role):
        for k in range(4):
            place = add_mod(self.me["y"], 4 - k, 4)
            pltpu.make_async_copy(self.src, self.out.at[role, place], self.recv.at[role, k]).wait()

    def sent(self):
        for role in range(2):
            for k in range(4):
                if role == 0 and k == 0:

                    @pl.when(jnp.logical_not(self.here))
                    def _():
                        self.copy(0, 0).wait_send()
                else:
                    self.copy(role, k).wait_send()


class Plane:
    def __init__(self, items, send, recv, collect):
        self.items, self.send, self.recv, self.collect = items, send, recv, collect
        self.me = where_am_i()
        c, xh = self.me["c"], self.me["xh"]
        self.here = xh == c
        self.mine, self.other = (xh, c) if collect else (c, xh)
        self.slot = (self.me["xl"] * 4 + self.me["z"]) * 2 + self.mine
        self.places = [(a, k, e) for k in (2, 1, 3, 0) for a in (1, 0) for e in range(2)]

    def target(self, a, k, e):
        me = self.me
        swapped = dict(c=e, xh=me["c"]) if self.collect else dict(c=me["xh"], xh=e)
        return dict(xl=add_mod(me["xl"], a, 2), z=add_mod(me["z"], k, 4), y=me["y"], **swapped)

    def origin(self, a, k, e):
        me = self.me
        swapped = dict(c=me["xh"], xh=e) if self.collect else dict(c=e, xh=me["c"])
        return dict(xl=add_mod(me["xl"], a, 2), z=add_mod(me["z"], 4 - k, 4), y=me["y"], **swapped)

    def number(self, a, k, e):
        return (add_mod(self.me["xl"], a, 2) * 4 + add_mod(self.me["z"], k, 4)) * 2 + e

    def greet(self):
        for a, k, e in self.places:
            if a == 0 and k == 0:

                @pl.when(jnp.logical_not(jnp.logical_and(self.here, e == self.mine)))
                def _(a=a, k=k, e=e):
                    signal(self.origin(a, k, e))
            else:
                signal(self.origin(a, k, e))
        return jnp.where(self.here, 15, 16)

    def start(self, i):
        block, place = self.items[i][:2]

        def copy(a, k, e):
            return remote(
                block(self.number(a, k, e)), place(self.slot), self.send.at[i], self.recv.at[i], self.target(a, k, e)
            )

        for a, k, e in self.places:
            if a == 0 and k == 0:
                is_self = jnp.logical_and(self.here, e == self.other)

                @pl.when(jnp.logical_not(is_self))
                def _(a=a, k=k, e=e):
                    copy(a, k, e).start()

                @pl.when(is_self)
                def _(a=a, k=k, e=e):
                    pltpu.make_async_copy(
                        block(self.number(a, k, e)), place(self.slot), self.recv.at[i]
                    ).start()
            else:
                copy(a, k, e).start()

    def arrive(self, i):
        whole = self.items[i][2]
        pltpu.make_async_copy(whole, whole, self.recv.at[i]).wait()

    def sent(self, i):
        whole, but_one = self.items[i][2:]

        @pl.when(self.here)
        def _():
            pltpu.make_async_copy(but_one, but_one, self.send.at[i]).wait()

        @pl.when(jnp.logical_not(self.here))
        def _():
            pltpu.make_async_copy(whole, whole, self.send.at[i]).wait()


def rows64(number):
    return pl.ds(pl.multiple_of(number * 64, 64), 64)


def spread_item(shard, target, cols=None):
    cols = pl.ds(0, target.shape[1]) if cols is None else cols
    return (
        lambda number: shard,
        lambda slot: target.at[rows64(slot), cols],
        target.at[:, cols],
        target.at[pl.ds(0, 960), cols],
    )


def collect_item(source, buf):
    return (
        lambda number: source.at[rows64(number)],
        lambda slot: buf.at[slot],
        buf,
        buf.at[pl.ds(0, 15)],
    )


def total_of(buf):
    total = buf[0].astype(F32)
    for s in range(1, 16):
        total = total + buf[s].astype(F32)
    return total


def thirds(row):
    high = row.astype(BF16).astype(F32)
    middle = (row - high).astype(BF16).astype(F32)
    low = row - high - middle
    index = lax.broadcasted_iota(jnp.int32, (8, row.shape[1]), 0)
    rows = jnp.where(index == 0, high, jnp.where(index == 1, middle, jnp.where(index == 2, low, 0.0)))
    return rows.astype(BF16)


def picked(values, start):
    rows = lax.broadcasted_iota(jnp.int32, (64, values.shape[1]), 0)
    cols = lax.broadcasted_iota(jnp.int32, (64, values.shape[1]), 1)
    chosen = (cols == rows + start).astype(F32)
    return lax.dot_general(chosen, values, RHS_T, precision=HIGH, preferred_element_type=F32)


def ring_places():
    me = where_am_i()
    y, c = me["y"], me["c"]
    return me, y, c, add_mod(y, 1, 4), add_mod(y, 3, 4), add_mod(y, 2, 4), 1 - c


class Owner:
    def __init__(self, blocks, stage, far, near, send, recv):
        self.blocks, self.stage, self.far, self.near = blocks, stage, far, near
        _, self.y, _, self.up, self.dn, op, _ = ring_places()
        self.ways = (self.up, self.dn)
        self.parts = (pl.ds(0, 32), pl.ds(32, 32))

        def go(k, source, target, side):
            return remote(source, target, send.at[k], recv.at[k], dict(y=self.ways[side]))

        self.first = [go(i, blocks(op).at[self.parts[i]], far.at[i], i) for i in range(2)]
        self.second = [
            go(2 + i, blocks(self.ways[i]).at[self.parts[1 - i]], near.at[i, self.parts[1 - i]], i)
            for i in range(2)
        ]
        self.third = [go(4 + i, stage.at[i], near.at[i, self.parts[i]], i) for i in range(2)]

    def begin(self):
        for step in self.first:
            step.start()

    def early(self, sides=(0, 1)):
        for i in sides:
            self.second[i].start()

    def relay(self):
        for i in range(2):
            self.first[i].wait_recv()
            mine = self.blocks(self.ways[i])[self.parts[i]]
            self.stage[i] = (mine.astype(F32) + self.far[i].astype(F32)).astype(BF16)
            self.third[i].start()

    def finish(self):
        for step in self.second + self.third:
            step.wait_recv()
        return self.blocks(self.y)[...].astype(F32) + self.near[0].astype(F32) + self.near[1].astype(F32)

    def sent(self):
        for step in self.first + self.second + self.third:
            step.wait_send()


class Gather:
    def __init__(self, out, chunk, send, recv):
        self.out, self.chunk, self.send, self.recv = out, chunk, send, recv
        _, y, c, up, dn, op, oc = ring_places()
        moves = [
            (y, c, None, dict(y=up)),
            (y, c, None, dict(y=dn)),
            (y, c, None, dict(c=oc)),
            (dn, c, 0, dict(y=up)),
            (dn, c, None, dict(c=oc)),
            (up, c, 1, dict(y=dn)),
            (up, c, None, dict(c=oc)),
            (op, c, 0, dict(c=oc)),
            (op, c, 1, dict(c=oc)),
        ]
        self.steps = []
        for k, (row, col, half, device) in enumerate(moves):
            start = (row * 2 + col) * 128 + chunk * 64
            if half is None:
                ref = out.at[pl.ds(pl.multiple_of(start, 64), 64)]
            else:
                ref = out.at[pl.ds(pl.multiple_of(start + half * 32, 32), 32)]
            self.steps.append(remote(ref, ref, send.at[k], recv.at[k], device))

    def begin(self):
        for k in (0, 1, 2):
            self.steps[k].start()

    def sides(self):
        self.steps[0].wait_recv()
        self.steps[3].start()
        self.steps[4].start()
        self.steps[1].wait_recv()
        self.steps[5].start()
        self.steps[6].start()

    def far(self):
        self.steps[3].wait_recv()
        self.steps[7].start()
        self.steps[5].wait_recv()
        self.steps[8].start()

    def pair_own(self):
        self.steps[2].wait_recv()

    def pair_sides(self):
        self.steps[4].wait_recv()
        self.steps[6].wait_recv()

    def pair_far(self):
        self.steps[7].wait_recv()
        self.steps[8].wait_recv()

    def sent(self):
        for step in self.steps:
            step.wait_send()


def gather_beside(gathers, block_work, last_work=None, after_sides=None):
    _, y, c, up, dn, op, oc = ring_places()
    for g in gathers:
        g.pair_own()
    block_work(y)
    for g in gathers:
        g.sides()
    if after_sides is not None:
        after_sides()
    for g in gathers:
        g.pair_sides()
    block_work(up)
    for g in gathers:
        g.far()
    block_work(dn)
    for g in gathers:
        g.pair_far()
    (last_work or block_work)(op)


class PairOwner:
    def __init__(self, terms, r, name):
        self.terms = terms
        get = lambda part: getattr(r, name + part)
        _, y, self.c, self.up, self.dn, self.op, oc = ring_places()
        self.pair, self.summed = get("_pair"), get("_summed")
        self.order = (self.op, self.up, self.dn, y)
        self.steps = [
            remote(
                terms.at[self.rows(b, oc)], self.pair.at[b], get("_psend").at[i], get("_precv").at[i], dict(c=oc)
            )
            for i, b in enumerate(self.order)
        ]
        self.owners = [
            Owner(
                lambda b, ch=ch: self.summed.at[b, pl.ds(ch * 64, 64)],
                get("_stage").at[ch],
                get("_far").at[ch],
                get("_near").at[ch],
                get("_rsend").at[ch],
                get("_rrecv").at[ch],
            )
            for ch in range(2)
        ]

    def rows(self, b, c):
        return pl.ds(pl.multiple_of((b * 2 + c) * 128, 128), 128)

    def push(self, i):
        self.steps[i].start()

    def pull(self, i):
        b = self.order[i]
        self.steps[i].wait_recv()
        self.summed[b] = (self.terms[self.rows(b, self.c)].astype(F32) + self.pair[b].astype(F32)).astype(BF16)

    def sent(self):
        for step in self.steps:
            step.wait_send()
        for owner in self.owners:
            owner.sent()


def pair_owner_scratch(name):
    return {
        name + "_pair": pltpu.VMEM((4, 128, 1024), BF16),
        name + "_summed": pltpu.VMEM((4, 128, 1024), BF16),
        name + "_stage": pltpu.VMEM((2, 2, 32, 1024), BF16),
        name + "_far": pltpu.VMEM((2, 2, 32, 1024), BF16),
        name + "_near": pltpu.VMEM((2, 2, 64, 1024), BF16),
        name + "_psend": pltpu.SemaphoreType.DMA((4,)),
        name + "_precv": pltpu.SemaphoreType.DMA((4,)),
        name + "_rsend": pltpu.SemaphoreType.DMA((2, 6)),
        name + "_rrecv": pltpu.SemaphoreType.DMA((2, 6)),
        name + "_asend": pltpu.SemaphoreType.DMA((2, 9)),
        name + "_arecv": pltpu.SemaphoreType.DMA((2, 9)),
    }


SCALE = 0.125
PACKET = 512 + 1024 + 1024 + 128 + 128
LHS_T = (((0,), (0,)), ((), ()))
RHS_T = (((1,), (1,)), ((), ()))


def rows256(b):
    return pl.ds(pl.multiple_of(b * 256, 256), 256)


def of_head(value, head, axis):
    index = lax.broadcasted_iota(jnp.int32, value.shape, axis)
    return jnp.where((index >= 64) == (head == 1), value, jnp.zeros_like(value))


def step_kernel(names, *refs):
    r = types.SimpleNamespace(**dict(zip(names, refs, strict=True)))
    me, y, c, up, dn, op, oc = ring_places()
    slot = y * 2 + c
    vocab, padded = r.table.shape[0], r.shard.shape[0]

    fetch = pltpu.make_async_copy(r.table, r.shard.at[pl.ds(0, vocab)], r.load.at[0])
    fetch_ids = pltpu.make_async_copy(r.ids, r.ids_here, r.load.at[1])
    fetch_ids.start()
    fetch.start()
    tokens = Ids(r.packet_in, r.got, r.isend, r.irecv)
    spread = Plane(
        [spread_item(r.qkv_s.at[i], r.qkv_w, pl.ds(i * 128, 128)) for i in range(3)]
        + [
            spread_item(r.out_s, r.out_w),
            spread_item(r.up_s, r.up_w),
            spread_item(r.head_s, r.head_w),
            spread_item(r.down_s, r.down_w),
        ],
        r.ssend,
        r.srecv,
        False,
    )
    collect = Plane(
        [
            (lambda number: r.packet, lambda slot: r.packets.at[slot], r.packets, r.packets.at[pl.ds(0, 15)]),
            collect_item(r.up_term, r.up_buf),
            collect_item(r.out_term, r.out_buf),
        ]
        + [collect_item(r.qkv_term.at[i], r.qkv_buf.at[i]) for i in range(3)],
        r.csend,
        r.crecv,
        True,
    )
    partner = dict(xl=1 - me["xl"], xh=1 - me["xh"])
    peers = [(k, e) for k in (2, 1, 3, 0) for e in range(2) if (k, e) != (0, 0)]
    for device in (dict(y=up), dict(y=dn), dict(c=oc), partner):
        signal(device)
    for k, e in peers:
        signal(dict(y=add_mod(y, (4 - k) % 4, 4), c=add_mod(c, e, 2)))
    greeted = tokens.greet() + spread.greet() + collect.greet() + 11
    if padded > vocab:
        r.shard[vocab:padded] = jnp.zeros((padded - vocab, 1024), BF16)
    fetch_ids.wait()
    line = lax.broadcasted_iota(jnp.int32, (8, 128), 0)
    r.packet_in[...] = jnp.where(line == 0, r.ids_here[...], jnp.where(line == 1, r.count[0], r.label[0]))
    pl.semaphore_wait(pltpu.get_barrier_semaphore(), greeted)
    tokens.start()
    for i in range(3):
        spread.start(i)

    base = (y * 2 + me["xh"]) * vocab
    lanes = lax.broadcasted_iota(jnp.int32, (64, 128), 1)

    def look_up(role, ch):
        for b in range(4):
            wanted = jnp.broadcast_to(r.got[role, b, 0:1, :], (128, 128)).T[ch * 64 : ch * 64 + 64] - base
            for tile in range(padded // 128):
                r.chosen[b * 64 : b * 64 + 64, tile * 128 : tile * 128 + 128] = jnp.where(
                    wanted == lanes + tile * 128, 1.0, 0.0
                ).astype(BF16)
        if role == 1 and ch == 0:
            fetch.wait()
        for part in range(4):
            cols = slice(part * 256, part * 256 + 256)
            found = jnp.dot(r.chosen[...], r.shard[:, cols], preferred_element_type=F32).astype(BF16)
            for b in range(4):
                r.rows[role, ch, b, :, cols] = found[b * 64 : b * 64 + 64]

    own = {
        (role, ch): Owner(
            lambda b, role=role, ch=ch: r.rows.at[role, ch, b],
            r.e_stage.at[role, ch],
            r.e_far.at[role, ch],
            r.e_near.at[role, ch],
            r.e_rsend.at[role, ch],
            r.e_rrecv.at[role, ch],
        )
        for role in range(2)
        for ch in range(2)
    }
    cross = [
        remote(r.total.at[ch], r.theirs.at[ch], r.xsend.at[ch], r.xrecv.at[ch], partner) for ch in range(2)
    ]
    tokens.arrive(1)
    look_up(1, 0)
    own[1, 0].begin()
    own[1, 0].early()
    look_up(1, 1)
    own[1, 1].begin()
    own[1, 1].early()
    own[1, 0].relay()
    tokens.arrive(0)
    look_up(0, 0)
    own[0, 0].begin()
    own[0, 0].early()
    own[1, 1].relay()
    r.total[0] = own[1, 0].finish().astype(BF16)
    cross[0].start()
    look_up(0, 1)
    own[0, 1].begin()
    own[0, 1].early()
    own[0, 0].relay()
    r.total[1] = own[1, 1].finish().astype(BF16)
    cross[1].start()
    spread.start(3)
    own[0, 1].relay()
    length, label = r.got[0, 0, 1:2, 0:1], r.got[0, 0, 2:3, 0:1]
    gathers = [Gather(r.normed, ch, r.e_asend.at[ch], r.e_arecv.at[ch]) for ch in range(2)]
    first = []

    def own_rows(ch):
        return pl.ds(pl.multiple_of(slot * 128 + ch * 64, 64), 64)

    for ch in range(2):
        mine = own[0, ch].finish()
        cross[ch].wait_recv()
        value = mine + r.theirs[ch].astype(F32)
        first.append(value)
        r.normed[own_rows(ch)] = normalize(value).astype(BF16)
        gathers[ch].begin()
    for i in range(4, 7):
        spread.start(i)
    for ch in range(2):
        r.first[ch * 64 : ch * 64 + 64] = first[ch]
    for i in range(3):
        spread.arrive(i)

    def project(b):
        r.qkv[rows256(b)] = jnp.dot(r.normed[rows256(b)], r.qkv_w[...], preferred_element_type=F32).astype(BF16)

    wide = [Gather(r.out_full, ch, r.wsend.at[ch], r.wrecv.at[ch]) for ch in range(2)]

    def widen():
        spread.arrive(3)
        r.out_full[pl.ds(pl.multiple_of(slot * 128, 128), 128)] = r.out_w[...].T
        for g in wide:
            g.begin()

    gather_beside(gathers, project, after_sides=widen)

    r.query_t[...] = (r.qkv[:, 0:128] * SCALE).T
    r.values_t[...] = r.qkv[:, 256:384].T
    seen = lax.broadcasted_iota(jnp.int32, (1024, 256), 0) < length

    def attend(b, head):
        cols = rows256(b)
        scores = jnp.dot(r.qkv[:, 128:256], of_head(r.query_t[:, cols], head, 0), preferred_element_type=F32)
        scores = jnp.where(seen, scores, -1e30)
        expo = jnp.exp(scores - jnp.max(scores, axis=0, keepdims=True))
        probs = (expo * (1.0 / jnp.sum(expo, axis=0, keepdims=True))).astype(BF16)
        r.probs_t[head, :, cols] = probs
        rows = slice(head * 64, head * 64 + 64)
        r.context_t[rows, cols] = jnp.dot(r.values_t[rows], probs, preferred_element_type=F32).astype(BF16)

    order = (op, up, dn, y)
    here128 = pl.ds(pl.multiple_of(slot * 128, 128), 128)

    def piece(i, e):
        return r.context.at[pl.ds(pl.multiple_of((order[i] * 2 + add_mod(c, e, 2)) * 128, 128), 128)]

    pieces = {
        (i, e): remote(
            piece(i, e),
            r.context_own.at[:, here128],
            r.tsend.at[i, e],
            r.trecv.at[i, e],
            dict(y=order[i], c=add_mod(c, e, 2)),
        )
        for i in range(4)
        for e in range(2)
        if (i, e) != (3, 0)
    }

    def hand_over(i):
        r.context[rows256(order[i])] = r.context_t[:, rows256(order[i])].T
        for e in range(2):
            if (i, e) in pieces:
                pieces[i, e].start()
            else:
                r.context_own[:, here128] = r.context[here128]

    for i, b in enumerate(order):
        attend(b, 0)
        if i == 3:
            wide[0].far()
        attend(b, 1)
        hand_over(i)
        if i == 0:
            for g in wide:
                g.sides()
    wide[1].far()
    for step in pieces.values():
        step.wait_recv()
    for g in wide:
        g.pair_own()
        g.pair_sides()
        g.pair_far()
    attn = jnp.dot(r.context_own[...], r.out_full[...], preferred_element_type=F32)
    more = [Gather(r.normed_two, ch, r.a_asend.at[ch], r.a_arecv.at[ch]) for ch in range(2)]
    for ch in range(2):
        second = (r.first[ch * 64 : ch * 64 + 64] + attn[ch * 64 : ch * 64 + 64]).astype(BF16)
        r.second[ch * 64 : ch * 64 + 64] = second
        r.normed_two[own_rows(ch)] = normalize(second.astype(F32)).astype(BF16)
        more[ch].begin()

    def live(start, size):
        return start + lax.broadcasted_iota(jnp.int32, (size, 1), 0) < length

    r.hidden_sum[...] = jnp.zeros((1, 512), F32)
    spread.arrive(4)

    def hidden_block(b):
        hidden = jnp.dot(r.normed_two[rows256(b)], r.up_w[...], preferred_element_type=F32)
        square = hidden * hidden
        inner = jnp.tanh(0.7978845608028654 * hidden * (1.0 + 0.044715 * square))
        half = 0.5 * (1.0 + inner)
        acted = (hidden * half).astype(BF16).astype(F32)
        r.slope[rows256(b)] = half + 0.5 * hidden * (1.0 - inner * inner) * (
            0.7978845608028654 + (0.7978845608028654 * 3.0 * 0.044715) * square
        )
        r.hidden_sum[...] += jnp.sum(jnp.where(live(b * 256, 256), acted, 0.0), axis=0, keepdims=True)

    gather_beside(more, hidden_block)

    spread.arrive(5)
    spread.arrive(6)
    hidden_sum = r.hidden_sum[...]
    own_sum = jnp.sum(jnp.where(live(slot * 128, 128), r.second[...].astype(F32), 0.0), axis=0, keepdims=True)
    pushed = lax.dot_general(thirds(hidden_sum), r.down_w[...], RHS_T, preferred_element_type=F32)
    r.parts[slot] = own_sum + jnp.sum(pushed, axis=0, keepdims=True)
    small = [
        remote(
            r.parts.at[slot],
            r.parts.at[slot],
            r.hsend.at[k, e],
            r.hrecv.at[k, e],
            dict(y=add_mod(y, k, 4), c=add_mod(c, e, 2)),
        )
        for k, e in peers
    ]
    for step in small:
        step.start()
    for step in small:
        step.wait()
    pooled = r.parts[0]
    for s in range(1, 8):
        pooled = pooled + r.parts[s]
    count = length.astype(F32)
    pooled = pooled / count
    final = normalize(pooled)
    logits = jnp.sum(jnp.dot(thirds(final), r.head_w[...], preferred_element_type=F32), axis=0, keepdims=True)
    top = jnp.max(logits, axis=-1, keepdims=True)
    total = jnp.log(jnp.sum(jnp.exp(logits - top), axis=-1, keepdims=True)) + top
    labels = (lax.broadcasted_iota(jnp.int32, logits.shape, 1) == label).astype(F32)
    loss = total - jnp.sum(logits * labels, axis=-1, keepdims=True)
    g_logits = (jnp.exp(logits - total) - labels) / 16.0
    g_final = lax.dot_general(thirds(g_logits), r.head_w[...], RHS_T, preferred_element_type=F32)
    per_token = normalize_back(pooled, jnp.sum(g_final, axis=0, keepdims=True)) / count
    rounded = per_token.astype(BF16)
    pulled = jnp.dot(rounded, r.down_w[...], preferred_element_type=F32)

    back = PairOwner(r.terms_back, r, "b")
    for i, b in enumerate(back.order):
        rows = rows256(b)
        grad = jnp.where(live(b * 256, 256), r.slope[rows] * pulled, 0.0).astype(BF16)
        r.g_pre[rows] = grad
        r.terms_back[rows] = lax.dot_general(
            grad, r.up_w[...], RHS_T, preferred_element_type=F32
        ).astype(BF16)
        back.push(i)
        if i == 2:
            back.pull(0)
            for owner in back.owners:
                owner.begin()
    for i in range(1, 4):
        back.pull(i)
        if i < 3:
            for owner in back.owners:
                owner.early((i - 1,))
    for block in range(4):
        cols = pl.ds(block * 256, 256)
        r.up_term[cols] = lax.dot_general(
            r.normed_two[:, cols], r.g_pre[...], LHS_T, preferred_element_type=F32
        ).astype(BF16)
    for owner in back.owners:
        owner.relay()
    r.packet[:, 0:512] = hidden_sum
    r.packet[:, 512:1536] = rounded.astype(F32)
    r.packet[:, 1536:2560] = final
    r.packet[:, 2560:2688] = g_logits
    r.packet[:, 2688:2816] = jnp.broadcast_to(loss, (1, 128))
    collect.start(1)
    collect.start(0)
    last = [Gather(r.g_second, ch, r.b_asend.at[ch], r.b_arecv.at[ch]) for ch in range(2)]
    for ch in range(2):
        grad = normalize_back(r.second[ch * 64 : ch * 64 + 64].astype(F32), back.owners[ch].finish())
        grad += jnp.where(live(slot * 128 + ch * 64, 64), per_token, 0.0)
        r.g_second[own_rows(ch)] = grad.astype(BF16)
        last[ch].begin()

    r.keys_t[...] = (r.qkv[:, 128:256] * SCALE).T
    r.grad_k[...] = jnp.zeros((1024, 128), F32)
    r.grad_v[...] = jnp.zeros((1024, 128), F32)

    def back_values(b):
        cols = rows256(b)
        g_context = jnp.dot(r.g_second[cols], r.out_w[...], preferred_element_type=F32)
        g_context_t = g_context.T
        g_context = g_context.astype(BF16)
        for head in range(2):
            r.grad_v[...] += jnp.dot(
                r.probs_t[head, :, cols], of_head(g_context, head, 1), preferred_element_type=F32
            )
        return g_context_t

    def back_scores(b, g_context_t):
        cols = rows256(b)
        product = g_context_t * r.context_t[:, cols].astype(F32)
        query = r.qkv[cols, 0:128] * SCALE
        for head in range(2):
            rows = slice(head * 64, head * 64 + 64)
            delta = jnp.sum(product[rows], axis=0, keepdims=True)
            moved = jnp.dot(
                r.qkv[:, 256:384], of_head(g_context_t, head, 0).astype(BF16), preferred_element_type=F32
            )
            g_scores = (r.probs_t[head, :, cols].astype(F32) * (moved - delta)).astype(BF16)
            r.grad_q[rows, cols] = jnp.dot(
                r.keys_t[rows], g_scores, preferred_element_type=F32
            ).astype(BF16)
            r.grad_k[...] += jnp.dot(g_scores, of_head(query, head, 1), preferred_element_type=F32)

    def send_term(piece, left):
        r.qkv_term[piece] = jnp.dot(left, r.normed[...], preferred_element_type=F32).T.astype(BF16)
        collect.start(3 + piece)

    def attend_back(b):
        back_scores(b, back_values(b))

    def attend_back_last(b):
        r.out_term[...] = jnp.dot(
            r.context_t[...], r.g_second[...], preferred_element_type=F32
        ).T.astype(BF16)
        collect.start(2)
        g_context_t = back_values(b)
        send_term(2, r.grad_v[...].T.astype(BF16))
        back_scores(b, g_context_t)
        send_term(0, r.grad_q[...])
        send_term(1, r.grad_k[...].T.astype(BF16))

    gather_beside(last, attend_back, attend_back_last)

    collect.arrive(0)
    begin = ((me["xl"] * 4 + me["z"]) * 2 + me["c"]) * 64
    packets = jnp.concatenate([r.packets[s] for s in range(16)], axis=0)
    r.down_grad[...] = jnp.dot(
        picked(packets[:, 512:1536], begin), packets[:, 0:512], precision=HIGH, preferred_element_type=F32
    )
    r.head_grad[...] = jnp.dot(
        picked(packets[:, 1536:2560], begin), packets[:, 2560:2688], precision=HIGH, preferred_element_type=F32
    )
    r.loss[...] = jnp.sum(packets[:, 2688:2816], axis=0, keepdims=True) / 16.0
    collect.arrive(1)
    r.up_grad[...] = total_of(r.up_buf)

    tokens.sent()
    for i in range(7):
        spread.sent(i)
    for owner in own.values():
        owner.sent()
    for step in cross:
        step.wait_send()
    for g in gathers + wide + more + last:
        g.sent()
    for step in pieces.values():
        step.wait_send()
    back.sent()
    for i in range(6):
        collect.sent(i)
    collect.arrive(2)
    r.out_grad[...] = total_of(r.out_buf)
    for piece in (2, 0, 1):
        collect.arrive(3 + piece)
        r.qkv_grad[piece] = total_of(r.qkv_buf.at[piece])


HBM = pl.BlockSpec(memory_space=pltpu.HBM)


def step(count, label, ids, table, qkv_s, out_s, up_s, down_s, head_s):
    padded = -(-table.shape[0] // 256) * 256
    inputs = dict(
        count=SM, label=SM, ids=HBM, table=HBM, qkv_s=HBM, out_s=HBM, up_s=HBM, down_s=HBM, head_s=HBM
    )
    outputs = dict(
        up_grad=jax.ShapeDtypeStruct((64, 512), F32),
        down_grad=jax.ShapeDtypeStruct((64, 512), F32),
        head_grad=jax.ShapeDtypeStruct((64, 128), F32),
        loss=jax.ShapeDtypeStruct((1, 128), F32),
        out_grad=jax.ShapeDtypeStruct((64, 128), F32),
        qkv_grad=jax.ShapeDtypeStruct((3, 64, 128), F32),
    )
    dma = pltpu.SemaphoreType.DMA
    vm = pltpu.VMEM
    scratch = dict(
        load=dma((2,)),
        ids_here=vm((1, 128), jnp.int32),
        packet_in=vm((8, 128), jnp.int32),
        got=vm((2, 4, 8, 128), jnp.int32),
        isend=dma((2, 4)),
        irecv=dma((2, 4)),
        ssend=dma((7,)),
        srecv=dma((7,)),
        csend=dma((6,)),
        crecv=dma((6,)),
        shard=vm((padded, 1024), BF16),
        chosen=vm((256, padded), BF16),
        rows=vm((2, 2, 4, 64, 1024), BF16),
        e_stage=vm((2, 2, 2, 32, 1024), BF16),
        e_far=vm((2, 2, 2, 32, 1024), BF16),
        e_near=vm((2, 2, 2, 64, 1024), BF16),
        e_rsend=dma((2, 2, 6)),
        e_rrecv=dma((2, 2, 6)),
        e_asend=dma((2, 9)),
        e_arecv=dma((2, 9)),
        total=vm((2, 64, 1024), BF16),
        theirs=vm((2, 64, 1024), BF16),
        xsend=dma((2,)),
        xrecv=dma((2,)),
        first=vm((128, 1024), F32),
        normed=vm((1024, 1024), BF16),
        qkv_w=vm((1024, 384), BF16),
        out_w=vm((1024, 128), BF16),
        up_w=vm((1024, 512), BF16),
        down_w=vm((1024, 512), BF16),
        head_w=vm((1024, 128), BF16),
        qkv=vm((1024, 384), BF16),
        query_t=vm((128, 1024), BF16),
        values_t=vm((128, 1024), BF16),
        keys_t=vm((128, 1024), BF16),
        out_full=vm((1024, 1024), BF16),
        wsend=dma((2, 9)),
        wrecv=dma((2, 9)),
        context=vm((1024, 128), BF16),
        context_own=vm((128, 1024), BF16),
        tsend=dma((4, 2)),
        trecv=dma((4, 2)),
        a_asend=dma((2, 9)),
        a_arecv=dma((2, 9)),
        probs_t=vm((2, 1024, 1024), BF16),
        context_t=vm((128, 1024), BF16),
        second=vm((128, 1024), BF16),
        normed_two=vm((1024, 1024), BF16),
        hidden_sum=vm((1, 512), F32),
        slope=vm((1024, 512), F32),
        parts=vm((8, 1, 1024), F32),
        hsend=dma((4, 2)),
        hrecv=dma((4, 2)),
        g_pre=vm((1024, 512), BF16),
        terms_back=vm((1024, 1024), BF16),
        **pair_owner_scratch("b"),
        up_term=vm((1024, 512), BF16),
        up_buf=vm((16, 64, 512), BF16),
        packet=vm((1, PACKET), F32),
        packets=vm((16, 1, PACKET), F32),
        g_second=vm((1024, 1024), BF16),
        grad_q=vm((128, 1024), BF16),
        grad_k=vm((1024, 128), F32),
        grad_v=vm((1024, 128), F32),
        out_term=vm((1024, 128), BF16),
        qkv_term=vm((3, 1024, 128), BF16),
        out_buf=vm((16, 64, 128), BF16),
        qkv_buf=vm((3, 16, 64, 128), BF16),
    )
    return pl.pallas_call(
        functools.partial(step_kernel, (*inputs, *outputs, *scratch)),
        out_shape=list(outputs.values()),
        in_specs=list(inputs.values()),
        out_specs=[VM] * len(outputs),
        scratch_shapes=list(scratch.values()),
        compiler_params=params(1, 54),
        name="step",
    )(count, label, ids, table, qkv_s, out_s, up_s, down_s, head_s)


def results_kernel(*refs):
    sources, targets, here, sems = refs[:5], refs[5:10], refs[10:15], refs[15]
    steps = [pltpu.make_async_copy(sources[i], here[i], sems.at[i]) for i in range(5)]
    for step in steps:
        step.start()
    for i in range(5):
        steps[i].wait()
        targets[i][...] = here[i][...]


def results(*arrays):
    return pl.pallas_call(
        results_kernel,
        out_shape=[
            jax.ShapeDtypeStruct((64, 512), F32),
            jax.ShapeDtypeStruct((64, 512), F32),
            jax.ShapeDtypeStruct((64, 128), F32),
            jax.ShapeDtypeStruct((64, 128), F32),
            jax.ShapeDtypeStruct((3, 64, 128), F32),
        ],
        in_specs=[HBM] * 5,
        out_specs=[VM] * 5,
        scratch_shapes=[pltpu.VMEM(a.shape, a.dtype) for a in arrays] + [pltpu.SemaphoreType.DMA((5,))],
        compiler_params=pltpu.CompilerParams(vmem_limit_bytes=67043328),
        name="results",
    )(*arrays)


def per_device(token_ids, lengths, teacher_bins, table, qkv_shard, out_shard, up_shard, down_shard, head_shard):
    up_grad, down_grad, head_grad, loss, out_grad, qkv_grad = step(
        lengths,
        teacher_bins,
        token_ids,
        table,
        jnp.transpose(qkv_shard, (1, 0, 2)),
        out_shard.T,
        up_shard,
        down_shard.T,
        head_shard,
    )
    up_grad, down_grad, head_grad, out_grad, qkv_grad = results(up_grad, down_grad, head_grad, out_grad, qkv_grad)
    return loss[0, 0], jnp.transpose(qkv_grad, (1, 0, 2)), out_grad.T, up_grad, down_grad.T, head_grad


def solution(mesh):
    fine = Mesh(mesh.devices.reshape(2, 4, 2, 4, 2), ("xl", "z", "c", "y", "xh"))
    dp, tensor = ("xl", "z", "c"), ("y", "xh")
    return jax.shard_map(
        per_device,
        mesh=fine,
        in_specs=(
            P(dp, tensor),
            P(dp),
            P(dp),
            P(tensor, None),
            P(dp, None, tensor),
            P(tensor, dp),
            P(dp, tensor),
            P(tensor, dp),
            P(dp, None),
        ),
        out_specs=(
            P(),
            P(dp, None, tensor),
            P(tensor, dp),
            P(dp, tensor),
            P(tensor, dp),
            P(dp, None),
        ),
        check_vma=False,
    )
```
